32 devices in a mesh: dp: 2 (over core), seq: 16 (over z, y, x).
Axes of the slice: x: 2, y: 2, z: 4, core: 2. Of those that a mesh axis runs over, the one named last changes fastest.
Arguments:
- hidden: bfloat16 [4, 2, 1024, 2048], P(None, 'dp', 'seq'), may hold values from -6 to 6
- prefix_lengths: int32 [4, 2], replicated, may hold values from 0 to 1023
- cotangent: bfloat16 [4, 2, 1024, 2048], P(None, 'dp', 'seq'), may hold values from -6 to 6
- first_gain: bfloat16 [2048], P(('dp', 'seq')), may hold values from 0.5 to 1.5
- first_shift: bfloat16 [2048], P(('dp', 'seq')), may hold values from -1.5 to 1.5
- triple_weight: bfloat16 [2048, 16, 3, 128], P('seq', 'dp'), may hold values from -0.125 to 0.125
- pair_bias: bfloat16 [4096], P(('dp', 'seq')), may hold values from -1.5 to 1.5
- dense_weight: bfloat16 [2048, 2048], P(('dp', 'seq')), may hold values from -0.375 to 0.375
- dense_shift: bfloat16 [2048], P(('dp', 'seq')), may hold values from -1.5 to 1.5
- second_gain: bfloat16 [2048], P(('dp', 'seq')), may hold values from 0.5 to 1.5
- second_shift: bfloat16 [2048], P(('dp', 'seq')), may hold values from -1.5 to 1.5
- expand_weight: bfloat16 [2048, 8192], P('seq', 'dp'), may hold values from -0.125 to 0.125
- expand_shift: bfloat16 [8192], P(('dp', 'seq')), may hold values from -1.5 to 1.5
- shrink_weight: bfloat16 [8192, 2048], P(('dp', 'seq')), may hold values from -0.09375 to 0.09375
- shrink_shift: bfloat16 [2048], P(('dp', 'seq')), may hold values from -1.5 to 1.5
Outputs:
- layer_output: bfloat16 [4, 2, 1024, 2048], P(None, 'dp', 'seq')
- hidden_grad: bfloat16 [4, 2, 1024, 2048], P(None, 'dp', 'seq')
- first_gain_grad: float32 [2048], P(('dp', 'seq'))
- first_shift_grad: float32 [2048], P(('dp', 'seq'))
- triple_weight_grad: float32 [2048, 16, 3, 128], P('seq', 'dp')
- pair_bias_grad: float32 [4096], P(('dp', 'seq'))
- dense_weight_grad: float32 [2048, 2048], P(('dp', 'seq'))
- dense_shift_grad: float32 [2048], P(('dp', 'seq'))
- second_gain_grad: float32 [2048], P(('dp', 'seq'))
- second_shift_grad: float32 [2048], P(('dp', 'seq'))
- expand_weight_grad: float32 [2048, 8192], P('seq', 'dp')
- expand_shift_grad: float32 [8192], P(('dp', 'seq'))
- shrink_weight_grad: float32 [8192, 2048], P(('dp', 'seq'))
- shrink_shift_grad: float32 [2048], P(('dp', 'seq'))
The draws below stay inside these ranges and needn't reach their ends.
All inputs are finite; a program needn't handle non-finite values.
Results may differ from the reference program's by a relative error of at most 0.017.
Values may be sent and summed in bfloat16 or wider, within the bound.
A program may use at most 320 MiB of HBM per device.

```python
import math
import jax
import jax.numpy as jnp
from jax import lax

D = 2048
HEADS = 16
HEAD_DIM = 128
FF = 8192
MICRO = 4
SEQS = 2
LENGTH = 1024


def place_ends(result, own_key, low, high):
    dims = result.shape
    index_at = [jax.random.randint(jax.random.fold_in(own_key, axis), (), 0, dims[axis]) for axis in range(len(dims))]
    result = result.at[tuple(index_at)].set(low)
    longest = dims.index(max(dims))
    index_at[longest] = (index_at[longest] + 1) % dims[longest]
    return result.at[tuple(index_at)].set(high)


def levels(rng, dims, shards, least, top_value):
    gain = 1.0
    for axis_at, blocks in shards:
        draws = jax.random.uniform(jax.random.fold_in(jax.random.fold_in(rng, 6), axis_at), (blocks,), jnp.float32, least / len(shards), top_value / len(shards))
        gain = gain * jnp.repeat(jnp.exp(draws), dims[axis_at] // blocks).reshape((-1,) + (1,) * (len(dims) - 1 - axis_at))
    return gain


def gaussian(own_key, dims, width, bound, split=(), kind=jnp.bfloat16):
    gain = levels(own_key, dims, split, -0.22, 0.18) if split else 1.0
    result = jax.random.normal(own_key, dims, jnp.float32) * width * gain
    return jnp.minimum(jnp.maximum(result, -bound), bound).astype(kind)


def setup_inputs(seed: int = 0) -> dict:
    key_of = jax.random.split(jax.random.key(seed), 16)
    return {
        "hidden": gaussian(key_of[0], (MICRO, SEQS, LENGTH, D), 1.0, 6.0, ((1, 2), (2, 16))),
        "prefix_lengths": place_ends(jax.random.randint(key_of[1], (MICRO, SEQS), 0, LENGTH), jax.random.fold_in(key_of[1], 1), 0, LENGTH - 1).astype(jnp.int32),
        "cotangent": gaussian(key_of[2], (MICRO, SEQS, LENGTH, D), 1.0, 6.0, ((1, 2), (2, 16))),
        "first_gain": jnp.clip(1.0 + 0.1 * jax.random.normal(key_of[3], (D,), jnp.float32), 0.5, 1.5).astype(jnp.bfloat16),
        "first_shift": gaussian(key_of[4], (D,), 0.3, 1.5, ((0, 32),)),
        "triple_weight": gaussian(key_of[5], (D, HEADS, 3, HEAD_DIM), D ** -0.5, 0.125, ((0, 16), (1, 2))),
        "pair_bias": gaussian(key_of[6], (2 * D,), 0.3, 1.5, ((0, 32),)),
        "dense_weight": gaussian(key_of[7], (D, D), (D // 8) ** -0.5, 0.375, ((0, 32),)),
        "dense_shift": gaussian(key_of[8], (D,), 0.3, 1.5, ((0, 32),)),
        "second_gain": jnp.clip(1.0 + 0.1 * jax.random.normal(key_of[9], (D,), jnp.float32), 0.5, 1.5).astype(jnp.bfloat16),
        "second_shift": gaussian(key_of[10], (D,), 0.3, 1.5, ((0, 32),)),
        "expand_weight": gaussian(key_of[11], (D, FF), D ** -0.5, 0.125, ((0, 16), (1, 2))),
        "expand_shift": gaussian(key_of[12], (FF,), 0.3, 1.5, ((0, 32),)),
        "shrink_weight": gaussian(key_of[13], (FF, D), (FF // 2) ** -0.5, 0.09375, ((0, 32),)),
        "shrink_shift": gaussian(key_of[14], (D,), 0.3, 1.5, ((0, 32),)),
    }


EPSILON = 1e-05
GELU_SCALE = 0.7978845608028654
HIGHEST = lax.Precision.HIGHEST

@jax.custom_vjp
def low(v):
    return lax.optimization_barrier(v.astype(jnp.bfloat16)).astype(jnp.float32)

@jax.custom_vjp
def low_back(v):
    return v

def low_keep(v):
    return (low(v), None)

def low_pass(kept, grad):
    return (grad,)

def back_keep(v):
    return (v, None)

def back_low(kept, grad):
    return (low(grad),)
low.defvjp(low_keep, low_pass)
low_back.defvjp(back_keep, back_low)

def matmul(left, right):
    return jnp.dot(left, right, precision=HIGHEST, preferred_element_type=jnp.float32)

def layer_norm(inputs, norm_gain, norm_shift):
    centered = inputs - lax.optimization_barrier(jnp.mean(inputs, -1, keepdims=True))
    variance = lax.optimization_barrier(jnp.mean(centered * centered, -1, keepdims=True))
    return centered * lax.rsqrt(variance + EPSILON) * norm_gain + norm_shift

def gelu_tanh(values):
    return 0.5 * values * (1.0 + jnp.tanh(GELU_SCALE * (values + 0.044715 * values * values * values)))

def head_slopes():
    return jnp.power(jnp.float32(2.0), -8.0 * (jnp.arange(HEADS, dtype=jnp.float32) + 1.0) / HEADS)

def attend(queries, keys, values, prefix):
    seq_length = queries.shape[0]
    block_rows = min(512, seq_length)
    block_count = seq_length // block_rows
    score_scale = 1.0 / math.sqrt(HEAD_DIM)
    slopes = head_slopes()
    key_pos = jnp.arange(seq_length, dtype=jnp.int32)

    def one_block(block_index):
        first_row = (block_index * block_rows).astype(jnp.int32)
        query_rows = lax.dynamic_slice_in_dim(queries, first_row, block_rows, 0)
        query_pos = first_row + jnp.arange(block_rows, dtype=jnp.int32)
        raw_scores = jnp.einsum('qhd,khd->hqk', query_rows, keys, precision=HIGHEST) * score_scale
        distance = jnp.abs(query_pos[:, None] - key_pos[None, :]).astype(jnp.float32)
        raw_scores = raw_scores - slopes[:, None, None] * distance[None]
        allowed = (key_pos[None, :] <= query_pos[:, None]) | (key_pos[None, :] < prefix)
        scores = jnp.where(allowed[None], low_back(raw_scores), jnp.float32(-1e+30))
        row_max = lax.optimization_barrier(jnp.max(scores, -1, keepdims=True))
        powers = jnp.exp(scores - row_max)
        soft_probs = powers / lax.optimization_barrier(jnp.sum(powers, -1, keepdims=True))
        return jnp.einsum('hqk,khd->qhd', low(soft_probs), values, precision=HIGHEST)
    blocks_out = lax.map(jax.checkpoint(one_block), jnp.arange(block_count, dtype=jnp.int32))
    return blocks_out.reshape(seq_length, HEADS * HEAD_DIM)

def sequence_forward(params, inputs, prefix):
    first_gain, first_shift, triple_weight, pair_bias, dense_weight, dense_shift, second_gain, second_shift, expand_weight, expand_shift, shrink_weight, shrink_shift = params
    seq_length = inputs.shape[0]
    normed = low(layer_norm(inputs, first_gain, first_shift))
    pair_heads = pair_bias.reshape(HEADS, 2, HEAD_DIM)
    bias_full = jnp.stack([pair_heads[:, 0], jnp.zeros((HEADS, HEAD_DIM), jnp.float32), pair_heads[:, 1]], 1).reshape(3 * D)
    projected = low(low_back(matmul(normed, triple_weight.reshape(D, 3 * D)) + bias_full))
    grouped = projected.reshape(seq_length, HEADS, 3, HEAD_DIM)
    attn_mix = low(low_back(attend(grouped[:, :, 0], grouped[:, :, 1], grouped[:, :, 2], prefix)))
    branch_one = low_back(matmul(attn_mix, dense_weight) + dense_shift)
    middle = inputs + branch_one
    normed_two = low(layer_norm(middle, second_gain, second_shift))
    hidden_pre = low_back(matmul(normed_two, expand_weight) + expand_shift)
    activated = low(gelu_tanh(hidden_pre))
    branch_two = low_back(matmul(activated, shrink_weight) + shrink_shift)
    return middle + branch_two

def reference(hidden, prefix_lengths, cotangent, first_gain, first_shift, triple_weight, pair_bias, dense_weight, dense_shift, second_gain, second_shift, expand_weight, expand_shift, shrink_weight, shrink_shift):
    params = jax.tree.map(lambda weight_array: weight_array.astype(jnp.float32), (first_gain, first_shift, triple_weight, pair_bias, dense_weight, dense_shift, second_gain, second_shift, expand_weight, expand_shift, shrink_weight, shrink_shift))
    inputs = hidden.astype(jnp.float32).reshape(MICRO * SEQS, LENGTH, D)
    prefixes = prefix_lengths.reshape(MICRO * SEQS).astype(jnp.int32)
    checked = jax.checkpoint(sequence_forward)

    def forward(weights_in, inputs_in):
        return lax.map(lambda seq_pair: checked(weights_in, seq_pair[0], seq_pair[1]), (inputs_in, prefixes))
    outputs, pull_back = jax.vjp(forward, params, inputs)
    grad_params, grad_inputs = pull_back(cotangent.astype(jnp.float32).reshape(outputs.shape))
    return (outputs.astype(jnp.bfloat16).reshape(hidden.shape), grad_inputs.astype(jnp.bfloat16).reshape(hidden.shape), grad_params[0], grad_params[1], grad_params[2], grad_params[3], grad_params[4], grad_params[5], grad_params[6], grad_params[7], grad_params[8], grad_params[9], grad_params[10], grad_params[11])
```

```python
import math

import jax
import jax.numpy as jnp
from jax import lax
from jax.sharding import Mesh
from jax.sharding import PartitionSpec as P

EPSILON = 1e-05
GELU_SCALE = 0.7978845608028654


def layer_norm(inputs, norm_gain, norm_shift):
    centered = inputs - jnp.mean(inputs, -1, keepdims=True)
    variance = jnp.mean(centered * centered, -1, keepdims=True)
    return centered * lax.rsqrt(variance + EPSILON) * norm_gain + norm_shift


def gelu_tanh(values):
    return (
        0.5 * values * (1.0 + jnp.tanh(GELU_SCALE * (values + 0.044715 * values * values * values)))
    )


def split_norm(inputs, gain_rows, shift_rows):
    return layer_norm(inputs, gain_rows[None, :, None, :], shift_rows[None, :, None, :])


def place_half(values, half_index, group_count):
    chosen = (jnp.arange(group_count, dtype=jnp.int32) == half_index).astype(values.dtype)
    return (chosen[:, None] * values.reshape(1, -1)).reshape(-1)


def shards(
    hidden,
    prefix_lengths,
    cotangent,
    first_gain,
    first_shift,
    triple_weight,
    pair_bias,
    dense_weight,
    dense_shift,
    second_gain,
    second_shift,
    expand_weight,
    expand_shift,
    shrink_weight,
    shrink_shift,
):
    wide_type = jnp.float32
    half_type = jnp.bfloat16
    seq_count = lax.axis_size("seq")
    group_count = lax.axis_size("dp")
    dp_index = lax.axis_index("dp")
    seq_index = lax.axis_index("seq")
    micro_count = hidden.shape[0]
    seq_rows = hidden.shape[2]
    model_width = hidden.shape[3]
    seq_length = seq_rows * seq_count
    local_heads = triple_weight.shape[1]
    head_dim = triple_weight.shape[3]
    head_total = local_heads * group_count
    pair_local = micro_count * group_count * local_heads // seq_count
    unit_local = expand_weight.shape[1]
    project_width = 3 * local_heads * head_dim
    token_total = micro_count * group_count * seq_rows
    score_scale = 1.0 / math.sqrt(head_dim)
    block_rows = min(512, seq_length)
    block_count = seq_length // block_rows
    key_pos = jnp.arange(seq_length, dtype=jnp.int32)
    gathered = (
        lax.all_gather(triple_weight, "seq", axis=0, tiled=True),
        lax.all_gather(dense_weight, "seq", axis=0, tiled=True),
        lax.all_gather(expand_weight, "seq", axis=0, tiled=True),
        lax.all_gather(shrink_weight, "seq", axis=0, tiled=True),
        lax.all_gather(first_gain, "seq", axis=0, tiled=True),
        lax.all_gather(first_shift, "seq", axis=0, tiled=True),
        lax.all_gather(pair_bias, "seq", axis=0, tiled=True),
        lax.all_gather(dense_shift, "seq", axis=0, tiled=True),
        lax.all_gather(second_gain, "seq", axis=0, tiled=True),
        lax.all_gather(second_shift, "seq", axis=0, tiled=True),
        lax.all_gather(expand_shift, "seq", axis=0, tiled=True),
        lax.all_gather(shrink_shift, "seq", axis=0, tiled=True),
    )
    triple_full, dense_full, expand_full, shrink_full = (
        gathered[0],
        gathered[1],
        gathered[2],
        gathered[3],
    )
    row_sets = (
        lax.all_gather(hidden, "dp", axis=1, tiled=True),
        lax.all_gather(cotangent, "dp", axis=1, tiled=True),
        lax.all_gather(gathered[4], "dp", axis=0, tiled=True),
        lax.all_gather(gathered[5], "dp", axis=0, tiled=True),
        lax.all_gather(gathered[6], "dp", axis=0, tiled=True),
        lax.all_gather(gathered[7], "dp", axis=0, tiled=True),
        lax.all_gather(gathered[8], "dp", axis=0, tiled=True),
        lax.all_gather(gathered[9], "dp", axis=0, tiled=True),
        lax.all_gather(gathered[10], "dp", axis=0, tiled=True),
        lax.all_gather(gathered[11], "dp", axis=0, tiled=True),
    )
    hidden_both = row_sets[0]
    upstream_low = row_sets[1]
    gain_one, shift_one, pair_full, dense_bias, gain_two, shift_two, expand_bias, shrink_bias = [
        vector.astype(wide_type) for vector in row_sets[2:]
    ]
    inputs_both = hidden_both.astype(wide_type)
    normed_low = layer_norm(inputs_both, gain_one, shift_one).astype(half_type)
    pair_heads = lax.dynamic_slice_in_dim(
        pair_full.reshape(head_total, 2, head_dim), dp_index * local_heads, local_heads, 0
    )
    triple_bias = jnp.stack(
        [pair_heads[:, 0], jnp.zeros_like(pair_heads[:, 0]), pair_heads[:, 1]], 0
    )
    projected = jnp.einsum(
        "mstd,dhce->cmshte", normed_low, triple_full, preferred_element_type=wide_type
    )
    projected = projected + triple_bias[:, None, None, :, None, :]
    project_low = projected.astype(half_type).reshape(3, seq_count, pair_local, seq_rows, head_dim)
    pair_rows = lax.all_to_all(project_low, "seq", split_axis=1, concat_axis=3, tiled=True)[:, 0]
    query_all, key_all, value_all = (pair_rows[0], pair_rows[1], pair_rows[2])
    pair_index = seq_index * pair_local + jnp.arange(pair_local, dtype=jnp.int32)
    head_index = dp_index * local_heads + pair_index % local_heads
    sequence_index = pair_index // local_heads
    slopes = jnp.power(jnp.float32(2.0), -8.0 * (head_index.astype(wide_type) + 1.0) / head_total)
    prefix_flat = prefix_lengths.reshape(-1)
    prefix_slots = jnp.arange(prefix_flat.shape[0], dtype=jnp.int32)
    prefixes = jnp.sum(
        jnp.where(prefix_slots[None, :] == sequence_index[:, None], prefix_flat[None, :], 0), 1
    )

    def block_scores(pair_item, first_row):
        query_block = lax.dynamic_slice_in_dim(
            lax.dynamic_index_in_dim(query_all, pair_item, 0, False), first_row, block_rows, 0
        )
        keys_item = lax.dynamic_index_in_dim(key_all, pair_item, 0, False)
        head_slope = lax.dynamic_index_in_dim(slopes, pair_item, 0, False)
        prefix = lax.dynamic_index_in_dim(prefixes, pair_item, 0, False)
        query_pos = first_row + jnp.arange(block_rows, dtype=jnp.int32)
        raw_scores = (
            jnp.einsum("qe,ke->qk", query_block, keys_item, preferred_element_type=wide_type)
            * score_scale
        )
        distance = jnp.abs(query_pos[:, None] - key_pos[None, :]).astype(wide_type)
        raw_scores = raw_scores - head_slope * distance
        allowed = (key_pos[None, :] <= query_pos[:, None]) | (key_pos[None, :] < prefix)
        return (query_block, jnp.where(allowed, raw_scores, jnp.float32(-1e30)))

    def forward_block(flat_index):
        pair_item = flat_index // block_count
        first_row = flat_index % block_count * block_rows
        query_block, scores = block_scores(pair_item, first_row)
        row_max = jnp.max(scores, -1, keepdims=True)
        powers = jnp.exp(scores - row_max)
        row_total = jnp.sum(powers, -1, keepdims=True)
        probs_low = (powers / row_total).astype(half_type)
        values_item = lax.dynamic_index_in_dim(value_all, pair_item, 0, False)
        mixed = jnp.dot(probs_low, values_item, preferred_element_type=wide_type).astype(half_type)
        return (mixed, (row_max + jnp.log(row_total))[:, 0])

    mixed_blocks, log_blocks = lax.map(
        forward_block, jnp.arange(pair_local * block_count, dtype=jnp.int32)
    )
    mixed_pairs = mixed_blocks.reshape(pair_local, seq_count, seq_rows, head_dim)
    log_totals = log_blocks.reshape(pair_local, seq_length)
    mixed_home = lax.all_to_all(mixed_pairs, "seq", split_axis=1, concat_axis=0, tiled=True)
    mixed_tokens = jnp.transpose(
        mixed_home.reshape(micro_count, group_count, local_heads, seq_rows, head_dim),
        (0, 1, 3, 2, 4),
    ).reshape(micro_count, group_count, seq_rows, local_heads * head_dim)
    dense_part = jnp.einsum(
        "mstk,kf->mstf", mixed_tokens, dense_full, preferred_element_type=wide_type
    )
    attention_sum = lax.psum(dense_part.astype(jnp.bfloat16), "dp").astype(jnp.float32)
    middle = inputs_both + attention_sum + dense_bias
    gain_rows_two = jnp.broadcast_to(gain_two[None, :], (group_count, model_width))
    shift_rows_two = jnp.broadcast_to(shift_two[None, :], (group_count, model_width))
    normed_two, norm_two_pull = jax.vjp(split_norm, middle, gain_rows_two, shift_rows_two)
    normed_two_low = normed_two.astype(half_type)
    unit_bias = lax.dynamic_slice_in_dim(expand_bias, dp_index * unit_local, unit_local, 0)
    hidden_pre = (
        jnp.einsum("mstd,df->mstf", normed_two_low, expand_full, preferred_element_type=wide_type)
        + unit_bias
    )
    activated_value, gelu_pull = jax.vjp(gelu_tanh, hidden_pre)
    activated_low = activated_value.astype(half_type)
    feed_part = jnp.einsum(
        "mstf,fd->mstd", activated_low, shrink_full, preferred_element_type=wide_type
    )
    feed_sum = lax.psum_scatter(
        feed_part.astype(jnp.bfloat16), "dp", scatter_dimension=1, tiled=True
    ).astype(jnp.float32)
    middle_own = lax.dynamic_slice_in_dim(middle, dp_index, 1, 1)
    layer_output = (middle_own + feed_sum + shrink_bias).astype(half_type)
    triple_back, dense_back, expand_back, shrink_back = (
        lax.all_gather(triple_weight, "seq", axis=0, tiled=True),
        lax.all_gather(dense_weight, "seq", axis=0, tiled=True),
        lax.all_gather(expand_weight, "seq", axis=0, tiled=True),
        lax.all_gather(shrink_weight, "seq", axis=0, tiled=True),
    )
    grad_act = jnp.einsum(
        "mstd,fd->mstf", upstream_low, shrink_back, preferred_element_type=wide_type
    )
    grad_pre_low = gelu_pull(grad_act)[0].astype(half_type)
    norm_two_part = jnp.einsum(
        "mstf,df->mstd", grad_pre_low, expand_back, preferred_element_type=wide_type
    )
    grad_normed_two = lax.psum(norm_two_part.astype(jnp.bfloat16), "dp").astype(jnp.float32)
    grad_middle_norm, grad_gain_rows_two, grad_shift_rows_two = norm_two_pull(grad_normed_two)
    grad_middle = upstream_low.astype(wide_type) + grad_middle_norm
    grad_branch_low = grad_middle.astype(half_type)
    go_pairs = jnp.einsum(
        "mstf,hef->mshte",
        grad_branch_low,
        dense_back.reshape(local_heads, head_dim, model_width),
        preferred_element_type=wide_type,
    ).astype(half_type)
    go_pairs = go_pairs.reshape(seq_count, pair_local, seq_rows, head_dim)
    grad_mixed_pairs = lax.all_to_all(go_pairs, "seq", split_axis=0, concat_axis=2, tiled=True)[0]

    def backward_item(pair_item):
        keys_item = lax.dynamic_index_in_dim(key_all, pair_item, 0, False)
        values_item = lax.dynamic_index_in_dim(value_all, pair_item, 0, False)
        grad_mixed_item = lax.dynamic_index_in_dim(grad_mixed_pairs, pair_item, 0, False)
        totals_item = lax.dynamic_index_in_dim(log_totals, pair_item, 0, False)

        def backward_block(running, block_index):
            key_grad, value_grad = running
            first_row = block_index * block_rows
            query_block, scores = block_scores(pair_item, first_row)
            soft_probs = jnp.exp(
                scores - lax.dynamic_slice_in_dim(totals_item, first_row, block_rows, 0)[:, None]
            )
            grad_block = lax.dynamic_slice_in_dim(grad_mixed_item, first_row, block_rows, 0)
            grad_probs = jnp.einsum(
                "qe,ke->qk", grad_block, values_item, preferred_element_type=wide_type
            )
            row_inner = jnp.sum(grad_probs * soft_probs, -1, keepdims=True)
            grad_scores_low = (soft_probs * (grad_probs - row_inner)).astype(half_type)
            query_grad = (
                jnp.dot(grad_scores_low, keys_item, preferred_element_type=wide_type) * score_scale
            )
            key_grad = (
                key_grad
                + jnp.einsum(
                    "qk,qe->ke", grad_scores_low, query_block, preferred_element_type=wide_type
                )
                * score_scale
            )
            value_grad = value_grad + jnp.einsum(
                "qk,qe->ke",
                soft_probs.astype(half_type),
                grad_block,
                preferred_element_type=wide_type,
            )
            return ((key_grad, value_grad), query_grad)

        zero_rows = jnp.zeros((seq_length, head_dim), wide_type)
        (key_grad, value_grad), query_grads = lax.scan(
            backward_block, (zero_rows, zero_rows), jnp.arange(block_count, dtype=jnp.int32)
        )
        return jnp.stack(
            [query_grads.reshape(seq_length, head_dim), key_grad, value_grad], 0
        ).astype(half_type)

    grad_pairs = lax.map(backward_item, jnp.arange(pair_local, dtype=jnp.int32))
    grad_split = grad_pairs.reshape(pair_local, 3, seq_count, seq_rows, head_dim)
    grad_home = lax.all_to_all(grad_split, "seq", split_axis=2, concat_axis=0, tiled=True)
    grad_project_low = jnp.transpose(
        grad_home.reshape(micro_count, group_count, local_heads, 3, seq_rows, head_dim),
        (0, 1, 4, 2, 3, 5),
    ).reshape(micro_count, group_count, seq_rows, project_width)
    norm_one_part = jnp.einsum(
        "mstc,dc->mstd",
        grad_project_low,
        triple_back.reshape(model_width, project_width),
        preferred_element_type=wide_type,
    )
    grad_normed_one = lax.psum_scatter(
        norm_one_part.astype(jnp.bfloat16), "dp", scatter_dimension=1, tiled=True
    ).astype(jnp.float32)
    inputs_own = hidden.astype(wide_type)
    grad_inputs_norm, grad_gain_one, grad_shift_one = jax.vjp(
        layer_norm, inputs_own, gain_one, shift_one
    )[1](grad_normed_one)
    grad_middle_own = lax.dynamic_slice_in_dim(grad_middle, dp_index, 1, 1)
    hidden_grad = (grad_middle_own + grad_inputs_norm).astype(half_type)
    head_sums = jnp.sum(
        grad_project_low.reshape(micro_count, group_count, seq_rows, local_heads, 3, head_dim),
        (0, 1, 2),
        dtype=wide_type,
    )
    pair_grad = place_half(jnp.stack([head_sums[:, 0], head_sums[:, 2]], 1), dp_index, group_count)
    unit_grad = place_half(jnp.sum(grad_pre_low, (0, 1, 2), dtype=wide_type), dp_index, group_count)
    dense_shift_term = jnp.sum(
        lax.dynamic_slice_in_dim(grad_branch_low, dp_index, 1, 1), (0, 1, 2), dtype=wide_type
    )
    shrink_shift_term = jnp.sum(cotangent, (0, 1, 2), dtype=wide_type)
    gain_two_term = lax.dynamic_index_in_dim(grad_gain_rows_two, dp_index, 0, False)
    shift_two_term = lax.dynamic_index_in_dim(grad_shift_rows_two, dp_index, 0, False)
    vector_sums = (
        lax.psum_scatter(grad_gain_one, ("dp", "seq"), scatter_dimension=0, tiled=True),
        lax.psum_scatter(grad_shift_one, ("dp", "seq"), scatter_dimension=0, tiled=True),
        lax.psum_scatter(pair_grad, ("dp", "seq"), scatter_dimension=0, tiled=True),
        lax.psum_scatter(dense_shift_term, ("dp", "seq"), scatter_dimension=0, tiled=True),
        lax.psum_scatter(gain_two_term, ("dp", "seq"), scatter_dimension=0, tiled=True),
        lax.psum_scatter(shift_two_term, ("dp", "seq"), scatter_dimension=0, tiled=True),
        lax.psum_scatter(unit_grad, ("dp", "seq"), scatter_dimension=0, tiled=True),
        lax.psum_scatter(shrink_shift_term, ("dp", "seq"), scatter_dimension=0, tiled=True),
    )
    normed_flat = normed_low.reshape(token_total, model_width)
    project_flat = grad_project_low.reshape(token_total, project_width)
    normed_two_flat = normed_two_low.reshape(token_total, model_width)
    pre_flat = grad_pre_low.reshape(token_total, unit_local)
    column_sums = lax.psum_scatter(
        jnp.concatenate(
            [
                jnp.einsum(
                    "tr,tc->rc", normed_flat, project_flat, preferred_element_type=wide_type
                ),
                jnp.einsum(
                    "tr,tc->rc", normed_two_flat, pre_flat, preferred_element_type=wide_type
                ),
            ],
            1,
        ),
        "seq",
        scatter_dimension=0,
        tiled=True,
    )
    triple_grad = column_sums[:, :project_width].reshape(
        model_width // seq_count, local_heads, 3, head_dim
    )
    expand_grad = column_sums[:, project_width:]
    dense_rows = dense_weight.shape[0]
    shrink_rows = shrink_weight.shape[0]
    row_block = dense_rows + shrink_rows
    mixed_flat = mixed_tokens.reshape(token_total, local_heads * head_dim)
    branch_flat = grad_branch_low.reshape(token_total, model_width)
    active_flat = activated_low.reshape(token_total, unit_local)
    upstream_flat = upstream_low.reshape(token_total, model_width)
    block_number = row_block * lax.axis_size("seq") // row_block
    dense_term = jnp.einsum("tr,td->rd", mixed_flat, branch_flat, preferred_element_type=wide_type)
    shrink_term = jnp.einsum(
        "tr,td->rd", active_flat, upstream_flat, preferred_element_type=wide_type
    )
    row_sums = lax.psum_scatter(
        jnp.concatenate(
            [
                dense_term.reshape(block_number, dense_rows, model_width),
                shrink_term.reshape(block_number, shrink_rows, model_width),
            ],
            1,
        ).reshape(row_block * lax.axis_size("seq"), model_width),
        "seq",
        scatter_dimension=0,
        tiled=True,
    )
    dense_grad = row_sums[:dense_rows]
    shrink_grad = row_sums[dense_rows:]
    return (
        layer_output,
        hidden_grad,
        vector_sums[0],
        vector_sums[1],
        triple_grad,
        vector_sums[2],
        dense_grad,
        vector_sums[3],
        vector_sums[4],
        vector_sums[5],
        expand_grad,
        vector_sums[6],
        shrink_grad,
        vector_sums[7],
    )


def spread_rows(rows):
    return lax.all_to_all(rows, "z", split_axis=0, concat_axis=0, tiled=True)


def gather_columns(blocks):
    turned = lax.all_to_all(blocks, ("y", "x"), split_axis=0, concat_axis=0, tiled=True)
    return lax.all_gather(
        turned.reshape(-1, turned.shape[2]), "z", axis=0, tiled=True
    )


def scatter_columns(term, plane):
    own = lax.psum_scatter(term, "z", scatter_dimension=0, tiled=True)
    blocks = own.reshape(plane, own.shape[0] // plane, own.shape[1])
    return lax.all_to_all(blocks, ("y", "x"), split_axis=0, concat_axis=0, tiled=True)


def token_positions(index, rows_y, rows_x, depth, seq_rows):
    own_rows = depth * seq_rows
    chip = index // own_rows
    block = index % own_rows // seq_rows
    return (block * (rows_y * rows_x) + chip) * seq_rows + index % seq_rows


def attend_forward(
    projected, slopes, prefixes, cores, own_heads, head_dim, rows_y, rows_x, depth, seq_rows
):
    wide = jnp.float32
    length = projected.shape[0] // cores
    scale = 1.0 / math.sqrt(head_dim)
    grouped = projected.reshape(cores, length, own_heads, 3, head_dim)
    pos = token_positions(
        jnp.arange(length, dtype=jnp.int32), rows_y, rows_x, depth, seq_rows
    )

    def one(pair):
        seq, head = pair // own_heads, pair % own_heads
        item = grouped[seq, :, head]
        scores = jnp.einsum("qe,ke->qk", item[:, 0], item[:, 1], preferred_element_type=wide)
        distance = jnp.abs(pos[:, None] - pos[None, :]).astype(wide)
        scores = scores * scale - slopes[head] * distance
        allowed = (pos[None, :] <= pos[:, None]) | (pos[None, :] < prefixes[seq])
        scores = jnp.where(allowed, scores, jnp.float32(-1e30))
        row_max = jnp.max(scores, -1, keepdims=True)
        powers = jnp.exp(scores - row_max)
        total = jnp.sum(powers, -1, keepdims=True)
        probs = (powers / total).astype(jnp.bfloat16)
        mixed = jnp.dot(probs, item[:, 2], preferred_element_type=wide).astype(jnp.bfloat16)
        return mixed, (row_max + jnp.log(total))[:, 0]

    mixed, totals = lax.map(one, jnp.arange(cores * own_heads, dtype=jnp.int32))
    mixed = mixed.reshape(cores, own_heads, length, head_dim).transpose(0, 2, 1, 3)
    return mixed.reshape(cores * length, own_heads * head_dim), totals


def attend_backward(
    projected,
    grad_mixed,
    totals,
    slopes,
    prefixes,
    cores,
    own_heads,
    head_dim,
    rows_y,
    rows_x,
    depth,
    seq_rows,
):
    wide = jnp.float32
    half = jnp.bfloat16
    length = projected.shape[0] // cores
    scale = 1.0 / math.sqrt(head_dim)
    grouped = projected.reshape(cores, length, own_heads, 3, head_dim)
    upstream = grad_mixed.reshape(cores, length, own_heads, head_dim)
    pos = token_positions(
        jnp.arange(length, dtype=jnp.int32), rows_y, rows_x, depth, seq_rows
    )

    def one(pair):
        seq, head = pair // own_heads, pair % own_heads
        item = grouped[seq, :, head]
        grad = upstream[seq, :, head]
        scores = jnp.einsum("qe,ke->qk", item[:, 0], item[:, 1], preferred_element_type=wide)
        distance = jnp.abs(pos[:, None] - pos[None, :]).astype(wide)
        scores = scores * scale - slopes[head] * distance
        allowed = (pos[None, :] <= pos[:, None]) | (pos[None, :] < prefixes[seq])
        scores = jnp.where(allowed, scores, jnp.float32(-1e30))
        probs = jnp.exp(scores - totals[pair][:, None])
        grad_probs = jnp.einsum("qe,ke->qk", grad, item[:, 2], preferred_element_type=wide)
        inner = jnp.sum(grad_probs * probs, -1, keepdims=True)
        grad_scores = (probs * (grad_probs - inner)).astype(half)
        query = jnp.dot(grad_scores, item[:, 1], preferred_element_type=wide) * scale
        key = jnp.einsum("qk,qe->ke", grad_scores, item[:, 0], preferred_element_type=wide) * scale
        value = jnp.einsum("qk,qe->ke", probs.astype(half), grad, preferred_element_type=wide)
        return jnp.stack([query, key, value], 1).astype(half)

    grads = lax.map(one, jnp.arange(cores * own_heads, dtype=jnp.int32))
    grads = grads.reshape(cores, own_heads, length, 3, head_dim).transpose(0, 2, 1, 3, 4)
    return grads.reshape(cores * length, own_heads * 3 * head_dim)


def planar(
    hidden,
    prefix_lengths,
    cotangent,
    first_gain,
    first_shift,
    triple_weight,
    pair_bias,
    dense_weight,
    dense_shift,
    second_gain,
    second_shift,
    expand_weight,
    expand_shift,
    shrink_weight,
    shrink_shift,
):
    wide = jnp.float32
    half = jnp.bfloat16
    cores = lax.axis_size("dp")
    depth = lax.axis_size("z")
    rows_y = lax.axis_size("y")
    rows_x = lax.axis_size("x")
    plane = rows_y * rows_x
    core = lax.axis_index("dp")
    at_y = lax.axis_index("y")
    at_x = lax.axis_index("x")
    place = at_y * rows_x + at_x
    seq_rows = hidden.shape[2]
    width = hidden.shape[3]
    head_dim = triple_weight.shape[3]
    heads = triple_weight.shape[1]
    own_heads = heads // plane
    length = seq_rows * depth * plane
    own_rows = seq_rows * depth
    units = expand_weight.shape[1]
    own_units = units // plane
    row_block = expand_weight.shape[0]
    shrink_rows = shrink_weight.shape[0]
    group = ("dp", "y", "x")

    pieces = [
        first_gain,
        first_shift,
        dense_shift,
        second_gain,
        second_shift,
        shrink_shift,
        pair_bias,
        expand_shift,
    ]
    packed = lax.all_gather(
        jnp.concatenate(pieces), ("dp", "z", "y", "x"), axis=0, tiled=False
    ).reshape(-1, sum(p.shape[0] for p in pieces))
    vectors = []
    offset = 0
    for piece in pieces:
        vectors.append(packed[:, offset : offset + piece.shape[0]].reshape(-1).astype(wide))
        offset += piece.shape[0]
    gain_one, shift_one, dense_bias, gain_two, shift_two, shrink_bias, pair_full, unit_full = vectors
    pair_heads = pair_full.reshape(cores, rows_x, own_heads, rows_y, 2, head_dim)[
        core, at_x, :, at_y
    ]
    triple_bias = jnp.stack(
        [pair_heads[:, 0], jnp.zeros_like(pair_heads[:, 0]), pair_heads[:, 1]], 1
    ).reshape(-1)
    unit_bias = unit_full.reshape(cores, depth, plane, shrink_rows)[core, :, place].reshape(-1)

    triple_own = gather_columns(
        triple_weight.reshape(row_block, rows_x, own_heads, rows_y, 3 * head_dim)
        .transpose(3, 1, 0, 2, 4)
        .reshape(plane, row_block, own_heads * 3 * head_dim)
    )
    expand_own = gather_columns(
        expand_weight.reshape(row_block, depth, plane, shrink_rows)
        .transpose(2, 0, 1, 3)
        .reshape(plane, row_block, own_units)
    )
    shrink_own = lax.all_gather(shrink_weight, "z", axis=0, tiled=True)
    dense_rows = lax.all_gather(dense_weight, ("z", "x"), axis=0, tiled=True)
    dense_own = lax.dynamic_slice_in_dim(
        dense_rows, at_x * own_heads * head_dim, own_heads * head_dim, 0
    )

    inputs = spread_rows(hidden[:, 0]).reshape(own_rows, width).astype(wide)
    upstream = spread_rows(cotangent[:, 0]).reshape(own_rows, width)

    def gather_tokens(rows):
        return lax.all_gather(rows, group, axis=0, tiled=True)

    def scatter_tokens(partial):
        return lax.psum_scatter(partial, group, scatter_dimension=0, tiled=True).astype(wide)

    normed_own = layer_norm(inputs, gain_one, shift_one).astype(half)
    normed = gather_tokens(normed_own)
    upstream_all = gather_tokens(upstream)
    projected = (
        jnp.dot(normed, triple_own, preferred_element_type=wide) + triple_bias
    ).astype(half)

    head_index = core * heads + at_x * own_heads * rows_y + jnp.arange(own_heads) * rows_y + at_y
    slopes = jnp.power(
        jnp.float32(2.0), -8.0 * (head_index.astype(wide) + 1.0) / (heads * cores)
    )
    at_z = lax.axis_index("z")
    prefixes = lax.dynamic_index_in_dim(prefix_lengths, at_z, 0, False)
    mixed, log_totals = attend_forward(
        projected, slopes, prefixes, cores, own_heads, head_dim, rows_y, rows_x, depth, seq_rows
    )
    dense_part = jnp.dot(mixed, dense_own, preferred_element_type=wide).astype(half)
    middle = inputs + scatter_tokens(dense_part) + dense_bias
    normed_two_own, norm_two_pull = jax.vjp(layer_norm, middle, gain_two, shift_two)
    normed_two = gather_tokens(normed_two_own.astype(half))
    hidden_pre = jnp.dot(normed_two, expand_own, preferred_element_type=wide) + unit_bias
    activated, gelu_pull = jax.vjp(gelu_tanh, hidden_pre)
    activated = activated.astype(half)
    feed_part = jnp.dot(activated, shrink_own, preferred_element_type=wide).astype(half)
    layer_output = (middle + scatter_tokens(feed_part) + shrink_bias).astype(half)
    layer_output = spread_rows(layer_output.reshape(depth, seq_rows, width))[:, None]

    grad_act = jnp.einsum("tf,uf->tu", upstream_all, shrink_own, preferred_element_type=wide)
    grad_pre = gelu_pull(grad_act)[0].astype(half)
    norm_two_part = jnp.einsum(
        "tu,du->td", grad_pre, expand_own, preferred_element_type=wide
    ).astype(half)
    grad_norm_two, gain_two_term, shift_two_term = norm_two_pull(scatter_tokens(norm_two_part))
    grad_middle = upstream.astype(wide) + grad_norm_two
    branch_own = grad_middle.astype(half)
    branch = gather_tokens(branch_own)
    shrink_term = jnp.einsum(
        "tu,td->ud", activated, upstream_all, preferred_element_type=wide
    ).astype(half)
    shrink_grad = lax.psum_scatter(shrink_term, "z", scatter_dimension=0, tiled=True).astype(wide)
    expand_term = jnp.einsum(
        "td,tu->du", normed_two, grad_pre, preferred_element_type=wide
    ).astype(half)
    expand_grad = (
        scatter_columns(expand_term, plane)
        .reshape(plane, row_block, depth, shrink_rows)
        .transpose(1, 2, 0, 3)
        .reshape(row_block, units)
        .astype(wide)
    )

    grad_mixed = jnp.einsum("tf,ef->te", branch, dense_own, preferred_element_type=wide).astype(
        half
    )
    dense_term = jnp.einsum("te,tf->ef", mixed, branch, preferred_element_type=wide).astype(half)
    dense_wide = lax.dynamic_update_slice_in_dim(
        jnp.zeros_like(dense_rows), dense_term, at_x * own_heads * head_dim, 0
    )
    dense_grad = lax.psum_scatter(
        dense_wide, ("z", "x"), scatter_dimension=0, tiled=True
    ).astype(wide)
    grad_project = attend_backward(
        projected,
        grad_mixed,
        log_totals,
        slopes,
        prefixes,
        cores,
        own_heads,
        head_dim,
        rows_y,
        rows_x,
        depth,
        seq_rows,
    )
    norm_one_part = jnp.einsum(
        "tc,dc->td", grad_project, triple_own, preferred_element_type=wide
    ).astype(half)
    grad_norm_one, gain_one_term, shift_one_term = jax.vjp(
        layer_norm, inputs, gain_one, shift_one
    )[1](scatter_tokens(norm_one_part))
    hidden_grad = (grad_middle + grad_norm_one).astype(half)
    hidden_grad = spread_rows(hidden_grad.reshape(depth, seq_rows, width))[:, None]
    triple_term = jnp.einsum(
        "td,tc->dc", normed, grad_project, preferred_element_type=wide
    ).astype(half)
    triple_grad = (
        scatter_columns(triple_term, plane)
        .reshape(rows_y, rows_x, row_block, own_heads, 3 * head_dim)
        .transpose(2, 1, 3, 0, 4)
        .reshape(row_block, heads, 3, head_dim)
        .astype(wide)
    )

    head_sums = jnp.sum(grad_project, 0, dtype=wide).reshape(own_heads, 3, head_dim)
    pair_term = jnp.stack([head_sums[:, 0], head_sums[:, 2]], 1)
    pair_zero = jnp.zeros((cores, rows_x, own_heads, rows_y, 2, head_dim), wide)
    pair_wide = lax.dynamic_update_slice(
        pair_zero, pair_term[None, None, :, None], (core, at_x, 0, at_y, 0, 0)
    ).reshape(-1)
    unit_term = jnp.sum(grad_pre, 0, dtype=wide).reshape(1, depth, 1, shrink_rows)
    unit_wide = lax.dynamic_update_slice(
        jnp.zeros((cores, depth, plane, shrink_rows), wide), unit_term, (core, 0, place, 0)
    ).reshape(-1)
    terms = [
        gain_one_term,
        shift_one_term,
        jnp.sum(branch_own, 0, dtype=wide),
        gain_two_term,
        shift_two_term,
        jnp.sum(upstream, 0, dtype=wide),
        pair_wide,
        unit_wide,
    ]
    devices = cores * depth * plane
    summed = lax.psum_scatter(
        jnp.concatenate([t.reshape(devices, -1) for t in terms], 1),
        ("dp", "z", "y", "x"),
        scatter_dimension=0,
        tiled=True,
    ).reshape(-1)
    vector_grads = []
    offset = 0
    for piece in pieces:
        vector_grads.append(summed[offset : offset + piece.shape[0]])
        offset += piece.shape[0]
    return (
        layer_output,
        hidden_grad,
        vector_grads[0],
        vector_grads[1],
        triple_grad,
        vector_grads[6],
        dense_grad,
        vector_grads[2],
        vector_grads[3],
        vector_grads[4],
        expand_grad,
        vector_grads[7],
        shrink_grad,
        vector_grads[5],
    )


def solution(mesh):
    depth = 4
    sides = (2, 2)
    planar_plan = mesh.shape["seq"] == depth * sides[0] * sides[1]
    if planar_plan:
        grid = Mesh(
            mesh.devices.reshape(mesh.shape["dp"], depth, *sides), ("dp", "z", "y", "x")
        )
        seq = ("z", "y", "x")
    else:
        grid = mesh
        seq = ("seq",)
    tokens = P(None, "dp", seq, None)
    vector = P(("dp",) + seq)
    matrix = P(("dp",) + seq, None)
    placed = (
        tokens,
        P(),
        tokens,
        vector,
        vector,
        P(seq, "dp", None, None),
        vector,
        matrix,
        vector,
        vector,
        vector,
        P(seq, "dp"),
        vector,
        matrix,
        vector,
    )
    results = (
        tokens,
        tokens,
        vector,
        vector,
        P(seq, "dp", None, None),
        vector,
        matrix,
        vector,
        vector,
        vector,
        P(seq, "dp"),
        vector,
        matrix,
        vector,
    )
    return jax.shard_map(
        planar if planar_plan else shards,
        mesh=grid,
        in_specs=placed,
        out_specs=results,
        check_vma=False,
    )
```

```python
import functools
import math

import jax
import jax.numpy as jnp
from jax import lax
from jax.experimental import pallas as pl
from jax.experimental.pallas import tpu as pltpu
from jax.sharding import Mesh
from jax.sharding import PartitionSpec as P

EPSILON = 1e-05
GELU_SCALE = 0.7978845608028654


def layer_norm(inputs, norm_gain, norm_shift):
    centered = inputs - jnp.mean(inputs, -1, keepdims=True)
    variance = jnp.mean(centered * centered, -1, keepdims=True)
    return centered * lax.rsqrt(variance + EPSILON) * norm_gain + norm_shift


def gelu_tanh(values):
    return (
        0.5 * values * (1.0 + jnp.tanh(GELU_SCALE * (values + 0.044715 * values * values * values)))
    )


def split_norm(inputs, gain_rows, shift_rows):
    return layer_norm(inputs, gain_rows[None, :, None, :], shift_rows[None, :, None, :])


def place_half(values, half_index, group_count):
    chosen = (jnp.arange(group_count, dtype=jnp.int32) == half_index).astype(values.dtype)
    return (chosen[:, None] * values.reshape(1, -1)).reshape(-1)


def shards(
    hidden,
    prefix_lengths,
    cotangent,
    first_gain,
    first_shift,
    triple_weight,
    pair_bias,
    dense_weight,
    dense_shift,
    second_gain,
    second_shift,
    expand_weight,
    expand_shift,
    shrink_weight,
    shrink_shift,
):
    wide_type = jnp.float32
    half_type = jnp.bfloat16
    seq_count = lax.axis_size("seq")
    group_count = lax.axis_size("dp")
    dp_index = lax.axis_index("dp")
    seq_index = lax.axis_index("seq")
    micro_count = hidden.shape[0]
    seq_rows = hidden.shape[2]
    model_width = hidden.shape[3]
    seq_length = seq_rows * seq_count
    local_heads = triple_weight.shape[1]
    head_dim = triple_weight.shape[3]
    head_total = local_heads * group_count
    pair_local = micro_count * group_count * local_heads // seq_count
    unit_local = expand_weight.shape[1]
    project_width = 3 * local_heads * head_dim
    token_total = micro_count * group_count * seq_rows
    score_scale = 1.0 / math.sqrt(head_dim)
    block_rows = min(512, seq_length)
    block_count = seq_length // block_rows
    key_pos = jnp.arange(seq_length, dtype=jnp.int32)
    gathered = (
        lax.all_gather(triple_weight, "seq", axis=0, tiled=True),
        lax.all_gather(dense_weight, "seq", axis=0, tiled=True),
        lax.all_gather(expand_weight, "seq", axis=0, tiled=True),
        lax.all_gather(shrink_weight, "seq", axis=0, tiled=True),
        lax.all_gather(first_gain, "seq", axis=0, tiled=True),
        lax.all_gather(first_shift, "seq", axis=0, tiled=True),
        lax.all_gather(pair_bias, "seq", axis=0, tiled=True),
        lax.all_gather(dense_shift, "seq", axis=0, tiled=True),
        lax.all_gather(second_gain, "seq", axis=0, tiled=True),
        lax.all_gather(second_shift, "seq", axis=0, tiled=True),
        lax.all_gather(expand_shift, "seq", axis=0, tiled=True),
        lax.all_gather(shrink_shift, "seq", axis=0, tiled=True),
    )
    triple_full, dense_full, expand_full, shrink_full = (
        gathered[0],
        gathered[1],
        gathered[2],
        gathered[3],
    )
    row_sets = (
        lax.all_gather(hidden, "dp", axis=1, tiled=True),
        lax.all_gather(cotangent, "dp", axis=1, tiled=True),
        lax.all_gather(gathered[4], "dp", axis=0, tiled=True),
        lax.all_gather(gathered[5], "dp", axis=0, tiled=True),
        lax.all_gather(gathered[6], "dp", axis=0, tiled=True),
        lax.all_gather(gathered[7], "dp", axis=0, tiled=True),
        lax.all_gather(gathered[8], "dp", axis=0, tiled=True),
        lax.all_gather(gathered[9], "dp", axis=0, tiled=True),
        lax.all_gather(gathered[10], "dp", axis=0, tiled=True),
        lax.all_gather(gathered[11], "dp", axis=0, tiled=True),
    )
    hidden_both = row_sets[0]
    upstream_low = row_sets[1]
    gain_one, shift_one, pair_full, dense_bias, gain_two, shift_two, expand_bias, shrink_bias = [
        vector.astype(wide_type) for vector in row_sets[2:]
    ]
    inputs_both = hidden_both.astype(wide_type)
    normed_low = layer_norm(inputs_both, gain_one, shift_one).astype(half_type)
    pair_heads = lax.dynamic_slice_in_dim(
        pair_full.reshape(head_total, 2, head_dim), dp_index * local_heads, local_heads, 0
    )
    triple_bias = jnp.stack(
        [pair_heads[:, 0], jnp.zeros_like(pair_heads[:, 0]), pair_heads[:, 1]], 0
    )
    projected = jnp.einsum(
        "mstd,dhce->cmshte", normed_low, triple_full, preferred_element_type=wide_type
    )
    projected = projected + triple_bias[:, None, None, :, None, :]
    project_low = projected.astype(half_type).reshape(3, seq_count, pair_local, seq_rows, head_dim)
    pair_rows = lax.all_to_all(project_low, "seq", split_axis=1, concat_axis=3, tiled=True)[:, 0]
    query_all, key_all, value_all = (pair_rows[0], pair_rows[1], pair_rows[2])
    pair_index = seq_index * pair_local + jnp.arange(pair_local, dtype=jnp.int32)
    head_index = dp_index * local_heads + pair_index % local_heads
    sequence_index = pair_index // local_heads
    slopes = jnp.power(jnp.float32(2.0), -8.0 * (head_index.astype(wide_type) + 1.0) / head_total)
    prefix_flat = prefix_lengths.reshape(-1)
    prefix_slots = jnp.arange(prefix_flat.shape[0], dtype=jnp.int32)
    prefixes = jnp.sum(
        jnp.where(prefix_slots[None, :] == sequence_index[:, None], prefix_flat[None, :], 0), 1
    )

    def block_scores(pair_item, first_row):
        query_block = lax.dynamic_slice_in_dim(
            lax.dynamic_index_in_dim(query_all, pair_item, 0, False), first_row, block_rows, 0
        )
        keys_item = lax.dynamic_index_in_dim(key_all, pair_item, 0, False)
        head_slope = lax.dynamic_index_in_dim(slopes, pair_item, 0, False)
        prefix = lax.dynamic_index_in_dim(prefixes, pair_item, 0, False)
        query_pos = first_row + jnp.arange(block_rows, dtype=jnp.int32)
        raw_scores = (
            jnp.einsum("qe,ke->qk", query_block, keys_item, preferred_element_type=wide_type)
            * score_scale
        )
        distance = jnp.abs(query_pos[:, None] - key_pos[None, :]).astype(wide_type)
        raw_scores = raw_scores - head_slope * distance
        allowed = (key_pos[None, :] <= query_pos[:, None]) | (key_pos[None, :] < prefix)
        return (query_block, jnp.where(allowed, raw_scores, jnp.float32(-1e30)))

    def forward_block(flat_index):
        pair_item = flat_index // block_count
        first_row = flat_index % block_count * block_rows
        query_block, scores = block_scores(pair_item, first_row)
        row_max = jnp.max(scores, -1, keepdims=True)
        powers = jnp.exp(scores - row_max)
        row_total = jnp.sum(powers, -1, keepdims=True)
        probs_low = (powers / row_total).astype(half_type)
        values_item = lax.dynamic_index_in_dim(value_all, pair_item, 0, False)
        mixed = jnp.dot(probs_low, values_item, preferred_element_type=wide_type).astype(half_type)
        return (mixed, (row_max + jnp.log(row_total))[:, 0])

    mixed_blocks, log_blocks = lax.map(
        forward_block, jnp.arange(pair_local * block_count, dtype=jnp.int32)
    )
    mixed_pairs = mixed_blocks.reshape(pair_local, seq_count, seq_rows, head_dim)
    log_totals = log_blocks.reshape(pair_local, seq_length)
    mixed_home = lax.all_to_all(mixed_pairs, "seq", split_axis=1, concat_axis=0, tiled=True)
    mixed_tokens = jnp.transpose(
        mixed_home.reshape(micro_count, group_count, local_heads, seq_rows, head_dim),
        (0, 1, 3, 2, 4),
    ).reshape(micro_count, group_count, seq_rows, local_heads * head_dim)
    dense_part = jnp.einsum(
        "mstk,kf->mstf", mixed_tokens, dense_full, preferred_element_type=wide_type
    )
    attention_sum = lax.psum(dense_part.astype(jnp.bfloat16), "dp").astype(jnp.float32)
    middle = inputs_both + attention_sum + dense_bias
    gain_rows_two = jnp.broadcast_to(gain_two[None, :], (group_count, model_width))
    shift_rows_two = jnp.broadcast_to(shift_two[None, :], (group_count, model_width))
    normed_two, norm_two_pull = jax.vjp(split_norm, middle, gain_rows_two, shift_rows_two)
    normed_two_low = normed_two.astype(half_type)
    unit_bias = lax.dynamic_slice_in_dim(expand_bias, dp_index * unit_local, unit_local, 0)
    hidden_pre = (
        jnp.einsum("mstd,df->mstf", normed_two_low, expand_full, preferred_element_type=wide_type)
        + unit_bias
    )
    activated_value, gelu_pull = jax.vjp(gelu_tanh, hidden_pre)
    activated_low = activated_value.astype(half_type)
    feed_part = jnp.einsum(
        "mstf,fd->mstd", activated_low, shrink_full, preferred_element_type=wide_type
    )
    feed_sum = lax.psum_scatter(
        feed_part.astype(jnp.bfloat16), "dp", scatter_dimension=1, tiled=True
    ).astype(jnp.float32)
    middle_own = lax.dynamic_slice_in_dim(middle, dp_index, 1, 1)
    layer_output = (middle_own + feed_sum + shrink_bias).astype(half_type)
    triple_back, dense_back, expand_back, shrink_back = (
        lax.all_gather(triple_weight, "seq", axis=0, tiled=True),
        lax.all_gather(dense_weight, "seq", axis=0, tiled=True),
        lax.all_gather(expand_weight, "seq", axis=0, tiled=True),
        lax.all_gather(shrink_weight, "seq", axis=0, tiled=True),
    )
    grad_act = jnp.einsum(
        "mstd,fd->mstf", upstream_low, shrink_back, preferred_element_type=wide_type
    )
    grad_pre_low = gelu_pull(grad_act)[0].astype(half_type)
    norm_two_part = jnp.einsum(
        "mstf,df->mstd", grad_pre_low, expand_back, preferred_element_type=wide_type
    )
    grad_normed_two = lax.psum(norm_two_part.astype(jnp.bfloat16), "dp").astype(jnp.float32)
    grad_middle_norm, grad_gain_rows_two, grad_shift_rows_two = norm_two_pull(grad_normed_two)
    grad_middle = upstream_low.astype(wide_type) + grad_middle_norm
    grad_branch_low = grad_middle.astype(half_type)
    go_pairs = jnp.einsum(
        "mstf,hef->mshte",
        grad_branch_low,
        dense_back.reshape(local_heads, head_dim, model_width),
        preferred_element_type=wide_type,
    ).astype(half_type)
    go_pairs = go_pairs.reshape(seq_count, pair_local, seq_rows, head_dim)
    grad_mixed_pairs = lax.all_to_all(go_pairs, "seq", split_axis=0, concat_axis=2, tiled=True)[0]

    def backward_item(pair_item):
        keys_item = lax.dynamic_index_in_dim(key_all, pair_item, 0, False)
        values_item = lax.dynamic_index_in_dim(value_all, pair_item, 0, False)
        grad_mixed_item = lax.dynamic_index_in_dim(grad_mixed_pairs, pair_item, 0, False)
        totals_item = lax.dynamic_index_in_dim(log_totals, pair_item, 0, False)

        def backward_block(running, block_index):
            key_grad, value_grad = running
            first_row = block_index * block_rows
            query_block, scores = block_scores(pair_item, first_row)
            soft_probs = jnp.exp(
                scores - lax.dynamic_slice_in_dim(totals_item, first_row, block_rows, 0)[:, None]
            )
            grad_block = lax.dynamic_slice_in_dim(grad_mixed_item, first_row, block_rows, 0)
            grad_probs = jnp.einsum(
                "qe,ke->qk", grad_block, values_item, preferred_element_type=wide_type
            )
            row_inner = jnp.sum(grad_probs * soft_probs, -1, keepdims=True)
            grad_scores_low = (soft_probs * (grad_probs - row_inner)).astype(half_type)
            query_grad = (
                jnp.dot(grad_scores_low, keys_item, preferred_element_type=wide_type) * score_scale
            )
            key_grad = (
                key_grad
                + jnp.einsum(
                    "qk,qe->ke", grad_scores_low, query_block, preferred_element_type=wide_type
                )
                * score_scale
            )
            value_grad = value_grad + jnp.einsum(
                "qk,qe->ke",
                soft_probs.astype(half_type),
                grad_block,
                preferred_element_type=wide_type,
            )
            return ((key_grad, value_grad), query_grad)

        zero_rows = jnp.zeros((seq_length, head_dim), wide_type)
        (key_grad, value_grad), query_grads = lax.scan(
            backward_block, (zero_rows, zero_rows), jnp.arange(block_count, dtype=jnp.int32)
        )
        return jnp.stack(
            [query_grads.reshape(seq_length, head_dim), key_grad, value_grad], 0
        ).astype(half_type)

    grad_pairs = lax.map(backward_item, jnp.arange(pair_local, dtype=jnp.int32))
    grad_split = grad_pairs.reshape(pair_local, 3, seq_count, seq_rows, head_dim)
    grad_home = lax.all_to_all(grad_split, "seq", split_axis=2, concat_axis=0, tiled=True)
    grad_project_low = jnp.transpose(
        grad_home.reshape(micro_count, group_count, local_heads, 3, seq_rows, head_dim),
        (0, 1, 4, 2, 3, 5),
    ).reshape(micro_count, group_count, seq_rows, project_width)
    norm_one_part = jnp.einsum(
        "mstc,dc->mstd",
        grad_project_low,
        triple_back.reshape(model_width, project_width),
        preferred_element_type=wide_type,
    )
    grad_normed_one = lax.psum_scatter(
        norm_one_part.astype(jnp.bfloat16), "dp", scatter_dimension=1, tiled=True
    ).astype(jnp.float32)
    inputs_own = hidden.astype(wide_type)
    grad_inputs_norm, grad_gain_one, grad_shift_one = jax.vjp(
        layer_norm, inputs_own, gain_one, shift_one
    )[1](grad_normed_one)
    grad_middle_own = lax.dynamic_slice_in_dim(grad_middle, dp_index, 1, 1)
    hidden_grad = (grad_middle_own + grad_inputs_norm).astype(half_type)
    head_sums = jnp.sum(
        grad_project_low.reshape(micro_count, group_count, seq_rows, local_heads, 3, head_dim),
        (0, 1, 2),
        dtype=wide_type,
    )
    pair_grad = place_half(jnp.stack([head_sums[:, 0], head_sums[:, 2]], 1), dp_index, group_count)
    unit_grad = place_half(jnp.sum(grad_pre_low, (0, 1, 2), dtype=wide_type), dp_index, group_count)
    dense_shift_term = jnp.sum(
        lax.dynamic_slice_in_dim(grad_branch_low, dp_index, 1, 1), (0, 1, 2), dtype=wide_type
    )
    shrink_shift_term = jnp.sum(cotangent, (0, 1, 2), dtype=wide_type)
    gain_two_term = lax.dynamic_index_in_dim(grad_gain_rows_two, dp_index, 0, False)
    shift_two_term = lax.dynamic_index_in_dim(grad_shift_rows_two, dp_index, 0, False)
    vector_sums = (
        lax.psum_scatter(grad_gain_one, ("dp", "seq"), scatter_dimension=0, tiled=True),
        lax.psum_scatter(grad_shift_one, ("dp", "seq"), scatter_dimension=0, tiled=True),
        lax.psum_scatter(pair_grad, ("dp", "seq"), scatter_dimension=0, tiled=True),
        lax.psum_scatter(dense_shift_term, ("dp", "seq"), scatter_dimension=0, tiled=True),
        lax.psum_scatter(gain_two_term, ("dp", "seq"), scatter_dimension=0, tiled=True),
        lax.psum_scatter(shift_two_term, ("dp", "seq"), scatter_dimension=0, tiled=True),
        lax.psum_scatter(unit_grad, ("dp", "seq"), scatter_dimension=0, tiled=True),
        lax.psum_scatter(shrink_shift_term, ("dp", "seq"), scatter_dimension=0, tiled=True),
    )
    normed_flat = normed_low.reshape(token_total, model_width)
    project_flat = grad_project_low.reshape(token_total, project_width)
    normed_two_flat = normed_two_low.reshape(token_total, model_width)
    pre_flat = grad_pre_low.reshape(token_total, unit_local)
    column_sums = lax.psum_scatter(
        jnp.concatenate(
            [
                jnp.einsum(
                    "tr,tc->rc", normed_flat, project_flat, preferred_element_type=wide_type
                ),
                jnp.einsum(
                    "tr,tc->rc", normed_two_flat, pre_flat, preferred_element_type=wide_type
                ),
            ],
            1,
        ),
        "seq",
        scatter_dimension=0,
        tiled=True,
    )
    triple_grad = column_sums[:, :project_width].reshape(
        model_width // seq_count, local_heads, 3, head_dim
    )
    expand_grad = column_sums[:, project_width:]
    dense_rows = dense_weight.shape[0]
    shrink_rows = shrink_weight.shape[0]
    row_block = dense_rows + shrink_rows
    mixed_flat = mixed_tokens.reshape(token_total, local_heads * head_dim)
    branch_flat = grad_branch_low.reshape(token_total, model_width)
    active_flat = activated_low.reshape(token_total, unit_local)
    upstream_flat = upstream_low.reshape(token_total, model_width)
    block_number = row_block * lax.axis_size("seq") // row_block
    dense_term = jnp.einsum("tr,td->rd", mixed_flat, branch_flat, preferred_element_type=wide_type)
    shrink_term = jnp.einsum(
        "tr,td->rd", active_flat, upstream_flat, preferred_element_type=wide_type
    )
    row_sums = lax.psum_scatter(
        jnp.concatenate(
            [
                dense_term.reshape(block_number, dense_rows, model_width),
                shrink_term.reshape(block_number, shrink_rows, model_width),
            ],
            1,
        ).reshape(row_block * lax.axis_size("seq"), model_width),
        "seq",
        scatter_dimension=0,
        tiled=True,
    )
    dense_grad = row_sums[:dense_rows]
    shrink_grad = row_sums[dense_rows:]
    return (
        layer_output,
        hidden_grad,
        vector_sums[0],
        vector_sums[1],
        triple_grad,
        vector_sums[2],
        dense_grad,
        vector_sums[3],
        vector_sums[4],
        vector_sums[5],
        expand_grad,
        vector_sums[6],
        shrink_grad,
        vector_sums[7],
    )


CHUNKS = 4
LOG2E = 1.4426950408889634
MESH = pl.DeviceIdType.MESH


def remote(src, dst, send, recv, peer):
    return pltpu.make_async_remote_copy(
        src_ref=src,
        dst_ref=dst,
        send_sem=send,
        recv_sem=recv,
        device_id=peer,
        device_id_type=MESH,
    )


def greet(peers):
    barrier = pltpu.get_barrier_semaphore()
    for peer in peers:
        pl.semaphore_signal(barrier, inc=1, device_id=peer, device_id_type=MESH)
    pl.semaphore_wait(barrier, len(peers))


class Corner:
    def __init__(self):
        self.c = lax.axis_index("dp")
        self.y = lax.axis_index("y")
        self.x = lax.axis_index("x")
        self.ax = self.x + (1 - self.c) * (1 - 2 * self.x)
        self.ay = self.y + self.c * (1 - 2 * self.y)
        self.bx = self.x + self.c * (1 - 2 * self.x)
        self.by = self.y + (1 - self.c) * (1 - 2 * self.y)
        self.dx = 1 - self.x
        self.dy = 1 - self.y
        self.peer_a = {"y": self.ay, "x": self.ax}
        self.peer_b = {"y": self.by, "x": self.bx}
        self.sibling = {"dp": 1 - self.c}

    def slots(self, core):
        return [
            (core * 2 + y) * 2 + x
            for y, x in (
                (self.dy, self.dx),
                (self.by, self.bx),
                (self.ay, self.ax),
                (self.y, self.x),
            )
        ]


def gather_kernel(rows_ref, all_ref, local_sem, send, recv):
    at = Corner()
    slot_d, slot_b, slot_a, me = at.slots(at.c)
    step = rows_ref.shape[0] // CHUNKS
    greet([at.peer_a, at.peer_b, at.sibling])
    local = pltpu.make_async_copy(rows_ref, all_ref.at[me], local_sem)
    local.start()

    def copy(kind, k, slot, peer):
        part = pl.ds(k * step, step)
        src = rows_ref.at[part] if kind < 3 else all_ref.at[slot, part]
        return remote(src, all_ref.at[slot, part], send.at[kind, k], recv.at[kind, k], peer)

    def arrived(kind, k, slot, peer):
        part = pl.ds(k * step, step)
        block = all_ref.at[slot, part]
        remote(block, block, send.at[kind, k], recv.at[kind, k], peer).wait_recv()

    sent = []

    def start(kind, k, slot, peer):
        one = copy(kind, k, slot, peer)
        one.start()
        sent.append(one)

    for k in range(CHUNKS):
        start(0, k, me, at.peer_a)
        start(1, k, me, at.peer_b)
    for k in range(CHUNKS):
        start(2, k, me, at.sibling)
    for k in range(CHUNKS):
        arrived(0, k, slot_a, at.peer_a)
        start(3, k, slot_a, at.peer_b)
        start(4, k, slot_a, at.sibling)
    for k in range(CHUNKS):
        arrived(1, k, slot_b, at.peer_b)
        start(5, k, slot_b, at.sibling)
    for k in range(CHUNKS):
        arrived(3, k, slot_d, at.peer_b)
        start(6, k, slot_d, at.sibling)
    other_d, other_b, other_a, other_me = at.slots(1 - at.c)
    for k in range(CHUNKS):
        arrived(2, k, other_me, at.sibling)
        arrived(4, k, other_b, at.sibling)
        arrived(5, k, other_a, at.sibling)
        arrived(6, k, other_d, at.sibling)
    for one in sent:
        one.wait_send()
    local.wait()


def gather_tokens(rows):
    count, width = rows.shape
    return pl.pallas_call(
        gather_kernel,
        out_shape=jax.ShapeDtypeStruct((8, count, width), rows.dtype),
        in_specs=[pl.BlockSpec(memory_space=pl.ANY)],
        out_specs=pl.BlockSpec(memory_space=pl.ANY),
        scratch_shapes=[
            pltpu.SemaphoreType.DMA,
            pltpu.SemaphoreType.DMA((7, CHUNKS)),
            pltpu.SemaphoreType.DMA((7, CHUNKS)),
        ],
        compiler_params=pltpu.CompilerParams(collective_id=1, has_side_effects=True),
        cost_estimate=pl.CostEstimate(
            flops=0, bytes_accessed=16 * count * width * 4, transcendentals=0
        ),
        name="gather_tokens",
    )(rows).reshape(8 * count, width)


def scatter_kernel(part_ref, own_ref, from_core, from_b, from_a, send, recv):
    at = Corner()
    slot_d, slot_b, slot_a, me = at.slots(at.c)
    other_d, other_b, other_a, other_me = at.slots(1 - at.c)
    step = own_ref.shape[0] // CHUNKS
    wide = jnp.float32
    greet([at.peer_a, at.peer_b, at.sibling])
    sent = []

    def start(kind, k, src, dst, peer):
        one = remote(src, dst, send.at[kind, k], recv.at[kind, k], peer)
        one.start()
        sent.append(one)

    def arrived(kind, k, dst, peer):
        remote(dst, dst, send.at[kind, k], recv.at[kind, k], peer).wait_recv()

    for q, slot in enumerate((other_d, other_a, other_b, other_me)):
        for k in range(CHUNKS):
            part = pl.ds(k * step, step)
            start(q, k, part_ref.at[slot, part], from_core.at[q, part], at.sibling)
    for q, slot in enumerate((slot_d, slot_b)):
        for k in range(CHUNKS):
            part = pl.ds(k * step, step)
            arrived(q, k, from_core.at[q, part], at.sibling)
            total = part_ref[slot, part].astype(wide) + from_core[q, part].astype(wide)
            from_core[q, part] = total.astype(from_core.dtype)
            start(4 + q, k, from_core.at[q, part], from_b.at[q, part], at.peer_b)
    for k in range(CHUNKS):
        part = pl.ds(k * step, step)
        arrived(2, k, from_core.at[2, part], at.sibling)
        arrived(4, k, from_b.at[0, part], at.peer_b)
        total = part_ref[slot_a, part].astype(wide) + from_core[2, part].astype(wide)
        total = total + from_b[0, part].astype(wide)
        from_core[2, part] = total.astype(from_core.dtype)
        start(6, k, from_core.at[2, part], from_a.at[part], at.peer_a)
    for k in range(CHUNKS):
        part = pl.ds(k * step, step)
        arrived(3, k, from_core.at[3, part], at.sibling)
        arrived(5, k, from_b.at[1, part], at.peer_b)
        arrived(6, k, from_a.at[part], at.peer_a)
        total = part_ref[me, part].astype(wide) + from_core[3, part].astype(wide)
        total = total + from_b[1, part].astype(wide)
        own_ref[part] = total + from_a[part].astype(wide)
    for one in sent:
        one.wait_send()


def scatter_tokens(partial):
    count, width = partial.shape[0] // 8, partial.shape[1]
    return pl.pallas_call(
        scatter_kernel,
        out_shape=jax.ShapeDtypeStruct((count, width), jnp.float32),
        in_specs=[pl.BlockSpec(memory_space=pltpu.VMEM)],
        out_specs=pl.BlockSpec(memory_space=pltpu.VMEM),
        scratch_shapes=[
            pltpu.VMEM((4, count, width), partial.dtype),
            pltpu.VMEM((2, count, width), partial.dtype),
            pltpu.VMEM((count, width), partial.dtype),
            pltpu.SemaphoreType.DMA((7, CHUNKS)),
            pltpu.SemaphoreType.DMA((7, CHUNKS)),
        ],
        compiler_params=pltpu.CompilerParams(
            collective_id=2, has_side_effects=True, vmem_limit_bytes=40 * 2**20
        ),
        cost_estimate=pl.CostEstimate(
            flops=0, bytes_accessed=16 * count * width * 4, transcendentals=0
        ),
        name="scatter_tokens",
    )(partial.reshape(8, count, width))


def exchange_kernel(n_deep, n_flat, gathers, reduces, *refs):
    refs = list(refs)
    take = lambda n: [refs.pop(0) for _ in range(n)]
    deep_in, flat_in = take(n_deep), take(n_flat)
    vec_in = take(gathers + reduces)
    deep_out, flat_out = take(n_deep), take(n_flat)
    vec_out = take(gathers + reduces)
    near = take(reduces)
    far = take(reduces)
    here = take(reduces)
    send, recv = take(2)
    c, z = lax.axis_index("dp"), lax.axis_index("z")
    place = lax.axis_index("y") * 2 + lax.axis_index("x")
    rank = c * 4 + place

    def deep(i):
        return lax.rem(z + i, 4)

    def flat(i):
        return lax.rem(place + i, 4)

    def wide(i):
        return lax.rem(rank + i, 8)

    def deep_peer(i):
        return {"z": deep(i)}

    def flat_peer(i):
        return {"y": flat(i) // 2, "x": lax.rem(flat(i), 2)}

    def wide_peer(i):
        return {
            "dp": wide(i) // 4,
            "y": lax.rem(wide(i), 4) // 2,
            "x": lax.rem(wide(i), 2),
        }

    others = range(1, 4)
    peers = []
    if n_deep or gathers or reduces:
        peers += [deep_peer(i) for i in others]
    if gathers or reduces:
        peers += [wide_peer(i) for i in range(1, 8)]
    elif n_flat:
        peers += [flat_peer(i) for i in others]
    greet(peers)
    sent, waits = [], []
    count = [0]

    def post(src, dst, peer, landing):
        k = count[0]
        count[0] += 1
        one = remote(src, dst, send.at[k], recv.at[k], peer)
        one.start()
        sent.append(one)
        return remote(landing, landing, send.at[k], recv.at[k], peer)

    stage = []
    for i in range(1, 8) if gathers or reduces else ():
        if gathers:
            stage.append(
                post(
                    vec_in[0], vec_out[0].at[z, rank], wide_peer(i), vec_out[0].at[z, wide(8 - i)]
                )
            )
        else:
            stage.append(
                post(vec_in[0].at[wide(i)], near[0].at[rank], wide_peer(i), near[0].at[wide(8 - i)])
            )
    for index, me, peer, ins, outs in (
        (deep, z, deep_peer, deep_in, deep_out),
        (flat, place, flat_peer, flat_in, flat_out),
    ):
        for src, dst in zip(ins, outs):
            for i in others:
                waits.append(post(src.at[index(i)], dst.at[me], peer(i), dst.at[index(4 - i)]))
    for me, ins, outs in ((z, deep_in, deep_out), (place, flat_in, flat_out)):
        for src, dst in zip(ins, outs):
            dst[me] = src[me]
    if gathers:
        vec_out[0][z, rank] = vec_in[0][...]
        for one in stage:
            one.wait_recv()
        for i in others:
            waits.append(
                post(vec_out[0].at[z], vec_out[0].at[z], deep_peer(i), vec_out[0].at[deep(4 - i)])
            )
    if reduces:
        near[0][rank] = vec_in[0][rank]
        for one in stage:
            one.wait_recv()
        here[0][...] = jnp.sum(near[0][...], 0)
        last = []
        for i in others:
            last.append(
                post(here[0].at[deep(i)], far[0].at[z], deep_peer(i), far[0].at[deep(4 - i)])
            )
        far[0][z] = here[0][z]
        for one in last:
            one.wait_recv()
        vec_out[0][...] = jnp.sum(far[0][...], 0)
    for one in waits:
        one.wait_recv()
    for one in sent:
        one.wait_send()


def exchange(identity, deep, flat, gathered=None, reduced=None):
    vectors = [v for v in (gathered, reduced) if v is not None]
    shapes = [jax.ShapeDtypeStruct(a.shape, a.dtype) for a in (*deep, *flat)]
    scratch = []
    copies = 3 * (len(deep) + len(flat))
    if gathered is not None:
        shapes.append(jax.ShapeDtypeStruct((4, 8) + gathered.shape, gathered.dtype))
    if reduced is not None:
        tile = reduced.shape[2:]
        shapes.append(jax.ShapeDtypeStruct(tile, reduced.dtype))
        scratch = [
            pltpu.VMEM((8, 4) + tile, reduced.dtype),
            pltpu.VMEM((4,) + tile, reduced.dtype),
            pltpu.VMEM((4,) + tile, reduced.dtype),
        ]
    copies += 10 * len(vectors)
    operands = [*deep, *flat, *vectors]
    moved = sum(a.size * a.dtype.itemsize for a in operands)
    return pl.pallas_call(
        functools.partial(
            exchange_kernel, len(deep), len(flat), int(gathered is not None), int(reduced is not None)
        ),
        out_shape=shapes,
        in_specs=[pl.BlockSpec(memory_space=pltpu.VMEM)] * len(operands),
        out_specs=[pl.BlockSpec(memory_space=pltpu.VMEM)] * len(shapes),
        scratch_shapes=scratch
        + [pltpu.SemaphoreType.DMA((copies,)), pltpu.SemaphoreType.DMA((copies,))],
        compiler_params=pltpu.CompilerParams(
            collective_id=identity, has_side_effects=True, vmem_limit_bytes=40 * 2**20
        ),
        cost_estimate=pl.CostEstimate(flops=0, bytes_accessed=16 * moved, transcendentals=0),
        name=f"exchange_{identity}",
    )(*operands)


def scores_of(item_ref, first, block, slope, prefix, depth, seq_rows):
    length = item_ref.shape[0]
    head_dim = item_ref.shape[1] // 3
    own_rows = depth * seq_rows
    chips = length // own_rows

    def position(index):
        chip = index // own_rows
        rest = index % own_rows
        return ((rest // seq_rows) * chips + chip) * seq_rows + rest % seq_rows

    queries = item_ref[first : first + block, :head_dim]
    keys = item_ref[:, head_dim : 2 * head_dim]
    raw = lax.dot_general(
        keys, queries, (((1,), (1,)), ((), ())), preferred_element_type=jnp.float32
    )
    key_pos = position(lax.broadcasted_iota(jnp.int32, (length, 1), 0))
    query_pos = position(first + lax.broadcasted_iota(jnp.int32, (1, block), 1))
    bound = jnp.where(key_pos < prefix, -1, key_pos)
    distance = jnp.abs(
        query_pos.astype(jnp.float32) - key_pos.astype(jnp.float32)
    )
    scores = raw * (LOG2E / math.sqrt(head_dim)) - (slope * LOG2E) * distance
    return jnp.where(bound <= query_pos, scores, jnp.float32(-1e30))


def forward_kernel(depth, seq_rows, block, prefix_ref, slope_ref, item_ref, mixed_ref, total_ref):
    prefix = prefix_ref[pl.program_id(0)]
    slope = slope_ref[pl.program_id(1)]
    length = item_ref.shape[0]
    head_dim = item_ref.shape[1] // 3
    for first in range(0, length, block):
        scores = scores_of(item_ref, first, block, slope, prefix, depth, seq_rows)
        top = jnp.max(scores, 0, keepdims=True)
        powers = jnp.exp2(scores - top)
        total = jnp.sum(powers, 0, keepdims=True)
        probs = (powers * (1.0 / total)).astype(jnp.bfloat16)
        mixed = lax.dot_general(
            probs,
            item_ref[:, 2 * head_dim :],
            (((0,), (0,)), ((), ())),
            preferred_element_type=jnp.float32,
        )
        mixed_ref[first : first + block, :] = mixed.astype(mixed_ref.dtype)
        total_ref[0, :, first : first + block] = top + jnp.log2(total)


def attend_forward(projected, slopes, prefixes, own_heads, head_dim, depth, seq_rows):
    cores = prefixes.shape[0]
    length = projected.shape[0] // cores
    block = min(256, length)
    scores = cores * own_heads * length * length
    return pl.pallas_call(
        functools.partial(forward_kernel, depth, seq_rows, block),
        grid=(cores, own_heads),
        out_shape=[
            jax.ShapeDtypeStruct((cores * length, own_heads * head_dim), projected.dtype),
            jax.ShapeDtypeStruct((cores * own_heads, 1, length), jnp.float32),
        ],
        in_specs=[
            pl.BlockSpec(memory_space=pltpu.SMEM),
            pl.BlockSpec(memory_space=pltpu.SMEM),
            pl.BlockSpec((length, 3 * head_dim), lambda s, h: (s, h)),
        ],
        out_specs=[
            pl.BlockSpec((length, head_dim), lambda s, h: (s, h)),
            pl.BlockSpec((1, 1, length), lambda s, h: (s * own_heads + h, 0, 0)),
        ],
        compiler_params=pltpu.CompilerParams(vmem_limit_bytes=48 * 2**20),
        cost_estimate=pl.CostEstimate(
            flops=4 * scores * head_dim,
            bytes_accessed=2 * projected.size * 2,
            transcendentals=scores,
        ),
        name="attend_forward",
    )(prefixes, slopes, projected)


def backward_kernel(
    depth, seq_rows, block, prefix_ref, slope_ref, item_ref, grad_ref, total_ref, out_ref, key_sum, value_sum
):
    prefix = prefix_ref[pl.program_id(0)]
    slope = slope_ref[pl.program_id(1)]
    length = item_ref.shape[0]
    head_dim = item_ref.shape[1] // 3
    scale = 1.0 / math.sqrt(head_dim)
    half = jnp.bfloat16
    wide = jnp.float32
    for first in range(0, length, block):
        scores = scores_of(item_ref, first, block, slope, prefix, depth, seq_rows)
        probs = jnp.exp2(scores - total_ref[0, :, first : first + block])
        grad = grad_ref[first : first + block, :]
        grad_probs = lax.dot_general(
            item_ref[:, 2 * head_dim :],
            grad,
            (((1,), (1,)), ((), ())),
            preferred_element_type=wide,
        )
        inner = jnp.sum(grad_probs * probs, 0, keepdims=True)
        grad_scores = (probs * (grad_probs - inner)).astype(half)
        key_term = jnp.dot(
            grad_scores, item_ref[first : first + block, :head_dim], preferred_element_type=wide
        )
        value_term = jnp.dot(probs.astype(half), grad, preferred_element_type=wide)
        query_grad = lax.dot_general(
            grad_scores,
            item_ref[:, head_dim : 2 * head_dim],
            (((0,), (0,)), ((), ())),
            preferred_element_type=wide,
        )
        out_ref[first : first + block, :head_dim] = (query_grad * scale).astype(half)
        if first == 0:
            key_sum[...] = key_term
            value_sum[...] = value_term
        else:
            key_sum[...] += key_term
            value_sum[...] += value_term
    out_ref[:, head_dim : 2 * head_dim] = (key_sum[...] * scale).astype(half)
    out_ref[:, 2 * head_dim :] = value_sum[...].astype(half)


def attend_backward(
    projected, grad_mixed, totals, slopes, prefixes, own_heads, head_dim, depth, seq_rows
):
    cores = prefixes.shape[0]
    length = projected.shape[0] // cores
    block = min(256, length)
    scores = cores * own_heads * length * length
    return pl.pallas_call(
        functools.partial(backward_kernel, depth, seq_rows, block),
        grid=(cores, own_heads),
        out_shape=jax.ShapeDtypeStruct(projected.shape, projected.dtype),
        in_specs=[
            pl.BlockSpec(memory_space=pltpu.SMEM),
            pl.BlockSpec(memory_space=pltpu.SMEM),
            pl.BlockSpec((length, 3 * head_dim), lambda s, h: (s, h)),
            pl.BlockSpec((length, head_dim), lambda s, h: (s, h)),
            pl.BlockSpec((1, 1, length), lambda s, h: (s * own_heads + h, 0, 0)),
        ],
        out_specs=pl.BlockSpec((length, 3 * head_dim), lambda s, h: (s, h)),
        scratch_shapes=[
            pltpu.VMEM((length, head_dim), jnp.float32),
            pltpu.VMEM((length, head_dim), jnp.float32),
        ],
        compiler_params=pltpu.CompilerParams(vmem_limit_bytes=48 * 2**20),
        cost_estimate=pl.CostEstimate(
            flops=10 * scores * head_dim,
            bytes_accessed=2 * projected.size * 2,
            transcendentals=scores,
        ),
        name="attend_backward",
    )(prefixes, slopes, projected, grad_mixed, totals)


def planar(
    hidden,
    prefix_lengths,
    cotangent,
    first_gain,
    first_shift,
    triple_weight,
    pair_bias,
    dense_weight,
    dense_shift,
    second_gain,
    second_shift,
    expand_weight,
    expand_shift,
    shrink_weight,
    shrink_shift,
):
    wide = jnp.float32
    half = jnp.bfloat16
    cores = lax.axis_size("dp")
    depth = lax.axis_size("z")
    rows_y = lax.axis_size("y")
    rows_x = lax.axis_size("x")
    plane = rows_y * rows_x
    core = lax.axis_index("dp")
    at_y = lax.axis_index("y")
    at_x = lax.axis_index("x")
    place = at_y * rows_x + at_x
    seq_rows = hidden.shape[2]
    width = hidden.shape[3]
    head_dim = triple_weight.shape[3]
    heads = triple_weight.shape[1]
    own_heads = heads // plane
    own_rows = seq_rows * depth
    units = expand_weight.shape[1]
    own_units = units // plane
    row_block = expand_weight.shape[0]
    shrink_rows = shrink_weight.shape[0]

    pieces = [
        first_gain,
        first_shift,
        dense_shift,
        second_gain,
        second_shift,
        shrink_shift,
        pair_bias,
        expand_shift,
    ]
    piece_total = sum(p.shape[0] for p in pieces)
    lanes = 128
    vector_rows = -(-piece_total // (lanes * 16)) * 16
    vector_tile = jnp.pad(
        jnp.concatenate(pieces), (0, vector_rows * lanes - piece_total)
    ).reshape(vector_rows, lanes)
    triple_blocks = (
        triple_weight.reshape(row_block, rows_x, own_heads, rows_y, 3 * head_dim)
        .transpose(3, 1, 0, 2, 4)
        .reshape(plane, row_block, own_heads * 3 * head_dim)
    )
    expand_blocks = (
        expand_weight.reshape(row_block, depth, plane, shrink_rows)
        .transpose(2, 0, 1, 3)
        .reshape(plane, row_block, own_units)
    )
    inputs, upstream, triple_turned, expand_turned, packed = exchange(
        3, (hidden[:, 0], cotangent[:, 0]), (triple_blocks, expand_blocks), gathered=vector_tile
    )
    packed = (
        packed.reshape(depth, cores, plane, vector_rows * lanes)
        .transpose(1, 0, 2, 3)
        .reshape(-1, vector_rows * lanes)
    )
    vectors = []
    offset = 0
    for piece in pieces:
        vectors.append(packed[:, offset : offset + piece.shape[0]].reshape(-1).astype(wide))
        offset += piece.shape[0]
    gain_one, shift_one, dense_bias, gain_two, shift_two, shrink_bias, pair_full, unit_full = vectors
    pair_heads = pair_full.reshape(cores, rows_x, own_heads, rows_y, 2, head_dim)[
        core, at_x, :, at_y
    ]
    triple_bias = jnp.stack(
        [pair_heads[:, 0], jnp.zeros_like(pair_heads[:, 0]), pair_heads[:, 1]], 1
    ).reshape(-1)
    unit_bias = unit_full.reshape(cores, depth, plane, shrink_rows)[core, :, place].reshape(-1)

    triple_own = lax.all_gather(
        triple_turned.reshape(-1, triple_turned.shape[2]), "z", axis=0, tiled=True
    )
    expand_own = lax.all_gather(
        expand_turned.reshape(-1, expand_turned.shape[2]), "z", axis=0, tiled=True
    )
    shrink_own = lax.all_gather(shrink_weight, "z", axis=0, tiled=True)
    dense_rows = lax.all_gather(dense_weight, ("z", "x"), axis=0, tiled=True)
    dense_own = lax.dynamic_slice_in_dim(
        dense_rows, at_x * own_heads * head_dim, own_heads * head_dim, 0
    )

    inputs = inputs.reshape(own_rows, width).astype(wide)
    upstream = upstream.reshape(own_rows, width)

    normed_own = layer_norm(inputs, gain_one, shift_one).astype(half)
    normed = gather_tokens(normed_own)
    upstream_all = gather_tokens(upstream)
    projected = (
        jnp.dot(normed, triple_own, preferred_element_type=wide) + triple_bias
    ).astype(half)

    head_index = core * heads + at_x * own_heads * rows_y + jnp.arange(own_heads) * rows_y + at_y
    slopes = jnp.power(
        jnp.float32(2.0), -8.0 * (head_index.astype(wide) + 1.0) / (heads * cores)
    )
    at_z = lax.axis_index("z")
    prefixes = lax.dynamic_index_in_dim(prefix_lengths, at_z, 0, False)
    mixed, log_totals = attend_forward(
        projected, slopes, prefixes, own_heads, head_dim, depth, seq_rows
    )
    dense_part = jnp.dot(mixed, dense_own, preferred_element_type=wide).astype(half)
    middle = inputs + scatter_tokens(dense_part) + dense_bias
    normed_two_own, norm_two_pull = jax.vjp(layer_norm, middle, gain_two, shift_two)
    normed_two = gather_tokens(normed_two_own.astype(half))
    hidden_pre = jnp.dot(normed_two, expand_own, preferred_element_type=wide) + unit_bias
    activated, gelu_pull = jax.vjp(gelu_tanh, hidden_pre)
    activated = activated.astype(half)
    feed_part = jnp.dot(activated, shrink_own, preferred_element_type=wide).astype(half)
    layer_output = (middle + scatter_tokens(feed_part) + shrink_bias).astype(half)

    grad_act = jnp.einsum("tf,uf->tu", upstream_all, shrink_own, preferred_element_type=wide)
    grad_pre = gelu_pull(grad_act)[0].astype(half)
    norm_two_part = jnp.einsum(
        "tu,du->td", grad_pre, expand_own, preferred_element_type=wide
    ).astype(half)
    grad_norm_two, gain_two_term, shift_two_term = norm_two_pull(scatter_tokens(norm_two_part))
    grad_middle = upstream.astype(wide) + grad_norm_two
    branch_own = grad_middle.astype(half)
    branch = gather_tokens(branch_own)
    shrink_term = jnp.einsum(
        "tu,td->ud", activated, upstream_all, preferred_element_type=wide
    ).astype(half)
    shrink_grad = lax.psum_scatter(shrink_term, "z", scatter_dimension=0, tiled=True).astype(wide)
    expand_term = jnp.einsum(
        "td,tu->du", normed_two, grad_pre, preferred_element_type=wide
    ).astype(half)
    expand_turned = lax.psum_scatter(expand_term, "z", scatter_dimension=0, tiled=True)
    grad_mixed = jnp.einsum("tf,ef->te", branch, dense_own, preferred_element_type=wide).astype(
        half
    )
    dense_term = jnp.einsum("te,tf->ef", mixed, branch, preferred_element_type=wide).astype(half)
    dense_wide = lax.dynamic_update_slice_in_dim(
        jnp.zeros_like(dense_rows), dense_term, at_x * own_heads * head_dim, 0
    )
    dense_grad = lax.psum_scatter(
        dense_wide, ("z", "x"), scatter_dimension=0, tiled=True
    ).astype(wide)
    grad_project = attend_backward(
        projected,
        grad_mixed,
        log_totals,
        slopes,
        prefixes,
        own_heads,
        head_dim,
        depth,
        seq_rows,
    )
    norm_one_part = jnp.einsum(
        "tc,dc->td", grad_project, triple_own, preferred_element_type=wide
    ).astype(half)
    grad_norm_one, gain_one_term, shift_one_term = jax.vjp(
        layer_norm, inputs, gain_one, shift_one
    )[1](scatter_tokens(norm_one_part))
    hidden_grad = (grad_middle + grad_norm_one).astype(half)
    triple_term = jnp.einsum(
        "td,tc->dc", normed, grad_project, preferred_element_type=wide
    ).astype(half)
    triple_turned = lax.psum_scatter(triple_term, "z", scatter_dimension=0, tiled=True)

    head_sums = jnp.sum(grad_project, 0, dtype=wide).reshape(own_heads, 3, head_dim)
    pair_term = jnp.stack([head_sums[:, 0], head_sums[:, 2]], 1)
    pair_zero = jnp.zeros((cores, rows_x, own_heads, rows_y, 2, head_dim), wide)
    pair_wide = lax.dynamic_update_slice(
        pair_zero, pair_term[None, None, :, None], (core, at_x, 0, at_y, 0, 0)
    ).reshape(-1)
    unit_term = jnp.sum(grad_pre, 0, dtype=wide).reshape(1, depth, 1, shrink_rows)
    unit_wide = lax.dynamic_update_slice(
        jnp.zeros((cores, depth, plane, shrink_rows), wide), unit_term, (core, 0, place, 0)
    ).reshape(-1)
    terms = [
        gain_one_term,
        shift_one_term,
        jnp.sum(branch_own, 0, dtype=wide),
        gain_two_term,
        shift_two_term,
        jnp.sum(upstream, 0, dtype=wide),
        pair_wide,
        unit_wide,
    ]
    devices = cores * depth * plane
    term_rows = -(-piece_total // (lanes * 8)) * 8
    term_tiles = jnp.pad(
        jnp.concatenate([t.reshape(devices, -1) for t in terms], 1),
        ((0, 0), (0, term_rows * lanes - piece_total)),
    )
    term_tiles = (
        term_tiles.reshape(cores, depth, plane, term_rows, lanes)
        .transpose(0, 2, 1, 3, 4)
        .reshape(cores * plane, depth, term_rows, lanes)
    )
    layer_output, hidden_grad, expand_grad, summed = exchange(
        4,
        (layer_output.reshape(depth, seq_rows, width), hidden_grad.reshape(depth, seq_rows, width)),
        (expand_turned.reshape(plane, row_block, own_units),),
        reduced=term_tiles,
    )
    layer_output = layer_output[:, None]
    hidden_grad = hidden_grad[:, None]
    expand_grad = (
        expand_grad.reshape(plane, row_block, depth, shrink_rows)
        .transpose(1, 2, 0, 3)
        .reshape(row_block, units)
        .astype(wide)
    )
    (triple_grad,) = exchange(5, (), (triple_turned.reshape(plane, row_block, -1),))
    triple_grad = (
        triple_grad.reshape(rows_y, rows_x, row_block, own_heads, 3 * head_dim)
        .transpose(2, 1, 3, 0, 4)
        .reshape(row_block, heads, 3, head_dim)
        .astype(wide)
    )
    summed = summed.reshape(-1)
    vector_grads = []
    offset = 0
    for piece in pieces:
        vector_grads.append(summed[offset : offset + piece.shape[0]])
        offset += piece.shape[0]
    return (
        layer_output,
        hidden_grad,
        vector_grads[0],
        vector_grads[1],
        triple_grad,
        vector_grads[6],
        dense_grad,
        vector_grads[2],
        vector_grads[3],
        vector_grads[4],
        expand_grad,
        vector_grads[7],
        shrink_grad,
        vector_grads[5],
    )


def solution(mesh):
    depth = 4
    sides = (2, 2)
    planar_plan = mesh.shape["seq"] == depth * sides[0] * sides[1]
    if planar_plan:
        grid = Mesh(
            mesh.devices.reshape(mesh.shape["dp"], depth, *sides), ("dp", "z", "y", "x")
        )
        seq = ("z", "y", "x")
    else:
        grid = mesh
        seq = ("seq",)
    tokens = P(None, "dp", seq, None)
    vector = P(("dp",) + seq)
    matrix = P(("dp",) + seq, None)
    placed = (
        tokens,
        P(),
        tokens,
        vector,
        vector,
        P(seq, "dp", None, None),
        vector,
        matrix,
        vector,
        vector,
        vector,
        P(seq, "dp"),
        vector,
        matrix,
        vector,
    )
    results = (
        tokens,
        tokens,
        vector,
        vector,
        P(seq, "dp", None, None),
        vector,
        matrix,
        vector,
        vector,
        vector,
        P(seq, "dp"),
        vector,
        matrix,
        vector,
    )
    return jax.shard_map(
        planar if planar_plan else shards,
        mesh=grid,
        in_specs=placed,
        out_specs=results,
        check_vma=False,
    )
```

```python
import functools
import math

import jax
import jax.numpy as jnp
from jax import lax
from jax.experimental import pallas as pl
from jax.experimental.pallas import tpu as pltpu
from jax.sharding import Mesh
from jax.sharding import PartitionSpec as P


EPSILON = 1e-05
GELU_SCALE = 0.7978845608028654


def layer_norm(inputs, norm_gain, norm_shift):
    centered = inputs - jnp.mean(inputs, -1, keepdims=True)
    variance = jnp.mean(centered * centered, -1, keepdims=True)
    return centered * lax.rsqrt(variance + EPSILON) * norm_gain + norm_shift


def gelu_tanh(values):
    return (
        0.5 * values * (1.0 + jnp.tanh(GELU_SCALE * (values + 0.044715 * values * values * values)))
    )


def split_norm(inputs, gain_rows, shift_rows):
    return layer_norm(inputs, gain_rows[None, :, None, :], shift_rows[None, :, None, :])


def place_half(values, half_index, group_count):
    chosen = (jnp.arange(group_count, dtype=jnp.int32) == half_index).astype(values.dtype)
    return (chosen[:, None] * values.reshape(1, -1)).reshape(-1)


def shards(
    hidden,
    prefix_lengths,
    cotangent,
    first_gain,
    first_shift,
    triple_weight,
    pair_bias,
    dense_weight,
    dense_shift,
    second_gain,
    second_shift,
    expand_weight,
    expand_shift,
    shrink_weight,
    shrink_shift,
):
    wide_type = jnp.float32
    half_type = jnp.bfloat16
    seq_count = lax.axis_size("seq")
    group_count = lax.axis_size("dp")
    dp_index = lax.axis_index("dp")
    seq_index = lax.axis_index("seq")
    micro_count = hidden.shape[0]
    seq_rows = hidden.shape[2]
    model_width = hidden.shape[3]
    seq_length = seq_rows * seq_count
    local_heads = triple_weight.shape[1]
    head_dim = triple_weight.shape[3]
    head_total = local_heads * group_count
    pair_local = micro_count * group_count * local_heads // seq_count
    unit_local = expand_weight.shape[1]
    project_width = 3 * local_heads * head_dim
    token_total = micro_count * group_count * seq_rows
    score_scale = 1.0 / math.sqrt(head_dim)
    block_rows = min(512, seq_length)
    block_count = seq_length // block_rows
    key_pos = jnp.arange(seq_length, dtype=jnp.int32)
    gathered = (
        lax.all_gather(triple_weight, "seq", axis=0, tiled=True),
        lax.all_gather(dense_weight, "seq", axis=0, tiled=True),
        lax.all_gather(expand_weight, "seq", axis=0, tiled=True),
        lax.all_gather(shrink_weight, "seq", axis=0, tiled=True),
        lax.all_gather(first_gain, "seq", axis=0, tiled=True),
        lax.all_gather(first_shift, "seq", axis=0, tiled=True),
        lax.all_gather(pair_bias, "seq", axis=0, tiled=True),
        lax.all_gather(dense_shift, "seq", axis=0, tiled=True),
        lax.all_gather(second_gain, "seq", axis=0, tiled=True),
        lax.all_gather(second_shift, "seq", axis=0, tiled=True),
        lax.all_gather(expand_shift, "seq", axis=0, tiled=True),
        lax.all_gather(shrink_shift, "seq", axis=0, tiled=True),
    )
    triple_full, dense_full, expand_full, shrink_full = (
        gathered[0],
        gathered[1],
        gathered[2],
        gathered[3],
    )
    row_sets = (
        lax.all_gather(hidden, "dp", axis=1, tiled=True),
        lax.all_gather(cotangent, "dp", axis=1, tiled=True),
        lax.all_gather(gathered[4], "dp", axis=0, tiled=True),
        lax.all_gather(gathered[5], "dp", axis=0, tiled=True),
        lax.all_gather(gathered[6], "dp", axis=0, tiled=True),
        lax.all_gather(gathered[7], "dp", axis=0, tiled=True),
        lax.all_gather(gathered[8], "dp", axis=0, tiled=True),
        lax.all_gather(gathered[9], "dp", axis=0, tiled=True),
        lax.all_gather(gathered[10], "dp", axis=0, tiled=True),
        lax.all_gather(gathered[11], "dp", axis=0, tiled=True),
    )
    hidden_both = row_sets[0]
    upstream_low = row_sets[1]
    gain_one, shift_one, pair_full, dense_bias, gain_two, shift_two, expand_bias, shrink_bias = [
        vector.astype(wide_type) for vector in row_sets[2:]
    ]
    inputs_both = hidden_both.astype(wide_type)
    normed_low = layer_norm(inputs_both, gain_one, shift_one).astype(half_type)
    pair_heads = lax.dynamic_slice_in_dim(
        pair_full.reshape(head_total, 2, head_dim), dp_index * local_heads, local_heads, 0
    )
    triple_bias = jnp.stack(
        [pair_heads[:, 0], jnp.zeros_like(pair_heads[:, 0]), pair_heads[:, 1]], 0
    )
    projected = jnp.einsum(
        "mstd,dhce->cmshte", normed_low, triple_full, preferred_element_type=wide_type
    )
    projected = projected + triple_bias[:, None, None, :, None, :]
    project_low = projected.astype(half_type).reshape(3, seq_count, pair_local, seq_rows, head_dim)
    pair_rows = lax.all_to_all(project_low, "seq", split_axis=1, concat_axis=3, tiled=True)[:, 0]
    query_all, key_all, value_all = (pair_rows[0], pair_rows[1], pair_rows[2])
    pair_index = seq_index * pair_local + jnp.arange(pair_local, dtype=jnp.int32)
    head_index = dp_index * local_heads + pair_index % local_heads
    sequence_index = pair_index // local_heads
    slopes = jnp.power(jnp.float32(2.0), -8.0 * (head_index.astype(wide_type) + 1.0) / head_total)
    prefix_flat = prefix_lengths.reshape(-1)
    prefix_slots = jnp.arange(prefix_flat.shape[0], dtype=jnp.int32)
    prefixes = jnp.sum(
        jnp.where(prefix_slots[None, :] == sequence_index[:, None], prefix_flat[None, :], 0), 1
    )

    def block_scores(pair_item, first_row):
        query_block = lax.dynamic_slice_in_dim(
            lax.dynamic_index_in_dim(query_all, pair_item, 0, False), first_row, block_rows, 0
        )
        keys_item = lax.dynamic_index_in_dim(key_all, pair_item, 0, False)
        head_slope = lax.dynamic_index_in_dim(slopes, pair_item, 0, False)
        prefix = lax.dynamic_index_in_dim(prefixes, pair_item, 0, False)
        query_pos = first_row + jnp.arange(block_rows, dtype=jnp.int32)
        raw_scores = (
            jnp.einsum("qe,ke->qk", query_block, keys_item, preferred_element_type=wide_type)
            * score_scale
        )
        distance = jnp.abs(query_pos[:, None] - key_pos[None, :]).astype(wide_type)
        raw_scores = raw_scores - head_slope * distance
        allowed = (key_pos[None, :] <= query_pos[:, None]) | (key_pos[None, :] < prefix)
        return (query_block, jnp.where(allowed, raw_scores, jnp.float32(-1e30)))

    def forward_block(flat_index):
        pair_item = flat_index // block_count
        first_row = flat_index % block_count * block_rows
        _, scores = block_scores(pair_item, first_row)
        row_max = jnp.max(scores, -1, keepdims=True)
        powers = jnp.exp(scores - row_max)
        row_total = jnp.sum(powers, -1, keepdims=True)
        probs_low = (powers / row_total).astype(half_type)
        values_item = lax.dynamic_index_in_dim(value_all, pair_item, 0, False)
        mixed = jnp.dot(probs_low, values_item, preferred_element_type=wide_type).astype(half_type)
        return (mixed, (row_max + jnp.log(row_total))[:, 0])

    mixed_blocks, log_blocks = lax.map(
        forward_block, jnp.arange(pair_local * block_count, dtype=jnp.int32)
    )
    mixed_pairs = mixed_blocks.reshape(pair_local, seq_count, seq_rows, head_dim)
    log_totals = log_blocks.reshape(pair_local, seq_length)
    mixed_home = lax.all_to_all(mixed_pairs, "seq", split_axis=1, concat_axis=0, tiled=True)
    mixed_tokens = jnp.transpose(
        mixed_home.reshape(micro_count, group_count, local_heads, seq_rows, head_dim),
        (0, 1, 3, 2, 4),
    ).reshape(micro_count, group_count, seq_rows, local_heads * head_dim)
    dense_part = jnp.einsum(
        "mstk,kf->mstf", mixed_tokens, dense_full, preferred_element_type=wide_type
    )
    attention_sum = lax.psum(dense_part.astype(jnp.bfloat16), "dp").astype(jnp.float32)
    middle = inputs_both + attention_sum + dense_bias
    gain_rows_two = jnp.broadcast_to(gain_two[None, :], (group_count, model_width))
    shift_rows_two = jnp.broadcast_to(shift_two[None, :], (group_count, model_width))
    normed_two, norm_two_pull = jax.vjp(split_norm, middle, gain_rows_two, shift_rows_two)
    normed_two_low = normed_two.astype(half_type)
    unit_bias = lax.dynamic_slice_in_dim(expand_bias, dp_index * unit_local, unit_local, 0)
    hidden_pre = (
        jnp.einsum("mstd,df->mstf", normed_two_low, expand_full, preferred_element_type=wide_type)
        + unit_bias
    )
    activated_value, gelu_pull = jax.vjp(gelu_tanh, hidden_pre)
    activated_low = activated_value.astype(half_type)
    feed_part = jnp.einsum(
        "mstf,fd->mstd", activated_low, shrink_full, preferred_element_type=wide_type
    )
    feed_sum = lax.psum_scatter(
        feed_part.astype(jnp.bfloat16), "dp", scatter_dimension=1, tiled=True
    ).astype(jnp.float32)
    middle_own = lax.dynamic_slice_in_dim(middle, dp_index, 1, 1)
    layer_output = (middle_own + feed_sum + shrink_bias).astype(half_type)
    triple_back, dense_back, expand_back, shrink_back = (
        lax.all_gather(triple_weight, "seq", axis=0, tiled=True),
        lax.all_gather(dense_weight, "seq", axis=0, tiled=True),
        lax.all_gather(expand_weight, "seq", axis=0, tiled=True),
        lax.all_gather(shrink_weight, "seq", axis=0, tiled=True),
    )
    grad_act = jnp.einsum(
        "mstd,fd->mstf", upstream_low, shrink_back, preferred_element_type=wide_type
    )
    grad_pre_low = gelu_pull(grad_act)[0].astype(half_type)
    norm_two_part = jnp.einsum(
        "mstf,df->mstd", grad_pre_low, expand_back, preferred_element_type=wide_type
    )
    grad_normed_two = lax.psum(norm_two_part.astype(jnp.bfloat16), "dp").astype(jnp.float32)
    grad_middle_norm, grad_gain_rows_two, grad_shift_rows_two = norm_two_pull(grad_normed_two)
    grad_middle = upstream_low.astype(wide_type) + grad_middle_norm
    grad_branch_low = grad_middle.astype(half_type)
    go_pairs = jnp.einsum(
        "mstf,hef->mshte",
        grad_branch_low,
        dense_back.reshape(local_heads, head_dim, model_width),
        preferred_element_type=wide_type,
    ).astype(half_type)
    go_pairs = go_pairs.reshape(seq_count, pair_local, seq_rows, head_dim)
    grad_mixed_pairs = lax.all_to_all(go_pairs, "seq", split_axis=0, concat_axis=2, tiled=True)[0]

    def backward_item(pair_item):
        keys_item = lax.dynamic_index_in_dim(key_all, pair_item, 0, False)
        values_item = lax.dynamic_index_in_dim(value_all, pair_item, 0, False)
        grad_mixed_item = lax.dynamic_index_in_dim(grad_mixed_pairs, pair_item, 0, False)
        totals_item = lax.dynamic_index_in_dim(log_totals, pair_item, 0, False)

        def backward_block(running, block_index):
            key_grad, value_grad = running
            first_row = block_index * block_rows
            query_block, scores = block_scores(pair_item, first_row)
            soft_probs = jnp.exp(
                scores - lax.dynamic_slice_in_dim(totals_item, first_row, block_rows, 0)[:, None]
            )
            grad_block = lax.dynamic_slice_in_dim(grad_mixed_item, first_row, block_rows, 0)
            grad_probs = jnp.einsum(
                "qe,ke->qk", grad_block, values_item, preferred_element_type=wide_type
            )
            row_inner = jnp.sum(grad_probs * soft_probs, -1, keepdims=True)
            grad_scores_low = (soft_probs * (grad_probs - row_inner)).astype(half_type)
            query_grad = (
                jnp.dot(grad_scores_low, keys_item, preferred_element_type=wide_type) * score_scale
            )
            key_grad = (
                key_grad
                + jnp.einsum(
                    "qk,qe->ke", grad_scores_low, query_block, preferred_element_type=wide_type
                )
                * score_scale
            )
            value_grad = value_grad + jnp.einsum(
                "qk,qe->ke",
                soft_probs.astype(half_type),
                grad_block,
                preferred_element_type=wide_type,
            )
            return ((key_grad, value_grad), query_grad)

        zero_rows = jnp.zeros((seq_length, head_dim), wide_type)
        (key_grad, value_grad), query_grads = lax.scan(
            backward_block, (zero_rows, zero_rows), jnp.arange(block_count, dtype=jnp.int32)
        )
        return jnp.stack(
            [query_grads.reshape(seq_length, head_dim), key_grad, value_grad], 0
        ).astype(half_type)

    grad_pairs = lax.map(backward_item, jnp.arange(pair_local, dtype=jnp.int32))
    grad_split = grad_pairs.reshape(pair_local, 3, seq_count, seq_rows, head_dim)
    grad_home = lax.all_to_all(grad_split, "seq", split_axis=2, concat_axis=0, tiled=True)
    grad_project_low = jnp.transpose(
        grad_home.reshape(micro_count, group_count, local_heads, 3, seq_rows, head_dim),
        (0, 1, 4, 2, 3, 5),
    ).reshape(micro_count, group_count, seq_rows, project_width)
    norm_one_part = jnp.einsum(
        "mstc,dc->mstd",
        grad_project_low,
        triple_back.reshape(model_width, project_width),
        preferred_element_type=wide_type,
    )
    grad_normed_one = lax.psum_scatter(
        norm_one_part.astype(jnp.bfloat16), "dp", scatter_dimension=1, tiled=True
    ).astype(jnp.float32)
    inputs_own = hidden.astype(wide_type)
    grad_inputs_norm, grad_gain_one, grad_shift_one = jax.vjp(
        layer_norm, inputs_own, gain_one, shift_one
    )[1](grad_normed_one)
    grad_middle_own = lax.dynamic_slice_in_dim(grad_middle, dp_index, 1, 1)
    hidden_grad = (grad_middle_own + grad_inputs_norm).astype(half_type)
    head_sums = jnp.sum(
        grad_project_low.reshape(micro_count, group_count, seq_rows, local_heads, 3, head_dim),
        (0, 1, 2),
        dtype=wide_type,
    )
    pair_grad = place_half(jnp.stack([head_sums[:, 0], head_sums[:, 2]], 1), dp_index, group_count)
    unit_grad = place_half(jnp.sum(grad_pre_low, (0, 1, 2), dtype=wide_type), dp_index, group_count)
    dense_shift_term = jnp.sum(
        lax.dynamic_slice_in_dim(grad_branch_low, dp_index, 1, 1), (0, 1, 2), dtype=wide_type
    )
    shrink_shift_term = jnp.sum(cotangent, (0, 1, 2), dtype=wide_type)
    gain_two_term = lax.dynamic_index_in_dim(grad_gain_rows_two, dp_index, 0, False)
    shift_two_term = lax.dynamic_index_in_dim(grad_shift_rows_two, dp_index, 0, False)
    vector_sums = (
        lax.psum_scatter(grad_gain_one, ("dp", "seq"), scatter_dimension=0, tiled=True),
        lax.psum_scatter(grad_shift_one, ("dp", "seq"), scatter_dimension=0, tiled=True),
        lax.psum_scatter(pair_grad, ("dp", "seq"), scatter_dimension=0, tiled=True),
        lax.psum_scatter(dense_shift_term, ("dp", "seq"), scatter_dimension=0, tiled=True),
        lax.psum_scatter(gain_two_term, ("dp", "seq"), scatter_dimension=0, tiled=True),
        lax.psum_scatter(shift_two_term, ("dp", "seq"), scatter_dimension=0, tiled=True),
        lax.psum_scatter(unit_grad, ("dp", "seq"), scatter_dimension=0, tiled=True),
        lax.psum_scatter(shrink_shift_term, ("dp", "seq"), scatter_dimension=0, tiled=True),
    )
    normed_flat = normed_low.reshape(token_total, model_width)
    project_flat = grad_project_low.reshape(token_total, project_width)
    normed_two_flat = normed_two_low.reshape(token_total, model_width)
    pre_flat = grad_pre_low.reshape(token_total, unit_local)
    column_sums = lax.psum_scatter(
        jnp.concatenate(
            [
                jnp.einsum(
                    "tr,tc->rc", normed_flat, project_flat, preferred_element_type=wide_type
                ),
                jnp.einsum(
                    "tr,tc->rc", normed_two_flat, pre_flat, preferred_element_type=wide_type
                ),
            ],
            1,
        ),
        "seq",
        scatter_dimension=0,
        tiled=True,
    )
    triple_grad = column_sums[:, :project_width].reshape(
        model_width // seq_count, local_heads, 3, head_dim
    )
    expand_grad = column_sums[:, project_width:]
    dense_rows = dense_weight.shape[0]
    shrink_rows = shrink_weight.shape[0]
    row_block = dense_rows + shrink_rows
    mixed_flat = mixed_tokens.reshape(token_total, local_heads * head_dim)
    branch_flat = grad_branch_low.reshape(token_total, model_width)
    active_flat = activated_low.reshape(token_total, unit_local)
    upstream_flat = upstream_low.reshape(token_total, model_width)
    block_number = row_block * lax.axis_size("seq") // row_block
    dense_term = jnp.einsum("tr,td->rd", mixed_flat, branch_flat, preferred_element_type=wide_type)
    shrink_term = jnp.einsum(
        "tr,td->rd", active_flat, upstream_flat, preferred_element_type=wide_type
    )
    row_sums = lax.psum_scatter(
        jnp.concatenate(
            [
                dense_term.reshape(block_number, dense_rows, model_width),
                shrink_term.reshape(block_number, shrink_rows, model_width),
            ],
            1,
        ).reshape(row_block * lax.axis_size("seq"), model_width),
        "seq",
        scatter_dimension=0,
        tiled=True,
    )
    dense_grad = row_sums[:dense_rows]
    shrink_grad = row_sums[dense_rows:]
    return (
        layer_output,
        hidden_grad,
        vector_sums[0],
        vector_sums[1],
        triple_grad,
        vector_sums[2],
        dense_grad,
        vector_sums[3],
        vector_sums[4],
        vector_sums[5],
        expand_grad,
        vector_sums[6],
        shrink_grad,
        vector_sums[7],
    )


CHUNKS = 4
LOG2E = 1.4426950408889634
MESH = pl.DeviceIdType.MESH


def remote(src, dst, send, recv, peer):
    return pltpu.make_async_remote_copy(
        src_ref=src,
        dst_ref=dst,
        send_sem=send,
        recv_sem=recv,
        device_id=peer,
        device_id_type=MESH,
    )


def greet(peers):
    barrier = pltpu.get_barrier_semaphore()
    for peer in peers:
        pl.semaphore_signal(barrier, inc=1, device_id=peer, device_id_type=MESH)
    pl.semaphore_wait(barrier, len(peers))


class Corner:
    def __init__(self):
        self.c = lax.axis_index("dp")
        self.y = lax.axis_index("y")
        self.x = lax.axis_index("x")
        self.ax = self.x + (1 - self.c) * (1 - 2 * self.x)
        self.ay = self.y + self.c * (1 - 2 * self.y)
        self.bx = self.x + self.c * (1 - 2 * self.x)
        self.by = self.y + (1 - self.c) * (1 - 2 * self.y)
        self.dx = 1 - self.x
        self.dy = 1 - self.y
        self.peer_a = {"y": self.ay, "x": self.ax}
        self.peer_b = {"y": self.by, "x": self.bx}
        self.sibling = {"dp": 1 - self.c}

    def slots(self, core):
        return [
            (core * 2 + y) * 2 + x
            for y, x in (
                (self.dy, self.dx),
                (self.by, self.bx),
                (self.ay, self.ax),
                (self.y, self.x),
            )
        ]


def gather_kernel(deep, *refs):
    if deep:
        rows_ref, deep_ref, all_ref, moved_ref, local_sem, send, recv, deep_send, deep_recv = refs
    else:
        rows_ref, all_ref, local_sem, send, recv = refs
    at = Corner()
    slot_d, slot_b, slot_a, me = at.slots(at.c)
    step = rows_ref.shape[0] // CHUNKS
    peers = [at.peer_a, at.peer_b, at.sibling]
    sent, moves = [], []
    if deep:
        z = lax.axis_index("z")
        plane_at = [lax.rem(z + i, 4) for i in range(4)]
        peers += [{"z": plane_at[i]} for i in range(1, 4)]
    greet(peers)
    locals_ = [pltpu.make_async_copy(rows_ref, all_ref.at[me], local_sem.at[0])]
    if deep:
        locals_.append(pltpu.make_async_copy(deep_ref.at[z], moved_ref.at[z], local_sem.at[1]))
    for one in locals_:
        one.start()

    def copy(kind, k, slot, peer):
        part = pl.ds(k * step, step)
        src = rows_ref.at[part] if kind < 3 else all_ref.at[slot, part]
        return remote(src, all_ref.at[slot, part], send.at[kind, k], recv.at[kind, k], peer)

    def arrived(kind, k, slot, peer):
        part = pl.ds(k * step, step)
        block = all_ref.at[slot, part]
        remote(block, block, send.at[kind, k], recv.at[kind, k], peer).wait_recv()

    def start(kind, k, slot, peer):
        one = copy(kind, k, slot, peer)
        one.start()
        sent.append(one)

    for i in range(1, 4) if deep else ():
        sems = deep_send.at[i - 1], deep_recv.at[i - 1]
        one = remote(deep_ref.at[plane_at[i]], moved_ref.at[z], *sems, {"z": plane_at[i]})
        one.start()
        sent.append(one)
        landing = moved_ref.at[plane_at[4 - i]]
        moves.append(remote(landing, landing, *sems, {"z": plane_at[i]}))
    for k in range(CHUNKS):
        start(0, k, me, at.peer_a)
        start(1, k, me, at.peer_b)
    for k in range(CHUNKS):
        start(2, k, me, at.sibling)
    for k in range(CHUNKS):
        arrived(0, k, slot_a, at.peer_a)
        start(3, k, slot_a, at.peer_b)
        start(4, k, slot_a, at.sibling)
    for k in range(CHUNKS):
        arrived(1, k, slot_b, at.peer_b)
        start(5, k, slot_b, at.sibling)
    for k in range(CHUNKS):
        arrived(3, k, slot_d, at.peer_b)
        start(6, k, slot_d, at.sibling)
    other_d, other_b, other_a, other_me = at.slots(1 - at.c)
    for k in range(CHUNKS):
        arrived(2, k, other_me, at.sibling)
        arrived(4, k, other_b, at.sibling)
        arrived(5, k, other_a, at.sibling)
        arrived(6, k, other_d, at.sibling)
    for one in moves:
        one.wait_recv()
    for one in sent:
        one.wait_send()
    for one in locals_:
        one.wait()


def gather_tokens(rows, deep=None):
    count, width = rows.shape
    operands = [rows]
    shapes = [jax.ShapeDtypeStruct((8, count, width), rows.dtype)]
    scratch = [
        pltpu.SemaphoreType.DMA((2,)),
        pltpu.SemaphoreType.DMA((7, CHUNKS)),
        pltpu.SemaphoreType.DMA((7, CHUNKS)),
    ]
    if deep is not None:
        operands.append(deep)
        shapes.append(jax.ShapeDtypeStruct(deep.shape, deep.dtype))
        scratch += [pltpu.SemaphoreType.DMA((3,)), pltpu.SemaphoreType.DMA((3,))]
    all_rows, *moved = pl.pallas_call(
        functools.partial(gather_kernel, deep is not None),
        out_shape=shapes,
        in_specs=[pl.BlockSpec(memory_space=pl.ANY)] * len(operands),
        out_specs=[pl.BlockSpec(memory_space=pl.ANY)] * len(shapes),
        scratch_shapes=scratch,
        compiler_params=pltpu.CompilerParams(
            collective_id=1 if deep is None else 6, has_side_effects=True
        ),
        cost_estimate=pl.CostEstimate(
            flops=0, bytes_accessed=16 * count * width * 4, transcendentals=0
        ),
        name="gather_tokens",
    )(*operands)
    return (all_rows.reshape(8 * count, width), *moved)


def after(value, *others):
    return lax.optimization_barrier((value, *others))[0]


def scatter_kernel(part_ref, own_ref, from_core, from_b, from_a, send, recv):
    at = Corner()
    slot_d, slot_b, slot_a, me = at.slots(at.c)
    other_d, other_b, other_a, other_me = at.slots(1 - at.c)
    step = own_ref.shape[0] // CHUNKS
    wide = jnp.float32
    greet([at.peer_a, at.peer_b, at.sibling])
    sent = []

    def start(kind, k, src, dst, peer):
        one = remote(src, dst, send.at[kind, k], recv.at[kind, k], peer)
        one.start()
        sent.append(one)

    def arrived(kind, k, dst, peer):
        remote(dst, dst, send.at[kind, k], recv.at[kind, k], peer).wait_recv()

    for q, slot in enumerate((other_d, other_a, other_b, other_me)):
        for k in range(CHUNKS):
            part = pl.ds(k * step, step)
            start(q, k, part_ref.at[slot, part], from_core.at[q, part], at.sibling)
    for q, slot in enumerate((slot_d, slot_b)):
        for k in range(CHUNKS):
            part = pl.ds(k * step, step)
            arrived(q, k, from_core.at[q, part], at.sibling)
            total = part_ref[slot, part].astype(wide) + from_core[q, part].astype(wide)
            from_core[q, part] = total.astype(from_core.dtype)
            start(4 + q, k, from_core.at[q, part], from_b.at[q, part], at.peer_b)
    for k in range(CHUNKS):
        part = pl.ds(k * step, step)
        arrived(2, k, from_core.at[2, part], at.sibling)
        arrived(4, k, from_b.at[0, part], at.peer_b)
        total = part_ref[slot_a, part].astype(wide) + from_core[2, part].astype(wide)
        total = total + from_b[0, part].astype(wide)
        from_core[2, part] = total.astype(from_core.dtype)
        start(6, k, from_core.at[2, part], from_a.at[part], at.peer_a)
    for k in range(CHUNKS):
        part = pl.ds(k * step, step)
        arrived(3, k, from_core.at[3, part], at.sibling)
        arrived(5, k, from_b.at[1, part], at.peer_b)
        arrived(6, k, from_a.at[part], at.peer_a)
        total = part_ref[me, part].astype(wide) + from_core[3, part].astype(wide)
        total = total + from_b[1, part].astype(wide)
        own_ref[part] = total + from_a[part].astype(wide)
    for one in sent:
        one.wait_send()


def scatter_tokens(partial):
    count, width = partial.shape[0] // 8, partial.shape[1]
    return pl.pallas_call(
        scatter_kernel,
        out_shape=jax.ShapeDtypeStruct((count, width), jnp.float32),
        in_specs=[pl.BlockSpec(memory_space=pltpu.VMEM)],
        out_specs=pl.BlockSpec(memory_space=pltpu.VMEM),
        scratch_shapes=[
            pltpu.VMEM((4, count, width), partial.dtype),
            pltpu.VMEM((2, count, width), partial.dtype),
            pltpu.VMEM((count, width), partial.dtype),
            pltpu.SemaphoreType.DMA((7, CHUNKS)),
            pltpu.SemaphoreType.DMA((7, CHUNKS)),
        ],
        compiler_params=pltpu.CompilerParams(
            collective_id=2, has_side_effects=True, vmem_limit_bytes=40 * 2**20
        ),
        cost_estimate=pl.CostEstimate(
            flops=0, bytes_accessed=16 * count * width * 4, transcendentals=0
        ),
        name="scatter_tokens",
    )(partial.reshape(8, count, width))


def exchange_kernel(last, n_flat, *refs):
    refs = list(refs)
    take = lambda n: [refs.pop(0) for _ in range(n)]
    deep_in, turn_in, *flat_in = take(2 + n_flat)
    (vec_in,) = take(1)
    deep_out, turn_out, *flat_out = take(2 + n_flat)
    (vec_out,) = take(1)
    if last:
        columns_out, flat_out = flat_out, take(n_flat)
        near, far, here = take(3)
    send, recv = take(2)
    c, z = lax.axis_index("dp"), lax.axis_index("z")
    y, x = lax.axis_index("y"), lax.axis_index("x")
    place = y * 2 + x
    rank = c * 4 + place

    def deep(i):
        return lax.rem(z + i, 4)

    def flat(i):
        return lax.rem(place + i, 4)

    def wide(i):
        return lax.rem(rank + i, 8)

    def deep_peer(i):
        return {"z": deep(i)}

    def flat_peer(i):
        return {"y": flat(i) // 2, "x": lax.rem(flat(i), 2)}

    def wide_peer(i):
        return {
            "dp": wide(i) // 4,
            "y": lax.rem(wide(i), 4) // 2,
            "x": lax.rem(wide(i), 2),
        }

    low = lax.rem(z, 2)
    turn_from = {"z": z - low + 1 - x, "x": low}
    turn_to = {"z": z - low + x, "x": 1 - low}
    if last:
        turn_from, turn_to = turn_to, turn_from
    others = range(1, 4)
    greet([deep_peer(i) for i in others] + [wide_peer(i) for i in range(1, 8)])
    sent, waits = [], []
    count = [0]

    def post(src, dst, peer, landing):
        k = count[0]
        count[0] += 1
        one = remote(src, dst, send.at[k], recv.at[k], peer)
        one.start()
        sent.append(one)
        return remote(landing, landing, send.at[k], recv.at[k], peer)

    stage = []
    for i in range(1, 8):
        if last:
            landing = near.at[wide(8 - i)]
            stage.append(post(vec_in.at[wide(i)], near.at[rank], wide_peer(i), landing))
        else:
            landing = vec_out.at[z, wide(8 - i)]
            stage.append(post(vec_in, vec_out.at[z, rank], wide_peer(i), landing))
    for i in others:
        landing = deep_out.at[deep(4 - i)]
        waits.append(post(deep_in.at[deep(i)], deep_out.at[z], deep_peer(i), landing))
    for src, dst in zip(flat_in, flat_out):
        for i in others:
            landing = dst.at[flat(4 - i)]
            waits.append(post(src.at[flat(i)], dst.at[place], flat_peer(i), landing))
    waits.append(post(turn_in, turn_out, turn_to, turn_out))
    deep_out[z] = deep_in[z]
    for src, dst in zip(flat_in, flat_out):
        dst[place] = src[place]
    if last:
        near[rank] = vec_in[rank]
        for one in stage:
            one.wait_recv()
        here[...] = jnp.sum(near[...], 0)
        stage = []
        for i in others:
            landing = far.at[deep(4 - i)]
            stage.append(post(here.at[deep(i)], far.at[z], deep_peer(i), landing))
        far[z] = here[z]
        for one in stage:
            one.wait_recv()
        vec_out[...] = jnp.sum(far[...], 0)
    else:
        vec_out[z, rank] = vec_in[...]
        for one in stage:
            one.wait_recv()
        for i in others:
            landing = vec_out.at[deep(4 - i)]
            waits.append(post(vec_out.at[z], vec_out.at[z], deep_peer(i), landing))
    for one in waits[3:]:
        one.wait_recv()
    if last:
        for (steps, order), blocks, columns in zip(last, flat_out, columns_out):
            step = blocks.shape[2] // steps
            for i in range(steps):
                for p in range(4):
                    first = (i * 4 + order[p]) * step
                    columns[:, first : first + step] = blocks[p, :, i * step : (i + 1) * step]
    for one in waits[:3]:
        one.wait_recv()
    for one in sent:
        one.wait_send()


def exchange(deep, turned, flat, vector, last=None):
    tile = vector.shape[2:] if last else vector.shape
    shapes = [jax.ShapeDtypeStruct(a.shape, a.dtype) for a in (deep, turned)]
    blocks = [(a.shape, a.dtype) for a in flat]
    scratch = []
    if last:
        shapes += [jax.ShapeDtypeStruct((s[1], 4 * s[2]), t) for s, t in blocks]
        shapes.append(jax.ShapeDtypeStruct(tile, vector.dtype))
        scratch = [pltpu.VMEM(*b) for b in blocks]
        scratch += [
            pltpu.VMEM((8, 4) + tile, vector.dtype),
            pltpu.VMEM((4,) + tile, vector.dtype),
            pltpu.VMEM((4,) + tile, vector.dtype),
        ]
    else:
        shapes += [jax.ShapeDtypeStruct(*b) for b in blocks]
        shapes.append(jax.ShapeDtypeStruct((4, 8) + tile, vector.dtype))
    copies = 3 * (1 + len(flat)) + 1 + 10
    operands = [deep, turned, *flat, vector]
    moved = sum(a.size * a.dtype.itemsize for a in operands)
    return pl.pallas_call(
        functools.partial(exchange_kernel, last, len(flat)),
        out_shape=shapes,
        in_specs=[pl.BlockSpec(memory_space=pltpu.VMEM)] * len(operands),
        out_specs=[pl.BlockSpec(memory_space=pltpu.VMEM)] * len(shapes),
        scratch_shapes=scratch
        + [pltpu.SemaphoreType.DMA((copies,)), pltpu.SemaphoreType.DMA((copies,))],
        compiler_params=pltpu.CompilerParams(
            collective_id=4 if last else 3, has_side_effects=True, vmem_limit_bytes=40 * 2**20
        ),
        cost_estimate=pl.CostEstimate(flops=0, bytes_accessed=16 * moved, transcendentals=0),
        name="exchange",
    )(*operands)


def scores_of(item_ref, first, block, slope, prefix, depth, seq_rows):
    length = item_ref.shape[0]
    head_dim = item_ref.shape[1] // 3
    own_rows = depth * seq_rows
    chips = length // own_rows

    def position(index):
        chip = index // own_rows
        rest = index % own_rows
        return ((rest // seq_rows) * chips + chip) * seq_rows + rest % seq_rows

    queries = item_ref[first : first + block, :head_dim]
    keys = item_ref[:, head_dim : 2 * head_dim]
    raw = lax.dot_general(
        keys, queries, (((1,), (1,)), ((), ())), preferred_element_type=jnp.float32
    )
    key_pos = position(lax.broadcasted_iota(jnp.int32, (length, 1), 0))
    query_pos = position(first + lax.broadcasted_iota(jnp.int32, (1, block), 1))
    bound = jnp.where(key_pos < prefix, -1, key_pos)
    distance = jnp.abs(
        query_pos.astype(jnp.float32) - key_pos.astype(jnp.float32)
    )
    scores = raw * (LOG2E / math.sqrt(head_dim)) - (slope * LOG2E) * distance
    return jnp.where(bound <= query_pos, scores, jnp.float32(-1e30))


def forward_kernel(depth, seq_rows, block, prefix_ref, slope_ref, item_ref, mixed_ref, total_ref):
    prefix = prefix_ref[pl.program_id(0)]
    slope = slope_ref[pl.program_id(1)]
    length = item_ref.shape[0]
    head_dim = item_ref.shape[1] // 3
    for first in range(0, length, block):
        scores = scores_of(item_ref, first, block, slope, prefix, depth, seq_rows)
        top = jnp.max(scores, 0, keepdims=True)
        powers = jnp.exp2(scores - top)
        total = jnp.sum(powers, 0, keepdims=True)
        probs = (powers * (1.0 / total)).astype(jnp.bfloat16)
        mixed = lax.dot_general(
            probs,
            item_ref[:, 2 * head_dim :],
            (((0,), (0,)), ((), ())),
            preferred_element_type=jnp.float32,
        )
        mixed_ref[first : first + block, :] = mixed.astype(mixed_ref.dtype)
        total_ref[0, :, first : first + block] = top + jnp.log2(total)


def attend_forward(projected, slopes, prefixes, own_heads, head_dim, depth, seq_rows):
    cores = prefixes.shape[0]
    length = projected.shape[0] // cores
    block = min(256, length)
    scores = cores * own_heads * length * length
    return pl.pallas_call(
        functools.partial(forward_kernel, depth, seq_rows, block),
        grid=(cores, own_heads),
        out_shape=[
            jax.ShapeDtypeStruct((cores * length, own_heads * head_dim), projected.dtype),
            jax.ShapeDtypeStruct((cores * own_heads, 1, length), jnp.float32),
        ],
        in_specs=[
            pl.BlockSpec(memory_space=pltpu.SMEM),
            pl.BlockSpec(memory_space=pltpu.SMEM),
            pl.BlockSpec((length, 3 * head_dim), lambda s, h: (s, h)),
        ],
        out_specs=[
            pl.BlockSpec((length, head_dim), lambda s, h: (s, h)),
            pl.BlockSpec((1, 1, length), lambda s, h: (s * own_heads + h, 0, 0)),
        ],
        compiler_params=pltpu.CompilerParams(vmem_limit_bytes=48 * 2**20),
        cost_estimate=pl.CostEstimate(
            flops=4 * scores * head_dim,
            bytes_accessed=2 * projected.size * 2,
            transcendentals=scores,
        ),
        name="attend_forward",
    )(prefixes, slopes, projected)


def backward_kernel(
    depth, seq_rows, block, prefix_ref, slope_ref, item_ref, grad_ref, total_ref, out_ref, key_sum, value_sum
):
    prefix = prefix_ref[pl.program_id(0)]
    slope = slope_ref[pl.program_id(1)]
    length = item_ref.shape[0]
    head_dim = item_ref.shape[1] // 3
    scale = 1.0 / math.sqrt(head_dim)
    half = jnp.bfloat16
    wide = jnp.float32
    for first in range(0, length, block):
        scores = scores_of(item_ref, first, block, slope, prefix, depth, seq_rows)
        probs = jnp.exp2(scores - total_ref[0, :, first : first + block])
        grad = grad_ref[first : first + block, :]
        grad_probs = lax.dot_general(
            item_ref[:, 2 * head_dim :],
            grad,
            (((1,), (1,)), ((), ())),
            preferred_element_type=wide,
        )
        inner = jnp.sum(grad_probs * probs, 0, keepdims=True)
        grad_scores = (probs * (grad_probs - inner)).astype(half)
        key_term = jnp.dot(
            grad_scores, item_ref[first : first + block, :head_dim], preferred_element_type=wide
        )
        value_term = jnp.dot(probs.astype(half), grad, preferred_element_type=wide)
        query_grad = lax.dot_general(
            grad_scores,
            item_ref[:, head_dim : 2 * head_dim],
            (((0,), (0,)), ((), ())),
            preferred_element_type=wide,
        )
        out_ref[first : first + block, :head_dim] = (query_grad * scale).astype(half)
        if first == 0:
            key_sum[...] = key_term
            value_sum[...] = value_term
        else:
            key_sum[...] += key_term
            value_sum[...] += value_term
    out_ref[:, head_dim : 2 * head_dim] = (key_sum[...] * scale).astype(half)
    out_ref[:, 2 * head_dim :] = value_sum[...].astype(half)


def attend_backward(
    projected, grad_mixed, totals, slopes, prefixes, own_heads, head_dim, depth, seq_rows
):
    cores = prefixes.shape[0]
    length = projected.shape[0] // cores
    block = min(256, length)
    scores = cores * own_heads * length * length
    return pl.pallas_call(
        functools.partial(backward_kernel, depth, seq_rows, block),
        grid=(cores, own_heads),
        out_shape=jax.ShapeDtypeStruct(projected.shape, projected.dtype),
        in_specs=[
            pl.BlockSpec(memory_space=pltpu.SMEM),
            pl.BlockSpec(memory_space=pltpu.SMEM),
            pl.BlockSpec((length, 3 * head_dim), lambda s, h: (s, h)),
            pl.BlockSpec((length, head_dim), lambda s, h: (s, h)),
            pl.BlockSpec((1, 1, length), lambda s, h: (s * own_heads + h, 0, 0)),
        ],
        out_specs=pl.BlockSpec((length, 3 * head_dim), lambda s, h: (s, h)),
        scratch_shapes=[
            pltpu.VMEM((length, head_dim), jnp.float32),
            pltpu.VMEM((length, head_dim), jnp.float32),
        ],
        compiler_params=pltpu.CompilerParams(vmem_limit_bytes=48 * 2**20),
        cost_estimate=pl.CostEstimate(
            flops=10 * scores * head_dim,
            bytes_accessed=2 * projected.size * 2,
            transcendentals=scores,
        ),
        name="attend_backward",
    )(prefixes, slopes, projected, grad_mixed, totals)


def planar(
    hidden,
    prefix_lengths,
    cotangent,
    first_gain,
    first_shift,
    triple_weight,
    pair_bias,
    dense_weight,
    dense_shift,
    second_gain,
    second_shift,
    expand_weight,
    expand_shift,
    shrink_weight,
    shrink_shift,
):
    wide = jnp.float32
    half = jnp.bfloat16
    cores = lax.axis_size("dp")
    depth = lax.axis_size("z")
    rows_y = lax.axis_size("y")
    rows_x = lax.axis_size("x")
    plane = rows_y * rows_x
    core = lax.axis_index("dp")
    at_y = lax.axis_index("y")
    at_x = lax.axis_index("x")
    place = at_y * rows_x + at_x
    seq_rows = hidden.shape[2]
    width = hidden.shape[3]
    head_dim = triple_weight.shape[3]
    heads = triple_weight.shape[1]
    own_heads = heads // plane
    own_rows = seq_rows * depth
    units = expand_weight.shape[1]
    own_units = units // plane
    row_block = expand_weight.shape[0]
    shrink_rows = shrink_weight.shape[0]

    pieces = [
        first_gain,
        first_shift,
        dense_shift,
        second_gain,
        second_shift,
        shrink_shift,
        pair_bias,
        expand_shift,
    ]
    piece_total = sum(p.shape[0] for p in pieces)
    lanes = 128
    vector_rows = -(-piece_total // (lanes * 16)) * 16
    vector_tile = jnp.pad(
        jnp.concatenate(pieces), (0, vector_rows * lanes - piece_total)
    ).reshape(vector_rows, lanes)
    triple_blocks = (
        triple_weight.reshape(row_block, own_heads, rows_x, rows_y, 3 * head_dim)[:, :, ::-1]
        .transpose(3, 2, 0, 1, 4)
        .reshape(plane, row_block, own_heads * 3 * head_dim)
    )
    expand_blocks = (
        expand_weight.reshape(row_block, depth, plane, shrink_rows)
        .transpose(2, 0, 1, 3)
        .reshape(plane, row_block, own_units)
    )
    inputs, dense_turned, triple_turned, expand_turned, packed = exchange(
        hidden[:, 0], dense_weight, (triple_blocks, expand_blocks), vector_tile
    )
    packed = (
        packed.reshape(depth, cores, plane, vector_rows * lanes)
        .transpose(1, 0, 2, 3)
        .reshape(-1, vector_rows * lanes)
    )
    vectors = []
    offset = 0
    for piece in pieces:
        vectors.append(packed[:, offset : offset + piece.shape[0]].reshape(-1).astype(wide))
        offset += piece.shape[0]
    gain_one, shift_one, dense_bias, gain_two, shift_two, shrink_bias, pair_full, unit_full = vectors
    pair_heads = pair_full.reshape(cores, own_heads, rows_x, rows_y, 2, head_dim)[
        core, :, 1 - at_x, at_y
    ]
    triple_bias = jnp.stack(
        [pair_heads[:, 0], jnp.zeros_like(pair_heads[:, 0]), pair_heads[:, 1]], 1
    ).reshape(-1)
    unit_bias = unit_full.reshape(cores, depth, plane, shrink_rows)[core, :, place].reshape(-1)

    triple_own = lax.all_gather(
        triple_turned.reshape(-1, triple_turned.shape[2]), "z", axis=0, tiled=True
    )
    inputs = inputs.reshape(own_rows, width).astype(wide)

    normed_own = layer_norm(inputs, gain_one, shift_one).astype(half)
    (normed,) = gather_tokens(normed_own)
    dense_own = lax.all_gather(after(dense_turned, normed), "z", axis=0, tiled=True)
    expand_own = lax.all_gather(
        after(expand_turned, normed).reshape(-1, own_units), "z", axis=0, tiled=True
    )
    projected = (
        jnp.dot(normed, triple_own, preferred_element_type=wide) + triple_bias
    ).astype(half)

    shrink_own = lax.all_gather(after(shrink_weight, projected), "z", axis=0, tiled=True)
    head_index = core * heads + jnp.arange(own_heads) * plane + (1 - at_x) * rows_y + at_y
    slopes = jnp.power(
        jnp.float32(2.0), -8.0 * (head_index.astype(wide) + 1.0) / (heads * cores)
    )
    at_z = lax.axis_index("z")
    prefixes = lax.dynamic_index_in_dim(prefix_lengths, at_z, 0, False)
    mixed, log_totals = attend_forward(
        projected, slopes, prefixes, own_heads, head_dim, depth, seq_rows
    )
    dense_part = jnp.dot(mixed, dense_own, preferred_element_type=wide).astype(half)
    dense_sum = scatter_tokens(dense_part)
    middle = inputs + dense_sum + dense_bias
    normed_two_own, norm_two_pull = jax.vjp(layer_norm, middle, gain_two, shift_two)
    normed_two, upstream = gather_tokens(normed_two_own.astype(half), cotangent[:, 0])
    upstream = upstream.reshape(own_rows, width)
    hidden_pre = jnp.dot(normed_two, expand_own, preferred_element_type=wide) + unit_bias
    (upstream_all,) = gather_tokens(upstream)
    activated, gelu_pull = jax.vjp(gelu_tanh, hidden_pre)
    activated = activated.astype(half)
    grad_act = jnp.einsum("tf,uf->tu", upstream_all, shrink_own, preferred_element_type=wide)
    grad_pre = gelu_pull(grad_act)[0].astype(half)
    shrink_term = jnp.einsum(
        "tu,td->ud", activated, upstream_all, preferred_element_type=wide
    ).astype(half)
    shrink_grad = lax.psum_scatter(shrink_term, "z", scatter_dimension=0, tiled=True)
    expand_term = jnp.einsum(
        "td,tu->du", normed_two, grad_pre, preferred_element_type=wide
    ).astype(half)
    expand_turned = lax.psum_scatter(expand_term, "z", scatter_dimension=0, tiled=True)
    feed_part = jnp.dot(activated, shrink_own, preferred_element_type=wide).astype(half)
    feed_sum = scatter_tokens(after(feed_part, shrink_term, expand_term))
    layer_output = (middle + feed_sum + shrink_bias).astype(half)

    norm_two_part = jnp.einsum(
        "tu,du->td", grad_pre, expand_own, preferred_element_type=wide
    ).astype(half)
    norm_two_sum = scatter_tokens(after(norm_two_part, feed_sum))
    grad_norm_two, gain_two_term, shift_two_term = norm_two_pull(norm_two_sum)
    grad_middle = upstream.astype(wide) + grad_norm_two
    branch_own = grad_middle.astype(half)
    branch, layer_output = gather_tokens(branch_own, layer_output.reshape(depth, seq_rows, width))

    grad_mixed = jnp.einsum("tf,ef->te", branch, dense_own, preferred_element_type=wide).astype(
        half
    )
    dense_term = jnp.einsum("te,tf->ef", mixed, branch, preferred_element_type=wide).astype(half)
    dense_turned = lax.psum_scatter(dense_term, "z", scatter_dimension=0, tiled=True)
    grad_project = attend_backward(
        projected,
        after(grad_mixed, dense_term),
        log_totals,
        slopes,
        prefixes,
        own_heads,
        head_dim,
        depth,
        seq_rows,
    )
    triple_term = jnp.einsum(
        "td,tc->dc", normed, grad_project, preferred_element_type=wide
    ).astype(half)
    triple_turned = lax.psum_scatter(triple_term, "z", scatter_dimension=0, tiled=True)
    norm_one_part = jnp.einsum(
        "tc,dc->td", grad_project, triple_own, preferred_element_type=wide
    ).astype(half)
    norm_one_sum = scatter_tokens(after(norm_one_part, triple_term))
    grad_norm_one, gain_one_term, shift_one_term = jax.vjp(
        layer_norm, inputs, gain_one, shift_one
    )[1](norm_one_sum)
    hidden_grad = (grad_middle + grad_norm_one).astype(half)
    head_sums = jnp.sum(grad_project, 0, dtype=wide).reshape(own_heads, 3, head_dim)
    pair_term = jnp.stack([head_sums[:, 0], head_sums[:, 2]], 1)
    pair_zero = jnp.zeros((cores, own_heads, rows_x, rows_y, 2, head_dim), wide)
    pair_wide = lax.dynamic_update_slice(
        pair_zero, pair_term[None, :, None, None], (core, 0, 1 - at_x, at_y, 0, 0)
    ).reshape(-1)
    unit_term = jnp.sum(grad_pre, 0, dtype=wide).reshape(1, depth, 1, shrink_rows)
    unit_wide = lax.dynamic_update_slice(
        jnp.zeros((cores, depth, plane, shrink_rows), wide), unit_term, (core, 0, place, 0)
    ).reshape(-1)
    terms = [
        gain_one_term,
        shift_one_term,
        jnp.sum(branch_own, 0, dtype=wide),
        gain_two_term,
        shift_two_term,
        jnp.sum(upstream, 0, dtype=wide),
        pair_wide,
        unit_wide,
    ]
    devices = cores * depth * plane
    term_rows = -(-piece_total // (lanes * 8)) * 8
    term_tiles = jnp.pad(
        jnp.concatenate([t.reshape(devices, -1) for t in terms], 1),
        ((0, 0), (0, term_rows * lanes - piece_total)),
    )
    term_tiles = (
        term_tiles.reshape(cores, depth, plane, term_rows, lanes)
        .transpose(0, 2, 1, 3, 4)
        .reshape(cores * plane, depth, term_rows, lanes)
    )
    hidden_grad, dense_grad, triple_grad, expand_grad, summed = exchange(
        hidden_grad.reshape(depth, seq_rows, width),
        dense_turned,
        (
            triple_turned.reshape(plane, row_block, -1),
            expand_turned.reshape(plane, row_block, own_units),
        ),
        term_tiles,
        last=((own_heads, (2, 0, 3, 1)), (depth, (0, 1, 2, 3))),
    )
    layer_output = layer_output[:, None]
    hidden_grad = hidden_grad[:, None]
    triple_grad = triple_grad.astype(wide).reshape(row_block, heads, 3, head_dim)
    summed = summed.reshape(-1)
    vector_grads = []
    offset = 0
    for piece in pieces:
        vector_grads.append(summed[offset : offset + piece.shape[0]])
        offset += piece.shape[0]
    return (
        layer_output,
        hidden_grad,
        vector_grads[0],
        vector_grads[1],
        triple_grad,
        vector_grads[6],
        dense_grad.astype(wide),
        vector_grads[2],
        vector_grads[3],
        vector_grads[4],
        expand_grad.astype(wide),
        vector_grads[7],
        shrink_grad.astype(wide),
        vector_grads[5],
    )


def layer(*args):
    return planar(*args)


def solution(mesh):
    depth = 4
    sides = (2, 2)
    planar_plan = mesh.shape["seq"] == depth * sides[0] * sides[1]
    if planar_plan:
        grid = Mesh(
            mesh.devices.reshape(mesh.shape["dp"], depth, *sides), ("dp", "z", "y", "x")
        )
        seq = ("z", "y", "x")
    else:
        grid = mesh
        seq = ("seq",)
    tokens = P(None, "dp", seq, None)
    vector = P(("dp",) + seq)
    matrix = P(("dp",) + seq, None)
    placed = (
        tokens,
        P(),
        tokens,
        vector,
        vector,
        P(seq, "dp", None, None),
        vector,
        matrix,
        vector,
        vector,
        vector,
        P(seq, "dp"),
        vector,
        matrix,
        vector,
    )
    results = (
        tokens,
        tokens,
        vector,
        vector,
        P(seq, "dp", None, None),
        vector,
        matrix,
        vector,
        vector,
        vector,
        P(seq, "dp"),
        vector,
        matrix,
        vector,
    )
    return jax.shard_map(
        layer if planar_plan else shards,
        mesh=grid,
        in_specs=placed,
        out_specs=results,
        check_vma=False,
    )
```

```python
import functools
import math

import jax
import jax.numpy as jnp
from jax import lax
from jax.experimental import pallas as pl
from jax.experimental.pallas import tpu as pltpu
from jax.sharding import Mesh
from jax.sharding import PartitionSpec as P


EPSILON = 1e-05
GELU_SCALE = 0.7978845608028654


def layer_norm(inputs, norm_gain, norm_shift):
    centered = inputs - jnp.mean(inputs, -1, keepdims=True)
    variance = jnp.mean(centered * centered, -1, keepdims=True)
    return centered * lax.rsqrt(variance + EPSILON) * norm_gain + norm_shift


def gelu_tanh(values):
    return (
        0.5 * values * (1.0 + jnp.tanh(GELU_SCALE * (values + 0.044715 * values * values * values)))
    )


def split_norm(inputs, gain_rows, shift_rows):
    return layer_norm(inputs, gain_rows[None, :, None, :], shift_rows[None, :, None, :])


def place_half(values, half_index, group_count):
    chosen = (jnp.arange(group_count, dtype=jnp.int32) == half_index).astype(values.dtype)
    return (chosen[:, None] * values.reshape(1, -1)).reshape(-1)


def shards(
    hidden,
    prefix_lengths,
    cotangent,
    first_gain,
    first_shift,
    triple_weight,
    pair_bias,
    dense_weight,
    dense_shift,
    second_gain,
    second_shift,
    expand_weight,
    expand_shift,
    shrink_weight,
    shrink_shift,
):
    wide_type = jnp.float32
    half_type = jnp.bfloat16
    seq_count = lax.axis_size("seq")
    group_count = lax.axis_size("dp")
    dp_index = lax.axis_index("dp")
    seq_index = lax.axis_index("seq")
    micro_count = hidden.shape[0]
    seq_rows = hidden.shape[2]
    model_width = hidden.shape[3]
    seq_length = seq_rows * seq_count
    local_heads = triple_weight.shape[1]
    head_dim = triple_weight.shape[3]
    head_total = local_heads * group_count
    pair_local = micro_count * group_count * local_heads // seq_count
    unit_local = expand_weight.shape[1]
    project_width = 3 * local_heads * head_dim
    token_total = micro_count * group_count * seq_rows
    score_scale = 1.0 / math.sqrt(head_dim)
    block_rows = min(512, seq_length)
    block_count = seq_length // block_rows
    key_pos = jnp.arange(seq_length, dtype=jnp.int32)
    gathered = (
        lax.all_gather(triple_weight, "seq", axis=0, tiled=True),
        lax.all_gather(dense_weight, "seq", axis=0, tiled=True),
        lax.all_gather(expand_weight, "seq", axis=0, tiled=True),
        lax.all_gather(shrink_weight, "seq", axis=0, tiled=True),
        lax.all_gather(first_gain, "seq", axis=0, tiled=True),
        lax.all_gather(first_shift, "seq", axis=0, tiled=True),
        lax.all_gather(pair_bias, "seq", axis=0, tiled=True),
        lax.all_gather(dense_shift, "seq", axis=0, tiled=True),
        lax.all_gather(second_gain, "seq", axis=0, tiled=True),
        lax.all_gather(second_shift, "seq", axis=0, tiled=True),
        lax.all_gather(expand_shift, "seq", axis=0, tiled=True),
        lax.all_gather(shrink_shift, "seq", axis=0, tiled=True),
    )
    triple_full, dense_full, expand_full, shrink_full = (
        gathered[0],
        gathered[1],
        gathered[2],
        gathered[3],
    )
    row_sets = (
        lax.all_gather(hidden, "dp", axis=1, tiled=True),
        lax.all_gather(cotangent, "dp", axis=1, tiled=True),
        lax.all_gather(gathered[4], "dp", axis=0, tiled=True),
        lax.all_gather(gathered[5], "dp", axis=0, tiled=True),
        lax.all_gather(gathered[6], "dp", axis=0, tiled=True),
        lax.all_gather(gathered[7], "dp", axis=0, tiled=True),
        lax.all_gather(gathered[8], "dp", axis=0, tiled=True),
        lax.all_gather(gathered[9], "dp", axis=0, tiled=True),
        lax.all_gather(gathered[10], "dp", axis=0, tiled=True),
        lax.all_gather(gathered[11], "dp", axis=0, tiled=True),
    )
    hidden_both = row_sets[0]
    upstream_low = row_sets[1]
    gain_one, shift_one, pair_full, dense_bias, gain_two, shift_two, expand_bias, shrink_bias = [
        vector.astype(wide_type) for vector in row_sets[2:]
    ]
    inputs_both = hidden_both.astype(wide_type)
    normed_low = layer_norm(inputs_both, gain_one, shift_one).astype(half_type)
    pair_heads = lax.dynamic_slice_in_dim(
        pair_full.reshape(head_total, 2, head_dim), dp_index * local_heads, local_heads, 0
    )
    triple_bias = jnp.stack(
        [pair_heads[:, 0], jnp.zeros_like(pair_heads[:, 0]), pair_heads[:, 1]], 0
    )
    projected = jnp.einsum(
        "mstd,dhce->cmshte", normed_low, triple_full, preferred_element_type=wide_type
    )
    projected = projected + triple_bias[:, None, None, :, None, :]
    project_low = projected.astype(half_type).reshape(3, seq_count, pair_local, seq_rows, head_dim)
    pair_rows = lax.all_to_all(project_low, "seq", split_axis=1, concat_axis=3, tiled=True)[:, 0]
    query_all, key_all, value_all = (pair_rows[0], pair_rows[1], pair_rows[2])
    pair_index = seq_index * pair_local + jnp.arange(pair_local, dtype=jnp.int32)
    head_index = dp_index * local_heads + pair_index % local_heads
    sequence_index = pair_index // local_heads
    slopes = jnp.power(jnp.float32(2.0), -8.0 * (head_index.astype(wide_type) + 1.0) / head_total)
    prefix_flat = prefix_lengths.reshape(-1)
    prefix_slots = jnp.arange(prefix_flat.shape[0], dtype=jnp.int32)
    prefixes = jnp.sum(
        jnp.where(prefix_slots[None, :] == sequence_index[:, None], prefix_flat[None, :], 0), 1
    )

    def block_scores(pair_item, first_row):
        query_block = lax.dynamic_slice_in_dim(
            lax.dynamic_index_in_dim(query_all, pair_item, 0, False), first_row, block_rows, 0
        )
        keys_item = lax.dynamic_index_in_dim(key_all, pair_item, 0, False)
        head_slope = lax.dynamic_index_in_dim(slopes, pair_item, 0, False)
        prefix = lax.dynamic_index_in_dim(prefixes, pair_item, 0, False)
        query_pos = first_row + jnp.arange(block_rows, dtype=jnp.int32)
        raw_scores = (
            jnp.einsum("qe,ke->qk", query_block, keys_item, preferred_element_type=wide_type)
            * score_scale
        )
        distance = jnp.abs(query_pos[:, None] - key_pos[None, :]).astype(wide_type)
        raw_scores = raw_scores - head_slope * distance
        allowed = (key_pos[None, :] <= query_pos[:, None]) | (key_pos[None, :] < prefix)
        return (query_block, jnp.where(allowed, raw_scores, jnp.float32(-1e30)))

    def forward_block(flat_index):
        pair_item = flat_index // block_count
        first_row = flat_index % block_count * block_rows
        _, scores = block_scores(pair_item, first_row)
        row_max = jnp.max(scores, -1, keepdims=True)
        powers = jnp.exp(scores - row_max)
        row_total = jnp.sum(powers, -1, keepdims=True)
        probs_low = (powers / row_total).astype(half_type)
        values_item = lax.dynamic_index_in_dim(value_all, pair_item, 0, False)
        mixed = jnp.dot(probs_low, values_item, preferred_element_type=wide_type).astype(half_type)
        return (mixed, (row_max + jnp.log(row_total))[:, 0])

    mixed_blocks, log_blocks = lax.map(
        forward_block, jnp.arange(pair_local * block_count, dtype=jnp.int32)
    )
    mixed_pairs = mixed_blocks.reshape(pair_local, seq_count, seq_rows, head_dim)
    log_totals = log_blocks.reshape(pair_local, seq_length)
    mixed_home = lax.all_to_all(mixed_pairs, "seq", split_axis=1, concat_axis=0, tiled=True)
    mixed_tokens = jnp.transpose(
        mixed_home.reshape(micro_count, group_count, local_heads, seq_rows, head_dim),
        (0, 1, 3, 2, 4),
    ).reshape(micro_count, group_count, seq_rows, local_heads * head_dim)
    dense_part = jnp.einsum(
        "mstk,kf->mstf", mixed_tokens, dense_full, preferred_element_type=wide_type
    )
    attention_sum = lax.psum(dense_part.astype(jnp.bfloat16), "dp").astype(jnp.float32)
    middle = inputs_both + attention_sum + dense_bias
    gain_rows_two = jnp.broadcast_to(gain_two[None, :], (group_count, model_width))
    shift_rows_two = jnp.broadcast_to(shift_two[None, :], (group_count, model_width))
    normed_two, norm_two_pull = jax.vjp(split_norm, middle, gain_rows_two, shift_rows_two)
    normed_two_low = normed_two.astype(half_type)
    unit_bias = lax.dynamic_slice_in_dim(expand_bias, dp_index * unit_local, unit_local, 0)
    hidden_pre = (
        jnp.einsum("mstd,df->mstf", normed_two_low, expand_full, preferred_element_type=wide_type)
        + unit_bias
    )
    activated_value, gelu_pull = jax.vjp(gelu_tanh, hidden_pre)
    activated_low = activated_value.astype(half_type)
    feed_part = jnp.einsum(
        "mstf,fd->mstd", activated_low, shrink_full, preferred_element_type=wide_type
    )
    feed_sum = lax.psum_scatter(
        feed_part.astype(jnp.bfloat16), "dp", scatter_dimension=1, tiled=True
    ).astype(jnp.float32)
    middle_own = lax.dynamic_slice_in_dim(middle, dp_index, 1, 1)
    layer_output = (middle_own + feed_sum + shrink_bias).astype(half_type)
    triple_back, dense_back, expand_back, shrink_back = (
        lax.all_gather(triple_weight, "seq", axis=0, tiled=True),
        lax.all_gather(dense_weight, "seq", axis=0, tiled=True),
        lax.all_gather(expand_weight, "seq", axis=0, tiled=True),
        lax.all_gather(shrink_weight, "seq", axis=0, tiled=True),
    )
    grad_act = jnp.einsum(
        "mstd,fd->mstf", upstream_low, shrink_back, preferred_element_type=wide_type
    )
    grad_pre_low = gelu_pull(grad_act)[0].astype(half_type)
    norm_two_part = jnp.einsum(
        "mstf,df->mstd", grad_pre_low, expand_back, preferred_element_type=wide_type
    )
    grad_normed_two = lax.psum(norm_two_part.astype(jnp.bfloat16), "dp").astype(jnp.float32)
    grad_middle_norm, grad_gain_rows_two, grad_shift_rows_two = norm_two_pull(grad_normed_two)
    grad_middle = upstream_low.astype(wide_type) + grad_middle_norm
    grad_branch_low = grad_middle.astype(half_type)
    go_pairs = jnp.einsum(
        "mstf,hef->mshte",
        grad_branch_low,
        dense_back.reshape(local_heads, head_dim, model_width),
        preferred_element_type=wide_type,
    ).astype(half_type)
    go_pairs = go_pairs.reshape(seq_count, pair_local, seq_rows, head_dim)
    grad_mixed_pairs = lax.all_to_all(go_pairs, "seq", split_axis=0, concat_axis=2, tiled=True)[0]

    def backward_item(pair_item):
        keys_item = lax.dynamic_index_in_dim(key_all, pair_item, 0, False)
        values_item = lax.dynamic_index_in_dim(value_all, pair_item, 0, False)
        grad_mixed_item = lax.dynamic_index_in_dim(grad_mixed_pairs, pair_item, 0, False)
        totals_item = lax.dynamic_index_in_dim(log_totals, pair_item, 0, False)

        def backward_block(running, block_index):
            key_grad, value_grad = running
            first_row = block_index * block_rows
            query_block, scores = block_scores(pair_item, first_row)
            soft_probs = jnp.exp(
                scores - lax.dynamic_slice_in_dim(totals_item, first_row, block_rows, 0)[:, None]
            )
            grad_block = lax.dynamic_slice_in_dim(grad_mixed_item, first_row, block_rows, 0)
            grad_probs = jnp.einsum(
                "qe,ke->qk", grad_block, values_item, preferred_element_type=wide_type
            )
            row_inner = jnp.sum(grad_probs * soft_probs, -1, keepdims=True)
            grad_scores_low = (soft_probs * (grad_probs - row_inner)).astype(half_type)
            query_grad = (
                jnp.dot(grad_scores_low, keys_item, preferred_element_type=wide_type) * score_scale
            )
            key_grad = (
                key_grad
                + jnp.einsum(
                    "qk,qe->ke", grad_scores_low, query_block, preferred_element_type=wide_type
                )
                * score_scale
            )
            value_grad = value_grad + jnp.einsum(
                "qk,qe->ke",
                soft_probs.astype(half_type),
                grad_block,
                preferred_element_type=wide_type,
            )
            return ((key_grad, value_grad), query_grad)

        zero_rows = jnp.zeros((seq_length, head_dim), wide_type)
        (key_grad, value_grad), query_grads = lax.scan(
            backward_block, (zero_rows, zero_rows), jnp.arange(block_count, dtype=jnp.int32)
        )
        return jnp.stack(
            [query_grads.reshape(seq_length, head_dim), key_grad, value_grad], 0
        ).astype(half_type)

    grad_pairs = lax.map(backward_item, jnp.arange(pair_local, dtype=jnp.int32))
    grad_split = grad_pairs.reshape(pair_local, 3, seq_count, seq_rows, head_dim)
    grad_home = lax.all_to_all(grad_split, "seq", split_axis=2, concat_axis=0, tiled=True)
    grad_project_low = jnp.transpose(
        grad_home.reshape(micro_count, group_count, local_heads, 3, seq_rows, head_dim),
        (0, 1, 4, 2, 3, 5),
    ).reshape(micro_count, group_count, seq_rows, project_width)
    norm_one_part = jnp.einsum(
        "mstc,dc->mstd",
        grad_project_low,
        triple_back.reshape(model_width, project_width),
        preferred_element_type=wide_type,
    )
    grad_normed_one = lax.psum_scatter(
        norm_one_part.astype(jnp.bfloat16), "dp", scatter_dimension=1, tiled=True
    ).astype(jnp.float32)
    inputs_own = hidden.astype(wide_type)
    grad_inputs_norm, grad_gain_one, grad_shift_one = jax.vjp(
        layer_norm, inputs_own, gain_one, shift_one
    )[1](grad_normed_one)
    grad_middle_own = lax.dynamic_slice_in_dim(grad_middle, dp_index, 1, 1)
    hidden_grad = (grad_middle_own + grad_inputs_norm).astype(half_type)
    head_sums = jnp.sum(
        grad_project_low.reshape(micro_count, group_count, seq_rows, local_heads, 3, head_dim),
        (0, 1, 2),
        dtype=wide_type,
    )
    pair_grad = place_half(jnp.stack([head_sums[:, 0], head_sums[:, 2]], 1), dp_index, group_count)
    unit_grad = place_half(jnp.sum(grad_pre_low, (0, 1, 2), dtype=wide_type), dp_index, group_count)
    dense_shift_term = jnp.sum(
        lax.dynamic_slice_in_dim(grad_branch_low, dp_index, 1, 1), (0, 1, 2), dtype=wide_type
    )
    shrink_shift_term = jnp.sum(cotangent, (0, 1, 2), dtype=wide_type)
    gain_two_term = lax.dynamic_index_in_dim(grad_gain_rows_two, dp_index, 0, False)
    shift_two_term = lax.dynamic_index_in_dim(grad_shift_rows_two, dp_index, 0, False)
    vector_sums = (
        lax.psum_scatter(grad_gain_one, ("dp", "seq"), scatter_dimension=0, tiled=True),
        lax.psum_scatter(grad_shift_one, ("dp", "seq"), scatter_dimension=0, tiled=True),
        lax.psum_scatter(pair_grad, ("dp", "seq"), scatter_dimension=0, tiled=True),
        lax.psum_scatter(dense_shift_term, ("dp", "seq"), scatter_dimension=0, tiled=True),
        lax.psum_scatter(gain_two_term, ("dp", "seq"), scatter_dimension=0, tiled=True),
        lax.psum_scatter(shift_two_term, ("dp", "seq"), scatter_dimension=0, tiled=True),
        lax.psum_scatter(unit_grad, ("dp", "seq"), scatter_dimension=0, tiled=True),
        lax.psum_scatter(shrink_shift_term, ("dp", "seq"), scatter_dimension=0, tiled=True),
    )
    normed_flat = normed_low.reshape(token_total, model_width)
    project_flat = grad_project_low.reshape(token_total, project_width)
    normed_two_flat = normed_two_low.reshape(token_total, model_width)
    pre_flat = grad_pre_low.reshape(token_total, unit_local)
    column_sums = lax.psum_scatter(
        jnp.concatenate(
            [
                jnp.einsum(
                    "tr,tc->rc", normed_flat, project_flat, preferred_element_type=wide_type
                ),
                jnp.einsum(
                    "tr,tc->rc", normed_two_flat, pre_flat, preferred_element_type=wide_type
                ),
            ],
            1,
        ),
        "seq",
        scatter_dimension=0,
        tiled=True,
    )
    triple_grad = column_sums[:, :project_width].reshape(
        model_width // seq_count, local_heads, 3, head_dim
    )
    expand_grad = column_sums[:, project_width:]
    dense_rows = dense_weight.shape[0]
    shrink_rows = shrink_weight.shape[0]
    row_block = dense_rows + shrink_rows
    mixed_flat = mixed_tokens.reshape(token_total, local_heads * head_dim)
    branch_flat = grad_branch_low.reshape(token_total, model_width)
    active_flat = activated_low.reshape(token_total, unit_local)
    upstream_flat = upstream_low.reshape(token_total, model_width)
    block_number = row_block * lax.axis_size("seq") // row_block
    dense_term = jnp.einsum("tr,td->rd", mixed_flat, branch_flat, preferred_element_type=wide_type)
    shrink_term = jnp.einsum(
        "tr,td->rd", active_flat, upstream_flat, preferred_element_type=wide_type
    )
    row_sums = lax.psum_scatter(
        jnp.concatenate(
            [
                dense_term.reshape(block_number, dense_rows, model_width),
                shrink_term.reshape(block_number, shrink_rows, model_width),
            ],
            1,
        ).reshape(row_block * lax.axis_size("seq"), model_width),
        "seq",
        scatter_dimension=0,
        tiled=True,
    )
    dense_grad = row_sums[:dense_rows]
    shrink_grad = row_sums[dense_rows:]
    return (
        layer_output,
        hidden_grad,
        vector_sums[0],
        vector_sums[1],
        triple_grad,
        vector_sums[2],
        dense_grad,
        vector_sums[3],
        vector_sums[4],
        vector_sums[5],
        expand_grad,
        vector_sums[6],
        shrink_grad,
        vector_sums[7],
    )


CHUNKS = 4
LOG2E = 1.4426950408889634
MESH = pl.DeviceIdType.MESH


def remote(src, dst, send, recv, peer):
    return pltpu.make_async_remote_copy(
        src_ref=src,
        dst_ref=dst,
        send_sem=send,
        recv_sem=recv,
        device_id=peer,
        device_id_type=MESH,
    )


def greet(peers):
    barrier = pltpu.get_barrier_semaphore()
    for peer in peers:
        pl.semaphore_signal(barrier, inc=1, device_id=peer, device_id_type=MESH)
    pl.semaphore_wait(barrier, len(peers))


class Corner:
    def __init__(self):
        self.c = lax.axis_index("dp")
        self.y = lax.axis_index("y")
        self.x = lax.axis_index("x")
        self.ax = self.x + (1 - self.c) * (1 - 2 * self.x)
        self.ay = self.y + self.c * (1 - 2 * self.y)
        self.bx = self.x + self.c * (1 - 2 * self.x)
        self.by = self.y + (1 - self.c) * (1 - 2 * self.y)
        self.dx = 1 - self.x
        self.dy = 1 - self.y
        self.peer_a = {"y": self.ay, "x": self.ax}
        self.peer_b = {"y": self.by, "x": self.bx}
        self.sibling = {"dp": 1 - self.c}

    def slots(self, core):
        return [
            (core * 2 + y) * 2 + x
            for y, x in (
                (self.dy, self.dx),
                (self.by, self.bx),
                (self.ay, self.ax),
                (self.y, self.x),
            )
        ]


def gather_kernel(deep, *refs):
    if deep:
        rows_ref, deep_ref, all_ref, moved_ref, local_sem, send, recv, deep_send, deep_recv = refs
    else:
        rows_ref, all_ref, local_sem, send, recv = refs
    at = Corner()
    slot_d, slot_b, slot_a, me = at.slots(at.c)
    step = rows_ref.shape[0] // CHUNKS
    peers = [at.peer_a, at.peer_b, at.sibling]
    sent, moves = [], []
    if deep:
        z = lax.axis_index("z")
        plane_at = [lax.rem(z + i, 4) for i in range(4)]
        peers += [{"z": plane_at[i]} for i in range(1, 4)]
    greet(peers)
    locals_ = [pltpu.make_async_copy(rows_ref, all_ref.at[me], local_sem.at[0])]
    if deep:
        locals_.append(pltpu.make_async_copy(deep_ref.at[z], moved_ref.at[z], local_sem.at[1]))
    for one in locals_:
        one.start()

    def copy(kind, k, slot, peer):
        part = pl.ds(k * step, step)
        src = rows_ref.at[part] if kind < 3 else all_ref.at[slot, part]
        return remote(src, all_ref.at[slot, part], send.at[kind, k], recv.at[kind, k], peer)

    def arrived(kind, k, slot, peer):
        part = pl.ds(k * step, step)
        block = all_ref.at[slot, part]
        remote(block, block, send.at[kind, k], recv.at[kind, k], peer).wait_recv()

    def start(kind, k, slot, peer):
        one = copy(kind, k, slot, peer)
        one.start()
        sent.append(one)

    for i in range(1, 4) if deep else ():
        sems = deep_send.at[i - 1], deep_recv.at[i - 1]
        one = remote(deep_ref.at[plane_at[i]], moved_ref.at[z], *sems, {"z": plane_at[i]})
        one.start()
        sent.append(one)
        landing = moved_ref.at[plane_at[4 - i]]
        moves.append(remote(landing, landing, *sems, {"z": plane_at[i]}))
    for k in range(CHUNKS):
        start(0, k, me, at.peer_a)
        start(1, k, me, at.peer_b)
    for k in range(CHUNKS):
        start(2, k, me, at.sibling)
    for k in range(CHUNKS):
        arrived(0, k, slot_a, at.peer_a)
        start(3, k, slot_a, at.peer_b)
        start(4, k, slot_a, at.sibling)
    for k in range(CHUNKS):
        arrived(1, k, slot_b, at.peer_b)
        start(5, k, slot_b, at.sibling)
    for k in range(CHUNKS):
        arrived(3, k, slot_d, at.peer_b)
        start(6, k, slot_d, at.sibling)
    other_d, other_b, other_a, other_me = at.slots(1 - at.c)
    for k in range(CHUNKS):
        arrived(2, k, other_me, at.sibling)
        arrived(4, k, other_b, at.sibling)
        arrived(5, k, other_a, at.sibling)
        arrived(6, k, other_d, at.sibling)
    for one in moves:
        one.wait_recv()
    for one in sent:
        one.wait_send()
    for one in locals_:
        one.wait()


def gather_tokens(rows, deep=None):
    count, width = rows.shape
    operands = [rows]
    shapes = [jax.ShapeDtypeStruct((8, count, width), rows.dtype)]
    scratch = [
        pltpu.SemaphoreType.DMA((2,)),
        pltpu.SemaphoreType.DMA((7, CHUNKS)),
        pltpu.SemaphoreType.DMA((7, CHUNKS)),
    ]
    if deep is not None:
        operands.append(deep)
        shapes.append(jax.ShapeDtypeStruct(deep.shape, deep.dtype))
        scratch += [pltpu.SemaphoreType.DMA((3,)), pltpu.SemaphoreType.DMA((3,))]
    all_rows, *moved = pl.pallas_call(
        functools.partial(gather_kernel, deep is not None),
        out_shape=shapes,
        in_specs=[pl.BlockSpec(memory_space=pl.ANY)] * len(operands),
        out_specs=[pl.BlockSpec(memory_space=pl.ANY)] * len(shapes),
        scratch_shapes=scratch,
        compiler_params=pltpu.CompilerParams(
            collective_id=1 if deep is None else 6, has_side_effects=True
        ),
        cost_estimate=pl.CostEstimate(
            flops=0, bytes_accessed=16 * count * width * 4, transcendentals=0
        ),
        name="gather_tokens",
    )(*operands)
    return (all_rows.reshape(8 * count, width), *moved)


def after(value, *others):
    return lax.optimization_barrier((value, *others))[0]


def scatter_kernel(
    turned, left_ref, right_ref, own_ref, part_ref, from_core, from_b, from_a, send, recv
):
    at = Corner()
    slot_d, slot_b, slot_a, me = at.slots(at.c)
    other_d, other_b, other_a, other_me = at.slots(1 - at.c)
    rows, width = own_ref.shape
    step = rows // CHUNKS
    wide = jnp.float32
    greet([at.peer_a, at.peer_b, at.sibling])
    sent = []

    def start(kind, k, src, dst, peer):
        one = remote(src, dst, send.at[kind, k], recv.at[kind, k], peer)
        one.start()
        sent.append(one)

    def arrived(kind, k, dst, peer):
        remote(dst, dst, send.at[kind, k], recv.at[kind, k], peer).wait_recv()

    tile = min(512, width)

    def multiply(slot):
        def columns(t, carry):
            part = pl.ds(pl.multiple_of(t * tile, tile), tile)
            right = right_ref[part] if turned else right_ref[:, part]
            product = lax.dot_general(
                left_ref[slot],
                right,
                (((1,), (1 if turned else 0,)), ((), ())),
                preferred_element_type=wide,
            )
            part_ref[slot, :, part] = product.astype(part_ref.dtype)
            return carry

        lax.fori_loop(0, width // tile, columns, 0)

    def to_sibling(q, slot):
        multiply(slot)
        for k in range(CHUNKS):
            part = pl.ds(k * step, step)
            start(q, k, part_ref.at[slot, part], from_core.at[q, part], at.sibling)

    def to_b(q, slot):
        for k in range(CHUNKS):
            part = pl.ds(k * step, step)
            arrived(q, k, from_core.at[q, part], at.sibling)
            total = part_ref[slot, part].astype(wide) + from_core[q, part].astype(wide)
            from_core[q, part] = total.astype(from_core.dtype)
            start(4 + q, k, from_core.at[q, part], from_b.at[q, part], at.peer_b)

    to_sibling(0, other_d)
    multiply(slot_d)
    to_sibling(1, other_a)
    to_b(0, slot_d)
    multiply(slot_b)
    to_b(1, slot_b)
    to_sibling(2, other_b)
    multiply(slot_a)
    for k in range(CHUNKS):
        part = pl.ds(k * step, step)
        arrived(2, k, from_core.at[2, part], at.sibling)
        arrived(4, k, from_b.at[0, part], at.peer_b)
        total = part_ref[slot_a, part].astype(wide) + from_core[2, part].astype(wide)
        total = total + from_b[0, part].astype(wide)
        from_core[2, part] = total.astype(from_core.dtype)
        start(6, k, from_core.at[2, part], from_a.at[part], at.peer_a)
    to_sibling(3, other_me)
    multiply(me)
    for k in range(CHUNKS):
        part = pl.ds(k * step, step)
        arrived(3, k, from_core.at[3, part], at.sibling)
        arrived(5, k, from_b.at[1, part], at.peer_b)
        arrived(6, k, from_a.at[part], at.peer_a)
        total = part_ref[me, part].astype(wide) + from_core[3, part].astype(wide)
        total = total + from_b[1, part].astype(wide)
        own_ref[part] = total + from_a[part].astype(wide)
    for one in sent:
        one.wait_send()


def scatter_tokens(identity, left, right, turned=False):
    count, depth = left.shape[0] // 8, left.shape[1]
    width = right.shape[0] if turned else right.shape[1]
    half = left.dtype
    return pl.pallas_call(
        functools.partial(scatter_kernel, turned),
        out_shape=jax.ShapeDtypeStruct((count, width), jnp.float32),
        in_specs=[pl.BlockSpec(memory_space=pltpu.VMEM)] * 2,
        out_specs=pl.BlockSpec(memory_space=pltpu.VMEM),
        scratch_shapes=[
            pltpu.VMEM((8, count, width), half),
            pltpu.VMEM((4, count, width), half),
            pltpu.VMEM((2, count, width), half),
            pltpu.VMEM((count, width), half),
            pltpu.SemaphoreType.DMA((7, CHUNKS)),
            pltpu.SemaphoreType.DMA((7, CHUNKS)),
        ],
        compiler_params=pltpu.CompilerParams(
            collective_id=identity, has_side_effects=True, vmem_limit_bytes=48 * 2**20
        ),
        cost_estimate=pl.CostEstimate(
            flops=2 * left.size * width, bytes_accessed=64 * count * width, transcendentals=0
        ),
        name="scatter_tokens",
    )(left.reshape(8, count, depth), right)


def exchange_kernel(last, n_deep, n_flat, n_vec, *refs):
    refs = list(refs)
    take = lambda n: [refs.pop(0) for _ in range(n)]
    deep_in, turn_in, flat_in, vec_in = take(n_deep), take(n_deep), take(n_flat), take(n_vec)
    deep_out, turn_out, flat_out, vec_out = take(n_deep), take(n_deep), take(n_flat), take(n_vec)
    if last:
        columns_out, flat_out = flat_out, take(n_flat)
        near, far, here = take(3)
    send, recv = take(2)
    c, z = lax.axis_index("dp"), lax.axis_index("z")
    y, x = lax.axis_index("y"), lax.axis_index("x")
    place = y * 2 + x
    rank = c * 4 + place

    def deep(i):
        return lax.rem(z + i, 4)

    def flat(i):
        return lax.rem(place + i, 4)

    def wide(i):
        return lax.rem(rank + i, 8)

    def deep_peer(i):
        return {"z": deep(i)}

    def flat_peer(i):
        return {"y": flat(i) // 2, "x": lax.rem(flat(i), 2)}

    def wide_peer(i):
        return {
            "dp": wide(i) // 4,
            "y": lax.rem(wide(i), 4) // 2,
            "x": lax.rem(wide(i), 2),
        }

    low = lax.rem(z, 2)
    turn_from = {"z": z - low + 1 - x, "x": low}
    turn_to = {"z": z - low + x, "x": 1 - low}
    if last:
        turn_from, turn_to = turn_to, turn_from
    others = range(1, 4)
    if n_vec:
        near_peers = [wide_peer(i) for i in range(1, 8)]
    else:
        near_peers = [flat_peer(i) for i in others]
    greet([deep_peer(i) for i in others] + near_peers)
    sent, waits = [], []
    count = [0]

    def post(src, dst, peer, landing):
        k = count[0]
        count[0] += 1
        one = remote(src, dst, send.at[k], recv.at[k], peer)
        one.start()
        sent.append(one)
        return remote(landing, landing, send.at[k], recv.at[k], peer)

    stage = []
    for i in range(1, 8) if n_vec else ():
        if last:
            landing = near.at[wide(8 - i)]
            stage.append(post(vec_in[0].at[wide(i)], near.at[rank], wide_peer(i), landing))
        else:
            landing = vec_out[0].at[z, wide(8 - i)]
            stage.append(post(vec_in[0], vec_out[0].at[z, rank], wide_peer(i), landing))
    late = []
    for src, dst in zip(deep_in, deep_out):
        for i in others:
            late.append(post(src.at[deep(i)], dst.at[z], deep_peer(i), dst.at[deep(4 - i)]))
    for src, dst in zip(flat_in, flat_out):
        for i in others:
            landing = dst.at[flat(4 - i)]
            waits.append(post(src.at[flat(i)], dst.at[place], flat_peer(i), landing))
    for src, dst in zip(turn_in, turn_out):
        late.append(post(src, dst, turn_to, dst))
    for src, dst in zip(deep_in, deep_out):
        dst[z] = src[z]
    for src, dst in zip(flat_in, flat_out):
        dst[place] = src[place]
    if last:
        near[rank] = vec_in[0][rank]
        for one in stage:
            one.wait_recv()
        here[...] = jnp.sum(near[...], 0)
        stage = []
        for i in others:
            landing = far.at[deep(4 - i)]
            stage.append(post(here.at[deep(i)], far.at[z], deep_peer(i), landing))
        far[z] = here[z]
        for one in stage:
            one.wait_recv()
        vec_out[0][...] = jnp.sum(far[...], 0)
    elif n_vec:
        vec_out[0][z, rank] = vec_in[0][...]
        for one in stage:
            one.wait_recv()
        for i in others:
            landing = vec_out[0].at[deep(4 - i)]
            late.append(post(vec_out[0].at[z], vec_out[0].at[z], deep_peer(i), landing))
    for one in waits:
        one.wait_recv()
    if last:
        for (steps, order), blocks, columns in zip(last, flat_out, columns_out):
            step = blocks.shape[2] // steps
            for i in range(steps):
                for p in range(4):
                    first = (i * 4 + order[p]) * step
                    columns[:, first : first + step] = blocks[p, :, i * step : (i + 1) * step]
    for one in late:
        one.wait_recv()
    for one in sent:
        one.wait_send()


def exchange(identity, deep, turned, flat, vector, last=None):
    if vector:
        tile = vector[0].shape[2:] if last else vector[0].shape
    shapes = [jax.ShapeDtypeStruct(a.shape, a.dtype) for a in (*deep, *turned)]
    blocks = [(a.shape, a.dtype) for a in flat]
    scratch = []
    if last:
        shapes += [jax.ShapeDtypeStruct((s[1], 4 * s[2]), t) for s, t in blocks]
        shapes.append(jax.ShapeDtypeStruct(tile, vector[0].dtype))
        scratch = [pltpu.VMEM(*b) for b in blocks]
        scratch += [
            pltpu.VMEM((8, 4) + tile, vector[0].dtype),
            pltpu.VMEM((4,) + tile, vector[0].dtype),
            pltpu.VMEM((4,) + tile, vector[0].dtype),
        ]
    else:
        shapes += [jax.ShapeDtypeStruct(*b) for b in blocks]
        if vector:
            shapes.append(jax.ShapeDtypeStruct((4, 8) + tile, vector[0].dtype))
    copies = 4 * len(deep) + 3 * len(flat) + 10 * len(vector)
    operands = [*deep, *turned, *flat, *vector]
    moved = sum(a.size * a.dtype.itemsize for a in operands)
    return pl.pallas_call(
        functools.partial(exchange_kernel, last, len(deep), len(flat), len(vector)),
        out_shape=shapes,
        in_specs=[pl.BlockSpec(memory_space=pltpu.VMEM)] * len(operands),
        out_specs=[pl.BlockSpec(memory_space=pltpu.VMEM)] * len(shapes),
        scratch_shapes=scratch
        + [pltpu.SemaphoreType.DMA((copies,)), pltpu.SemaphoreType.DMA((copies,))],
        compiler_params=pltpu.CompilerParams(
            collective_id=identity, has_side_effects=True, vmem_limit_bytes=40 * 2**20
        ),
        cost_estimate=pl.CostEstimate(flops=0, bytes_accessed=16 * moved, transcendentals=0),
        name="exchange",
    )(*operands)


def scores_of(item_ref, first, block, slope, prefix, depth, seq_rows):
    length = item_ref.shape[0]
    head_dim = item_ref.shape[1] // 3
    own_rows = depth * seq_rows
    chips = length // own_rows

    def position(index):
        chip = index // own_rows
        rest = index % own_rows
        return ((rest // seq_rows) * chips + chip) * seq_rows + rest % seq_rows

    queries = item_ref[first : first + block, :head_dim]
    keys = item_ref[:, head_dim : 2 * head_dim]
    raw = lax.dot_general(
        keys, queries, (((1,), (1,)), ((), ())), preferred_element_type=jnp.float32
    )
    key_pos = position(lax.broadcasted_iota(jnp.int32, (length, 1), 0))
    query_pos = position(first + lax.broadcasted_iota(jnp.int32, (1, block), 1))
    bound = jnp.where(key_pos < prefix, -1, key_pos)
    distance = jnp.abs(
        query_pos.astype(jnp.float32) - key_pos.astype(jnp.float32)
    )
    scores = raw * (LOG2E / math.sqrt(head_dim)) - (slope * LOG2E) * distance
    return jnp.where(bound <= query_pos, scores, jnp.float32(-1e30))


def forward_kernel(depth, seq_rows, block, prefix_ref, slope_ref, item_ref, mixed_ref, total_ref):
    prefix = prefix_ref[pl.program_id(0)]
    slope = slope_ref[pl.program_id(1)]
    length = item_ref.shape[0]
    head_dim = item_ref.shape[1] // 3
    for first in range(0, length, block):
        scores = scores_of(item_ref, first, block, slope, prefix, depth, seq_rows)
        top = jnp.max(scores, 0, keepdims=True)
        powers = jnp.exp2(scores - top)
        total = jnp.sum(powers, 0, keepdims=True)
        probs = (powers * (1.0 / total)).astype(jnp.bfloat16)
        mixed = lax.dot_general(
            probs,
            item_ref[:, 2 * head_dim :],
            (((0,), (0,)), ((), ())),
            preferred_element_type=jnp.float32,
        )
        mixed_ref[first : first + block, :] = mixed.astype(mixed_ref.dtype)
        total_ref[0, :, first : first + block] = top + jnp.log2(total)


def attend_forward(projected, slopes, prefixes, own_heads, head_dim, depth, seq_rows):
    cores = prefixes.shape[0]
    length = projected.shape[0] // cores
    block = min(256, length)
    scores = cores * own_heads * length * length
    return pl.pallas_call(
        functools.partial(forward_kernel, depth, seq_rows, block),
        grid=(cores, own_heads),
        out_shape=[
            jax.ShapeDtypeStruct((cores * length, own_heads * head_dim), projected.dtype),
            jax.ShapeDtypeStruct((cores * own_heads, 1, length), jnp.float32),
        ],
        in_specs=[
            pl.BlockSpec(memory_space=pltpu.SMEM),
            pl.BlockSpec(memory_space=pltpu.SMEM),
            pl.BlockSpec((length, 3 * head_dim), lambda s, h: (s, h)),
        ],
        out_specs=[
            pl.BlockSpec((length, head_dim), lambda s, h: (s, h)),
            pl.BlockSpec((1, 1, length), lambda s, h: (s * own_heads + h, 0, 0)),
        ],
        compiler_params=pltpu.CompilerParams(vmem_limit_bytes=48 * 2**20),
        cost_estimate=pl.CostEstimate(
            flops=4 * scores * head_dim,
            bytes_accessed=2 * projected.size * 2,
            transcendentals=scores,
        ),
        name="attend_forward",
    )(prefixes, slopes, projected)


def backward_kernel(
    depth, seq_rows, block, prefix_ref, slope_ref, item_ref, grad_ref, total_ref, out_ref, key_sum, value_sum
):
    prefix = prefix_ref[pl.program_id(0)]
    slope = slope_ref[pl.program_id(1)]
    length = item_ref.shape[0]
    head_dim = item_ref.shape[1] // 3
    scale = 1.0 / math.sqrt(head_dim)
    half = jnp.bfloat16
    wide = jnp.float32
    for first in range(0, length, block):
        scores = scores_of(item_ref, first, block, slope, prefix, depth, seq_rows)
        probs = jnp.exp2(scores - total_ref[0, :, first : first + block])
        grad = grad_ref[first : first + block, :]
        grad_probs = lax.dot_general(
            item_ref[:, 2 * head_dim :],
            grad,
            (((1,), (1,)), ((), ())),
            preferred_element_type=wide,
        )
        inner = jnp.sum(grad_probs * probs, 0, keepdims=True)
        grad_scores = (probs * (grad_probs - inner)).astype(half)
        key_term = jnp.dot(
            grad_scores, item_ref[first : first + block, :head_dim], preferred_element_type=wide
        )
        value_term = jnp.dot(probs.astype(half), grad, preferred_element_type=wide)
        query_grad = lax.dot_general(
            grad_scores,
            item_ref[:, head_dim : 2 * head_dim],
            (((0,), (0,)), ((), ())),
            preferred_element_type=wide,
        )
        out_ref[first : first + block, :head_dim] = (query_grad * scale).astype(half)
        if first == 0:
            key_sum[...] = key_term
            value_sum[...] = value_term
        else:
            key_sum[...] += key_term
            value_sum[...] += value_term
    out_ref[:, head_dim : 2 * head_dim] = (key_sum[...] * scale).astype(half)
    out_ref[:, 2 * head_dim :] = value_sum[...].astype(half)


def attend_backward(
    projected, grad_mixed, totals, slopes, prefixes, own_heads, head_dim, depth, seq_rows
):
    cores = prefixes.shape[0]
    length = projected.shape[0] // cores
    block = min(256, length)
    scores = cores * own_heads * length * length
    return pl.pallas_call(
        functools.partial(backward_kernel, depth, seq_rows, block),
        grid=(cores, own_heads),
        out_shape=jax.ShapeDtypeStruct(projected.shape, projected.dtype),
        in_specs=[
            pl.BlockSpec(memory_space=pltpu.SMEM),
            pl.BlockSpec(memory_space=pltpu.SMEM),
            pl.BlockSpec((length, 3 * head_dim), lambda s, h: (s, h)),
            pl.BlockSpec((length, head_dim), lambda s, h: (s, h)),
            pl.BlockSpec((1, 1, length), lambda s, h: (s * own_heads + h, 0, 0)),
        ],
        out_specs=pl.BlockSpec((length, 3 * head_dim), lambda s, h: (s, h)),
        scratch_shapes=[
            pltpu.VMEM((length, head_dim), jnp.float32),
            pltpu.VMEM((length, head_dim), jnp.float32),
        ],
        compiler_params=pltpu.CompilerParams(vmem_limit_bytes=48 * 2**20),
        cost_estimate=pl.CostEstimate(
            flops=10 * scores * head_dim,
            bytes_accessed=2 * projected.size * 2,
            transcendentals=scores,
        ),
        name="attend_backward",
    )(prefixes, slopes, projected, grad_mixed, totals)


def planar(
    hidden,
    prefix_lengths,
    cotangent,
    first_gain,
    first_shift,
    triple_weight,
    pair_bias,
    dense_weight,
    dense_shift,
    second_gain,
    second_shift,
    expand_weight,
    expand_shift,
    shrink_weight,
    shrink_shift,
):
    wide = jnp.float32
    half = jnp.bfloat16
    cores = lax.axis_size("dp")
    depth = lax.axis_size("z")
    rows_y = lax.axis_size("y")
    rows_x = lax.axis_size("x")
    plane = rows_y * rows_x
    core = lax.axis_index("dp")
    at_y = lax.axis_index("y")
    at_x = lax.axis_index("x")
    place = at_y * rows_x + at_x
    seq_rows = hidden.shape[2]
    width = hidden.shape[3]
    head_dim = triple_weight.shape[3]
    heads = triple_weight.shape[1]
    own_heads = heads // plane
    own_rows = seq_rows * depth
    units = expand_weight.shape[1]
    own_units = units // plane
    row_block = expand_weight.shape[0]
    shrink_rows = shrink_weight.shape[0]

    pieces = [
        first_gain,
        first_shift,
        dense_shift,
        second_gain,
        second_shift,
        shrink_shift,
        pair_bias,
        expand_shift,
    ]
    piece_total = sum(p.shape[0] for p in pieces)
    lanes = 128
    vector_rows = -(-piece_total // (lanes * 16)) * 16
    vector_tile = jnp.pad(
        jnp.concatenate(pieces), (0, vector_rows * lanes - piece_total)
    ).reshape(vector_rows, lanes)
    triple_blocks = (
        triple_weight.reshape(row_block, own_heads, rows_x, rows_y, 3 * head_dim)[:, :, ::-1]
        .transpose(3, 2, 0, 1, 4)
        .reshape(plane, row_block, own_heads * 3 * head_dim)
    )
    triple_turned, packed = exchange(3, (), (), (triple_blocks,), (vector_tile,))
    expand_blocks = (
        after(expand_weight, triple_turned).reshape(row_block, depth, plane, shrink_rows)
        .transpose(2, 0, 1, 3)
        .reshape(plane, row_block, own_units)
    )
    inputs, dense_turned, expand_turned = exchange(
        7, (hidden[:, 0],), (dense_weight,), (expand_blocks,), ()
    )
    packed = (
        packed.reshape(depth, cores, plane, vector_rows * lanes)
        .transpose(1, 0, 2, 3)
        .reshape(-1, vector_rows * lanes)
    )
    vectors = []
    offset = 0
    for piece in pieces:
        vectors.append(packed[:, offset : offset + piece.shape[0]].reshape(-1).astype(wide))
        offset += piece.shape[0]
    gain_one, shift_one, dense_bias, gain_two, shift_two, shrink_bias, pair_full, unit_full = vectors
    pair_heads = pair_full.reshape(cores, own_heads, rows_x, rows_y, 2, head_dim)[
        core, :, 1 - at_x, at_y
    ]
    triple_bias = jnp.stack(
        [pair_heads[:, 0], jnp.zeros_like(pair_heads[:, 0]), pair_heads[:, 1]], 1
    ).reshape(-1)
    unit_bias = unit_full.reshape(cores, depth, plane, shrink_rows)[core, :, place].reshape(-1)

    triple_own = lax.all_gather(
        triple_turned.reshape(-1, triple_turned.shape[2]), "z", axis=0, tiled=True
    )
    inputs = inputs.reshape(own_rows, width).astype(wide)

    normed_own = layer_norm(inputs, gain_one, shift_one).astype(half)
    (normed,) = gather_tokens(normed_own)
    dense_own = lax.all_gather(after(dense_turned, normed), "z", axis=0, tiled=True)
    expand_own = lax.all_gather(
        after(expand_turned, normed).reshape(-1, own_units), "z", axis=0, tiled=True
    )
    projected = (
        jnp.dot(normed, triple_own, preferred_element_type=wide) + triple_bias
    ).astype(half)

    shrink_own = lax.all_gather(after(shrink_weight, projected), "z", axis=0, tiled=True)
    head_index = core * heads + jnp.arange(own_heads) * plane + (1 - at_x) * rows_y + at_y
    slopes = jnp.power(
        jnp.float32(2.0), -8.0 * (head_index.astype(wide) + 1.0) / (heads * cores)
    )
    at_z = lax.axis_index("z")
    prefixes = lax.dynamic_index_in_dim(prefix_lengths, at_z, 0, False)
    mixed, log_totals = attend_forward(
        projected, slopes, prefixes, own_heads, head_dim, depth, seq_rows
    )
    dense_sum = scatter_tokens(2, mixed, dense_own)
    middle = inputs + dense_sum + dense_bias
    normed_two_own, norm_two_pull = jax.vjp(layer_norm, middle, gain_two, shift_two)
    normed_two, upstream = gather_tokens(normed_two_own.astype(half), cotangent[:, 0])
    upstream = upstream.reshape(own_rows, width)
    hidden_pre = jnp.dot(normed_two, expand_own, preferred_element_type=wide) + unit_bias
    (upstream_all,) = gather_tokens(upstream)
    activated, gelu_pull = jax.vjp(gelu_tanh, hidden_pre)
    activated = activated.astype(half)
    shrink_term = jnp.einsum(
        "tu,td->ud", activated, upstream_all, preferred_element_type=wide
    ).astype(half)
    shrink_own = after(shrink_own, shrink_term)
    grad_act = jnp.einsum("tf,uf->tu", upstream_all, shrink_own, preferred_element_type=wide)
    grad_pre = gelu_pull(grad_act)[0].astype(half)
    shrink_grad = lax.psum_scatter(shrink_term, "z", scatter_dimension=0, tiled=True)
    expand_term = jnp.einsum(
        "td,tu->du", normed_two, grad_pre, preferred_element_type=wide
    ).astype(half)
    expand_turned = lax.psum_scatter(expand_term, "z", scatter_dimension=0, tiled=True)
    feed_sum = scatter_tokens(8, after(activated, shrink_term, expand_term), shrink_own)
    layer_output = (middle + feed_sum + shrink_bias).astype(half)

    norm_two_sum = scatter_tokens(9, after(grad_pre, feed_sum), expand_own, True)
    grad_norm_two, gain_two_term, shift_two_term = norm_two_pull(norm_two_sum)
    grad_middle = upstream.astype(wide) + grad_norm_two
    branch_own = grad_middle.astype(half)
    branch, layer_output = gather_tokens(branch_own, layer_output.reshape(depth, seq_rows, width))

    grad_mixed = jnp.einsum("tf,ef->te", branch, dense_own, preferred_element_type=wide).astype(
        half
    )
    dense_term = jnp.einsum("te,tf->ef", mixed, branch, preferred_element_type=wide).astype(half)
    dense_turned = lax.psum_scatter(dense_term, "z", scatter_dimension=0, tiled=True)
    grad_project = attend_backward(
        projected,
        after(grad_mixed, dense_term),
        log_totals,
        slopes,
        prefixes,
        own_heads,
        head_dim,
        depth,
        seq_rows,
    )
    triple_term = jnp.einsum(
        "td,tc->dc", normed, grad_project, preferred_element_type=wide
    ).astype(half)
    triple_turned = lax.psum_scatter(triple_term, "z", scatter_dimension=0, tiled=True)
    norm_one_sum = scatter_tokens(10, after(grad_project, triple_term), triple_own, True)
    grad_norm_one, gain_one_term, shift_one_term = jax.vjp(
        layer_norm, inputs, gain_one, shift_one
    )[1](norm_one_sum)
    hidden_grad = (grad_middle + grad_norm_one).astype(half)
    head_sums = jnp.sum(grad_project, 0, dtype=wide).reshape(own_heads, 3, head_dim)
    pair_term = jnp.stack([head_sums[:, 0], head_sums[:, 2]], 1)
    pair_zero = jnp.zeros((cores, own_heads, rows_x, rows_y, 2, head_dim), wide)
    pair_wide = lax.dynamic_update_slice(
        pair_zero, pair_term[None, :, None, None], (core, 0, 1 - at_x, at_y, 0, 0)
    ).reshape(-1)
    unit_term = jnp.sum(grad_pre, 0, dtype=wide).reshape(1, depth, 1, shrink_rows)
    unit_wide = lax.dynamic_update_slice(
        jnp.zeros((cores, depth, plane, shrink_rows), wide), unit_term, (core, 0, place, 0)
    ).reshape(-1)
    terms = [
        gain_one_term,
        shift_one_term,
        jnp.sum(branch_own, 0, dtype=wide),
        gain_two_term,
        shift_two_term,
        jnp.sum(upstream, 0, dtype=wide),
        pair_wide,
        unit_wide,
    ]
    devices = cores * depth * plane
    term_rows = -(-piece_total // (lanes * 8)) * 8
    term_tiles = jnp.pad(
        jnp.concatenate([t.reshape(devices, -1) for t in terms], 1),
        ((0, 0), (0, term_rows * lanes - piece_total)),
    )
    term_tiles = (
        term_tiles.reshape(cores, depth, plane, term_rows, lanes)
        .transpose(0, 2, 1, 3, 4)
        .reshape(cores * plane, depth, term_rows, lanes)
    )
    hidden_grad, dense_grad, triple_grad, expand_grad, summed = exchange(
        4,
        (hidden_grad.reshape(depth, seq_rows, width),),
        (dense_turned,),
        (
            triple_turned.reshape(plane, row_block, -1),
            expand_turned.reshape(plane, row_block, own_units),
        ),
        (term_tiles,),
        last=((own_heads, (2, 0, 3, 1)), (depth, (0, 1, 2, 3))),
    )
    layer_output = layer_output[:, None]
    hidden_grad = hidden_grad[:, None]
    triple_grad = triple_grad.astype(wide).reshape(row_block, heads, 3, head_dim)
    summed = summed.reshape(-1)
    vector_grads = []
    offset = 0
    for piece in pieces:
        vector_grads.append(summed[offset : offset + piece.shape[0]])
        offset += piece.shape[0]
    return (
        layer_output,
        hidden_grad,
        vector_grads[0],
        vector_grads[1],
        triple_grad,
        vector_grads[6],
        dense_grad.astype(wide),
        vector_grads[2],
        vector_grads[3],
        vector_grads[4],
        expand_grad.astype(wide),
        vector_grads[7],
        shrink_grad.astype(wide),
        vector_grads[5],
    )


def layer(*args):
    return planar(*args)


def solution(mesh):
    depth = 4
    sides = (2, 2)
    planar_plan = mesh.shape["seq"] == depth * sides[0] * sides[1]
    if planar_plan:
        grid = Mesh(
            mesh.devices.reshape(mesh.shape["dp"], depth, *sides), ("dp", "z", "y", "x")
        )
        seq = ("z", "y", "x")
    else:
        grid = mesh
        seq = ("seq",)
    tokens = P(None, "dp", seq, None)
    vector = P(("dp",) + seq)
    matrix = P(("dp",) + seq, None)
    placed = (
        tokens,
        P(),
        tokens,
        vector,
        vector,
        P(seq, "dp", None, None),
        vector,
        matrix,
        vector,
        vector,
        vector,
        P(seq, "dp"),
        vector,
        matrix,
        vector,
    )
    results = (
        tokens,
        tokens,
        vector,
        vector,
        P(seq, "dp", None, None),
        vector,
        matrix,
        vector,
        vector,
        vector,
        P(seq, "dp"),
        vector,
        matrix,
        vector,
    )
    return jax.shard_map(
        layer if planar_plan else shards,
        mesh=grid,
        in_specs=placed,
        out_specs=results,
        check_vma=False,
    )
```

```python
import functools
import math

import jax
import jax.numpy as jnp
from jax import lax
from jax.experimental import pallas as pl
from jax.experimental.pallas import tpu as pltpu
from jax.sharding import Mesh
from jax.sharding import PartitionSpec as P


EPSILON = 1e-05
GELU_SCALE = 0.7978845608028654


def layer_norm(inputs, norm_gain, norm_shift):
    centered = inputs - jnp.mean(inputs, -1, keepdims=True)
    variance = jnp.mean(centered * centered, -1, keepdims=True)
    return centered * lax.rsqrt(variance + EPSILON) * norm_gain + norm_shift


def gelu_tanh(values):
    return (
        0.5 * values * (1.0 + jnp.tanh(GELU_SCALE * (values + 0.044715 * values * values * values)))
    )


def split_norm(inputs, gain_rows, shift_rows):
    return layer_norm(inputs, gain_rows[None, :, None, :], shift_rows[None, :, None, :])


def place_half(values, half_index, group_count):
    chosen = (jnp.arange(group_count, dtype=jnp.int32) == half_index).astype(values.dtype)
    return (chosen[:, None] * values.reshape(1, -1)).reshape(-1)


def shards(
    hidden,
    prefix_lengths,
    cotangent,
    first_gain,
    first_shift,
    triple_weight,
    pair_bias,
    dense_weight,
    dense_shift,
    second_gain,
    second_shift,
    expand_weight,
    expand_shift,
    shrink_weight,
    shrink_shift,
):
    wide_type = jnp.float32
    half_type = jnp.bfloat16
    seq_count = lax.axis_size("seq")
    group_count = lax.axis_size("dp")
    dp_index = lax.axis_index("dp")
    seq_index = lax.axis_index("seq")
    micro_count = hidden.shape[0]
    seq_rows = hidden.shape[2]
    model_width = hidden.shape[3]
    seq_length = seq_rows * seq_count
    local_heads = triple_weight.shape[1]
    head_dim = triple_weight.shape[3]
    head_total = local_heads * group_count
    pair_local = micro_count * group_count * local_heads // seq_count
    unit_local = expand_weight.shape[1]
    project_width = 3 * local_heads * head_dim
    token_total = micro_count * group_count * seq_rows
    score_scale = 1.0 / math.sqrt(head_dim)
    block_rows = min(512, seq_length)
    block_count = seq_length // block_rows
    key_pos = jnp.arange(seq_length, dtype=jnp.int32)
    gathered = (
        lax.all_gather(triple_weight, "seq", axis=0, tiled=True),
        lax.all_gather(dense_weight, "seq", axis=0, tiled=True),
        lax.all_gather(expand_weight, "seq", axis=0, tiled=True),
        lax.all_gather(shrink_weight, "seq", axis=0, tiled=True),
        lax.all_gather(first_gain, "seq", axis=0, tiled=True),
        lax.all_gather(first_shift, "seq", axis=0, tiled=True),
        lax.all_gather(pair_bias, "seq", axis=0, tiled=True),
        lax.all_gather(dense_shift, "seq", axis=0, tiled=True),
        lax.all_gather(second_gain, "seq", axis=0, tiled=True),
        lax.all_gather(second_shift, "seq", axis=0, tiled=True),
        lax.all_gather(expand_shift, "seq", axis=0, tiled=True),
        lax.all_gather(shrink_shift, "seq", axis=0, tiled=True),
    )
    triple_full, dense_full, expand_full, shrink_full = (
        gathered[0],
        gathered[1],
        gathered[2],
        gathered[3],
    )
    row_sets = (
        lax.all_gather(hidden, "dp", axis=1, tiled=True),
        lax.all_gather(cotangent, "dp", axis=1, tiled=True),
        lax.all_gather(gathered[4], "dp", axis=0, tiled=True),
        lax.all_gather(gathered[5], "dp", axis=0, tiled=True),
        lax.all_gather(gathered[6], "dp", axis=0, tiled=True),
        lax.all_gather(gathered[7], "dp", axis=0, tiled=True),
        lax.all_gather(gathered[8], "dp", axis=0, tiled=True),
        lax.all_gather(gathered[9], "dp", axis=0, tiled=True),
        lax.all_gather(gathered[10], "dp", axis=0, tiled=True),
        lax.all_gather(gathered[11], "dp", axis=0, tiled=True),
    )
    hidden_both = row_sets[0]
    upstream_low = row_sets[1]
    gain_one, shift_one, pair_full, dense_bias, gain_two, shift_two, expand_bias, shrink_bias = [
        vector.astype(wide_type) for vector in row_sets[2:]
    ]
    inputs_both = hidden_both.astype(wide_type)
    normed_low = layer_norm(inputs_both, gain_one, shift_one).astype(half_type)
    pair_heads = lax.dynamic_slice_in_dim(
        pair_full.reshape(head_total, 2, head_dim), dp_index * local_heads, local_heads, 0
    )
    triple_bias = jnp.stack(
        [pair_heads[:, 0], jnp.zeros_like(pair_heads[:, 0]), pair_heads[:, 1]], 0
    )
    projected = jnp.einsum(
        "mstd,dhce->cmshte", normed_low, triple_full, preferred_element_type=wide_type
    )
    projected = projected + triple_bias[:, None, None, :, None, :]
    project_low = projected.astype(half_type).reshape(3, seq_count, pair_local, seq_rows, head_dim)
    pair_rows = lax.all_to_all(project_low, "seq", split_axis=1, concat_axis=3, tiled=True)[:, 0]
    query_all, key_all, value_all = (pair_rows[0], pair_rows[1], pair_rows[2])
    pair_index = seq_index * pair_local + jnp.arange(pair_local, dtype=jnp.int32)
    head_index = dp_index * local_heads + pair_index % local_heads
    sequence_index = pair_index // local_heads
    slopes = jnp.power(jnp.float32(2.0), -8.0 * (head_index.astype(wide_type) + 1.0) / head_total)
    prefix_flat = prefix_lengths.reshape(-1)
    prefix_slots = jnp.arange(prefix_flat.shape[0], dtype=jnp.int32)
    prefixes = jnp.sum(
        jnp.where(prefix_slots[None, :] == sequence_index[:, None], prefix_flat[None, :], 0), 1
    )

    def block_scores(pair_item, first_row):
        query_block = lax.dynamic_slice_in_dim(
            lax.dynamic_index_in_dim(query_all, pair_item, 0, False), first_row, block_rows, 0
        )
        keys_item = lax.dynamic_index_in_dim(key_all, pair_item, 0, False)
        head_slope = lax.dynamic_index_in_dim(slopes, pair_item, 0, False)
        prefix = lax.dynamic_index_in_dim(prefixes, pair_item, 0, False)
        query_pos = first_row + jnp.arange(block_rows, dtype=jnp.int32)
        raw_scores = (
            jnp.einsum("qe,ke->qk", query_block, keys_item, preferred_element_type=wide_type)
            * score_scale
        )
        distance = jnp.abs(query_pos[:, None] - key_pos[None, :]).astype(wide_type)
        raw_scores = raw_scores - head_slope * distance
        allowed = (key_pos[None, :] <= query_pos[:, None]) | (key_pos[None, :] < prefix)
        return (query_block, jnp.where(allowed, raw_scores, jnp.float32(-1e30)))

    def forward_block(flat_index):
        pair_item = flat_index // block_count
        first_row = flat_index % block_count * block_rows
        _, scores = block_scores(pair_item, first_row)
        row_max = jnp.max(scores, -1, keepdims=True)
        powers = jnp.exp(scores - row_max)
        row_total = jnp.sum(powers, -1, keepdims=True)
        probs_low = (powers / row_total).astype(half_type)
        values_item = lax.dynamic_index_in_dim(value_all, pair_item, 0, False)
        mixed = jnp.dot(probs_low, values_item, preferred_element_type=wide_type).astype(half_type)
        return (mixed, (row_max + jnp.log(row_total))[:, 0])

    mixed_blocks, log_blocks = lax.map(
        forward_block, jnp.arange(pair_local * block_count, dtype=jnp.int32)
    )
    mixed_pairs = mixed_blocks.reshape(pair_local, seq_count, seq_rows, head_dim)
    log_totals = log_blocks.reshape(pair_local, seq_length)
    mixed_home = lax.all_to_all(mixed_pairs, "seq", split_axis=1, concat_axis=0, tiled=True)
    mixed_tokens = jnp.transpose(
        mixed_home.reshape(micro_count, group_count, local_heads, seq_rows, head_dim),
        (0, 1, 3, 2, 4),
    ).reshape(micro_count, group_count, seq_rows, local_heads * head_dim)
    dense_part = jnp.einsum(
        "mstk,kf->mstf", mixed_tokens, dense_full, preferred_element_type=wide_type
    )
    attention_sum = lax.psum(dense_part.astype(jnp.bfloat16), "dp").astype(jnp.float32)
    middle = inputs_both + attention_sum + dense_bias
    gain_rows_two = jnp.broadcast_to(gain_two[None, :], (group_count, model_width))
    shift_rows_two = jnp.broadcast_to(shift_two[None, :], (group_count, model_width))
    normed_two, norm_two_pull = jax.vjp(split_norm, middle, gain_rows_two, shift_rows_two)
    normed_two_low = normed_two.astype(half_type)
    unit_bias = lax.dynamic_slice_in_dim(expand_bias, dp_index * unit_local, unit_local, 0)
    hidden_pre = (
        jnp.einsum("mstd,df->mstf", normed_two_low, expand_full, preferred_element_type=wide_type)
        + unit_bias
    )
    activated_value, gelu_pull = jax.vjp(gelu_tanh, hidden_pre)
    activated_low = activated_value.astype(half_type)
    feed_part = jnp.einsum(
        "mstf,fd->mstd", activated_low, shrink_full, preferred_element_type=wide_type
    )
    feed_sum = lax.psum_scatter(
        feed_part.astype(jnp.bfloat16), "dp", scatter_dimension=1, tiled=True
    ).astype(jnp.float32)
    middle_own = lax.dynamic_slice_in_dim(middle, dp_index, 1, 1)
    layer_output = (middle_own + feed_sum + shrink_bias).astype(half_type)
    triple_back, dense_back, expand_back, shrink_back = (
        lax.all_gather(triple_weight, "seq", axis=0, tiled=True),
        lax.all_gather(dense_weight, "seq", axis=0, tiled=True),
        lax.all_gather(expand_weight, "seq", axis=0, tiled=True),
        lax.all_gather(shrink_weight, "seq", axis=0, tiled=True),
    )
    grad_act = jnp.einsum(
        "mstd,fd->mstf", upstream_low, shrink_back, preferred_element_type=wide_type
    )
    grad_pre_low = gelu_pull(grad_act)[0].astype(half_type)
    norm_two_part = jnp.einsum(
        "mstf,df->mstd", grad_pre_low, expand_back, preferred_element_type=wide_type
    )
    grad_normed_two = lax.psum(norm_two_part.astype(jnp.bfloat16), "dp").astype(jnp.float32)
    grad_middle_norm, grad_gain_rows_two, grad_shift_rows_two = norm_two_pull(grad_normed_two)
    grad_middle = upstream_low.astype(wide_type) + grad_middle_norm
    grad_branch_low = grad_middle.astype(half_type)
    go_pairs = jnp.einsum(
        "mstf,hef->mshte",
        grad_branch_low,
        dense_back.reshape(local_heads, head_dim, model_width),
        preferred_element_type=wide_type,
    ).astype(half_type)
    go_pairs = go_pairs.reshape(seq_count, pair_local, seq_rows, head_dim)
    grad_mixed_pairs = lax.all_to_all(go_pairs, "seq", split_axis=0, concat_axis=2, tiled=True)[0]

    def backward_item(pair_item):
        keys_item = lax.dynamic_index_in_dim(key_all, pair_item, 0, False)
        values_item = lax.dynamic_index_in_dim(value_all, pair_item, 0, False)
        grad_mixed_item = lax.dynamic_index_in_dim(grad_mixed_pairs, pair_item, 0, False)
        totals_item = lax.dynamic_index_in_dim(log_totals, pair_item, 0, False)

        def backward_block(running, block_index):
            key_grad, value_grad = running
            first_row = block_index * block_rows
            query_block, scores = block_scores(pair_item, first_row)
            soft_probs = jnp.exp(
                scores - lax.dynamic_slice_in_dim(totals_item, first_row, block_rows, 0)[:, None]
            )
            grad_block = lax.dynamic_slice_in_dim(grad_mixed_item, first_row, block_rows, 0)
            grad_probs = jnp.einsum(
                "qe,ke->qk", grad_block, values_item, preferred_element_type=wide_type
            )
            row_inner = jnp.sum(grad_probs * soft_probs, -1, keepdims=True)
            grad_scores_low = (soft_probs * (grad_probs - row_inner)).astype(half_type)
            query_grad = (
                jnp.dot(grad_scores_low, keys_item, preferred_element_type=wide_type) * score_scale
            )
            key_grad = (
                key_grad
                + jnp.einsum(
                    "qk,qe->ke", grad_scores_low, query_block, preferred_element_type=wide_type
                )
                * score_scale
            )
            value_grad = value_grad + jnp.einsum(
                "qk,qe->ke",
                soft_probs.astype(half_type),
                grad_block,
                preferred_element_type=wide_type,
            )
            return ((key_grad, value_grad), query_grad)

        zero_rows = jnp.zeros((seq_length, head_dim), wide_type)
        (key_grad, value_grad), query_grads = lax.scan(
            backward_block, (zero_rows, zero_rows), jnp.arange(block_count, dtype=jnp.int32)
        )
        return jnp.stack(
            [query_grads.reshape(seq_length, head_dim), key_grad, value_grad], 0
        ).astype(half_type)

    grad_pairs = lax.map(backward_item, jnp.arange(pair_local, dtype=jnp.int32))
    grad_split = grad_pairs.reshape(pair_local, 3, seq_count, seq_rows, head_dim)
    grad_home = lax.all_to_all(grad_split, "seq", split_axis=2, concat_axis=0, tiled=True)
    grad_project_low = jnp.transpose(
        grad_home.reshape(micro_count, group_count, local_heads, 3, seq_rows, head_dim),
        (0, 1, 4, 2, 3, 5),
    ).reshape(micro_count, group_count, seq_rows, project_width)
    norm_one_part = jnp.einsum(
        "mstc,dc->mstd",
        grad_project_low,
        triple_back.reshape(model_width, project_width),
        preferred_element_type=wide_type,
    )
    grad_normed_one = lax.psum_scatter(
        norm_one_part.astype(jnp.bfloat16), "dp", scatter_dimension=1, tiled=True
    ).astype(jnp.float32)
    inputs_own = hidden.astype(wide_type)
    grad_inputs_norm, grad_gain_one, grad_shift_one = jax.vjp(
        layer_norm, inputs_own, gain_one, shift_one
    )[1](grad_normed_one)
    grad_middle_own = lax.dynamic_slice_in_dim(grad_middle, dp_index, 1, 1)
    hidden_grad = (grad_middle_own + grad_inputs_norm).astype(half_type)
    head_sums = jnp.sum(
        grad_project_low.reshape(micro_count, group_count, seq_rows, local_heads, 3, head_dim),
        (0, 1, 2),
        dtype=wide_type,
    )
    pair_grad = place_half(jnp.stack([head_sums[:, 0], head_sums[:, 2]], 1), dp_index, group_count)
    unit_grad = place_half(jnp.sum(grad_pre_low, (0, 1, 2), dtype=wide_type), dp_index, group_count)
    dense_shift_term = jnp.sum(
        lax.dynamic_slice_in_dim(grad_branch_low, dp_index, 1, 1), (0, 1, 2), dtype=wide_type
    )
    shrink_shift_term = jnp.sum(cotangent, (0, 1, 2), dtype=wide_type)
    gain_two_term = lax.dynamic_index_in_dim(grad_gain_rows_two, dp_index, 0, False)
    shift_two_term = lax.dynamic_index_in_dim(grad_shift_rows_two, dp_index, 0, False)
    vector_sums = (
        lax.psum_scatter(grad_gain_one, ("dp", "seq"), scatter_dimension=0, tiled=True),
        lax.psum_scatter(grad_shift_one, ("dp", "seq"), scatter_dimension=0, tiled=True),
        lax.psum_scatter(pair_grad, ("dp", "seq"), scatter_dimension=0, tiled=True),
        lax.psum_scatter(dense_shift_term, ("dp", "seq"), scatter_dimension=0, tiled=True),
        lax.psum_scatter(gain_two_term, ("dp", "seq"), scatter_dimension=0, tiled=True),
        lax.psum_scatter(shift_two_term, ("dp", "seq"), scatter_dimension=0, tiled=True),
        lax.psum_scatter(unit_grad, ("dp", "seq"), scatter_dimension=0, tiled=True),
        lax.psum_scatter(shrink_shift_term, ("dp", "seq"), scatter_dimension=0, tiled=True),
    )
    normed_flat = normed_low.reshape(token_total, model_width)
    project_flat = grad_project_low.reshape(token_total, project_width)
    normed_two_flat = normed_two_low.reshape(token_total, model_width)
    pre_flat = grad_pre_low.reshape(token_total, unit_local)
    column_sums = lax.psum_scatter(
        jnp.concatenate(
            [
                jnp.einsum(
                    "tr,tc->rc", normed_flat, project_flat, preferred_element_type=wide_type
                ),
                jnp.einsum(
                    "tr,tc->rc", normed_two_flat, pre_flat, preferred_element_type=wide_type
                ),
            ],
            1,
        ),
        "seq",
        scatter_dimension=0,
        tiled=True,
    )
    triple_grad = column_sums[:, :project_width].reshape(
        model_width // seq_count, local_heads, 3, head_dim
    )
    expand_grad = column_sums[:, project_width:]
    dense_rows = dense_weight.shape[0]
    shrink_rows = shrink_weight.shape[0]
    row_block = dense_rows + shrink_rows
    mixed_flat = mixed_tokens.reshape(token_total, local_heads * head_dim)
    branch_flat = grad_branch_low.reshape(token_total, model_width)
    active_flat = activated_low.reshape(token_total, unit_local)
    upstream_flat = upstream_low.reshape(token_total, model_width)
    block_number = row_block * lax.axis_size("seq") // row_block
    dense_term = jnp.einsum("tr,td->rd", mixed_flat, branch_flat, preferred_element_type=wide_type)
    shrink_term = jnp.einsum(
        "tr,td->rd", active_flat, upstream_flat, preferred_element_type=wide_type
    )
    row_sums = lax.psum_scatter(
        jnp.concatenate(
            [
                dense_term.reshape(block_number, dense_rows, model_width),
                shrink_term.reshape(block_number, shrink_rows, model_width),
            ],
            1,
        ).reshape(row_block * lax.axis_size("seq"), model_width),
        "seq",
        scatter_dimension=0,
        tiled=True,
    )
    dense_grad = row_sums[:dense_rows]
    shrink_grad = row_sums[dense_rows:]
    return (
        layer_output,
        hidden_grad,
        vector_sums[0],
        vector_sums[1],
        triple_grad,
        vector_sums[2],
        dense_grad,
        vector_sums[3],
        vector_sums[4],
        vector_sums[5],
        expand_grad,
        vector_sums[6],
        shrink_grad,
        vector_sums[7],
    )


CHUNKS = 4
LOG2E = 1.4426950408889634
MESH = pl.DeviceIdType.MESH


def remote(src, dst, send, recv, peer):
    return pltpu.make_async_remote_copy(
        src_ref=src,
        dst_ref=dst,
        send_sem=send,
        recv_sem=recv,
        device_id=peer,
        device_id_type=MESH,
    )


def greet(peers):
    barrier = pltpu.get_barrier_semaphore()
    for peer in peers:
        pl.semaphore_signal(barrier, inc=1, device_id=peer, device_id_type=MESH)
    pl.semaphore_wait(barrier, len(peers))


class Corner:
    def __init__(self):
        self.c = lax.axis_index("dp")
        self.y = lax.axis_index("y")
        self.x = lax.axis_index("x")
        self.ax = self.x + (1 - self.c) * (1 - 2 * self.x)
        self.ay = self.y + self.c * (1 - 2 * self.y)
        self.bx = self.x + self.c * (1 - 2 * self.x)
        self.by = self.y + (1 - self.c) * (1 - 2 * self.y)
        self.dx = 1 - self.x
        self.dy = 1 - self.y
        self.peer_a = {"y": self.ay, "x": self.ax}
        self.peer_b = {"y": self.by, "x": self.bx}
        self.sibling = {"dp": 1 - self.c}

    def slots(self, core):
        return [
            (core * 2 + y) * 2 + x
            for y, x in (
                (self.dy, self.dx),
                (self.by, self.bx),
                (self.ay, self.ax),
                (self.y, self.x),
            )
        ]


def gather_kernel(deep, *refs):
    if deep:
        rows_ref, deep_ref, all_ref, moved_ref, local_sem, send, recv, deep_send, deep_recv = refs
    else:
        rows_ref, all_ref, local_sem, send, recv = refs
    at = Corner()
    slot_d, slot_b, slot_a, me = at.slots(at.c)
    step = rows_ref.shape[0] // CHUNKS
    peers = [at.peer_a, at.peer_b, at.sibling]
    sent, moves = [], []
    if deep:
        z = lax.axis_index("z")
        plane_at = [lax.rem(z + i, 4) for i in range(4)]
        peers += [{"z": plane_at[i]} for i in range(1, 4)]
    greet(peers)
    locals_ = [pltpu.make_async_copy(rows_ref, all_ref.at[me], local_sem.at[0])]
    if deep:
        locals_.append(pltpu.make_async_copy(deep_ref.at[z], moved_ref.at[z], local_sem.at[1]))
    for one in locals_:
        one.start()

    def copy(kind, k, slot, peer):
        part = pl.ds(k * step, step)
        src = rows_ref.at[part] if kind < 3 else all_ref.at[slot, part]
        return remote(src, all_ref.at[slot, part], send.at[kind, k], recv.at[kind, k], peer)

    def arrived(kind, k, slot, peer):
        part = pl.ds(k * step, step)
        block = all_ref.at[slot, part]
        remote(block, block, send.at[kind, k], recv.at[kind, k], peer).wait_recv()

    def start(kind, k, slot, peer):
        one = copy(kind, k, slot, peer)
        one.start()
        sent.append(one)

    for i in range(1, 4) if deep else ():
        sems = deep_send.at[i - 1], deep_recv.at[i - 1]
        one = remote(deep_ref.at[plane_at[i]], moved_ref.at[z], *sems, {"z": plane_at[i]})
        one.start()
        sent.append(one)
        landing = moved_ref.at[plane_at[4 - i]]
        moves.append(remote(landing, landing, *sems, {"z": plane_at[i]}))
    for k in range(CHUNKS):
        start(0, k, me, at.peer_a)
        start(1, k, me, at.peer_b)
    for k in range(CHUNKS):
        start(2, k, me, at.sibling)
    for k in range(CHUNKS):
        arrived(0, k, slot_a, at.peer_a)
        start(3, k, slot_a, at.peer_b)
        start(4, k, slot_a, at.sibling)
    for k in range(CHUNKS):
        arrived(1, k, slot_b, at.peer_b)
        start(5, k, slot_b, at.sibling)
    for k in range(CHUNKS):
        arrived(3, k, slot_d, at.peer_b)
        start(6, k, slot_d, at.sibling)
    other_d, other_b, other_a, other_me = at.slots(1 - at.c)
    for k in range(CHUNKS):
        arrived(2, k, other_me, at.sibling)
        arrived(4, k, other_b, at.sibling)
        arrived(5, k, other_a, at.sibling)
        arrived(6, k, other_d, at.sibling)
    for one in moves:
        one.wait_recv()
    for one in sent:
        one.wait_send()
    for one in locals_:
        one.wait()


def gather_tokens(rows, deep=None):
    count, width = rows.shape
    operands = [rows]
    shapes = [jax.ShapeDtypeStruct((8, count, width), rows.dtype)]
    scratch = [
        pltpu.SemaphoreType.DMA((2,)),
        pltpu.SemaphoreType.DMA((7, CHUNKS)),
        pltpu.SemaphoreType.DMA((7, CHUNKS)),
    ]
    if deep is not None:
        operands.append(deep)
        shapes.append(jax.ShapeDtypeStruct(deep.shape, deep.dtype))
        scratch += [pltpu.SemaphoreType.DMA((3,)), pltpu.SemaphoreType.DMA((3,))]
    all_rows, *moved = pl.pallas_call(
        functools.partial(gather_kernel, deep is not None),
        out_shape=shapes,
        in_specs=[pl.BlockSpec(memory_space=pl.ANY)] * len(operands),
        out_specs=[pl.BlockSpec(memory_space=pl.ANY)] * len(shapes),
        scratch_shapes=scratch,
        compiler_params=pltpu.CompilerParams(
            collective_id=1 if deep is None else 6, has_side_effects=True
        ),
        cost_estimate=pl.CostEstimate(
            flops=0, bytes_accessed=16 * count * width * 4, transcendentals=0
        ),
        name="gather_tokens",
    )(*operands)
    return (all_rows.reshape(8 * count, width), *moved)


def after(value, *others):
    return lax.optimization_barrier((value, *others))[0]


def scatter_kernel(turned, term, left_ref, right_ref, *refs):
    if term:
        rows_ref, grads_ref, own_ref, term_ref, *refs = refs
    else:
        own_ref, *refs = refs
    part_ref, from_core, from_b, from_a, send, recv = refs
    at = Corner()
    slot_d, slot_b, slot_a, me = at.slots(at.c)
    other_d, other_b, other_a, other_me = at.slots(1 - at.c)
    rows, width = own_ref.shape
    step = rows // CHUNKS
    wide = jnp.float32
    greet([at.peer_a, at.peer_b, at.sibling])
    sent = []

    def start(kind, k, src, dst, peer):
        one = remote(src, dst, send.at[kind, k], recv.at[kind, k], peer)
        one.start()
        sent.append(one)

    def arrived(kind, k, dst, peer):
        remote(dst, dst, send.at[kind, k], recv.at[kind, k], peer).wait_recv()

    tile = min(512, width)

    def multiply(slot, part=slice(None)):
        def columns(t, carry):
            cols = pl.ds(pl.multiple_of(t * tile, tile), tile)
            right = right_ref[cols] if turned else right_ref[:, cols]
            product = lax.dot_general(
                left_ref[slot, part],
                right,
                (((1,), (1 if turned else 0,)), ((), ())),
                preferred_element_type=wide,
            )
            part_ref[slot, part, cols] = product.astype(part_ref.dtype)
            return carry

        lax.fori_loop(0, width // tile, columns, 0)

    def multiply_term(first, last):
        if not term:
            return
        lanes = min(256, rows_ref.shape[1] // 8)

        def features(t, carry):
            cols = pl.ds(pl.multiple_of(t * lanes, lanes), lanes)
            product = lax.dot_general(
                rows_ref[:, cols],
                grads_ref[...],
                (((0,), (0,)), ((), ())),
                preferred_element_type=wide,
            )
            term_ref[cols] = product.astype(term_ref.dtype)
            return carry

        count = rows_ref.shape[1] // lanes
        lax.fori_loop(count * first // 8, count * last // 8, features, 0)

    def share(q, slot, chunks):
        for k in chunks:
            part = pl.ds(k * step, step)
            start(q, k, part_ref.at[slot, part], from_core.at[q, part], at.sibling)

    everything = range(CHUNKS)

    def to_b(q, slot, chunks):
        for k in chunks:
            part = pl.ds(k * step, step)
            arrived(q, k, from_core.at[q, part], at.sibling)
            total = part_ref[slot, part].astype(wide) + from_core[q, part].astype(wide)
            from_core[q, part] = total.astype(from_core.dtype)
            start(4 + q, k, from_core.at[q, part], from_b.at[q, part], at.peer_b)

    for h in range(2):
        multiply(other_d, slice(h * rows // 2, (h + 1) * rows // 2))
        share(0, other_d, everything[h * CHUNKS // 2 : (h + 1) * CHUNKS // 2])
    for h in range(2):
        multiply(slot_d, slice(h * rows // 2, (h + 1) * rows // 2))
        to_b(0, slot_d, everything[h * CHUNKS // 2 : (h + 1) * CHUNKS // 2])
    multiply(other_a)
    share(1, other_a, everything)
    multiply(slot_b)
    to_b(1, slot_b, everything)
    multiply(other_b)
    share(2, other_b, everything)
    multiply(slot_a)
    multiply_term(0, 2)
    for k in range(CHUNKS):
        part = pl.ds(k * step, step)
        arrived(2, k, from_core.at[2, part], at.sibling)
        arrived(4, k, from_b.at[0, part], at.peer_b)
        total = part_ref[slot_a, part].astype(wide) + from_core[2, part].astype(wide)
        total = total + from_b[0, part].astype(wide)
        from_core[2, part] = total.astype(from_core.dtype)
        start(6, k, from_core.at[2, part], from_a.at[part], at.peer_a)
    multiply(other_me)
    share(3, other_me, everything)
    multiply(me)
    multiply_term(2, 8)
    for k in range(CHUNKS):
        part = pl.ds(k * step, step)
        arrived(3, k, from_core.at[3, part], at.sibling)
        arrived(5, k, from_b.at[1, part], at.peer_b)
        arrived(6, k, from_a.at[part], at.peer_a)
        total = part_ref[me, part].astype(wide) + from_core[3, part].astype(wide)
        total = total + from_b[1, part].astype(wide)
        own_ref[part] = total + from_a[part].astype(wide)
    for one in sent:
        one.wait_send()


def scatter_tokens(identity, left, right, turned=False, term=()):
    count, depth = left.shape[0] // 8, left.shape[1]
    width = right.shape[0] if turned else right.shape[1]
    half = left.dtype
    shapes = [jax.ShapeDtypeStruct((count, width), jnp.float32)]
    if term:
        shapes.append(jax.ShapeDtypeStruct((term[0].shape[1], term[1].shape[1]), half))
    vmem = pl.BlockSpec(memory_space=pltpu.VMEM)
    return pl.pallas_call(
        functools.partial(scatter_kernel, turned, bool(term)),
        out_shape=shapes,
        in_specs=[vmem] * (2 + len(term)),
        out_specs=[vmem] * len(shapes),
        scratch_shapes=[
            pltpu.VMEM((8, count, width), half),
            pltpu.VMEM((4, count, width), half),
            pltpu.VMEM((2, count, width), half),
            pltpu.VMEM((count, width), half),
            pltpu.SemaphoreType.DMA((7, CHUNKS)),
            pltpu.SemaphoreType.DMA((7, CHUNKS)),
        ],
        compiler_params=pltpu.CompilerParams(
            collective_id=identity, has_side_effects=True, vmem_limit_bytes=58 * 2**20
        ),
        cost_estimate=pl.CostEstimate(
            flops=2 * left.size * width, bytes_accessed=64 * count * width, transcendentals=0
        ),
        name="scatter_tokens",
    )(left.reshape(8, count, depth), right, *term)


def exchange_kernel(last, *refs):
    refs = list(refs)
    take = lambda n: [refs.pop(0) for _ in range(n)]
    deep_in, turn_in, triple_in, expand_in, vec_in = take(5)
    deep_out, turn_out, triple_out, expand_out, vec_out = take(5)
    if last:
        triple_columns, expand_columns = triple_out, expand_out
        triple_out, expand_out, near, far, here = take(5)
    send, recv, local_sem = take(3)
    c, z = lax.axis_index("dp"), lax.axis_index("z")
    y, x = lax.axis_index("y"), lax.axis_index("x")
    place = y * 2 + x
    rank = c * 4 + place

    def deep(i):
        return lax.rem(z + i, 4)

    def flat(i):
        return lax.rem(place + i, 4)

    def wide(i):
        return lax.rem(rank + i, 8)

    def deep_peer(i):
        return {"z": deep(i)}

    def flat_peer(i):
        return {"y": flat(i) // 2, "x": lax.rem(flat(i), 2)}

    def wide_peer(i):
        return {
            "dp": wide(i) // 4,
            "y": lax.rem(wide(i), 4) // 2,
            "x": lax.rem(wide(i), 2),
        }

    low = lax.rem(z, 2)
    turn_from = {"z": z - low + 1 - x, "x": low}
    turn_to = {"z": z - low + x, "x": 1 - low}
    if last:
        turn_from, turn_to = turn_to, turn_from
    others = range(1, 4)
    greet([deep_peer(i) for i in others] + [wide_peer(i) for i in range(1, 8)])
    sent, waits, kept = [], [], []
    count = [0]

    def post(src, dst, peer, landing):
        k = count[0]
        count[0] += 1
        one = remote(src, dst, send.at[k], recv.at[k], peer)
        one.start()
        sent.append(one)
        return remote(landing, landing, send.at[k], recv.at[k], peer)

    def keep(src, dst):
        one = pltpu.make_async_copy(src, dst, local_sem.at[len(kept)])
        one.start()
        kept.append(one)

    def expand_parts(block):
        if last:
            return [(expand_in.at[block], expand_out.at[place])]
        step = expand_out.shape[2] // 4
        return [
            (
                expand_in.at[:, pl.ds(pl.multiple_of((i * 4 + block) * step, step), step)],
                expand_out.at[place, :, pl.ds(i * step, step)],
            )
            for i in range(4)
        ]

    stage, late = [], []
    for i in others:
        landing = triple_out.at[flat(4 - i)]
        waits.append(post(triple_in.at[flat(i)], triple_out.at[place], flat_peer(i), landing))
    for i in others:
        late.append(post(deep_in.at[deep(i)], deep_out.at[z], deep_peer(i), deep_out.at[deep(4 - i)]))
    for i in range(1, 8):
        if last:
            landing = near.at[wide(8 - i)]
            stage.append(post(vec_in.at[wide(i)], near.at[rank], wide_peer(i), landing))
        else:
            landing = vec_out.at[z, wide(8 - i)]
            stage.append(post(vec_in, vec_out.at[z, rank], wide_peer(i), landing))
    late.append(post(turn_in, turn_out, turn_to, turn_out))
    for i in others:
        for n, (src, dst) in enumerate(expand_parts(flat(i))):
            landing = expand_out.at[flat(4 - i)]
            if not last:
                step = expand_out.shape[2] // 4
                landing = landing.at[:, pl.ds(n * step, step)]
            waits.append(post(src, dst, flat_peer(i), landing))
    keep(deep_in.at[z], deep_out.at[z])
    keep(triple_in.at[place], triple_out.at[place])
    for src, dst in expand_parts(place):
        keep(src, dst)
    if last:
        own = pltpu.make_async_copy(vec_in.at[rank], near.at[rank], local_sem.at[len(kept)])
        own.start()
        for one in stage:
            one.wait_recv()
        own.wait()
        here[...] = jnp.sum(near[...], 0)
        stage = []
        for i in others:
            landing = far.at[deep(4 - i)]
            stage.append(post(here.at[deep(i)], far.at[z], deep_peer(i), landing))
        far[z] = here[z]
        for one in stage:
            one.wait_recv()
        vec_out[...] = jnp.sum(far[...], 0)
    else:
        own = pltpu.make_async_copy(vec_in, vec_out.at[z, rank], local_sem.at[len(kept)])
        own.start()
        for one in stage:
            one.wait_recv()
        own.wait()
        for i in others:
            landing = vec_out.at[deep(4 - i)]
            late.append(post(vec_out.at[z], vec_out.at[z], deep_peer(i), landing))
    for one in waits:
        one.wait_recv()
    for one in kept:
        one.wait()
    if last:
        for (steps, order), blocks, columns in zip(
            last, (triple_out, expand_out), (triple_columns, expand_columns)
        ):
            step = blocks.shape[2] // steps
            for i in range(steps):
                for p in range(4):
                    first = (i * 4 + order[p]) * step
                    columns[:, first : first + step] = blocks[p, :, i * step : (i + 1) * step]
    for one in late:
        one.wait_recv()
    for one in sent:
        one.wait_send()


def exchange(identity, deep, turned, triple, expand, vector, last=None):
    half = expand.dtype
    operands = [deep, turned, triple, expand, vector]
    shapes = [jax.ShapeDtypeStruct(a.shape, a.dtype) for a in (deep, turned)]
    hbm, vmem = pl.BlockSpec(memory_space=pl.ANY), pl.BlockSpec(memory_space=pltpu.VMEM)
    scratch = []
    if last:
        tile = vector.shape[2:]
        shapes += [jax.ShapeDtypeStruct((a.shape[1], 4 * a.shape[2]), half) for a in (triple, expand)]
        shapes.append(jax.ShapeDtypeStruct(tile, vector.dtype))
        scratch = [pltpu.VMEM(triple.shape, half), pltpu.VMEM(expand.shape, half)]
        scratch += [pltpu.VMEM(n + tile, vector.dtype) for n in ((8, 4), (4,), (4,))]
        places = [hbm, hbm, vmem, vmem, vmem]
    else:
        rows, columns = expand.shape
        shapes.append(jax.ShapeDtypeStruct(triple.shape, half))
        shapes.append(jax.ShapeDtypeStruct((4, rows, columns // 4), half))
        shapes.append(jax.ShapeDtypeStruct((4, 8) + vector.shape, vector.dtype))
        places = [hbm] * 5
    copies = 3 + 3 + 7 + 1 + 3 * (1 if last else 4) + 3
    moved = sum(a.size * a.dtype.itemsize for a in operands)
    return pl.pallas_call(
        functools.partial(exchange_kernel, last),
        out_shape=shapes,
        in_specs=[hbm] * 5,
        out_specs=places,
        scratch_shapes=scratch
        + [
            pltpu.SemaphoreType.DMA((copies,)),
            pltpu.SemaphoreType.DMA((copies,)),
            pltpu.SemaphoreType.DMA((8,)),
        ],
        compiler_params=pltpu.CompilerParams(
            collective_id=identity, has_side_effects=True, vmem_limit_bytes=24 * 2**20
        ),
        cost_estimate=pl.CostEstimate(flops=0, bytes_accessed=16 * moved, transcendentals=0),
        name="exchange",
    )(*operands)


def scores_of(item_ref, first, block, slope, prefix, depth, seq_rows):
    length = item_ref.shape[0]
    head_dim = item_ref.shape[1] // 3
    own_rows = depth * seq_rows
    chips = length // own_rows

    def position(index):
        chip = index // own_rows
        rest = index % own_rows
        return ((rest // seq_rows) * chips + chip) * seq_rows + rest % seq_rows

    queries = item_ref[first : first + block, :head_dim]
    keys = item_ref[:, head_dim : 2 * head_dim]
    raw = lax.dot_general(
        keys, queries, (((1,), (1,)), ((), ())), preferred_element_type=jnp.float32
    )
    key_pos = position(lax.broadcasted_iota(jnp.int32, (length, 1), 0))
    query_pos = position(first + lax.broadcasted_iota(jnp.int32, (1, block), 1))
    bound = jnp.where(key_pos < prefix, -1, key_pos)
    distance = jnp.abs(
        query_pos.astype(jnp.float32) - key_pos.astype(jnp.float32)
    )
    scores = raw * (LOG2E / math.sqrt(head_dim)) - (slope * LOG2E) * distance
    return jnp.where(bound <= query_pos, scores, jnp.float32(-1e30))


def forward_kernel(depth, seq_rows, block, prefix_ref, slope_ref, item_ref, mixed_ref, total_ref):
    prefix = prefix_ref[pl.program_id(0)]
    slope = slope_ref[pl.program_id(1)]
    length = item_ref.shape[0]
    head_dim = item_ref.shape[1] // 3
    for first in range(0, length, block):
        scores = scores_of(item_ref, first, block, slope, prefix, depth, seq_rows)
        top = jnp.max(scores, 0, keepdims=True)
        powers = jnp.exp2(scores - top)
        total = jnp.sum(powers, 0, keepdims=True)
        probs = (powers * (1.0 / total)).astype(jnp.bfloat16)
        mixed = lax.dot_general(
            probs,
            item_ref[:, 2 * head_dim :],
            (((0,), (0,)), ((), ())),
            preferred_element_type=jnp.float32,
        )
        mixed_ref[first : first + block, :] = mixed.astype(mixed_ref.dtype)
        total_ref[0, :, first : first + block] = top + jnp.log2(total)


def attend_forward(projected, slopes, prefixes, own_heads, head_dim, depth, seq_rows):
    cores = prefixes.shape[0]
    length = projected.shape[0] // cores
    block = min(256, length)
    scores = cores * own_heads * length * length
    return pl.pallas_call(
        functools.partial(forward_kernel, depth, seq_rows, block),
        grid=(cores, own_heads),
        out_shape=[
            jax.ShapeDtypeStruct((cores * length, own_heads * head_dim), projected.dtype),
            jax.ShapeDtypeStruct((cores * own_heads, 1, length), jnp.float32),
        ],
        in_specs=[
            pl.BlockSpec(memory_space=pltpu.SMEM),
            pl.BlockSpec(memory_space=pltpu.SMEM),
            pl.BlockSpec((length, 3 * head_dim), lambda s, h: (s, h)),
        ],
        out_specs=[
            pl.BlockSpec((length, head_dim), lambda s, h: (s, h)),
            pl.BlockSpec((1, 1, length), lambda s, h: (s * own_heads + h, 0, 0)),
        ],
        compiler_params=pltpu.CompilerParams(vmem_limit_bytes=48 * 2**20),
        cost_estimate=pl.CostEstimate(
            flops=4 * scores * head_dim,
            bytes_accessed=2 * projected.size * 2,
            transcendentals=scores,
        ),
        name="attend_forward",
    )(prefixes, slopes, projected)


def backward_kernel(
    depth, seq_rows, block, prefix_ref, slope_ref, item_ref, grad_ref, total_ref, out_ref, key_sum, value_sum
):
    prefix = prefix_ref[pl.program_id(0)]
    slope = slope_ref[pl.program_id(1)]
    length = item_ref.shape[0]
    head_dim = item_ref.shape[1] // 3
    scale = 1.0 / math.sqrt(head_dim)
    half = jnp.bfloat16
    wide = jnp.float32
    for first in range(0, length, block):
        scores = scores_of(item_ref, first, block, slope, prefix, depth, seq_rows)
        probs = jnp.exp2(scores - total_ref[0, :, first : first + block])
        grad = grad_ref[first : first + block, :]
        grad_probs = lax.dot_general(
            item_ref[:, 2 * head_dim :],
            grad,
            (((1,), (1,)), ((), ())),
            preferred_element_type=wide,
        )
        inner = jnp.sum(grad_probs * probs, 0, keepdims=True)
        grad_scores = (probs * (grad_probs - inner)).astype(half)
        key_term = jnp.dot(
            grad_scores, item_ref[first : first + block, :head_dim], preferred_element_type=wide
        )
        value_term = jnp.dot(probs.astype(half), grad, preferred_element_type=wide)
        query_grad = lax.dot_general(
            grad_scores,
            item_ref[:, head_dim : 2 * head_dim],
            (((0,), (0,)), ((), ())),
            preferred_element_type=wide,
        )
        out_ref[first : first + block, :head_dim] = (query_grad * scale).astype(half)
        if first == 0:
            key_sum[...] = key_term
            value_sum[...] = value_term
        else:
            key_sum[...] += key_term
            value_sum[...] += value_term
    out_ref[:, head_dim : 2 * head_dim] = (key_sum[...] * scale).astype(half)
    out_ref[:, 2 * head_dim :] = value_sum[...].astype(half)


def attend_backward(
    projected, grad_mixed, totals, slopes, prefixes, own_heads, head_dim, depth, seq_rows
):
    cores = prefixes.shape[0]
    length = projected.shape[0] // cores
    block = min(256, length)
    scores = cores * own_heads * length * length
    return pl.pallas_call(
        functools.partial(backward_kernel, depth, seq_rows, block),
        grid=(cores, own_heads),
        out_shape=jax.ShapeDtypeStruct(projected.shape, projected.dtype),
        in_specs=[
            pl.BlockSpec(memory_space=pltpu.SMEM),
            pl.BlockSpec(memory_space=pltpu.SMEM),
            pl.BlockSpec((length, 3 * head_dim), lambda s, h: (s, h)),
            pl.BlockSpec((length, head_dim), lambda s, h: (s, h)),
            pl.BlockSpec((1, 1, length), lambda s, h: (s * own_heads + h, 0, 0)),
        ],
        out_specs=pl.BlockSpec((length, 3 * head_dim), lambda s, h: (s, h)),
        scratch_shapes=[
            pltpu.VMEM((length, head_dim), jnp.float32),
            pltpu.VMEM((length, head_dim), jnp.float32),
        ],
        compiler_params=pltpu.CompilerParams(vmem_limit_bytes=48 * 2**20),
        cost_estimate=pl.CostEstimate(
            flops=10 * scores * head_dim,
            bytes_accessed=2 * projected.size * 2,
            transcendentals=scores,
        ),
        name="attend_backward",
    )(prefixes, slopes, projected, grad_mixed, totals)


def planar(
    hidden,
    prefix_lengths,
    cotangent,
    first_gain,
    first_shift,
    triple_weight,
    pair_bias,
    dense_weight,
    dense_shift,
    second_gain,
    second_shift,
    expand_weight,
    expand_shift,
    shrink_weight,
    shrink_shift,
):
    wide = jnp.float32
    half = jnp.bfloat16
    cores = lax.axis_size("dp")
    depth = lax.axis_size("z")
    rows_y = lax.axis_size("y")
    rows_x = lax.axis_size("x")
    plane = rows_y * rows_x
    core = lax.axis_index("dp")
    at_y = lax.axis_index("y")
    at_x = lax.axis_index("x")
    place = at_y * rows_x + at_x
    seq_rows = hidden.shape[2]
    width = hidden.shape[3]
    head_dim = triple_weight.shape[3]
    heads = triple_weight.shape[1]
    own_heads = heads // plane
    own_rows = seq_rows * depth
    units = expand_weight.shape[1]
    own_units = units // plane
    row_block = expand_weight.shape[0]
    shrink_rows = shrink_weight.shape[0]

    pieces = [
        first_gain,
        first_shift,
        dense_shift,
        second_gain,
        second_shift,
        shrink_shift,
        pair_bias,
        expand_shift,
    ]
    piece_total = sum(p.shape[0] for p in pieces)
    lanes = 128
    vector_rows = -(-piece_total // (lanes * 16)) * 16
    vector_tile = jnp.pad(
        jnp.concatenate(pieces), (0, vector_rows * lanes - piece_total)
    ).reshape(vector_rows, lanes)
    triple_blocks = (
        triple_weight.reshape(row_block, own_heads, rows_x, rows_y, 3 * head_dim)[:, :, ::-1]
        .transpose(3, 2, 0, 1, 4)
        .reshape(plane, row_block, own_heads * 3 * head_dim)
    )
    inputs, dense_turned, triple_turned, expand_turned, packed = exchange(
        3, hidden[:, 0], dense_weight, triple_blocks, expand_weight, vector_tile
    )
    packed = (
        packed.reshape(depth, cores, plane, vector_rows * lanes)
        .transpose(1, 0, 2, 3)
        .reshape(-1, vector_rows * lanes)
    )
    vectors = []
    offset = 0
    for piece in pieces:
        vectors.append(packed[:, offset : offset + piece.shape[0]].reshape(-1).astype(wide))
        offset += piece.shape[0]
    gain_one, shift_one, dense_bias, gain_two, shift_two, shrink_bias, pair_full, unit_full = vectors
    pair_heads = pair_full.reshape(cores, own_heads, rows_x, rows_y, 2, head_dim)[
        core, :, 1 - at_x, at_y
    ]
    triple_bias = jnp.stack(
        [pair_heads[:, 0], jnp.zeros_like(pair_heads[:, 0]), pair_heads[:, 1]], 1
    ).reshape(-1)
    unit_bias = unit_full.reshape(cores, depth, plane, shrink_rows)[core, :, place].reshape(-1)

    triple_own = lax.all_gather(
        triple_turned.reshape(-1, triple_turned.shape[2]), "z", axis=0, tiled=True
    )
    inputs = inputs.reshape(own_rows, width).astype(wide)

    normed_own = layer_norm(inputs, gain_one, shift_one).astype(half)
    (normed,) = gather_tokens(normed_own)
    dense_own = lax.all_gather(after(dense_turned, normed), "z", axis=0, tiled=True)
    expand_own = lax.all_gather(
        after(expand_turned, normed).reshape(-1, own_units), "z", axis=0, tiled=True
    )
    projected = (
        jnp.dot(normed, triple_own, preferred_element_type=wide) + triple_bias
    ).astype(half)

    shrink_own = lax.all_gather(after(shrink_weight, projected), "z", axis=0, tiled=True)
    head_index = core * heads + jnp.arange(own_heads) * plane + (1 - at_x) * rows_y + at_y
    slopes = jnp.power(
        jnp.float32(2.0), -8.0 * (head_index.astype(wide) + 1.0) / (heads * cores)
    )
    at_z = lax.axis_index("z")
    prefixes = lax.dynamic_index_in_dim(prefix_lengths, at_z, 0, False)
    mixed, log_totals = attend_forward(
        projected, slopes, prefixes, own_heads, head_dim, depth, seq_rows
    )
    (dense_sum,) = scatter_tokens(2, mixed, dense_own)
    middle = inputs + dense_sum + dense_bias
    normed_two_own, norm_two_pull = jax.vjp(layer_norm, middle, gain_two, shift_two)
    normed_two, upstream = gather_tokens(normed_two_own.astype(half), cotangent[:, 0])
    upstream = upstream.reshape(own_rows, width)
    hidden_pre = jnp.dot(normed_two, expand_own, preferred_element_type=wide) + unit_bias
    (upstream_all,) = gather_tokens(upstream)
    activated, gelu_pull = jax.vjp(gelu_tanh, hidden_pre)
    activated = activated.astype(half)
    shrink_term = jnp.einsum(
        "tu,td->ud", activated, upstream_all, preferred_element_type=wide
    ).astype(half)
    shrink_own = after(shrink_own, shrink_term)
    grad_act = jnp.einsum("tf,uf->tu", upstream_all, shrink_own, preferred_element_type=wide)
    grad_pre = gelu_pull(grad_act)[0].astype(half)
    shrink_grad = lax.psum_scatter(shrink_term, "z", scatter_dimension=0, tiled=True)
    feed_sum, expand_term = scatter_tokens(
        8, after(activated, shrink_term), shrink_own, term=(normed_two, grad_pre)
    )
    expand_turned = lax.psum_scatter(expand_term, "z", scatter_dimension=0, tiled=True)
    layer_output = (middle + feed_sum + shrink_bias).astype(half)

    (norm_two_sum,) = scatter_tokens(9, after(grad_pre, feed_sum), expand_own, True)
    grad_norm_two, gain_two_term, shift_two_term = norm_two_pull(norm_two_sum)
    grad_middle = upstream.astype(wide) + grad_norm_two
    branch_own = grad_middle.astype(half)
    branch, layer_output = gather_tokens(branch_own, layer_output.reshape(depth, seq_rows, width))

    grad_mixed = jnp.einsum("tf,ef->te", branch, dense_own, preferred_element_type=wide).astype(
        half
    )
    dense_term = jnp.einsum("te,tf->ef", mixed, branch, preferred_element_type=wide).astype(half)
    dense_turned = lax.psum_scatter(dense_term, "z", scatter_dimension=0, tiled=True)
    grad_project = attend_backward(
        projected,
        after(grad_mixed, dense_term),
        log_totals,
        slopes,
        prefixes,
        own_heads,
        head_dim,
        depth,
        seq_rows,
    )
    triple_term = jnp.einsum(
        "td,tc->dc", normed, grad_project, preferred_element_type=wide
    ).astype(half)
    triple_turned = lax.psum_scatter(triple_term, "z", scatter_dimension=0, tiled=True)
    (norm_one_sum,) = scatter_tokens(10, after(grad_project, triple_term), triple_own, True)
    grad_norm_one, gain_one_term, shift_one_term = jax.vjp(
        layer_norm, inputs, gain_one, shift_one
    )[1](norm_one_sum)
    hidden_grad = (grad_middle + grad_norm_one).astype(half)
    head_sums = jnp.sum(grad_project, 0, dtype=wide).reshape(own_heads, 3, head_dim)
    pair_term = jnp.stack([head_sums[:, 0], head_sums[:, 2]], 1)
    pair_zero = jnp.zeros((cores, own_heads, rows_x, rows_y, 2, head_dim), wide)
    pair_wide = lax.dynamic_update_slice(
        pair_zero, pair_term[None, :, None, None], (core, 0, 1 - at_x, at_y, 0, 0)
    ).reshape(-1)
    unit_term = jnp.sum(grad_pre, 0, dtype=wide).reshape(1, depth, 1, shrink_rows)
    unit_wide = lax.dynamic_update_slice(
        jnp.zeros((cores, depth, plane, shrink_rows), wide), unit_term, (core, 0, place, 0)
    ).reshape(-1)
    terms = [
        gain_one_term,
        shift_one_term,
        jnp.sum(branch_own, 0, dtype=wide),
        gain_two_term,
        shift_two_term,
        jnp.sum(upstream, 0, dtype=wide),
        pair_wide,
        unit_wide,
    ]
    devices = cores * depth * plane
    term_rows = -(-piece_total // (lanes * 8)) * 8
    term_tiles = jnp.pad(
        jnp.concatenate([t.reshape(devices, -1) for t in terms], 1),
        ((0, 0), (0, term_rows * lanes - piece_total)),
    )
    term_tiles = (
        term_tiles.reshape(cores, depth, plane, term_rows, lanes)
        .transpose(0, 2, 1, 3, 4)
        .reshape(cores * plane, depth, term_rows, lanes)
    )
    hidden_grad, dense_grad, triple_grad, expand_grad, summed = exchange(
        4,
        hidden_grad.reshape(depth, seq_rows, width),
        dense_turned,
        triple_turned.reshape(plane, row_block, -1),
        expand_turned.reshape(plane, row_block, own_units),
        term_tiles,
        last=((own_heads, (2, 0, 3, 1)), (depth, (0, 1, 2, 3))),
    )
    layer_output = layer_output[:, None]
    hidden_grad = hidden_grad[:, None]
    triple_grad = triple_grad.astype(wide).reshape(row_block, heads, 3, head_dim)
    summed = summed.reshape(-1)
    vector_grads = []
    offset = 0
    for piece in pieces:
        vector_grads.append(summed[offset : offset + piece.shape[0]])
        offset += piece.shape[0]
    return (
        layer_output,
        hidden_grad,
        vector_grads[0],
        vector_grads[1],
        triple_grad,
        vector_grads[6],
        dense_grad.astype(wide),
        vector_grads[2],
        vector_grads[3],
        vector_grads[4],
        expand_grad.astype(wide),
        vector_grads[7],
        shrink_grad.astype(wide),
        vector_grads[5],
    )


def layer(*args):
    return planar(*args)


def solution(mesh):
    depth = 4
    sides = (2, 2)
    planar_plan = mesh.shape["seq"] == depth * sides[0] * sides[1]
    if planar_plan:
        grid = Mesh(
            mesh.devices.reshape(mesh.shape["dp"], depth, *sides), ("dp", "z", "y", "x")
        )
        seq = ("z", "y", "x")
    else:
        grid = mesh
        seq = ("seq",)
    tokens = P(None, "dp", seq, None)
    vector = P(("dp",) + seq)
    matrix = P(("dp",) + seq, None)
    placed = (
        tokens,
        P(),
        tokens,
        vector,
        vector,
        P(seq, "dp", None, None),
        vector,
        matrix,
        vector,
        vector,
        vector,
        P(seq, "dp"),
        vector,
        matrix,
        vector,
    )
    results = (
        tokens,
        tokens,
        vector,
        vector,
        P(seq, "dp", None, None),
        vector,
        matrix,
        vector,
        vector,
        vector,
        P(seq, "dp"),
        vector,
        matrix,
        vector,
    )
    return jax.shard_map(
        layer if planar_plan else shards,
        mesh=grid,
        in_specs=placed,
        out_specs=results,
        check_vma=False,
    )
```

```python
import functools
import math

import jax
import jax.numpy as jnp
from jax import lax
from jax.experimental import pallas as pl
from jax.experimental.pallas import tpu as pltpu
from jax.sharding import Mesh
from jax.sharding import PartitionSpec as P


EPSILON = 1e-05
GELU_SCALE = 0.7978845608028654


def layer_norm(inputs, norm_gain, norm_shift):
    centered = inputs - jnp.mean(inputs, -1, keepdims=True)
    variance = jnp.mean(centered * centered, -1, keepdims=True)
    return centered * lax.rsqrt(variance + EPSILON) * norm_gain + norm_shift


def gelu_tanh(values):
    return (
        0.5 * values * (1.0 + jnp.tanh(GELU_SCALE * (values + 0.044715 * values * values * values)))
    )


def split_norm(inputs, gain_rows, shift_rows):
    return layer_norm(inputs, gain_rows[None, :, None, :], shift_rows[None, :, None, :])


def place_half(values, half_index, group_count):
    chosen = (jnp.arange(group_count, dtype=jnp.int32) == half_index).astype(values.dtype)
    return (chosen[:, None] * values.reshape(1, -1)).reshape(-1)


def shards(
    hidden,
    prefix_lengths,
    cotangent,
    first_gain,
    first_shift,
    triple_weight,
    pair_bias,
    dense_weight,
    dense_shift,
    second_gain,
    second_shift,
    expand_weight,
    expand_shift,
    shrink_weight,
    shrink_shift,
):
    wide_type = jnp.float32
    half_type = jnp.bfloat16
    seq_count = lax.axis_size("seq")
    group_count = lax.axis_size("dp")
    dp_index = lax.axis_index("dp")
    seq_index = lax.axis_index("seq")
    micro_count = hidden.shape[0]
    seq_rows = hidden.shape[2]
    model_width = hidden.shape[3]
    seq_length = seq_rows * seq_count
    local_heads = triple_weight.shape[1]
    head_dim = triple_weight.shape[3]
    head_total = local_heads * group_count
    pair_local = micro_count * group_count * local_heads // seq_count
    unit_local = expand_weight.shape[1]
    project_width = 3 * local_heads * head_dim
    token_total = micro_count * group_count * seq_rows
    score_scale = 1.0 / math.sqrt(head_dim)
    block_rows = min(512, seq_length)
    block_count = seq_length // block_rows
    key_pos = jnp.arange(seq_length, dtype=jnp.int32)
    gathered = (
        lax.all_gather(triple_weight, "seq", axis=0, tiled=True),
        lax.all_gather(dense_weight, "seq", axis=0, tiled=True),
        lax.all_gather(expand_weight, "seq", axis=0, tiled=True),
        lax.all_gather(shrink_weight, "seq", axis=0, tiled=True),
        lax.all_gather(first_gain, "seq", axis=0, tiled=True),
        lax.all_gather(first_shift, "seq", axis=0, tiled=True),
        lax.all_gather(pair_bias, "seq", axis=0, tiled=True),
        lax.all_gather(dense_shift, "seq", axis=0, tiled=True),
        lax.all_gather(second_gain, "seq", axis=0, tiled=True),
        lax.all_gather(second_shift, "seq", axis=0, tiled=True),
        lax.all_gather(expand_shift, "seq", axis=0, tiled=True),
        lax.all_gather(shrink_shift, "seq", axis=0, tiled=True),
    )
    triple_full, dense_full, expand_full, shrink_full = (
        gathered[0],
        gathered[1],
        gathered[2],
        gathered[3],
    )
    row_sets = (
        lax.all_gather(hidden, "dp", axis=1, tiled=True),
        lax.all_gather(cotangent, "dp", axis=1, tiled=True),
        lax.all_gather(gathered[4], "dp", axis=0, tiled=True),
        lax.all_gather(gathered[5], "dp", axis=0, tiled=True),
        lax.all_gather(gathered[6], "dp", axis=0, tiled=True),
        lax.all_gather(gathered[7], "dp", axis=0, tiled=True),
        lax.all_gather(gathered[8], "dp", axis=0, tiled=True),
        lax.all_gather(gathered[9], "dp", axis=0, tiled=True),
        lax.all_gather(gathered[10], "dp", axis=0, tiled=True),
        lax.all_gather(gathered[11], "dp", axis=0, tiled=True),
    )
    hidden_both = row_sets[0]
    upstream_low = row_sets[1]
    gain_one, shift_one, pair_full, dense_bias, gain_two, shift_two, expand_bias, shrink_bias = [
        vector.astype(wide_type) for vector in row_sets[2:]
    ]
    inputs_both = hidden_both.astype(wide_type)
    normed_low = layer_norm(inputs_both, gain_one, shift_one).astype(half_type)
    pair_heads = lax.dynamic_slice_in_dim(
        pair_full.reshape(head_total, 2, head_dim), dp_index * local_heads, local_heads, 0
    )
    triple_bias = jnp.stack(
        [pair_heads[:, 0], jnp.zeros_like(pair_heads[:, 0]), pair_heads[:, 1]], 0
    )
    projected = jnp.einsum(
        "mstd,dhce->cmshte", normed_low, triple_full, preferred_element_type=wide_type
    )
    projected = projected + triple_bias[:, None, None, :, None, :]
    project_low = projected.astype(half_type).reshape(3, seq_count, pair_local, seq_rows, head_dim)
    pair_rows = lax.all_to_all(project_low, "seq", split_axis=1, concat_axis=3, tiled=True)[:, 0]
    query_all, key_all, value_all = (pair_rows[0], pair_rows[1], pair_rows[2])
    pair_index = seq_index * pair_local + jnp.arange(pair_local, dtype=jnp.int32)
    head_index = dp_index * local_heads + pair_index % local_heads
    sequence_index = pair_index // local_heads
    slopes = jnp.power(jnp.float32(2.0), -8.0 * (head_index.astype(wide_type) + 1.0) / head_total)
    prefix_flat = prefix_lengths.reshape(-1)
    prefix_slots = jnp.arange(prefix_flat.shape[0], dtype=jnp.int32)
    prefixes = jnp.sum(
        jnp.where(prefix_slots[None, :] == sequence_index[:, None], prefix_flat[None, :], 0), 1
    )

    def block_scores(pair_item, first_row):
        query_block = lax.dynamic_slice_in_dim(
            lax.dynamic_index_in_dim(query_all, pair_item, 0, False), first_row, block_rows, 0
        )
        keys_item = lax.dynamic_index_in_dim(key_all, pair_item, 0, False)
        head_slope = lax.dynamic_index_in_dim(slopes, pair_item, 0, False)
        prefix = lax.dynamic_index_in_dim(prefixes, pair_item, 0, False)
        query_pos = first_row + jnp.arange(block_rows, dtype=jnp.int32)
        raw_scores = (
            jnp.einsum("qe,ke->qk", query_block, keys_item, preferred_element_type=wide_type)
            * score_scale
        )
        distance = jnp.abs(query_pos[:, None] - key_pos[None, :]).astype(wide_type)
        raw_scores = raw_scores - head_slope * distance
        allowed = (key_pos[None, :] <= query_pos[:, None]) | (key_pos[None, :] < prefix)
        return (query_block, jnp.where(allowed, raw_scores, jnp.float32(-1e30)))

    def forward_block(flat_index):
        pair_item = flat_index // block_count
        first_row = flat_index % block_count * block_rows
        _, scores = block_scores(pair_item, first_row)
        row_max = jnp.max(scores, -1, keepdims=True)
        powers = jnp.exp(scores - row_max)
        row_total = jnp.sum(powers, -1, keepdims=True)
        probs_low = (powers / row_total).astype(half_type)
        values_item = lax.dynamic_index_in_dim(value_all, pair_item, 0, False)
        mixed = jnp.dot(probs_low, values_item, preferred_element_type=wide_type).astype(half_type)
        return (mixed, (row_max + jnp.log(row_total))[:, 0])

    mixed_blocks, log_blocks = lax.map(
        forward_block, jnp.arange(pair_local * block_count, dtype=jnp.int32)
    )
    mixed_pairs = mixed_blocks.reshape(pair_local, seq_count, seq_rows, head_dim)
    log_totals = log_blocks.reshape(pair_local, seq_length)
    mixed_home = lax.all_to_all(mixed_pairs, "seq", split_axis=1, concat_axis=0, tiled=True)
    mixed_tokens = jnp.transpose(
        mixed_home.reshape(micro_count, group_count, local_heads, seq_rows, head_dim),
        (0, 1, 3, 2, 4),
    ).reshape(micro_count, group_count, seq_rows, local_heads * head_dim)
    dense_part = jnp.einsum(
        "mstk,kf->mstf", mixed_tokens, dense_full, preferred_element_type=wide_type
    )
    attention_sum = lax.psum(dense_part.astype(jnp.bfloat16), "dp").astype(jnp.float32)
    middle = inputs_both + attention_sum + dense_bias
    gain_rows_two = jnp.broadcast_to(gain_two[None, :], (group_count, model_width))
    shift_rows_two = jnp.broadcast_to(shift_two[None, :], (group_count, model_width))
    normed_two, norm_two_pull = jax.vjp(split_norm, middle, gain_rows_two, shift_rows_two)
    normed_two_low = normed_two.astype(half_type)
    unit_bias = lax.dynamic_slice_in_dim(expand_bias, dp_index * unit_local, unit_local, 0)
    hidden_pre = (
        jnp.einsum("mstd,df->mstf", normed_two_low, expand_full, preferred_element_type=wide_type)
        + unit_bias
    )
    activated_value, gelu_pull = jax.vjp(gelu_tanh, hidden_pre)
    activated_low = activated_value.astype(half_type)
    feed_part = jnp.einsum(
        "mstf,fd->mstd", activated_low, shrink_full, preferred_element_type=wide_type
    )
    feed_sum = lax.psum_scatter(
        feed_part.astype(jnp.bfloat16), "dp", scatter_dimension=1, tiled=True
    ).astype(jnp.float32)
    middle_own = lax.dynamic_slice_in_dim(middle, dp_index, 1, 1)
    layer_output = (middle_own + feed_sum + shrink_bias).astype(half_type)
    triple_back, dense_back, expand_back, shrink_back = (
        lax.all_gather(triple_weight, "seq", axis=0, tiled=True),
        lax.all_gather(dense_weight, "seq", axis=0, tiled=True),
        lax.all_gather(expand_weight, "seq", axis=0, tiled=True),
        lax.all_gather(shrink_weight, "seq", axis=0, tiled=True),
    )
    grad_act = jnp.einsum(
        "mstd,fd->mstf", upstream_low, shrink_back, preferred_element_type=wide_type
    )
    grad_pre_low = gelu_pull(grad_act)[0].astype(half_type)
    norm_two_part = jnp.einsum(
        "mstf,df->mstd", grad_pre_low, expand_back, preferred_element_type=wide_type
    )
    grad_normed_two = lax.psum(norm_two_part.astype(jnp.bfloat16), "dp").astype(jnp.float32)
    grad_middle_norm, grad_gain_rows_two, grad_shift_rows_two = norm_two_pull(grad_normed_two)
    grad_middle = upstream_low.astype(wide_type) + grad_middle_norm
    grad_branch_low = grad_middle.astype(half_type)
    go_pairs = jnp.einsum(
        "mstf,hef->mshte",
        grad_branch_low,
        dense_back.reshape(local_heads, head_dim, model_width),
        preferred_element_type=wide_type,
    ).astype(half_type)
    go_pairs = go_pairs.reshape(seq_count, pair_local, seq_rows, head_dim)
    grad_mixed_pairs = lax.all_to_all(go_pairs, "seq", split_axis=0, concat_axis=2, tiled=True)[0]

    def backward_item(pair_item):
        keys_item = lax.dynamic_index_in_dim(key_all, pair_item, 0, False)
        values_item = lax.dynamic_index_in_dim(value_all, pair_item, 0, False)
        grad_mixed_item = lax.dynamic_index_in_dim(grad_mixed_pairs, pair_item, 0, False)
        totals_item = lax.dynamic_index_in_dim(log_totals, pair_item, 0, False)

        def backward_block(running, block_index):
            key_grad, value_grad = running
            first_row = block_index * block_rows
            query_block, scores = block_scores(pair_item, first_row)
            soft_probs = jnp.exp(
                scores - lax.dynamic_slice_in_dim(totals_item, first_row, block_rows, 0)[:, None]
            )
            grad_block = lax.dynamic_slice_in_dim(grad_mixed_item, first_row, block_rows, 0)
            grad_probs = jnp.einsum(
                "qe,ke->qk", grad_block, values_item, preferred_element_type=wide_type
            )
            row_inner = jnp.sum(grad_probs * soft_probs, -1, keepdims=True)
            grad_scores_low = (soft_probs * (grad_probs - row_inner)).astype(half_type)
            query_grad = (
                jnp.dot(grad_scores_low, keys_item, preferred_element_type=wide_type) * score_scale
            )
            key_grad = (
                key_grad
                + jnp.einsum(
                    "qk,qe->ke", grad_scores_low, query_block, preferred_element_type=wide_type
                )
                * score_scale
            )
            value_grad = value_grad + jnp.einsum(
                "qk,qe->ke",
                soft_probs.astype(half_type),
                grad_block,
                preferred_element_type=wide_type,
            )
            return ((key_grad, value_grad), query_grad)

        zero_rows = jnp.zeros((seq_length, head_dim), wide_type)
        (key_grad, value_grad), query_grads = lax.scan(
            backward_block, (zero_rows, zero_rows), jnp.arange(block_count, dtype=jnp.int32)
        )
        return jnp.stack(
            [query_grads.reshape(seq_length, head_dim), key_grad, value_grad], 0
        ).astype(half_type)

    grad_pairs = lax.map(backward_item, jnp.arange(pair_local, dtype=jnp.int32))
    grad_split = grad_pairs.reshape(pair_local, 3, seq_count, seq_rows, head_dim)
    grad_home = lax.all_to_all(grad_split, "seq", split_axis=2, concat_axis=0, tiled=True)
    grad_project_low = jnp.transpose(
        grad_home.reshape(micro_count, group_count, local_heads, 3, seq_rows, head_dim),
        (0, 1, 4, 2, 3, 5),
    ).reshape(micro_count, group_count, seq_rows, project_width)
    norm_one_part = jnp.einsum(
        "mstc,dc->mstd",
        grad_project_low,
        triple_back.reshape(model_width, project_width),
        preferred_element_type=wide_type,
    )
    grad_normed_one = lax.psum_scatter(
        norm_one_part.astype(jnp.bfloat16), "dp", scatter_dimension=1, tiled=True
    ).astype(jnp.float32)
    inputs_own = hidden.astype(wide_type)
    grad_inputs_norm, grad_gain_one, grad_shift_one = jax.vjp(
        layer_norm, inputs_own, gain_one, shift_one
    )[1](grad_normed_one)
    grad_middle_own = lax.dynamic_slice_in_dim(grad_middle, dp_index, 1, 1)
    hidden_grad = (grad_middle_own + grad_inputs_norm).astype(half_type)
    head_sums = jnp.sum(
        grad_project_low.reshape(micro_count, group_count, seq_rows, local_heads, 3, head_dim),
        (0, 1, 2),
        dtype=wide_type,
    )
    pair_grad = place_half(jnp.stack([head_sums[:, 0], head_sums[:, 2]], 1), dp_index, group_count)
    unit_grad = place_half(jnp.sum(grad_pre_low, (0, 1, 2), dtype=wide_type), dp_index, group_count)
    dense_shift_term = jnp.sum(
        lax.dynamic_slice_in_dim(grad_branch_low, dp_index, 1, 1), (0, 1, 2), dtype=wide_type
    )
    shrink_shift_term = jnp.sum(cotangent, (0, 1, 2), dtype=wide_type)
    gain_two_term = lax.dynamic_index_in_dim(grad_gain_rows_two, dp_index, 0, False)
    shift_two_term = lax.dynamic_index_in_dim(grad_shift_rows_two, dp_index, 0, False)
    vector_sums = (
        lax.psum_scatter(grad_gain_one, ("dp", "seq"), scatter_dimension=0, tiled=True),
        lax.psum_scatter(grad_shift_one, ("dp", "seq"), scatter_dimension=0, tiled=True),
        lax.psum_scatter(pair_grad, ("dp", "seq"), scatter_dimension=0, tiled=True),
        lax.psum_scatter(dense_shift_term, ("dp", "seq"), scatter_dimension=0, tiled=True),
        lax.psum_scatter(gain_two_term, ("dp", "seq"), scatter_dimension=0, tiled=True),
        lax.psum_scatter(shift_two_term, ("dp", "seq"), scatter_dimension=0, tiled=True),
        lax.psum_scatter(unit_grad, ("dp", "seq"), scatter_dimension=0, tiled=True),
        lax.psum_scatter(shrink_shift_term, ("dp", "seq"), scatter_dimension=0, tiled=True),
    )
    normed_flat = normed_low.reshape(token_total, model_width)
    project_flat = grad_project_low.reshape(token_total, project_width)
    normed_two_flat = normed_two_low.reshape(token_total, model_width)
    pre_flat = grad_pre_low.reshape(token_total, unit_local)
    column_sums = lax.psum_scatter(
        jnp.concatenate(
            [
                jnp.einsum(
                    "tr,tc->rc", normed_flat, project_flat, preferred_element_type=wide_type
                ),
                jnp.einsum(
                    "tr,tc->rc", normed_two_flat, pre_flat, preferred_element_type=wide_type
                ),
            ],
            1,
        ),
        "seq",
        scatter_dimension=0,
        tiled=True,
    )
    triple_grad = column_sums[:, :project_width].reshape(
        model_width // seq_count, local_heads, 3, head_dim
    )
    expand_grad = column_sums[:, project_width:]
    dense_rows = dense_weight.shape[0]
    shrink_rows = shrink_weight.shape[0]
    row_block = dense_rows + shrink_rows
    mixed_flat = mixed_tokens.reshape(token_total, local_heads * head_dim)
    branch_flat = grad_branch_low.reshape(token_total, model_width)
    active_flat = activated_low.reshape(token_total, unit_local)
    upstream_flat = upstream_low.reshape(token_total, model_width)
    block_number = row_block * lax.axis_size("seq") // row_block
    dense_term = jnp.einsum("tr,td->rd", mixed_flat, branch_flat, preferred_element_type=wide_type)
    shrink_term = jnp.einsum(
        "tr,td->rd", active_flat, upstream_flat, preferred_element_type=wide_type
    )
    row_sums = lax.psum_scatter(
        jnp.concatenate(
            [
                dense_term.reshape(block_number, dense_rows, model_width),
                shrink_term.reshape(block_number, shrink_rows, model_width),
            ],
            1,
        ).reshape(row_block * lax.axis_size("seq"), model_width),
        "seq",
        scatter_dimension=0,
        tiled=True,
    )
    dense_grad = row_sums[:dense_rows]
    shrink_grad = row_sums[dense_rows:]
    return (
        layer_output,
        hidden_grad,
        vector_sums[0],
        vector_sums[1],
        triple_grad,
        vector_sums[2],
        dense_grad,
        vector_sums[3],
        vector_sums[4],
        vector_sums[5],
        expand_grad,
        vector_sums[6],
        shrink_grad,
        vector_sums[7],
    )


CHUNKS = 4
LOG2E = 1.4426950408889634
MESH = pl.DeviceIdType.MESH


def remote(src, dst, send, recv, peer):
    return pltpu.make_async_remote_copy(
        src_ref=src,
        dst_ref=dst,
        send_sem=send,
        recv_sem=recv,
        device_id=peer,
        device_id_type=MESH,
    )


def greet(peers):
    barrier = pltpu.get_barrier_semaphore()
    for peer in peers:
        pl.semaphore_signal(barrier, inc=1, device_id=peer, device_id_type=MESH)
    pl.semaphore_wait(barrier, len(peers))


class Corner:
    def __init__(self):
        self.c = lax.axis_index("dp")
        self.y = lax.axis_index("y")
        self.x = lax.axis_index("x")
        self.ax = self.x + (1 - self.c) * (1 - 2 * self.x)
        self.ay = self.y + self.c * (1 - 2 * self.y)
        self.bx = self.x + self.c * (1 - 2 * self.x)
        self.by = self.y + (1 - self.c) * (1 - 2 * self.y)
        self.dx = 1 - self.x
        self.dy = 1 - self.y
        self.peer_a = {"y": self.ay, "x": self.ax}
        self.peer_b = {"y": self.by, "x": self.bx}
        self.sibling = {"dp": 1 - self.c}

    def slots(self, core):
        return [
            (core * 2 + y) * 2 + x
            for y, x in (
                (self.dy, self.dx),
                (self.by, self.bx),
                (self.ay, self.ax),
                (self.y, self.x),
            )
        ]


def gather_kernel(deep, whole, *refs):
    if deep:
        rows_ref, deep_ref, all_ref, moved_ref, local_sem, send, recv, deep_send, deep_recv = refs
    else:
        rows_ref, all_ref, local_sem, send, recv = refs
    at = Corner()
    slot_d, slot_b, slot_a, me = at.slots(at.c)
    step = rows_ref.shape[0] // CHUNKS
    peers = [at.peer_a, at.peer_b, at.sibling]
    sent, moves = [], []
    if deep:
        z = lax.axis_index("z")
        plane_at = [lax.rem(z + i, 4) for i in range(4)]
        peers += [{"z": plane_at[i]} for i in range(1, 4)]
    greet(peers)
    locals_ = [pltpu.make_async_copy(rows_ref, all_ref.at[me], local_sem.at[0])]
    if deep:
        block = deep_ref if whole else deep_ref.at[z]
        locals_.append(pltpu.make_async_copy(block, moved_ref.at[z], local_sem.at[1]))
    for one in locals_:
        one.start()

    def copy(kind, k, slot, peer):
        part = pl.ds(k * step, step)
        src = rows_ref.at[part] if kind < 3 else all_ref.at[slot, part]
        return remote(src, all_ref.at[slot, part], send.at[kind, k], recv.at[kind, k], peer)

    def arrived(kind, k, slot, peer):
        part = pl.ds(k * step, step)
        block = all_ref.at[slot, part]
        remote(block, block, send.at[kind, k], recv.at[kind, k], peer).wait_recv()

    def start(kind, k, slot, peer):
        one = copy(kind, k, slot, peer)
        one.start()
        sent.append(one)

    for i in range(1, 4) if deep else ():
        sems = deep_send.at[i - 1], deep_recv.at[i - 1]
        block = deep_ref if whole else deep_ref.at[plane_at[i]]
        one = remote(block, moved_ref.at[z], *sems, {"z": plane_at[i]})
        one.start()
        sent.append(one)
        landing = moved_ref.at[plane_at[4 - i]]
        moves.append(remote(landing, landing, *sems, {"z": plane_at[i]}))
    for k in range(CHUNKS):
        start(0, k, me, at.peer_a)
        start(1, k, me, at.peer_b)
    for k in range(CHUNKS):
        start(2, k, me, at.sibling)
    for k in range(CHUNKS):
        arrived(0, k, slot_a, at.peer_a)
        start(3, k, slot_a, at.peer_b)
        start(4, k, slot_a, at.sibling)
    for k in range(CHUNKS):
        arrived(1, k, slot_b, at.peer_b)
        start(5, k, slot_b, at.sibling)
    for k in range(CHUNKS):
        arrived(3, k, slot_d, at.peer_b)
        start(6, k, slot_d, at.sibling)
    other_d, other_b, other_a, other_me = at.slots(1 - at.c)
    for k in range(CHUNKS):
        arrived(2, k, other_me, at.sibling)
        arrived(4, k, other_b, at.sibling)
        arrived(5, k, other_a, at.sibling)
        arrived(6, k, other_d, at.sibling)
    for one in moves:
        one.wait_recv()
    for one in sent:
        one.wait_send()
    for one in locals_:
        one.wait()


def gather_tokens(identity, rows, deep=None, whole=False):
    count, width = rows.shape
    operands = [rows]
    shapes = [jax.ShapeDtypeStruct((8, count, width), rows.dtype)]
    scratch = [
        pltpu.SemaphoreType.DMA((2,)),
        pltpu.SemaphoreType.DMA((7, CHUNKS)),
        pltpu.SemaphoreType.DMA((7, CHUNKS)),
    ]
    if deep is not None:
        operands.append(deep)
        moved_shape = (4,) + deep.shape if whole else deep.shape
        shapes.append(jax.ShapeDtypeStruct(moved_shape, deep.dtype))
        scratch += [pltpu.SemaphoreType.DMA((3,)), pltpu.SemaphoreType.DMA((3,))]
    all_rows, *moved = pl.pallas_call(
        functools.partial(gather_kernel, deep is not None, whole),
        out_shape=shapes,
        in_specs=[pl.BlockSpec(memory_space=pl.ANY)] * len(operands),
        out_specs=[pl.BlockSpec(memory_space=pl.ANY)] * len(shapes),
        scratch_shapes=scratch,
        compiler_params=pltpu.CompilerParams(
            collective_id=identity, has_side_effects=True
        ),
        cost_estimate=pl.CostEstimate(
            flops=0, bytes_accessed=16 * count * width * 4, transcendentals=0
        ),
        name="gather_tokens",
    )(*operands)
    return (all_rows.reshape(8 * count, width), *moved)


def after(value, *others):
    return lax.optimization_barrier((value, *others))[0]


def scatter_kernel(turned, term, left_ref, right_ref, *refs):
    if term:
        rows_ref, grads_ref, own_ref, term_ref, *refs = refs
    else:
        own_ref, *refs = refs
    part_ref, from_core, from_b, from_a, send, recv = refs
    at = Corner()
    slot_d, slot_b, slot_a, me = at.slots(at.c)
    other_d, other_b, other_a, other_me = at.slots(1 - at.c)
    _, width = own_ref.shape
    step = width // CHUNKS
    wide = jnp.float32
    greet([at.peer_a, at.peer_b, at.sibling])
    sent = []

    def start(kind, k, src, dst, peer):
        one = remote(src, dst, send.at[kind, k], recv.at[kind, k], peer)
        one.start()
        sent.append(one)

    def arrived(kind, k, dst, peer):
        remote(dst, dst, send.at[kind, k], recv.at[kind, k], peer).wait_recv()

    def multiply_columns(slot, cols):
        right = right_ref[cols] if turned else right_ref[:, cols]
        product = lax.dot_general(
            left_ref[slot],
            right,
            (((1,), (1 if turned else 0,)), ((), ())),
            preferred_element_type=wide,
        )
        part_ref[slot, :, cols] = product.astype(part_ref.dtype)

    def multiply(slot):
        def columns(t, carry):
            multiply_columns(slot, pl.ds(pl.multiple_of(t * step, step), step))
            return carry

        lax.fori_loop(0, CHUNKS, columns, 0)

    def multiply_term(first, last):
        if not term:
            return
        lanes = min(256, rows_ref.shape[1] // 8)

        def features(t, carry):
            cols = pl.ds(pl.multiple_of(t * lanes, lanes), lanes)
            product = lax.dot_general(
                rows_ref[:, cols],
                grads_ref[...],
                (((0,), (0,)), ((), ())),
                preferred_element_type=wide,
            )
            term_ref[cols] = product.astype(term_ref.dtype)
            return carry

        count = rows_ref.shape[1] // lanes
        lax.fori_loop(count * first // 8, count * last // 8, features, 0)

    def share(q, slot, chunks):
        for k in chunks:
            part = pl.ds(k * step, step)
            start(q, k, part_ref.at[slot, :, part], from_core.at[q, :, part], at.sibling)

    def to_b(q, slot, chunks):
        for k in chunks:
            part = pl.ds(k * step, step)
            arrived(q, k, from_core.at[q, :, part], at.sibling)
            total = part_ref[slot, :, part].astype(wide) + from_core[q, :, part].astype(wide)
            from_core[q, :, part] = total.astype(from_core.dtype)
            start(4 + q, k, from_core.at[q, :, part], from_b.at[q, :, part], at.peer_b)

    everything = range(CHUNKS)
    for k in everything:
        multiply_columns(other_d, pl.ds(k * step, step))
        share(0, other_d, [k])
        multiply_columns(slot_d, pl.ds(k * step, step))
        if k:
            to_b(0, slot_d, [k - 1])
    to_b(0, slot_d, [CHUNKS - 1])
    multiply(other_a)
    share(1, other_a, everything)
    multiply(slot_b)
    to_b(1, slot_b, everything)
    multiply(other_b)
    share(2, other_b, everything)
    multiply(slot_a)
    multiply_term(0, 2)
    for k in everything:
        part = pl.ds(k * step, step)
        arrived(2, k, from_core.at[2, :, part], at.sibling)
        arrived(4, k, from_b.at[0, :, part], at.peer_b)
        total = part_ref[slot_a, :, part].astype(wide) + from_core[2, :, part].astype(wide)
        total = total + from_b[0, :, part].astype(wide)
        from_core[2, :, part] = total.astype(from_core.dtype)
        start(6, k, from_core.at[2, :, part], from_a.at[:, part], at.peer_a)
    multiply(other_me)
    share(3, other_me, everything)
    multiply(me)
    multiply_term(2, 8)
    for k in everything:
        part = pl.ds(k * step, step)
        arrived(3, k, from_core.at[3, :, part], at.sibling)
        arrived(5, k, from_b.at[1, :, part], at.peer_b)
        arrived(6, k, from_a.at[:, part], at.peer_a)
        total = part_ref[me, :, part].astype(wide) + from_core[3, :, part].astype(wide)
        total = total + from_b[1, :, part].astype(wide)
        own_ref[:, part] = total + from_a[:, part].astype(wide)
    for one in sent:
        one.wait_send()


def scatter_tokens(identity, left, right, turned=False, term=()):
    count, depth = left.shape[0] // 8, left.shape[1]
    width = right.shape[0] if turned else right.shape[1]
    half = left.dtype
    shapes = [jax.ShapeDtypeStruct((count, width), jnp.float32)]
    if term:
        shapes.append(jax.ShapeDtypeStruct((term[0].shape[1], term[1].shape[1]), half))
    vmem = pl.BlockSpec(memory_space=pltpu.VMEM)
    return pl.pallas_call(
        functools.partial(scatter_kernel, turned, bool(term)),
        out_shape=shapes,
        in_specs=[vmem] * (2 + len(term)),
        out_specs=[vmem] * len(shapes),
        scratch_shapes=[
            pltpu.VMEM((8, count, width), half),
            pltpu.VMEM((4, count, width), half),
            pltpu.VMEM((2, count, width), half),
            pltpu.VMEM((count, width), half),
            pltpu.SemaphoreType.DMA((7, CHUNKS)),
            pltpu.SemaphoreType.DMA((7, CHUNKS)),
        ],
        compiler_params=pltpu.CompilerParams(
            collective_id=identity, has_side_effects=True, vmem_limit_bytes=58 * 2**20
        ),
        cost_estimate=pl.CostEstimate(
            flops=2 * left.size * width, bytes_accessed=64 * count * width, transcendentals=0
        ),
        name="scatter_tokens",
    )(left.reshape(8, count, depth), right, *term)


def exchange_kernel(last, triple_step, expand_step, *refs):
    refs = list(refs)
    take = lambda n: [refs.pop(0) for _ in range(n)]
    deep_in, turn_in, triple_in, expand_in, vec_in = take(5)
    deep_out, turn_out, triple_out, expand_out, vec_out = take(5)
    if last:
        triple_columns, expand_columns = triple_out, expand_out
        triple_out, expand_out, near, far, here = take(5)
    send, recv, local_sem = take(3)
    c, z = lax.axis_index("dp"), lax.axis_index("z")
    y, x = lax.axis_index("y"), lax.axis_index("x")
    place = y * 2 + x
    rank = c * 4 + place

    def deep(i):
        return lax.rem(z + i, 4)

    def flat(i):
        return lax.rem(place + i, 4)

    def wide(i):
        return lax.rem(rank + i, 8)

    def deep_peer(i):
        return {"z": deep(i)}

    def flat_peer(i):
        return {"y": flat(i) // 2, "x": lax.rem(flat(i), 2)}

    def wide_peer(i):
        return {
            "dp": wide(i) // 4,
            "y": lax.rem(wide(i), 4) // 2,
            "x": lax.rem(wide(i), 2),
        }

    low = lax.rem(z, 2)
    turn_from = {"z": z - low + 1 - x, "x": low}
    turn_to = {"z": z - low + x, "x": 1 - low}
    if last:
        turn_from, turn_to = turn_to, turn_from
    others = range(1, 4)
    greet([deep_peer(i) for i in others] + [wide_peer(i) for i in range(1, 8)])
    sent, waits, kept = [], [], []
    count = [0]

    def post(src, dst, peer, landing):
        k = count[0]
        count[0] += 1
        one = remote(src, dst, send.at[k], recv.at[k], peer)
        one.start()
        sent.append(one)
        return remote(landing, landing, send.at[k], recv.at[k], peer)

    def keep(src, dst):
        one = pltpu.make_async_copy(src, dst, local_sem.at[len(kept)])
        one.start()
        kept.append(one)

    def parts(src, dst, order, block):
        if last:
            return [(src.at[block], dst.at[place])]
        steps = src.shape[1] // 4 // order[0]
        step = order[0]
        return [
            (
                src.at[:, pl.ds(pl.multiple_of((i * 4 + order[1](block)) * step, step), step)],
                dst.at[place, :, pl.ds(i * step, step)],
            )
            for i in range(steps)
        ]

    def turn_columns(src, dst, order):
        for i in others:
            for n, (a, b) in enumerate(parts(src, dst, order, flat(i))):
                landing = dst.at[flat(4 - i)]
                if not last:
                    landing = landing.at[:, pl.ds(n * order[0], order[0])]
                waits.append(post(a, b, flat_peer(i), landing))

    triple_order = (triple_step, lambda p: 2 * (1 - lax.rem(p, 2)) + p // 2)
    expand_order = (expand_step, lambda p: p)
    stage, late = [], []
    turn_columns(triple_in, triple_out, triple_order)
    for i in others:
        late.append(post(deep_in.at[deep(i)], deep_out.at[z], deep_peer(i), deep_out.at[deep(4 - i)]))
    for i in range(1, 8):
        if last:
            landing = near.at[wide(8 - i)]
            stage.append(post(vec_in.at[wide(i)], near.at[rank], wide_peer(i), landing))
        else:
            landing = vec_out.at[z, wide(8 - i)]
            stage.append(post(vec_in, vec_out.at[z, rank], wide_peer(i), landing))
    late.append(post(turn_in, turn_out, turn_to, turn_out))
    turn_columns(expand_in, expand_out, expand_order)
    keep(deep_in.at[z], deep_out.at[z])
    for src, dst, order in (
        (triple_in, triple_out, triple_order),
        (expand_in, expand_out, expand_order),
    ):
        for a, b in parts(src, dst, order, place):
            keep(a, b)
    if last:
        own = pltpu.make_async_copy(vec_in.at[rank], near.at[rank], local_sem.at[len(kept)])
        own.start()
        for one in stage:
            one.wait_recv()
        own.wait()
        here[...] = jnp.sum(near[...], 0)
        stage = []
        for i in others:
            landing = far.at[deep(4 - i)]
            stage.append(post(here.at[deep(i)], far.at[z], deep_peer(i), landing))
        far[z] = here[z]
        for one in stage:
            one.wait_recv()
        vec_out[...] = jnp.sum(far[...], 0)
    else:
        own = pltpu.make_async_copy(vec_in, vec_out.at[z, rank], local_sem.at[len(kept)])
        own.start()
        for one in stage:
            one.wait_recv()
        own.wait()
        for i in others:
            landing = vec_out.at[deep(4 - i)]
            late.append(post(vec_out.at[z], vec_out.at[z], deep_peer(i), landing))
    for one in waits:
        one.wait_recv()
    for one in kept:
        one.wait()
    if last:
        for (steps, order), blocks, columns in zip(
            last, (triple_out, expand_out), (triple_columns, expand_columns)
        ):
            step = blocks.shape[2] // steps
            for i in range(steps):
                for p in range(4):
                    first = (i * 4 + order[p]) * step
                    columns[:, first : first + step] = blocks[p, :, i * step : (i + 1) * step]
    for one in late:
        one.wait_recv()
    for one in sent:
        one.wait_send()


def exchange(identity, deep, turned, triple, expand, vector, steps, last=None):
    half = expand.dtype
    operands = [deep, turned, triple, expand, vector]
    shapes = [jax.ShapeDtypeStruct(a.shape, a.dtype) for a in (deep, turned)]
    hbm, vmem = pl.BlockSpec(memory_space=pl.ANY), pl.BlockSpec(memory_space=pltpu.VMEM)
    scratch = []
    if last:
        tile = vector.shape[2:]
        shapes += [jax.ShapeDtypeStruct((a.shape[1], 4 * a.shape[2]), half) for a in (triple, expand)]
        shapes.append(jax.ShapeDtypeStruct(tile, vector.dtype))
        scratch = [pltpu.VMEM(triple.shape, half), pltpu.VMEM(expand.shape, half)]
        scratch += [pltpu.VMEM(n + tile, vector.dtype) for n in ((8, 4), (4,), (4,))]
        places = [hbm, hbm, vmem, vmem, vmem]
    else:
        for rows, columns in (triple.shape, expand.shape):
            shapes.append(jax.ShapeDtypeStruct((4, rows, columns // 4), half))
        shapes.append(jax.ShapeDtypeStruct((4, 8) + vector.shape, vector.dtype))
        places = [hbm] * 5
    copies = 3 + 7 + 1 + 3
    for whole, step in zip((triple, expand), steps):
        copies += 3 if last else 3 * (whole.shape[1] // 4 // step)
    moved = sum(a.size * a.dtype.itemsize for a in operands)
    return pl.pallas_call(
        functools.partial(exchange_kernel, last, *steps),
        out_shape=shapes,
        in_specs=[hbm] * 5,
        out_specs=places,
        scratch_shapes=scratch
        + [
            pltpu.SemaphoreType.DMA((copies,)),
            pltpu.SemaphoreType.DMA((copies,)),
            pltpu.SemaphoreType.DMA((16,)),
        ],
        compiler_params=pltpu.CompilerParams(
            collective_id=identity, has_side_effects=True, vmem_limit_bytes=24 * 2**20
        ),
        cost_estimate=pl.CostEstimate(flops=0, bytes_accessed=16 * moved, transcendentals=0),
        name="exchange",
    )(*operands)


def scores_of(item_ref, first, block, slope, prefix, depth, seq_rows):
    length = item_ref.shape[0]
    head_dim = item_ref.shape[1] // 3
    own_rows = depth * seq_rows
    chips = length // own_rows

    def position(index):
        chip = index // own_rows
        rest = index % own_rows
        return ((rest // seq_rows) * chips + chip) * seq_rows + rest % seq_rows

    queries = item_ref[first : first + block, :head_dim]
    keys = item_ref[:, head_dim : 2 * head_dim]
    raw = lax.dot_general(
        keys, queries, (((1,), (1,)), ((), ())), preferred_element_type=jnp.float32
    )
    key_pos = position(lax.broadcasted_iota(jnp.int32, (length, 1), 0))
    query_pos = position(first + lax.broadcasted_iota(jnp.int32, (1, block), 1))
    bound = jnp.where(key_pos < prefix, -1, key_pos)
    distance = jnp.abs(
        query_pos.astype(jnp.float32) - key_pos.astype(jnp.float32)
    )
    scores = raw * (LOG2E / math.sqrt(head_dim)) - (slope * LOG2E) * distance
    return jnp.where(bound <= query_pos, scores, jnp.float32(-1e30))


def forward_kernel(depth, seq_rows, block, prefix_ref, slope_ref, item_ref, mixed_ref, total_ref):
    prefix = prefix_ref[pl.program_id(0)]
    slope = slope_ref[pl.program_id(1)]
    length = item_ref.shape[0]
    head_dim = item_ref.shape[1] // 3
    for first in range(0, length, block):
        scores = scores_of(item_ref, first, block, slope, prefix, depth, seq_rows)
        top = jnp.max(scores, 0, keepdims=True)
        powers = jnp.exp2(scores - top)
        total = jnp.sum(powers, 0, keepdims=True)
        probs = (powers * (1.0 / total)).astype(jnp.bfloat16)
        mixed = lax.dot_general(
            probs,
            item_ref[:, 2 * head_dim :],
            (((0,), (0,)), ((), ())),
            preferred_element_type=jnp.float32,
        )
        mixed_ref[first : first + block, :] = mixed.astype(mixed_ref.dtype)
        total_ref[0, :, first : first + block] = top + jnp.log2(total)


def attend_forward(projected, slopes, prefixes, own_heads, head_dim, depth, seq_rows):
    cores = prefixes.shape[0]
    length = projected.shape[0] // cores
    block = min(256, length)
    scores = cores * own_heads * length * length
    return pl.pallas_call(
        functools.partial(forward_kernel, depth, seq_rows, block),
        grid=(cores, own_heads),
        out_shape=[
            jax.ShapeDtypeStruct((cores * length, own_heads * head_dim), projected.dtype),
            jax.ShapeDtypeStruct((cores * own_heads, 1, length), jnp.float32),
        ],
        in_specs=[
            pl.BlockSpec(memory_space=pltpu.SMEM),
            pl.BlockSpec(memory_space=pltpu.SMEM),
            pl.BlockSpec((length, 3 * head_dim), lambda s, h: (s, h)),
        ],
        out_specs=[
            pl.BlockSpec((length, head_dim), lambda s, h: (s, h)),
            pl.BlockSpec((1, 1, length), lambda s, h: (s * own_heads + h, 0, 0)),
        ],
        compiler_params=pltpu.CompilerParams(vmem_limit_bytes=48 * 2**20),
        cost_estimate=pl.CostEstimate(
            flops=4 * scores * head_dim,
            bytes_accessed=2 * projected.size * 2,
            transcendentals=scores,
        ),
        name="attend_forward",
    )(prefixes, slopes, projected)


def backward_kernel(
    depth, seq_rows, block, prefix_ref, slope_ref, item_ref, grad_ref, total_ref, out_ref, key_sum, value_sum
):
    prefix = prefix_ref[pl.program_id(0)]
    slope = slope_ref[pl.program_id(1)]
    length = item_ref.shape[0]
    head_dim = item_ref.shape[1] // 3
    scale = 1.0 / math.sqrt(head_dim)
    half = jnp.bfloat16
    wide = jnp.float32
    for first in range(0, length, block):
        scores = scores_of(item_ref, first, block, slope, prefix, depth, seq_rows)
        probs = jnp.exp2(scores - total_ref[0, :, first : first + block])
        grad = grad_ref[first : first + block, :]
        grad_probs = lax.dot_general(
            item_ref[:, 2 * head_dim :],
            grad,
            (((1,), (1,)), ((), ())),
            preferred_element_type=wide,
        )
        inner = jnp.sum(grad_probs * probs, 0, keepdims=True)
        grad_scores = (probs * (grad_probs - inner)).astype(half)
        key_term = jnp.dot(
            grad_scores, item_ref[first : first + block, :head_dim], preferred_element_type=wide
        )
        value_term = jnp.dot(probs.astype(half), grad, preferred_element_type=wide)
        query_grad = lax.dot_general(
            grad_scores,
            item_ref[:, head_dim : 2 * head_dim],
            (((0,), (0,)), ((), ())),
            preferred_element_type=wide,
        )
        out_ref[first : first + block, :head_dim] = (query_grad * scale).astype(half)
        if first == 0:
            key_sum[...] = key_term
            value_sum[...] = value_term
        else:
            key_sum[...] += key_term
            value_sum[...] += value_term
    out_ref[:, head_dim : 2 * head_dim] = (key_sum[...] * scale).astype(half)
    out_ref[:, 2 * head_dim :] = value_sum[...].astype(half)


def attend_backward(
    projected, grad_mixed, totals, slopes, prefixes, own_heads, head_dim, depth, seq_rows
):
    cores = prefixes.shape[0]
    length = projected.shape[0] // cores
    block = min(256, length)
    scores = cores * own_heads * length * length
    return pl.pallas_call(
        functools.partial(backward_kernel, depth, seq_rows, block),
        grid=(cores, own_heads),
        out_shape=jax.ShapeDtypeStruct(projected.shape, projected.dtype),
        in_specs=[
            pl.BlockSpec(memory_space=pltpu.SMEM),
            pl.BlockSpec(memory_space=pltpu.SMEM),
            pl.BlockSpec((length, 3 * head_dim), lambda s, h: (s, h)),
            pl.BlockSpec((length, head_dim), lambda s, h: (s, h)),
            pl.BlockSpec((1, 1, length), lambda s, h: (s * own_heads + h, 0, 0)),
        ],
        out_specs=pl.BlockSpec((length, 3 * head_dim), lambda s, h: (s, h)),
        scratch_shapes=[
            pltpu.VMEM((length, head_dim), jnp.float32),
            pltpu.VMEM((length, head_dim), jnp.float32),
        ],
        compiler_params=pltpu.CompilerParams(vmem_limit_bytes=48 * 2**20),
        cost_estimate=pl.CostEstimate(
            flops=10 * scores * head_dim,
            bytes_accessed=2 * projected.size * 2,
            transcendentals=scores,
        ),
        name="attend_backward",
    )(prefixes, slopes, projected, grad_mixed, totals)


def planar(
    hidden,
    prefix_lengths,
    cotangent,
    first_gain,
    first_shift,
    triple_weight,
    pair_bias,
    dense_weight,
    dense_shift,
    second_gain,
    second_shift,
    expand_weight,
    expand_shift,
    shrink_weight,
    shrink_shift,
):
    wide = jnp.float32
    half = jnp.bfloat16
    cores = lax.axis_size("dp")
    depth = lax.axis_size("z")
    rows_y = lax.axis_size("y")
    rows_x = lax.axis_size("x")
    plane = rows_y * rows_x
    core = lax.axis_index("dp")
    at_y = lax.axis_index("y")
    at_x = lax.axis_index("x")
    place = at_y * rows_x + at_x
    seq_rows = hidden.shape[2]
    width = hidden.shape[3]
    head_dim = triple_weight.shape[3]
    heads = triple_weight.shape[1]
    own_heads = heads // plane
    own_rows = seq_rows * depth
    units = expand_weight.shape[1]
    own_units = units // plane
    row_block = expand_weight.shape[0]
    shrink_rows = shrink_weight.shape[0]

    pieces = [
        first_gain,
        first_shift,
        dense_shift,
        second_gain,
        second_shift,
        shrink_shift,
        pair_bias,
        expand_shift,
    ]
    piece_total = sum(p.shape[0] for p in pieces)
    lanes = 128
    vector_rows = -(-piece_total // (lanes * 16)) * 16
    vector_tile = jnp.pad(
        jnp.concatenate(pieces), (0, vector_rows * lanes - piece_total)
    ).reshape(vector_rows, lanes)
    steps = (3 * head_dim, shrink_rows)
    inputs, dense_turned, triple_turned, expand_turned, packed = exchange(
        3,
        hidden[:, 0],
        dense_weight,
        triple_weight.reshape(row_block, heads * 3 * head_dim),
        expand_weight,
        vector_tile,
        steps,
    )
    packed = (
        packed.reshape(depth, cores, plane, vector_rows * lanes)
        .transpose(1, 0, 2, 3)
        .reshape(-1, vector_rows * lanes)
    )
    vectors = []
    offset = 0
    for piece in pieces:
        vectors.append(packed[:, offset : offset + piece.shape[0]].reshape(-1).astype(wide))
        offset += piece.shape[0]
    gain_one, shift_one, dense_bias, gain_two, shift_two, shrink_bias, pair_full, unit_full = vectors
    pair_heads = pair_full.reshape(cores, own_heads, rows_x, rows_y, 2, head_dim)[
        core, :, 1 - at_x, at_y
    ]
    triple_bias = jnp.stack(
        [pair_heads[:, 0], jnp.zeros_like(pair_heads[:, 0]), pair_heads[:, 1]], 1
    ).reshape(-1)
    unit_bias = unit_full.reshape(cores, depth, plane, shrink_rows)[core, :, place].reshape(-1)

    triple_own = lax.all_gather(
        triple_turned.reshape(-1, triple_turned.shape[2]), "z", axis=0, tiled=True
    )
    inputs = inputs.reshape(own_rows, width).astype(wide)

    normed_own = layer_norm(inputs, gain_one, shift_one).astype(half)
    normed, dense_own = gather_tokens(1, normed_own, dense_turned, True)
    dense_own = dense_own.reshape(own_heads * head_dim, width)
    expand_own = lax.all_gather(
        after(expand_turned, normed).reshape(-1, own_units), "z", axis=0, tiled=True
    )
    projected = (
        jnp.dot(normed, triple_own, preferred_element_type=wide) + triple_bias
    ).astype(half)

    shrink_own = lax.all_gather(after(shrink_weight, projected), "z", axis=0, tiled=True)
    head_index = core * heads + jnp.arange(own_heads) * plane + (1 - at_x) * rows_y + at_y
    slopes = jnp.power(
        jnp.float32(2.0), -8.0 * (head_index.astype(wide) + 1.0) / (heads * cores)
    )
    at_z = lax.axis_index("z")
    prefixes = lax.dynamic_index_in_dim(prefix_lengths, at_z, 0, False)
    mixed, log_totals = attend_forward(
        projected, slopes, prefixes, own_heads, head_dim, depth, seq_rows
    )
    (dense_sum,) = scatter_tokens(2, mixed, dense_own)
    middle = inputs + dense_sum + dense_bias
    normed_two_own, norm_two_pull = jax.vjp(layer_norm, middle, gain_two, shift_two)
    normed_two, upstream = gather_tokens(6, normed_two_own.astype(half), cotangent[:, 0])
    upstream = upstream.reshape(own_rows, width)
    hidden_pre = jnp.dot(normed_two, expand_own, preferred_element_type=wide) + unit_bias
    (upstream_all,) = gather_tokens(5, upstream)
    activated, gelu_pull = jax.vjp(gelu_tanh, hidden_pre)
    activated = activated.astype(half)
    shrink_term = jnp.einsum(
        "tu,td->ud", activated, upstream_all, preferred_element_type=wide
    ).astype(half)
    shrink_own = after(shrink_own, shrink_term)
    grad_act = jnp.einsum("tf,uf->tu", upstream_all, shrink_own, preferred_element_type=wide)
    grad_pre = gelu_pull(grad_act)[0].astype(half)
    shrink_grad = lax.psum_scatter(shrink_term, "z", scatter_dimension=0, tiled=True)
    feed_sum, expand_term = scatter_tokens(
        8, after(activated, shrink_term), shrink_own, term=(normed_two, grad_pre)
    )
    expand_turned = lax.psum_scatter(expand_term, "z", scatter_dimension=0, tiled=True)
    layer_output = (middle + feed_sum + shrink_bias).astype(half)

    (norm_two_sum,) = scatter_tokens(9, after(grad_pre, feed_sum), expand_own, True)
    grad_norm_two, gain_two_term, shift_two_term = norm_two_pull(norm_two_sum)
    grad_middle = upstream.astype(wide) + grad_norm_two
    branch_own = grad_middle.astype(half)
    branch, layer_output = gather_tokens(
        6, branch_own, layer_output.reshape(depth, seq_rows, width)
    )

    grad_mixed = jnp.einsum("tf,ef->te", branch, dense_own, preferred_element_type=wide).astype(
        half
    )
    dense_term = jnp.einsum("te,tf->ef", mixed, branch, preferred_element_type=wide).astype(half)
    dense_turned = lax.psum_scatter(dense_term, "z", scatter_dimension=0, tiled=True)
    grad_project = attend_backward(
        projected,
        after(grad_mixed, dense_term),
        log_totals,
        slopes,
        prefixes,
        own_heads,
        head_dim,
        depth,
        seq_rows,
    )
    triple_term = jnp.einsum(
        "td,tc->dc", normed, grad_project, preferred_element_type=wide
    ).astype(half)
    triple_turned = lax.psum_scatter(triple_term, "z", scatter_dimension=0, tiled=True)
    (norm_one_sum,) = scatter_tokens(10, after(grad_project, triple_term), triple_own, True)
    grad_norm_one, gain_one_term, shift_one_term = jax.vjp(
        layer_norm, inputs, gain_one, shift_one
    )[1](norm_one_sum)
    hidden_grad = (grad_middle + grad_norm_one).astype(half)
    head_sums = jnp.sum(grad_project, 0, dtype=wide).reshape(own_heads, 3, head_dim)
    pair_term = jnp.stack([head_sums[:, 0], head_sums[:, 2]], 1)
    pair_zero = jnp.zeros((cores, own_heads, rows_x, rows_y, 2, head_dim), wide)
    pair_wide = lax.dynamic_update_slice(
        pair_zero, pair_term[None, :, None, None], (core, 0, 1 - at_x, at_y, 0, 0)
    ).reshape(-1)
    unit_term = jnp.sum(grad_pre, 0, dtype=wide).reshape(1, depth, 1, shrink_rows)
    unit_wide = lax.dynamic_update_slice(
        jnp.zeros((cores, depth, plane, shrink_rows), wide), unit_term, (core, 0, place, 0)
    ).reshape(-1)
    terms = [
        gain_one_term,
        shift_one_term,
        jnp.sum(branch_own, 0, dtype=wide),
        gain_two_term,
        shift_two_term,
        jnp.sum(upstream, 0, dtype=wide),
        pair_wide,
        unit_wide,
    ]
    devices = cores * depth * plane
    term_rows = -(-piece_total // (lanes * 8)) * 8
    term_tiles = jnp.pad(
        jnp.concatenate([t.reshape(devices, -1) for t in terms], 1),
        ((0, 0), (0, term_rows * lanes - piece_total)),
    )
    term_tiles = (
        term_tiles.reshape(cores, depth, plane, term_rows, lanes)
        .transpose(0, 2, 1, 3, 4)
        .reshape(cores * plane, depth, term_rows, lanes)
    )
    hidden_grad, dense_grad, triple_grad, expand_grad, summed = exchange(
        4,
        hidden_grad.reshape(depth, seq_rows, width),
        dense_turned,
        triple_turned.reshape(plane, row_block, -1),
        expand_turned.reshape(plane, row_block, own_units),
        term_tiles,
        steps,
        last=((own_heads, (2, 0, 3, 1)), (depth, (0, 1, 2, 3))),
    )
    layer_output = layer_output[:, None]
    hidden_grad = hidden_grad[:, None]
    triple_grad = triple_grad.astype(wide).reshape(row_block, heads, 3, head_dim)
    summed = summed.reshape(-1)
    vector_grads = []
    offset = 0
    for piece in pieces:
        vector_grads.append(summed[offset : offset + piece.shape[0]])
        offset += piece.shape[0]
    return (
        layer_output,
        hidden_grad,
        vector_grads[0],
        vector_grads[1],
        triple_grad,
        vector_grads[6],
        dense_grad.astype(wide),
        vector_grads[2],
        vector_grads[3],
        vector_grads[4],
        expand_grad.astype(wide),
        vector_grads[7],
        shrink_grad.astype(wide),
        vector_grads[5],
    )


def layer(*args):
    return planar(*args)


def solution(mesh):
    depth = 4
    sides = (2, 2)
    planar_plan = mesh.shape["seq"] == depth * sides[0] * sides[1]
    if planar_plan:
        grid = Mesh(
            mesh.devices.reshape(mesh.shape["dp"], depth, *sides), ("dp", "z", "y", "x")
        )
        seq = ("z", "y", "x")
    else:
        grid = mesh
        seq = ("seq",)
    tokens = P(None, "dp", seq, None)
    vector = P(("dp",) + seq)
    matrix = P(("dp",) + seq, None)
    placed = (
        tokens,
        P(),
        tokens,
        vector,
        vector,
        P(seq, "dp", None, None),
        vector,
        matrix,
        vector,
        vector,
        vector,
        P(seq, "dp"),
        vector,
        matrix,
        vector,
    )
    results = (
        tokens,
        tokens,
        vector,
        vector,
        P(seq, "dp", None, None),
        vector,
        matrix,
        vector,
        vector,
        vector,
        P(seq, "dp"),
        vector,
        matrix,
        vector,
    )
    return jax.shard_map(
        layer if planar_plan else shards,
        mesh=grid,
        in_specs=placed,
        out_specs=results,
        check_vma=False,
    )
```

```python
import functools
import math

import jax
import jax.numpy as jnp
from jax import lax
from jax.experimental import pallas as pl
from jax.experimental.pallas import tpu as pltpu
from jax.sharding import Mesh
from jax.sharding import PartitionSpec as P


EPSILON = 1e-05
GELU_SCALE = 0.7978845608028654


def layer_norm(inputs, norm_gain, norm_shift):
    centered = inputs - jnp.mean(inputs, -1, keepdims=True)
    variance = jnp.mean(centered * centered, -1, keepdims=True)
    return centered * lax.rsqrt(variance + EPSILON) * norm_gain + norm_shift


def gelu_tanh(values):
    return (
        0.5 * values * (1.0 + jnp.tanh(GELU_SCALE * (values + 0.044715 * values * values * values)))
    )


def split_norm(inputs, gain_rows, shift_rows):
    return layer_norm(inputs, gain_rows[None, :, None, :], shift_rows[None, :, None, :])


def place_half(values, half_index, group_count):
    chosen = (jnp.arange(group_count, dtype=jnp.int32) == half_index).astype(values.dtype)
    return (chosen[:, None] * values.reshape(1, -1)).reshape(-1)


def shards(
    hidden,
    prefix_lengths,
    cotangent,
    first_gain,
    first_shift,
    triple_weight,
    pair_bias,
    dense_weight,
    dense_shift,
    second_gain,
    second_shift,
    expand_weight,
    expand_shift,
    shrink_weight,
    shrink_shift,
):
    wide_type = jnp.float32
    half_type = jnp.bfloat16
    seq_count = lax.axis_size("seq")
    group_count = lax.axis_size("dp")
    dp_index = lax.axis_index("dp")
    seq_index = lax.axis_index("seq")
    micro_count = hidden.shape[0]
    seq_rows = hidden.shape[2]
    model_width = hidden.shape[3]
    seq_length = seq_rows * seq_count
    local_heads = triple_weight.shape[1]
    head_dim = triple_weight.shape[3]
    head_total = local_heads * group_count
    pair_local = micro_count * group_count * local_heads // seq_count
    unit_local = expand_weight.shape[1]
    project_width = 3 * local_heads * head_dim
    token_total = micro_count * group_count * seq_rows
    score_scale = 1.0 / math.sqrt(head_dim)
    block_rows = min(512, seq_length)
    block_count = seq_length // block_rows
    key_pos = jnp.arange(seq_length, dtype=jnp.int32)
    gathered = (
        lax.all_gather(triple_weight, "seq", axis=0, tiled=True),
        lax.all_gather(dense_weight, "seq", axis=0, tiled=True),
        lax.all_gather(expand_weight, "seq", axis=0, tiled=True),
        lax.all_gather(shrink_weight, "seq", axis=0, tiled=True),
        lax.all_gather(first_gain, "seq", axis=0, tiled=True),
        lax.all_gather(first_shift, "seq", axis=0, tiled=True),
        lax.all_gather(pair_bias, "seq", axis=0, tiled=True),
        lax.all_gather(dense_shift, "seq", axis=0, tiled=True),
        lax.all_gather(second_gain, "seq", axis=0, tiled=True),
        lax.all_gather(second_shift, "seq", axis=0, tiled=True),
        lax.all_gather(expand_shift, "seq", axis=0, tiled=True),
        lax.all_gather(shrink_shift, "seq", axis=0, tiled=True),
    )
    triple_full, dense_full, expand_full, shrink_full = (
        gathered[0],
        gathered[1],
        gathered[2],
        gathered[3],
    )
    row_sets = (
        lax.all_gather(hidden, "dp", axis=1, tiled=True),
        lax.all_gather(cotangent, "dp", axis=1, tiled=True),
        lax.all_gather(gathered[4], "dp", axis=0, tiled=True),
        lax.all_gather(gathered[5], "dp", axis=0, tiled=True),
        lax.all_gather(gathered[6], "dp", axis=0, tiled=True),
        lax.all_gather(gathered[7], "dp", axis=0, tiled=True),
        lax.all_gather(gathered[8], "dp", axis=0, tiled=True),
        lax.all_gather(gathered[9], "dp", axis=0, tiled=True),
        lax.all_gather(gathered[10], "dp", axis=0, tiled=True),
        lax.all_gather(gathered[11], "dp", axis=0, tiled=True),
    )
    hidden_both = row_sets[0]
    upstream_low = row_sets[1]
    gain_one, shift_one, pair_full, dense_bias, gain_two, shift_two, expand_bias, shrink_bias = [
        vector.astype(wide_type) for vector in row_sets[2:]
    ]
    inputs_both = hidden_both.astype(wide_type)
    normed_low = layer_norm(inputs_both, gain_one, shift_one).astype(half_type)
    pair_heads = lax.dynamic_slice_in_dim(
        pair_full.reshape(head_total, 2, head_dim), dp_index * local_heads, local_heads, 0
    )
    triple_bias = jnp.stack(
        [pair_heads[:, 0], jnp.zeros_like(pair_heads[:, 0]), pair_heads[:, 1]], 0
    )
    projected = jnp.einsum(
        "mstd,dhce->cmshte", normed_low, triple_full, preferred_element_type=wide_type
    )
    projected = projected + triple_bias[:, None, None, :, None, :]
    project_low = projected.astype(half_type).reshape(3, seq_count, pair_local, seq_rows, head_dim)
    pair_rows = lax.all_to_all(project_low, "seq", split_axis=1, concat_axis=3, tiled=True)[:, 0]
    query_all, key_all, value_all = (pair_rows[0], pair_rows[1], pair_rows[2])
    pair_index = seq_index * pair_local + jnp.arange(pair_local, dtype=jnp.int32)
    head_index = dp_index * local_heads + pair_index % local_heads
    sequence_index = pair_index // local_heads
    slopes = jnp.power(jnp.float32(2.0), -8.0 * (head_index.astype(wide_type) + 1.0) / head_total)
    prefix_flat = prefix_lengths.reshape(-1)
    prefix_slots = jnp.arange(prefix_flat.shape[0], dtype=jnp.int32)
    prefixes = jnp.sum(
        jnp.where(prefix_slots[None, :] == sequence_index[:, None], prefix_flat[None, :], 0), 1
    )

    def block_scores(pair_item, first_row):
        query_block = lax.dynamic_slice_in_dim(
            lax.dynamic_index_in_dim(query_all, pair_item, 0, False), first_row, block_rows, 0
        )
        keys_item = lax.dynamic_index_in_dim(key_all, pair_item, 0, False)
        head_slope = lax.dynamic_index_in_dim(slopes, pair_item, 0, False)
        prefix = lax.dynamic_index_in_dim(prefixes, pair_item, 0, False)
        query_pos = first_row + jnp.arange(block_rows, dtype=jnp.int32)
        raw_scores = (
            jnp.einsum("qe,ke->qk", query_block, keys_item, preferred_element_type=wide_type)
            * score_scale
        )
        distance = jnp.abs(query_pos[:, None] - key_pos[None, :]).astype(wide_type)
        raw_scores = raw_scores - head_slope * distance
        allowed = (key_pos[None, :] <= query_pos[:, None]) | (key_pos[None, :] < prefix)
        return (query_block, jnp.where(allowed, raw_scores, jnp.float32(-1e30)))

    def forward_block(flat_index):
        pair_item = flat_index // block_count
        first_row = flat_index % block_count * block_rows
        _, scores = block_scores(pair_item, first_row)
        row_max = jnp.max(scores, -1, keepdims=True)
        powers = jnp.exp(scores - row_max)
        row_total = jnp.sum(powers, -1, keepdims=True)
        probs_low = (powers / row_total).astype(half_type)
        values_item = lax.dynamic_index_in_dim(value_all, pair_item, 0, False)
        mixed = jnp.dot(probs_low, values_item, preferred_element_type=wide_type).astype(half_type)
        return (mixed, (row_max + jnp.log(row_total))[:, 0])

    mixed_blocks, log_blocks = lax.map(
        forward_block, jnp.arange(pair_local * block_count, dtype=jnp.int32)
    )
    mixed_pairs = mixed_blocks.reshape(pair_local, seq_count, seq_rows, head_dim)
    log_totals = log_blocks.reshape(pair_local, seq_length)
    mixed_home = lax.all_to_all(mixed_pairs, "seq", split_axis=1, concat_axis=0, tiled=True)
    mixed_tokens = jnp.transpose(
        mixed_home.reshape(micro_count, group_count, local_heads, seq_rows, head_dim),
        (0, 1, 3, 2, 4),
    ).reshape(micro_count, group_count, seq_rows, local_heads * head_dim)
    dense_part = jnp.einsum(
        "mstk,kf->mstf", mixed_tokens, dense_full, preferred_element_type=wide_type
    )
    attention_sum = lax.psum(dense_part.astype(jnp.bfloat16), "dp").astype(jnp.float32)
    middle = inputs_both + attention_sum + dense_bias
    gain_rows_two = jnp.broadcast_to(gain_two[None, :], (group_count, model_width))
    shift_rows_two = jnp.broadcast_to(shift_two[None, :], (group_count, model_width))
    normed_two, norm_two_pull = jax.vjp(split_norm, middle, gain_rows_two, shift_rows_two)
    normed_two_low = normed_two.astype(half_type)
    unit_bias = lax.dynamic_slice_in_dim(expand_bias, dp_index * unit_local, unit_local, 0)
    hidden_pre = (
        jnp.einsum("mstd,df->mstf", normed_two_low, expand_full, preferred_element_type=wide_type)
        + unit_bias
    )
    activated_value, gelu_pull = jax.vjp(gelu_tanh, hidden_pre)
    activated_low = activated_value.astype(half_type)
    feed_part = jnp.einsum(
        "mstf,fd->mstd", activated_low, shrink_full, preferred_element_type=wide_type
    )
    feed_sum = lax.psum_scatter(
        feed_part.astype(jnp.bfloat16), "dp", scatter_dimension=1, tiled=True
    ).astype(jnp.float32)
    middle_own = lax.dynamic_slice_in_dim(middle, dp_index, 1, 1)
    layer_output = (middle_own + feed_sum + shrink_bias).astype(half_type)
    triple_back, dense_back, expand_back, shrink_back = (
        lax.all_gather(triple_weight, "seq", axis=0, tiled=True),
        lax.all_gather(dense_weight, "seq", axis=0, tiled=True),
        lax.all_gather(expand_weight, "seq", axis=0, tiled=True),
        lax.all_gather(shrink_weight, "seq", axis=0, tiled=True),
    )
    grad_act = jnp.einsum(
        "mstd,fd->mstf", upstream_low, shrink_back, preferred_element_type=wide_type
    )
    grad_pre_low = gelu_pull(grad_act)[0].astype(half_type)
    norm_two_part = jnp.einsum(
        "mstf,df->mstd", grad_pre_low, expand_back, preferred_element_type=wide_type
    )
    grad_normed_two = lax.psum(norm_two_part.astype(jnp.bfloat16), "dp").astype(jnp.float32)
    grad_middle_norm, grad_gain_rows_two, grad_shift_rows_two = norm_two_pull(grad_normed_two)
    grad_middle = upstream_low.astype(wide_type) + grad_middle_norm
    grad_branch_low = grad_middle.astype(half_type)
    go_pairs = jnp.einsum(
        "mstf,hef->mshte",
        grad_branch_low,
        dense_back.reshape(local_heads, head_dim, model_width),
        preferred_element_type=wide_type,
    ).astype(half_type)
    go_pairs = go_pairs.reshape(seq_count, pair_local, seq_rows, head_dim)
    grad_mixed_pairs = lax.all_to_all(go_pairs, "seq", split_axis=0, concat_axis=2, tiled=True)[0]

    def backward_item(pair_item):
        keys_item = lax.dynamic_index_in_dim(key_all, pair_item, 0, False)
        values_item = lax.dynamic_index_in_dim(value_all, pair_item, 0, False)
        grad_mixed_item = lax.dynamic_index_in_dim(grad_mixed_pairs, pair_item, 0, False)
        totals_item = lax.dynamic_index_in_dim(log_totals, pair_item, 0, False)

        def backward_block(running, block_index):
            key_grad, value_grad = running
            first_row = block_index * block_rows
            query_block, scores = block_scores(pair_item, first_row)
            soft_probs = jnp.exp(
                scores - lax.dynamic_slice_in_dim(totals_item, first_row, block_rows, 0)[:, None]
            )
            grad_block = lax.dynamic_slice_in_dim(grad_mixed_item, first_row, block_rows, 0)
            grad_probs = jnp.einsum(
                "qe,ke->qk", grad_block, values_item, preferred_element_type=wide_type
            )
            row_inner = jnp.sum(grad_probs * soft_probs, -1, keepdims=True)
            grad_scores_low = (soft_probs * (grad_probs - row_inner)).astype(half_type)
            query_grad = (
                jnp.dot(grad_scores_low, keys_item, preferred_element_type=wide_type) * score_scale
            )
            key_grad = (
                key_grad
                + jnp.einsum(
                    "qk,qe->ke", grad_scores_low, query_block, preferred_element_type=wide_type
                )
                * score_scale
            )
            value_grad = value_grad + jnp.einsum(
                "qk,qe->ke",
                soft_probs.astype(half_type),
                grad_block,
                preferred_element_type=wide_type,
            )
            return ((key_grad, value_grad), query_grad)

        zero_rows = jnp.zeros((seq_length, head_dim), wide_type)
        (key_grad, value_grad), query_grads = lax.scan(
            backward_block, (zero_rows, zero_rows), jnp.arange(block_count, dtype=jnp.int32)
        )
        return jnp.stack(
            [query_grads.reshape(seq_length, head_dim), key_grad, value_grad], 0
        ).astype(half_type)

    grad_pairs = lax.map(backward_item, jnp.arange(pair_local, dtype=jnp.int32))
    grad_split = grad_pairs.reshape(pair_local, 3, seq_count, seq_rows, head_dim)
    grad_home = lax.all_to_all(grad_split, "seq", split_axis=2, concat_axis=0, tiled=True)
    grad_project_low = jnp.transpose(
        grad_home.reshape(micro_count, group_count, local_heads, 3, seq_rows, head_dim),
        (0, 1, 4, 2, 3, 5),
    ).reshape(micro_count, group_count, seq_rows, project_width)
    norm_one_part = jnp.einsum(
        "mstc,dc->mstd",
        grad_project_low,
        triple_back.reshape(model_width, project_width),
        preferred_element_type=wide_type,
    )
    grad_normed_one = lax.psum_scatter(
        norm_one_part.astype(jnp.bfloat16), "dp", scatter_dimension=1, tiled=True
    ).astype(jnp.float32)
    inputs_own = hidden.astype(wide_type)
    grad_inputs_norm, grad_gain_one, grad_shift_one = jax.vjp(
        layer_norm, inputs_own, gain_one, shift_one
    )[1](grad_normed_one)
    grad_middle_own = lax.dynamic_slice_in_dim(grad_middle, dp_index, 1, 1)
    hidden_grad = (grad_middle_own + grad_inputs_norm).astype(half_type)
    head_sums = jnp.sum(
        grad_project_low.reshape(micro_count, group_count, seq_rows, local_heads, 3, head_dim),
        (0, 1, 2),
        dtype=wide_type,
    )
    pair_grad = place_half(jnp.stack([head_sums[:, 0], head_sums[:, 2]], 1), dp_index, group_count)
    unit_grad = place_half(jnp.sum(grad_pre_low, (0, 1, 2), dtype=wide_type), dp_index, group_count)
    dense_shift_term = jnp.sum(
        lax.dynamic_slice_in_dim(grad_branch_low, dp_index, 1, 1), (0, 1, 2), dtype=wide_type
    )
    shrink_shift_term = jnp.sum(cotangent, (0, 1, 2), dtype=wide_type)
    gain_two_term = lax.dynamic_index_in_dim(grad_gain_rows_two, dp_index, 0, False)
    shift_two_term = lax.dynamic_index_in_dim(grad_shift_rows_two, dp_index, 0, False)
    vector_sums = (
        lax.psum_scatter(grad_gain_one, ("dp", "seq"), scatter_dimension=0, tiled=True),
        lax.psum_scatter(grad_shift_one, ("dp", "seq"), scatter_dimension=0, tiled=True),
        lax.psum_scatter(pair_grad, ("dp", "seq"), scatter_dimension=0, tiled=True),
        lax.psum_scatter(dense_shift_term, ("dp", "seq"), scatter_dimension=0, tiled=True),
        lax.psum_scatter(gain_two_term, ("dp", "seq"), scatter_dimension=0, tiled=True),
        lax.psum_scatter(shift_two_term, ("dp", "seq"), scatter_dimension=0, tiled=True),
        lax.psum_scatter(unit_grad, ("dp", "seq"), scatter_dimension=0, tiled=True),
        lax.psum_scatter(shrink_shift_term, ("dp", "seq"), scatter_dimension=0, tiled=True),
    )
    normed_flat = normed_low.reshape(token_total, model_width)
    project_flat = grad_project_low.reshape(token_total, project_width)
    normed_two_flat = normed_two_low.reshape(token_total, model_width)
    pre_flat = grad_pre_low.reshape(token_total, unit_local)
    column_sums = lax.psum_scatter(
        jnp.concatenate(
            [
                jnp.einsum(
                    "tr,tc->rc", normed_flat, project_flat, preferred_element_type=wide_type
                ),
                jnp.einsum(
                    "tr,tc->rc", normed_two_flat, pre_flat, preferred_element_type=wide_type
                ),
            ],
            1,
        ),
        "seq",
        scatter_dimension=0,
        tiled=True,
    )
    triple_grad = column_sums[:, :project_width].reshape(
        model_width // seq_count, local_heads, 3, head_dim
    )
    expand_grad = column_sums[:, project_width:]
    dense_rows = dense_weight.shape[0]
    shrink_rows = shrink_weight.shape[0]
    row_block = dense_rows + shrink_rows
    mixed_flat = mixed_tokens.reshape(token_total, local_heads * head_dim)
    branch_flat = grad_branch_low.reshape(token_total, model_width)
    active_flat = activated_low.reshape(token_total, unit_local)
    upstream_flat = upstream_low.reshape(token_total, model_width)
    block_number = row_block * lax.axis_size("seq") // row_block
    dense_term = jnp.einsum("tr,td->rd", mixed_flat, branch_flat, preferred_element_type=wide_type)
    shrink_term = jnp.einsum(
        "tr,td->rd", active_flat, upstream_flat, preferred_element_type=wide_type
    )
    row_sums = lax.psum_scatter(
        jnp.concatenate(
            [
                dense_term.reshape(block_number, dense_rows, model_width),
                shrink_term.reshape(block_number, shrink_rows, model_width),
            ],
            1,
        ).reshape(row_block * lax.axis_size("seq"), model_width),
        "seq",
        scatter_dimension=0,
        tiled=True,
    )
    dense_grad = row_sums[:dense_rows]
    shrink_grad = row_sums[dense_rows:]
    return (
        layer_output,
        hidden_grad,
        vector_sums[0],
        vector_sums[1],
        triple_grad,
        vector_sums[2],
        dense_grad,
        vector_sums[3],
        vector_sums[4],
        vector_sums[5],
        expand_grad,
        vector_sums[6],
        shrink_grad,
        vector_sums[7],
    )


CHUNKS = 4
LOG2E = 1.4426950408889634
MESH = pl.DeviceIdType.MESH


def remote(src, dst, send, recv, peer):
    return pltpu.make_async_remote_copy(
        src_ref=src,
        dst_ref=dst,
        send_sem=send,
        recv_sem=recv,
        device_id=peer,
        device_id_type=MESH,
    )


def greet(peers):
    barrier = pltpu.get_barrier_semaphore()
    for peer in peers:
        pl.semaphore_signal(barrier, inc=1, device_id=peer, device_id_type=MESH)
    pl.semaphore_wait(barrier, len(peers))


class Corner:
    def __init__(self):
        self.c = lax.axis_index("dp")
        self.y = lax.axis_index("y")
        self.x = lax.axis_index("x")
        self.ax = self.x + (1 - self.c) * (1 - 2 * self.x)
        self.ay = self.y + self.c * (1 - 2 * self.y)
        self.bx = self.x + self.c * (1 - 2 * self.x)
        self.by = self.y + (1 - self.c) * (1 - 2 * self.y)
        self.dx = 1 - self.x
        self.dy = 1 - self.y
        self.peer_a = {"y": self.ay, "x": self.ax}
        self.peer_b = {"y": self.by, "x": self.bx}
        self.sibling = {"dp": 1 - self.c}

    def slots(self, core):
        return [
            (core * 2 + y) * 2 + x
            for y, x in (
                (self.dy, self.dx),
                (self.by, self.bx),
                (self.ay, self.ax),
                (self.y, self.x),
            )
        ]


def gather_kernel(deep, whole, *refs):
    if deep:
        rows_ref, deep_ref, all_ref, moved_ref, local_sem, send, recv, deep_send, deep_recv = refs
    else:
        rows_ref, all_ref, local_sem, send, recv = refs
    at = Corner()
    slot_d, slot_b, slot_a, me = at.slots(at.c)
    step = rows_ref.shape[0] // CHUNKS
    peers = [at.peer_a, at.peer_b, at.sibling]
    sent, moves = [], []
    if deep:
        z = lax.axis_index("z")
        plane_at = [lax.rem(z + i, 4) for i in range(4)]
        peers += [{"z": plane_at[i]} for i in range(1, 4)]
    greet(peers)
    locals_ = [pltpu.make_async_copy(rows_ref, all_ref.at[me], local_sem.at[0])]
    if deep:
        block = deep_ref if whole else deep_ref.at[z]
        locals_.append(pltpu.make_async_copy(block, moved_ref.at[z], local_sem.at[1]))
    for one in locals_:
        one.start()

    def copy(kind, k, slot, peer):
        part = pl.ds(k * step, step)
        src = rows_ref.at[part] if kind < 3 else all_ref.at[slot, part]
        return remote(src, all_ref.at[slot, part], send.at[kind, k], recv.at[kind, k], peer)

    def arrived(kind, k, slot, peer):
        part = pl.ds(k * step, step)
        block = all_ref.at[slot, part]
        remote(block, block, send.at[kind, k], recv.at[kind, k], peer).wait_recv()

    def start(kind, k, slot, peer):
        one = copy(kind, k, slot, peer)
        one.start()
        sent.append(one)

    for i in range(1, 4) if deep else ():
        sems = deep_send.at[i - 1], deep_recv.at[i - 1]
        block = deep_ref if whole else deep_ref.at[plane_at[i]]
        one = remote(block, moved_ref.at[z], *sems, {"z": plane_at[i]})
        one.start()
        sent.append(one)
        landing = moved_ref.at[plane_at[4 - i]]
        moves.append(remote(landing, landing, *sems, {"z": plane_at[i]}))
    for k in range(CHUNKS):
        start(0, k, me, at.peer_a)
        start(1, k, me, at.peer_b)
    for k in range(CHUNKS):
        start(2, k, me, at.sibling)
    for k in range(CHUNKS):
        arrived(0, k, slot_a, at.peer_a)
        start(3, k, slot_a, at.peer_b)
        start(4, k, slot_a, at.sibling)
    for k in range(CHUNKS):
        arrived(1, k, slot_b, at.peer_b)
        start(5, k, slot_b, at.sibling)
    for k in range(CHUNKS):
        arrived(3, k, slot_d, at.peer_b)
        start(6, k, slot_d, at.sibling)
    other_d, other_b, other_a, other_me = at.slots(1 - at.c)
    for k in range(CHUNKS):
        arrived(2, k, other_me, at.sibling)
        arrived(4, k, other_b, at.sibling)
        arrived(5, k, other_a, at.sibling)
        arrived(6, k, other_d, at.sibling)
    for one in moves:
        one.wait_recv()
    for one in sent:
        one.wait_send()
    for one in locals_:
        one.wait()


def gather_tokens(identity, rows, deep=None, whole=False):
    count, width = rows.shape
    operands = [rows]
    shapes = [jax.ShapeDtypeStruct((8, count, width), rows.dtype)]
    scratch = [
        pltpu.SemaphoreType.DMA((2,)),
        pltpu.SemaphoreType.DMA((7, CHUNKS)),
        pltpu.SemaphoreType.DMA((7, CHUNKS)),
    ]
    if deep is not None:
        operands.append(deep)
        moved_shape = (4,) + deep.shape if whole else deep.shape
        shapes.append(jax.ShapeDtypeStruct(moved_shape, deep.dtype))
        scratch += [pltpu.SemaphoreType.DMA((3,)), pltpu.SemaphoreType.DMA((3,))]
    all_rows, *moved = pl.pallas_call(
        functools.partial(gather_kernel, deep is not None, whole),
        out_shape=shapes,
        in_specs=[pl.BlockSpec(memory_space=pl.ANY)] * len(operands),
        out_specs=[pl.BlockSpec(memory_space=pl.ANY)] * len(shapes),
        scratch_shapes=scratch,
        compiler_params=pltpu.CompilerParams(
            collective_id=identity, has_side_effects=True
        ),
        cost_estimate=pl.CostEstimate(
            flops=0, bytes_accessed=16 * count * width * 4, transcendentals=0
        ),
        name="gather_tokens",
    )(*operands)
    return (all_rows.reshape(8 * count, width), *moved)


def after(value, *others):
    return lax.optimization_barrier((value, *others))[0]


def scatter_kernel(turned, term, left_ref, right_ref, *refs):
    if term:
        rows_ref, grads_ref, own_ref, term_ref, *refs = refs
    else:
        own_ref, *refs = refs
    part_ref, from_core, from_b, from_a, send, recv = refs
    at = Corner()
    slot_d, slot_b, slot_a, me = at.slots(at.c)
    other_d, other_b, other_a, other_me = at.slots(1 - at.c)
    _, width = own_ref.shape
    step = width // CHUNKS
    wide = jnp.float32
    greet([at.peer_a, at.peer_b, at.sibling])
    sent = []

    def start(kind, k, src, dst, peer):
        one = remote(src, dst, send.at[kind, k], recv.at[kind, k], peer)
        one.start()
        sent.append(one)

    def arrived(kind, k, dst, peer):
        remote(dst, dst, send.at[kind, k], recv.at[kind, k], peer).wait_recv()

    def multiply_columns(slot, cols):
        right = right_ref[cols] if turned else right_ref[:, cols]
        product = lax.dot_general(
            left_ref[slot],
            right,
            (((1,), (1 if turned else 0,)), ((), ())),
            preferred_element_type=wide,
        )
        part_ref[slot, :, cols] = product.astype(part_ref.dtype)

    def multiply(slot):
        def columns(t, carry):
            multiply_columns(slot, pl.ds(pl.multiple_of(t * step, step), step))
            return carry

        lax.fori_loop(0, CHUNKS, columns, 0)

    def multiply_term(first, last):
        if not term:
            return
        lanes = min(256, rows_ref.shape[1] // 8)

        def features(t, carry):
            cols = pl.ds(pl.multiple_of(t * lanes, lanes), lanes)
            product = lax.dot_general(
                rows_ref[:, cols],
                grads_ref[...],
                (((0,), (0,)), ((), ())),
                preferred_element_type=wide,
            )
            term_ref[cols] = product.astype(term_ref.dtype)
            return carry

        count = rows_ref.shape[1] // lanes
        lax.fori_loop(count * first // 8, count * last // 8, features, 0)

    def share(q, slot, chunks):
        for k in chunks:
            part = pl.ds(k * step, step)
            start(q, k, part_ref.at[slot, :, part], from_core.at[q, :, part], at.sibling)

    def to_b(q, slot, chunks):
        for k in chunks:
            part = pl.ds(k * step, step)
            arrived(q, k, from_core.at[q, :, part], at.sibling)
            total = part_ref[slot, :, part].astype(wide) + from_core[q, :, part].astype(wide)
            from_core[q, :, part] = total.astype(from_core.dtype)
            start(4 + q, k, from_core.at[q, :, part], from_b.at[q, :, part], at.peer_b)

    everything = range(CHUNKS)
    for k in everything:
        multiply_columns(other_d, pl.ds(k * step, step))
        share(0, other_d, [k])
        multiply_columns(slot_d, pl.ds(k * step, step))
        if k:
            to_b(0, slot_d, [k - 1])
    to_b(0, slot_d, [CHUNKS - 1])
    multiply(other_a)
    share(1, other_a, everything)
    multiply(slot_b)
    to_b(1, slot_b, everything)
    multiply(other_b)
    share(2, other_b, everything)
    multiply(slot_a)
    multiply_term(0, 2)
    for k in everything:
        part = pl.ds(k * step, step)
        arrived(2, k, from_core.at[2, :, part], at.sibling)
        arrived(4, k, from_b.at[0, :, part], at.peer_b)
        total = part_ref[slot_a, :, part].astype(wide) + from_core[2, :, part].astype(wide)
        total = total + from_b[0, :, part].astype(wide)
        from_core[2, :, part] = total.astype(from_core.dtype)
        start(6, k, from_core.at[2, :, part], from_a.at[:, part], at.peer_a)
    multiply(other_me)
    share(3, other_me, everything)
    multiply(me)
    multiply_term(2, 8)
    for k in everything:
        part = pl.ds(k * step, step)
        arrived(3, k, from_core.at[3, :, part], at.sibling)
        arrived(5, k, from_b.at[1, :, part], at.peer_b)
        arrived(6, k, from_a.at[:, part], at.peer_a)
        total = part_ref[me, :, part].astype(wide) + from_core[3, :, part].astype(wide)
        total = total + from_b[1, :, part].astype(wide)
        own_ref[:, part] = total + from_a[:, part].astype(wide)
    for one in sent:
        one.wait_send()


def scatter_tokens(identity, left, right, turned=False, term=()):
    count, depth = left.shape[0] // 8, left.shape[1]
    width = right.shape[0] if turned else right.shape[1]
    half = left.dtype
    shapes = [jax.ShapeDtypeStruct((count, width), jnp.float32)]
    if term:
        shapes.append(jax.ShapeDtypeStruct((term[0].shape[1], term[1].shape[1]), half))
    vmem = pl.BlockSpec(memory_space=pltpu.VMEM)
    return pl.pallas_call(
        functools.partial(scatter_kernel, turned, bool(term)),
        out_shape=shapes,
        in_specs=[vmem] * (2 + len(term)),
        out_specs=[vmem] * len(shapes),
        scratch_shapes=[
            pltpu.VMEM((8, count, width), half),
            pltpu.VMEM((4, count, width), half),
            pltpu.VMEM((2, count, width), half),
            pltpu.VMEM((count, width), half),
            pltpu.SemaphoreType.DMA((7, CHUNKS)),
            pltpu.SemaphoreType.DMA((7, CHUNKS)),
        ],
        compiler_params=pltpu.CompilerParams(
            collective_id=identity, has_side_effects=True, vmem_limit_bytes=58 * 2**20
        ),
        cost_estimate=pl.CostEstimate(
            flops=2 * left.size * width, bytes_accessed=64 * count * width, transcendentals=0
        ),
        name="scatter_tokens",
    )(left.reshape(8, count, depth), right, *term)


def exchange_kernel(last, triple_step, expand_step, *refs):
    refs = list(refs)
    take = lambda n: [refs.pop(0) for _ in range(n)]
    deep_in, turn_in, triple_in, expand_in, vec_in = take(5)
    deep_out, turn_out, triple_out, expand_out, vec_out = take(5)
    if last:
        triple_columns, expand_columns = triple_out, expand_out
        triple_out, expand_out, near, far, here = take(5)
    send, recv, local_sem = take(3)
    c, z = lax.axis_index("dp"), lax.axis_index("z")
    y, x = lax.axis_index("y"), lax.axis_index("x")
    place = y * 2 + x
    rank = c * 4 + place

    def deep(i):
        return lax.rem(z + i, 4)

    def flat(i):
        return lax.rem(place + i, 4)

    def wide(i):
        return lax.rem(rank + i, 8)

    def deep_peer(i):
        return {"z": deep(i)}

    def flat_peer(i):
        return {"y": flat(i) // 2, "x": lax.rem(flat(i), 2)}

    def wide_peer(i):
        return {
            "dp": wide(i) // 4,
            "y": lax.rem(wide(i), 4) // 2,
            "x": lax.rem(wide(i), 2),
        }

    low = lax.rem(z, 2)
    turn_from = {"z": z - low + 1 - x, "x": low}
    turn_to = {"z": z - low + x, "x": 1 - low}
    if last:
        turn_from, turn_to = turn_to, turn_from
    others = range(1, 4)
    greet([deep_peer(i) for i in others] + [wide_peer(i) for i in range(1, 8)])
    sent, waits, kept = [], [], []
    count = [0]

    def post(src, dst, peer, landing):
        k = count[0]
        count[0] += 1
        one = remote(src, dst, send.at[k], recv.at[k], peer)
        one.start()
        sent.append(one)
        return remote(landing, landing, send.at[k], recv.at[k], peer)

    def keep(src, dst):
        one = pltpu.make_async_copy(src, dst, local_sem.at[len(kept)])
        one.start()
        kept.append(one)

    def parts(src, dst, order, block):
        if last:
            return [(src.at[block], dst.at[place])]
        steps = src.shape[1] // 4 // order[0]
        step = order[0]
        return [
            (
                src.at[:, pl.ds(pl.multiple_of((i * 4 + order[1](block)) * step, step), step)],
                dst.at[place, :, pl.ds(i * step, step)],
            )
            for i in range(steps)
        ]

    def turn_columns(src, dst, order):
        for i in others:
            for n, (a, b) in enumerate(parts(src, dst, order, flat(i))):
                landing = dst.at[flat(4 - i)]
                if not last:
                    landing = landing.at[:, pl.ds(n * order[0], order[0])]
                waits.append(post(a, b, flat_peer(i), landing))

    triple_order = (triple_step, lambda p: 2 * (1 - lax.rem(p, 2)) + p // 2)
    expand_order = (expand_step, lambda p: p)
    stage, late = [], []
    turn_columns(triple_in, triple_out, triple_order)
    for i in others:
        late.append(post(deep_in.at[deep(i)], deep_out.at[z], deep_peer(i), deep_out.at[deep(4 - i)]))
    for i in range(1, 8):
        if last:
            landing = near.at[wide(8 - i)]
            stage.append(post(vec_in.at[wide(i)], near.at[rank], wide_peer(i), landing))
        else:
            landing = vec_out.at[z, wide(8 - i)]
            stage.append(post(vec_in, vec_out.at[z, rank], wide_peer(i), landing))
    late.append(post(turn_in, turn_out, turn_to, turn_out))
    turn_columns(expand_in, expand_out, expand_order)
    keep(deep_in.at[z], deep_out.at[z])
    for src, dst, order in (
        (triple_in, triple_out, triple_order),
        (expand_in, expand_out, expand_order),
    ):
        for a, b in parts(src, dst, order, place):
            keep(a, b)
    if last:
        own = pltpu.make_async_copy(vec_in.at[rank], near.at[rank], local_sem.at[len(kept)])
        own.start()
        for one in stage:
            one.wait_recv()
        own.wait()
        here[...] = jnp.sum(near[...], 0)
        stage = []
        for i in others:
            landing = far.at[deep(4 - i)]
            stage.append(post(here.at[deep(i)], far.at[z], deep_peer(i), landing))
        far[z] = here[z]
        for one in stage:
            one.wait_recv()
        vec_out[...] = jnp.sum(far[...], 0)
    else:
        own = pltpu.make_async_copy(vec_in, vec_out.at[z, rank], local_sem.at[len(kept)])
        own.start()
        for one in stage:
            one.wait_recv()
        own.wait()
        for i in others:
            landing = vec_out.at[deep(4 - i)]
            late.append(post(vec_out.at[z], vec_out.at[z], deep_peer(i), landing))
    for one in waits:
        one.wait_recv()
    for one in kept:
        one.wait()
    if last:
        for (steps, order), blocks, columns in zip(
            last, (triple_out, expand_out), (triple_columns, expand_columns)
        ):
            step = blocks.shape[2] // steps
            for i in range(steps):
                for p in range(4):
                    first = (i * 4 + order[p]) * step
                    columns[:, first : first + step] = blocks[p, :, i * step : (i + 1) * step]
    for one in late:
        one.wait_recv()
    for one in sent:
        one.wait_send()


def exchange(identity, deep, turned, triple, expand, vector, steps, last=None):
    half = expand.dtype
    operands = [deep, turned, triple, expand, vector]
    shapes = [jax.ShapeDtypeStruct(a.shape, a.dtype) for a in (deep, turned)]
    hbm, vmem = pl.BlockSpec(memory_space=pl.ANY), pl.BlockSpec(memory_space=pltpu.VMEM)
    scratch = []
    if last:
        tile = vector.shape[2:]
        shapes += [jax.ShapeDtypeStruct((a.shape[1], 4 * a.shape[2]), half) for a in (triple, expand)]
        shapes.append(jax.ShapeDtypeStruct(tile, vector.dtype))
        scratch = [pltpu.VMEM(triple.shape, half), pltpu.VMEM(expand.shape, half)]
        scratch += [pltpu.VMEM(n + tile, vector.dtype) for n in ((8, 4), (4,), (4,))]
        places = [hbm, hbm, vmem, vmem, vmem]
    else:
        for rows, columns in (triple.shape, expand.shape):
            shapes.append(jax.ShapeDtypeStruct((4, rows, columns // 4), half))
        shapes.append(jax.ShapeDtypeStruct((4, 8) + vector.shape, vector.dtype))
        places = [hbm] * 5
    copies = 3 + 7 + 1 + 3
    for whole, step in zip((triple, expand), steps):
        copies += 3 if last else 3 * (whole.shape[1] // 4 // step)
    moved = sum(a.size * a.dtype.itemsize for a in operands)
    return pl.pallas_call(
        functools.partial(exchange_kernel, last, *steps),
        out_shape=shapes,
        in_specs=[hbm] * 5,
        out_specs=places,
        scratch_shapes=scratch
        + [
            pltpu.SemaphoreType.DMA((copies,)),
            pltpu.SemaphoreType.DMA((copies,)),
            pltpu.SemaphoreType.DMA((16,)),
        ],
        compiler_params=pltpu.CompilerParams(
            collective_id=identity, has_side_effects=True, vmem_limit_bytes=24 * 2**20
        ),
        cost_estimate=pl.CostEstimate(flops=0, bytes_accessed=16 * moved, transcendentals=0),
        name="exchange",
    )(*operands)


def scores_of(item_ref, first, block, slope, prefix, depth, seq_rows):
    length = item_ref.shape[0]
    head_dim = item_ref.shape[1] // 3
    own_rows = depth * seq_rows
    chips = length // own_rows

    def position(index):
        chip = index // own_rows
        rest = index % own_rows
        return ((rest // seq_rows) * chips + chip) * seq_rows + rest % seq_rows

    queries = item_ref[first : first + block, :head_dim]
    keys = item_ref[:, head_dim : 2 * head_dim]
    raw = lax.dot_general(
        keys, queries, (((1,), (1,)), ((), ())), preferred_element_type=jnp.float32
    )
    key_pos = position(lax.broadcasted_iota(jnp.int32, (length, 1), 0))
    query_pos = position(first + lax.broadcasted_iota(jnp.int32, (1, block), 1))
    bound = jnp.where(key_pos < prefix, -1, key_pos)
    distance = jnp.abs(
        query_pos.astype(jnp.float32) - key_pos.astype(jnp.float32)
    )
    scores = raw * (LOG2E / math.sqrt(head_dim)) - (slope * LOG2E) * distance
    return jnp.where(bound <= query_pos, scores, jnp.float32(-1e30))


def forward_kernel(depth, seq_rows, block, prefix_ref, slope_ref, item_ref, mixed_ref, total_ref):
    prefix = prefix_ref[pl.program_id(0)]
    slope = slope_ref[pl.program_id(1)]
    length = item_ref.shape[0]
    head_dim = item_ref.shape[1] // 3
    for first in range(0, length, block):
        scores = scores_of(item_ref, first, block, slope, prefix, depth, seq_rows)
        top = jnp.max(scores, 0, keepdims=True)
        powers = jnp.exp2(scores - top)
        total = jnp.sum(powers, 0, keepdims=True)
        probs = (powers * (1.0 / total)).astype(jnp.bfloat16)
        mixed = lax.dot_general(
            probs,
            item_ref[:, 2 * head_dim :],
            (((0,), (0,)), ((), ())),
            preferred_element_type=jnp.float32,
        )
        mixed_ref[first : first + block, :] = mixed.astype(mixed_ref.dtype)
        total_ref[0, :, first : first + block] = top + jnp.log2(total)


def attend_forward(projected, slopes, prefixes, own_heads, head_dim, depth, seq_rows):
    cores = prefixes.shape[0]
    length = projected.shape[0] // cores
    block = min(256, length)
    scores = cores * own_heads * length * length
    return pl.pallas_call(
        functools.partial(forward_kernel, depth, seq_rows, block),
        grid=(cores, own_heads),
        out_shape=[
            jax.ShapeDtypeStruct((cores * length, own_heads * head_dim), projected.dtype),
            jax.ShapeDtypeStruct((cores * own_heads, 1, length), jnp.float32),
        ],
        in_specs=[
            pl.BlockSpec(memory_space=pltpu.SMEM),
            pl.BlockSpec(memory_space=pltpu.SMEM),
            pl.BlockSpec((length, 3 * head_dim), lambda s, h: (s, h)),
        ],
        out_specs=[
            pl.BlockSpec((length, head_dim), lambda s, h: (s, h)),
            pl.BlockSpec((1, 1, length), lambda s, h: (s * own_heads + h, 0, 0)),
        ],
        compiler_params=pltpu.CompilerParams(vmem_limit_bytes=48 * 2**20),
        cost_estimate=pl.CostEstimate(
            flops=4 * scores * head_dim,
            bytes_accessed=2 * projected.size * 2,
            transcendentals=scores,
        ),
        name="attend_forward",
    )(prefixes, slopes, projected)


def backward_kernel(
    depth, seq_rows, block, prefix_ref, slope_ref, item_ref, grad_ref, total_ref, out_ref, key_sum, value_sum
):
    prefix = prefix_ref[pl.program_id(0)]
    slope = slope_ref[pl.program_id(1)]
    length = item_ref.shape[0]
    head_dim = item_ref.shape[1] // 3
    scale = 1.0 / math.sqrt(head_dim)
    half = jnp.bfloat16
    wide = jnp.float32
    for first in range(0, length, block):
        scores = scores_of(item_ref, first, block, slope, prefix, depth, seq_rows)
        probs = jnp.exp2(scores - total_ref[0, :, first : first + block])
        grad = grad_ref[first : first + block, :]
        grad_probs = lax.dot_general(
            item_ref[:, 2 * head_dim :],
            grad,
            (((1,), (1,)), ((), ())),
            preferred_element_type=wide,
        )
        inner = jnp.sum(grad_probs * probs, 0, keepdims=True)
        grad_scores = (probs * (grad_probs - inner)).astype(half)
        key_term = jnp.dot(
            grad_scores, item_ref[first : first + block, :head_dim], preferred_element_type=wide
        )
        value_term = jnp.dot(probs.astype(half), grad, preferred_element_type=wide)
        query_grad = lax.dot_general(
            grad_scores,
            item_ref[:, head_dim : 2 * head_dim],
            (((0,), (0,)), ((), ())),
            preferred_element_type=wide,
        )
        out_ref[first : first + block, :head_dim] = (query_grad * scale).astype(half)
        if first == 0:
            key_sum[...] = key_term
            value_sum[...] = value_term
        else:
            key_sum[...] += key_term
            value_sum[...] += value_term
    out_ref[:, head_dim : 2 * head_dim] = (key_sum[...] * scale).astype(half)
    out_ref[:, 2 * head_dim :] = value_sum[...].astype(half)


def attend_backward(
    projected, grad_mixed, totals, slopes, prefixes, own_heads, head_dim, depth, seq_rows
):
    cores = prefixes.shape[0]
    length = projected.shape[0] // cores
    block = min(256, length)
    scores = cores * own_heads * length * length
    return pl.pallas_call(
        functools.partial(backward_kernel, depth, seq_rows, block),
        grid=(cores, own_heads),
        out_shape=jax.ShapeDtypeStruct(projected.shape, projected.dtype),
        in_specs=[
            pl.BlockSpec(memory_space=pltpu.SMEM),
            pl.BlockSpec(memory_space=pltpu.SMEM),
            pl.BlockSpec((length, 3 * head_dim), lambda s, h: (s, h)),
            pl.BlockSpec((length, head_dim), lambda s, h: (s, h)),
            pl.BlockSpec((1, 1, length), lambda s, h: (s * own_heads + h, 0, 0)),
        ],
        out_specs=pl.BlockSpec((length, 3 * head_dim), lambda s, h: (s, h)),
        scratch_shapes=[
            pltpu.VMEM((length, head_dim), jnp.float32),
            pltpu.VMEM((length, head_dim), jnp.float32),
        ],
        compiler_params=pltpu.CompilerParams(vmem_limit_bytes=48 * 2**20),
        cost_estimate=pl.CostEstimate(
            flops=10 * scores * head_dim,
            bytes_accessed=2 * projected.size * 2,
            transcendentals=scores,
        ),
        name="attend_backward",
    )(prefixes, slopes, projected, grad_mixed, totals)


def planar(
    hidden,
    prefix_lengths,
    cotangent,
    first_gain,
    first_shift,
    triple_weight,
    pair_bias,
    dense_weight,
    dense_shift,
    second_gain,
    second_shift,
    expand_weight,
    expand_shift,
    shrink_weight,
    shrink_shift,
):
    wide = jnp.float32
    half = jnp.bfloat16
    cores = lax.axis_size("dp")
    depth = lax.axis_size("z")
    rows_y = lax.axis_size("y")
    rows_x = lax.axis_size("x")
    plane = rows_y * rows_x
    core = lax.axis_index("dp")
    at_y = lax.axis_index("y")
    at_x = lax.axis_index("x")
    place = at_y * rows_x + at_x
    seq_rows = hidden.shape[2]
    width = hidden.shape[3]
    head_dim = triple_weight.shape[3]
    heads = triple_weight.shape[1]
    own_heads = heads // plane
    own_rows = seq_rows * depth
    units = expand_weight.shape[1]
    own_units = units // plane
    row_block = expand_weight.shape[0]
    shrink_rows = shrink_weight.shape[0]

    pieces = [
        first_gain,
        first_shift,
        dense_shift,
        second_gain,
        second_shift,
        shrink_shift,
        pair_bias,
        expand_shift,
    ]
    piece_total = sum(p.shape[0] for p in pieces)
    lanes = 128
    vector_rows = -(-piece_total // (lanes * 16)) * 16
    vector_tile = jnp.pad(
        jnp.concatenate(pieces), (0, vector_rows * lanes - piece_total)
    ).reshape(vector_rows, lanes)
    steps = (3 * head_dim, shrink_rows)
    shrink_half = shrink_rows // 2
    shrink_low = lax.all_gather(shrink_weight[:shrink_half], "z", axis=0)
    inputs, dense_turned, triple_turned, expand_turned, packed = exchange(
        3,
        hidden[:, 0],
        dense_weight,
        triple_weight.reshape(row_block, heads * 3 * head_dim),
        expand_weight,
        vector_tile,
        steps,
    )
    packed = (
        packed.reshape(depth, cores, plane, vector_rows * lanes)
        .transpose(1, 0, 2, 3)
        .reshape(-1, vector_rows * lanes)
    )
    vectors = []
    offset = 0
    for piece in pieces:
        vectors.append(packed[:, offset : offset + piece.shape[0]].reshape(-1).astype(wide))
        offset += piece.shape[0]
    gain_one, shift_one, dense_bias, gain_two, shift_two, shrink_bias, pair_full, unit_full = vectors
    pair_heads = pair_full.reshape(cores, own_heads, rows_x, rows_y, 2, head_dim)[
        core, :, 1 - at_x, at_y
    ]
    triple_bias = jnp.stack(
        [pair_heads[:, 0], jnp.zeros_like(pair_heads[:, 0]), pair_heads[:, 1]], 1
    ).reshape(-1)
    unit_bias = unit_full.reshape(cores, depth, plane, shrink_rows)[core, :, place].reshape(-1)

    triple_own = lax.all_gather(
        triple_turned.reshape(-1, triple_turned.shape[2]), "z", axis=0, tiled=True
    )
    inputs = inputs.reshape(own_rows, width).astype(wide)

    normed_own = layer_norm(inputs, gain_one, shift_one).astype(half)
    normed, upstream = gather_tokens(6, normed_own, cotangent[:, 0])
    upstream = upstream.reshape(own_rows, width)
    upstream_all, dense_own = gather_tokens(1, upstream, dense_turned, True)
    dense_own = dense_own.reshape(own_heads * head_dim, width)
    expand_own = lax.all_gather(
        after(expand_turned, normed).reshape(-1, own_units), "z", axis=0, tiled=True
    )
    projected = (
        jnp.dot(normed, triple_own, preferred_element_type=wide) + triple_bias
    ).astype(half)

    shrink_high = lax.all_gather(after(shrink_weight, projected)[shrink_half:], "z", axis=0)
    head_index = core * heads + jnp.arange(own_heads) * plane + (1 - at_x) * rows_y + at_y
    slopes = jnp.power(
        jnp.float32(2.0), -8.0 * (head_index.astype(wide) + 1.0) / (heads * cores)
    )
    at_z = lax.axis_index("z")
    prefixes = lax.dynamic_index_in_dim(prefix_lengths, at_z, 0, False)
    mixed, log_totals = attend_forward(
        projected, slopes, prefixes, own_heads, head_dim, depth, seq_rows
    )
    (dense_sum,) = scatter_tokens(2, mixed, dense_own)
    middle = inputs + dense_sum + dense_bias
    normed_two_own, norm_two_pull = jax.vjp(layer_norm, middle, gain_two, shift_two)
    (normed_two,) = gather_tokens(5, normed_two_own.astype(half))
    hidden_pre = jnp.dot(normed_two, expand_own, preferred_element_type=wide) + unit_bias
    activated, gelu_pull = jax.vjp(gelu_tanh, hidden_pre)
    activated = activated.astype(half)
    shrink_term = jnp.einsum(
        "tu,td->ud", activated, upstream_all, preferred_element_type=wide
    ).astype(half)
    shrink_high = after(shrink_high, shrink_term)
    shrink_own = jnp.concatenate([shrink_low, shrink_high], 1).reshape(own_units, width)
    grad_act = jnp.einsum("tf,uf->tu", upstream_all, shrink_own, preferred_element_type=wide)
    grad_pre = gelu_pull(grad_act)[0].astype(half)
    shrink_grad = lax.psum_scatter(shrink_term, "z", scatter_dimension=0, tiled=True)
    feed_sum, expand_term = scatter_tokens(
        8, after(activated, shrink_term), shrink_own, term=(normed_two, grad_pre)
    )
    expand_turned = lax.psum_scatter(expand_term, "z", scatter_dimension=0, tiled=True)
    layer_output = (middle + feed_sum + shrink_bias).astype(half)

    (norm_two_sum,) = scatter_tokens(9, after(grad_pre, feed_sum), expand_own, True)
    grad_norm_two, gain_two_term, shift_two_term = norm_two_pull(norm_two_sum)
    grad_middle = upstream.astype(wide) + grad_norm_two
    branch_own = grad_middle.astype(half)
    branch, layer_output = gather_tokens(
        6, branch_own, layer_output.reshape(depth, seq_rows, width)
    )

    grad_mixed = jnp.einsum("tf,ef->te", branch, dense_own, preferred_element_type=wide).astype(
        half
    )
    dense_term = jnp.einsum("te,tf->ef", mixed, branch, preferred_element_type=wide).astype(half)
    dense_turned = lax.psum_scatter(dense_term, "z", scatter_dimension=0, tiled=True)
    grad_project = attend_backward(
        projected,
        after(grad_mixed, dense_term),
        log_totals,
        slopes,
        prefixes,
        own_heads,
        head_dim,
        depth,
        seq_rows,
    )
    triple_term = jnp.einsum(
        "td,tc->dc", normed, grad_project, preferred_element_type=wide
    ).astype(half)
    triple_turned = lax.psum_scatter(triple_term, "z", scatter_dimension=0, tiled=True)
    (norm_one_sum,) = scatter_tokens(10, after(grad_project, triple_term), triple_own, True)
    grad_norm_one, gain_one_term, shift_one_term = jax.vjp(
        layer_norm, inputs, gain_one, shift_one
    )[1](norm_one_sum)
    hidden_grad = (grad_middle + grad_norm_one).astype(half)
    head_sums = jnp.sum(grad_project, 0, dtype=wide).reshape(own_heads, 3, head_dim)
    pair_term = jnp.stack([head_sums[:, 0], head_sums[:, 2]], 1)
    pair_zero = jnp.zeros((cores, own_heads, rows_x, rows_y, 2, head_dim), wide)
    pair_wide = lax.dynamic_update_slice(
        pair_zero, pair_term[None, :, None, None], (core, 0, 1 - at_x, at_y, 0, 0)
    ).reshape(-1)
    unit_term = jnp.sum(grad_pre, 0, dtype=wide).reshape(1, depth, 1, shrink_rows)
    unit_wide = lax.dynamic_update_slice(
        jnp.zeros((cores, depth, plane, shrink_rows), wide), unit_term, (core, 0, place, 0)
    ).reshape(-1)
    terms = [
        gain_one_term,
        shift_one_term,
        jnp.sum(branch_own, 0, dtype=wide),
        gain_two_term,
        shift_two_term,
        jnp.sum(upstream, 0, dtype=wide),
        pair_wide,
        unit_wide,
    ]
    devices = cores * depth * plane
    term_rows = -(-piece_total // (lanes * 8)) * 8
    term_tiles = jnp.pad(
        jnp.concatenate([t.reshape(devices, -1) for t in terms], 1),
        ((0, 0), (0, term_rows * lanes - piece_total)),
    )
    term_tiles = (
        term_tiles.reshape(cores, depth, plane, term_rows, lanes)
        .transpose(0, 2, 1, 3, 4)
        .reshape(cores * plane, depth, term_rows, lanes)
    )
    hidden_grad, dense_grad, triple_grad, expand_grad, summed = exchange(
        4,
        hidden_grad.reshape(depth, seq_rows, width),
        dense_turned,
        triple_turned.reshape(plane, row_block, -1),
        expand_turned.reshape(plane, row_block, own_units),
        term_tiles,
        steps,
        last=((own_heads, (2, 0, 3, 1)), (depth, (0, 1, 2, 3))),
    )
    layer_output = layer_output[:, None]
    hidden_grad = hidden_grad[:, None]
    triple_grad = triple_grad.astype(wide).reshape(row_block, heads, 3, head_dim)
    summed = summed.reshape(-1)
    vector_grads = []
    offset = 0
    for piece in pieces:
        vector_grads.append(summed[offset : offset + piece.shape[0]])
        offset += piece.shape[0]
    return (
        layer_output,
        hidden_grad,
        vector_grads[0],
        vector_grads[1],
        triple_grad,
        vector_grads[6],
        dense_grad.astype(wide),
        vector_grads[2],
        vector_grads[3],
        vector_grads[4],
        expand_grad.astype(wide),
        vector_grads[7],
        shrink_grad.astype(wide),
        vector_grads[5],
    )


def layer(*args):
    return planar(*args)


def solution(mesh):
    depth = 4
    sides = (2, 2)
    planar_plan = mesh.shape["seq"] == depth * sides[0] * sides[1]
    if planar_plan:
        grid = Mesh(
            mesh.devices.reshape(mesh.shape["dp"], depth, *sides), ("dp", "z", "y", "x")
        )
        seq = ("z", "y", "x")
    else:
        grid = mesh
        seq = ("seq",)
    tokens = P(None, "dp", seq, None)
    vector = P(("dp",) + seq)
    matrix = P(("dp",) + seq, None)
    placed = (
        tokens,
        P(),
        tokens,
        vector,
        vector,
        P(seq, "dp", None, None),
        vector,
        matrix,
        vector,
        vector,
        vector,
        P(seq, "dp"),
        vector,
        matrix,
        vector,
    )
    results = (
        tokens,
        tokens,
        vector,
        vector,
        P(seq, "dp", None, None),
        vector,
        matrix,
        vector,
        vector,
        vector,
        P(seq, "dp"),
        vector,
        matrix,
        vector,
    )
    return jax.shard_map(
        layer if planar_plan else shards,
        mesh=grid,
        in_specs=placed,
        out_specs=results,
        check_vma=False,
    )
```

```python
import functools
import math

import jax
import jax.numpy as jnp
from jax import lax
from jax.experimental import pallas as pl
from jax.experimental.pallas import tpu as pltpu
from jax.sharding import Mesh
from jax.sharding import PartitionSpec as P


EPSILON = 1e-05
GELU_SCALE = 0.7978845608028654


def layer_norm(inputs, norm_gain, norm_shift):
    centered = inputs - jnp.mean(inputs, -1, keepdims=True)
    variance = jnp.mean(centered * centered, -1, keepdims=True)
    return centered * lax.rsqrt(variance + EPSILON) * norm_gain + norm_shift


def gelu_tanh(values):
    return (
        0.5 * values * (1.0 + jnp.tanh(GELU_SCALE * (values + 0.044715 * values * values * values)))
    )


def split_norm(inputs, gain_rows, shift_rows):
    return layer_norm(inputs, gain_rows[None, :, None, :], shift_rows[None, :, None, :])


def place_half(values, half_index, group_count):
    chosen = (jnp.arange(group_count, dtype=jnp.int32) == half_index).astype(values.dtype)
    return (chosen[:, None] * values.reshape(1, -1)).reshape(-1)


def shards(
    hidden,
    prefix_lengths,
    cotangent,
    first_gain,
    first_shift,
    triple_weight,
    pair_bias,
    dense_weight,
    dense_shift,
    second_gain,
    second_shift,
    expand_weight,
    expand_shift,
    shrink_weight,
    shrink_shift,
):
    wide_type = jnp.float32
    half_type = jnp.bfloat16
    seq_count = lax.axis_size("seq")
    group_count = lax.axis_size("dp")
    dp_index = lax.axis_index("dp")
    seq_index = lax.axis_index("seq")
    micro_count = hidden.shape[0]
    seq_rows = hidden.shape[2]
    model_width = hidden.shape[3]
    seq_length = seq_rows * seq_count
    local_heads = triple_weight.shape[1]
    head_dim = triple_weight.shape[3]
    head_total = local_heads * group_count
    pair_local = micro_count * group_count * local_heads // seq_count
    unit_local = expand_weight.shape[1]
    project_width = 3 * local_heads * head_dim
    token_total = micro_count * group_count * seq_rows
    score_scale = 1.0 / math.sqrt(head_dim)
    block_rows = min(512, seq_length)
    block_count = seq_length // block_rows
    key_pos = jnp.arange(seq_length, dtype=jnp.int32)
    gathered = (
        lax.all_gather(triple_weight, "seq", axis=0, tiled=True),
        lax.all_gather(dense_weight, "seq", axis=0, tiled=True),
        lax.all_gather(expand_weight, "seq", axis=0, tiled=True),
        lax.all_gather(shrink_weight, "seq", axis=0, tiled=True),
        lax.all_gather(first_gain, "seq", axis=0, tiled=True),
        lax.all_gather(first_shift, "seq", axis=0, tiled=True),
        lax.all_gather(pair_bias, "seq", axis=0, tiled=True),
        lax.all_gather(dense_shift, "seq", axis=0, tiled=True),
        lax.all_gather(second_gain, "seq", axis=0, tiled=True),
        lax.all_gather(second_shift, "seq", axis=0, tiled=True),
        lax.all_gather(expand_shift, "seq", axis=0, tiled=True),
        lax.all_gather(shrink_shift, "seq", axis=0, tiled=True),
    )
    triple_full, dense_full, expand_full, shrink_full = (
        gathered[0],
        gathered[1],
        gathered[2],
        gathered[3],
    )
    row_sets = (
        lax.all_gather(hidden, "dp", axis=1, tiled=True),
        lax.all_gather(cotangent, "dp", axis=1, tiled=True),
        lax.all_gather(gathered[4], "dp", axis=0, tiled=True),
        lax.all_gather(gathered[5], "dp", axis=0, tiled=True),
        lax.all_gather(gathered[6], "dp", axis=0, tiled=True),
        lax.all_gather(gathered[7], "dp", axis=0, tiled=True),
        lax.all_gather(gathered[8], "dp", axis=0, tiled=True),
        lax.all_gather(gathered[9], "dp", axis=0, tiled=True),
        lax.all_gather(gathered[10], "dp", axis=0, tiled=True),
        lax.all_gather(gathered[11], "dp", axis=0, tiled=True),
    )
    hidden_both = row_sets[0]
    upstream_low = row_sets[1]
    gain_one, shift_one, pair_full, dense_bias, gain_two, shift_two, expand_bias, shrink_bias = [
        vector.astype(wide_type) for vector in row_sets[2:]
    ]
    inputs_both = hidden_both.astype(wide_type)
    normed_low = layer_norm(inputs_both, gain_one, shift_one).astype(half_type)
    pair_heads = lax.dynamic_slice_in_dim(
        pair_full.reshape(head_total, 2, head_dim), dp_index * local_heads, local_heads, 0
    )
    triple_bias = jnp.stack(
        [pair_heads[:, 0], jnp.zeros_like(pair_heads[:, 0]), pair_heads[:, 1]], 0
    )
    projected = jnp.einsum(
        "mstd,dhce->cmshte", normed_low, triple_full, preferred_element_type=wide_type
    )
    projected = projected + triple_bias[:, None, None, :, None, :]
    project_low = projected.astype(half_type).reshape(3, seq_count, pair_local, seq_rows, head_dim)
    pair_rows = lax.all_to_all(project_low, "seq", split_axis=1, concat_axis=3, tiled=True)[:, 0]
    query_all, key_all, value_all = (pair_rows[0], pair_rows[1], pair_rows[2])
    pair_index = seq_index * pair_local + jnp.arange(pair_local, dtype=jnp.int32)
    head_index = dp_index * local_heads + pair_index % local_heads
    sequence_index = pair_index // local_heads
    slopes = jnp.power(jnp.float32(2.0), -8.0 * (head_index.astype(wide_type) + 1.0) / head_total)
    prefix_flat = prefix_lengths.reshape(-1)
    prefix_slots = jnp.arange(prefix_flat.shape[0], dtype=jnp.int32)
    prefixes = jnp.sum(
        jnp.where(prefix_slots[None, :] == sequence_index[:, None], prefix_flat[None, :], 0), 1
    )

    def block_scores(pair_item, first_row):
        query_block = lax.dynamic_slice_in_dim(
            lax.dynamic_index_in_dim(query_all, pair_item, 0, False), first_row, block_rows, 0
        )
        keys_item = lax.dynamic_index_in_dim(key_all, pair_item, 0, False)
        head_slope = lax.dynamic_index_in_dim(slopes, pair_item, 0, False)
        prefix = lax.dynamic_index_in_dim(prefixes, pair_item, 0, False)
        query_pos = first_row + jnp.arange(block_rows, dtype=jnp.int32)
        raw_scores = (
            jnp.einsum("qe,ke->qk", query_block, keys_item, preferred_element_type=wide_type)
            * score_scale
        )
        distance = jnp.abs(query_pos[:, None] - key_pos[None, :]).astype(wide_type)
        raw_scores = raw_scores - head_slope * distance
        allowed = (key_pos[None, :] <= query_pos[:, None]) | (key_pos[None, :] < prefix)
        return (query_block, jnp.where(allowed, raw_scores, jnp.float32(-1e30)))

    def forward_block(flat_index):
        pair_item = flat_index // block_count
        first_row = flat_index % block_count * block_rows
        _, scores = block_scores(pair_item, first_row)
        row_max = jnp.max(scores, -1, keepdims=True)
        powers = jnp.exp(scores - row_max)
        row_total = jnp.sum(powers, -1, keepdims=True)
        probs_low = (powers / row_total).astype(half_type)
        values_item = lax.dynamic_index_in_dim(value_all, pair_item, 0, False)
        mixed = jnp.dot(probs_low, values_item, preferred_element_type=wide_type).astype(half_type)
        return (mixed, (row_max + jnp.log(row_total))[:, 0])

    mixed_blocks, log_blocks = lax.map(
        forward_block, jnp.arange(pair_local * block_count, dtype=jnp.int32)
    )
    mixed_pairs = mixed_blocks.reshape(pair_local, seq_count, seq_rows, head_dim)
    log_totals = log_blocks.reshape(pair_local, seq_length)
    mixed_home = lax.all_to_all(mixed_pairs, "seq", split_axis=1, concat_axis=0, tiled=True)
    mixed_tokens = jnp.transpose(
        mixed_home.reshape(micro_count, group_count, local_heads, seq_rows, head_dim),
        (0, 1, 3, 2, 4),
    ).reshape(micro_count, group_count, seq_rows, local_heads * head_dim)
    dense_part = jnp.einsum(
        "mstk,kf->mstf", mixed_tokens, dense_full, preferred_element_type=wide_type
    )
    attention_sum = lax.psum(dense_part.astype(jnp.bfloat16), "dp").astype(jnp.float32)
    middle = inputs_both + attention_sum + dense_bias
    gain_rows_two = jnp.broadcast_to(gain_two[None, :], (group_count, model_width))
    shift_rows_two = jnp.broadcast_to(shift_two[None, :], (group_count, model_width))
    normed_two, norm_two_pull = jax.vjp(split_norm, middle, gain_rows_two, shift_rows_two)
    normed_two_low = normed_two.astype(half_type)
    unit_bias = lax.dynamic_slice_in_dim(expand_bias, dp_index * unit_local, unit_local, 0)
    hidden_pre = (
        jnp.einsum("mstd,df->mstf", normed_two_low, expand_full, preferred_element_type=wide_type)
        + unit_bias
    )
    activated_value, gelu_pull = jax.vjp(gelu_tanh, hidden_pre)
    activated_low = activated_value.astype(half_type)
    feed_part = jnp.einsum(
        "mstf,fd->mstd", activated_low, shrink_full, preferred_element_type=wide_type
    )
    feed_sum = lax.psum_scatter(
        feed_part.astype(jnp.bfloat16), "dp", scatter_dimension=1, tiled=True
    ).astype(jnp.float32)
    middle_own = lax.dynamic_slice_in_dim(middle, dp_index, 1, 1)
    layer_output = (middle_own + feed_sum + shrink_bias).astype(half_type)
    triple_back, dense_back, expand_back, shrink_back = (
        lax.all_gather(triple_weight, "seq", axis=0, tiled=True),
        lax.all_gather(dense_weight, "seq", axis=0, tiled=True),
        lax.all_gather(expand_weight, "seq", axis=0, tiled=True),
        lax.all_gather(shrink_weight, "seq", axis=0, tiled=True),
    )
    grad_act = jnp.einsum(
        "mstd,fd->mstf", upstream_low, shrink_back, preferred_element_type=wide_type
    )
    grad_pre_low = gelu_pull(grad_act)[0].astype(half_type)
    norm_two_part = jnp.einsum(
        "mstf,df->mstd", grad_pre_low, expand_back, preferred_element_type=wide_type
    )
    grad_normed_two = lax.psum(norm_two_part.astype(jnp.bfloat16), "dp").astype(jnp.float32)
    grad_middle_norm, grad_gain_rows_two, grad_shift_rows_two = norm_two_pull(grad_normed_two)
    grad_middle = upstream_low.astype(wide_type) + grad_middle_norm
    grad_branch_low = grad_middle.astype(half_type)
    go_pairs = jnp.einsum(
        "mstf,hef->mshte",
        grad_branch_low,
        dense_back.reshape(local_heads, head_dim, model_width),
        preferred_element_type=wide_type,
    ).astype(half_type)
    go_pairs = go_pairs.reshape(seq_count, pair_local, seq_rows, head_dim)
    grad_mixed_pairs = lax.all_to_all(go_pairs, "seq", split_axis=0, concat_axis=2, tiled=True)[0]

    def backward_item(pair_item):
        keys_item = lax.dynamic_index_in_dim(key_all, pair_item, 0, False)
        values_item = lax.dynamic_index_in_dim(value_all, pair_item, 0, False)
        grad_mixed_item = lax.dynamic_index_in_dim(grad_mixed_pairs, pair_item, 0, False)
        totals_item = lax.dynamic_index_in_dim(log_totals, pair_item, 0, False)

        def backward_block(running, block_index):
            key_grad, value_grad = running
            first_row = block_index * block_rows
            query_block, scores = block_scores(pair_item, first_row)
            soft_probs = jnp.exp(
                scores - lax.dynamic_slice_in_dim(totals_item, first_row, block_rows, 0)[:, None]
            )
            grad_block = lax.dynamic_slice_in_dim(grad_mixed_item, first_row, block_rows, 0)
            grad_probs = jnp.einsum(
                "qe,ke->qk", grad_block, values_item, preferred_element_type=wide_type
            )
            row_inner = jnp.sum(grad_probs * soft_probs, -1, keepdims=True)
            grad_scores_low = (soft_probs * (grad_probs - row_inner)).astype(half_type)
            query_grad = (
                jnp.dot(grad_scores_low, keys_item, preferred_element_type=wide_type) * score_scale
            )
            key_grad = (
                key_grad
                + jnp.einsum(
                    "qk,qe->ke", grad_scores_low, query_block, preferred_element_type=wide_type
                )
                * score_scale
            )
            value_grad = value_grad + jnp.einsum(
                "qk,qe->ke",
                soft_probs.astype(half_type),
                grad_block,
                preferred_element_type=wide_type,
            )
            return ((key_grad, value_grad), query_grad)

        zero_rows = jnp.zeros((seq_length, head_dim), wide_type)
        (key_grad, value_grad), query_grads = lax.scan(
            backward_block, (zero_rows, zero_rows), jnp.arange(block_count, dtype=jnp.int32)
        )
        return jnp.stack(
            [query_grads.reshape(seq_length, head_dim), key_grad, value_grad], 0
        ).astype(half_type)

    grad_pairs = lax.map(backward_item, jnp.arange(pair_local, dtype=jnp.int32))
    grad_split = grad_pairs.reshape(pair_local, 3, seq_count, seq_rows, head_dim)
    grad_home = lax.all_to_all(grad_split, "seq", split_axis=2, concat_axis=0, tiled=True)
    grad_project_low = jnp.transpose(
        grad_home.reshape(micro_count, group_count, local_heads, 3, seq_rows, head_dim),
        (0, 1, 4, 2, 3, 5),
    ).reshape(micro_count, group_count, seq_rows, project_width)
    norm_one_part = jnp.einsum(
        "mstc,dc->mstd",
        grad_project_low,
        triple_back.reshape(model_width, project_width),
        preferred_element_type=wide_type,
    )
    grad_normed_one = lax.psum_scatter(
        norm_one_part.astype(jnp.bfloat16), "dp", scatter_dimension=1, tiled=True
    ).astype(jnp.float32)
    inputs_own = hidden.astype(wide_type)
    grad_inputs_norm, grad_gain_one, grad_shift_one = jax.vjp(
        layer_norm, inputs_own, gain_one, shift_one
    )[1](grad_normed_one)
    grad_middle_own = lax.dynamic_slice_in_dim(grad_middle, dp_index, 1, 1)
    hidden_grad = (grad_middle_own + grad_inputs_norm).astype(half_type)
    head_sums = jnp.sum(
        grad_project_low.reshape(micro_count, group_count, seq_rows, local_heads, 3, head_dim),
        (0, 1, 2),
        dtype=wide_type,
    )
    pair_grad = place_half(jnp.stack([head_sums[:, 0], head_sums[:, 2]], 1), dp_index, group_count)
    unit_grad = place_half(jnp.sum(grad_pre_low, (0, 1, 2), dtype=wide_type), dp_index, group_count)
    dense_shift_term = jnp.sum(
        lax.dynamic_slice_in_dim(grad_branch_low, dp_index, 1, 1), (0, 1, 2), dtype=wide_type
    )
    shrink_shift_term = jnp.sum(cotangent, (0, 1, 2), dtype=wide_type)
    gain_two_term = lax.dynamic_index_in_dim(grad_gain_rows_two, dp_index, 0, False)
    shift_two_term = lax.dynamic_index_in_dim(grad_shift_rows_two, dp_index, 0, False)
    vector_sums = (
        lax.psum_scatter(grad_gain_one, ("dp", "seq"), scatter_dimension=0, tiled=True),
        lax.psum_scatter(grad_shift_one, ("dp", "seq"), scatter_dimension=0, tiled=True),
        lax.psum_scatter(pair_grad, ("dp", "seq"), scatter_dimension=0, tiled=True),
        lax.psum_scatter(dense_shift_term, ("dp", "seq"), scatter_dimension=0, tiled=True),
        lax.psum_scatter(gain_two_term, ("dp", "seq"), scatter_dimension=0, tiled=True),
        lax.psum_scatter(shift_two_term, ("dp", "seq"), scatter_dimension=0, tiled=True),
        lax.psum_scatter(unit_grad, ("dp", "seq"), scatter_dimension=0, tiled=True),
        lax.psum_scatter(shrink_shift_term, ("dp", "seq"), scatter_dimension=0, tiled=True),
    )
    normed_flat = normed_low.reshape(token_total, model_width)
    project_flat = grad_project_low.reshape(token_total, project_width)
    normed_two_flat = normed_two_low.reshape(token_total, model_width)
    pre_flat = grad_pre_low.reshape(token_total, unit_local)
    column_sums = lax.psum_scatter(
        jnp.concatenate(
            [
                jnp.einsum(
                    "tr,tc->rc", normed_flat, project_flat, preferred_element_type=wide_type
                ),
                jnp.einsum(
                    "tr,tc->rc", normed_two_flat, pre_flat, preferred_element_type=wide_type
                ),
            ],
            1,
        ),
        "seq",
        scatter_dimension=0,
        tiled=True,
    )
    triple_grad = column_sums[:, :project_width].reshape(
        model_width // seq_count, local_heads, 3, head_dim
    )
    expand_grad = column_sums[:, project_width:]
    dense_rows = dense_weight.shape[0]
    shrink_rows = shrink_weight.shape[0]
    row_block = dense_rows + shrink_rows
    mixed_flat = mixed_tokens.reshape(token_total, local_heads * head_dim)
    branch_flat = grad_branch_low.reshape(token_total, model_width)
    active_flat = activated_low.reshape(token_total, unit_local)
    upstream_flat = upstream_low.reshape(token_total, model_width)
    block_number = row_block * lax.axis_size("seq") // row_block
    dense_term = jnp.einsum("tr,td->rd", mixed_flat, branch_flat, preferred_element_type=wide_type)
    shrink_term = jnp.einsum(
        "tr,td->rd", active_flat, upstream_flat, preferred_element_type=wide_type
    )
    row_sums = lax.psum_scatter(
        jnp.concatenate(
            [
                dense_term.reshape(block_number, dense_rows, model_width),
                shrink_term.reshape(block_number, shrink_rows, model_width),
            ],
            1,
        ).reshape(row_block * lax.axis_size("seq"), model_width),
        "seq",
        scatter_dimension=0,
        tiled=True,
    )
    dense_grad = row_sums[:dense_rows]
    shrink_grad = row_sums[dense_rows:]
    return (
        layer_output,
        hidden_grad,
        vector_sums[0],
        vector_sums[1],
        triple_grad,
        vector_sums[2],
        dense_grad,
        vector_sums[3],
        vector_sums[4],
        vector_sums[5],
        expand_grad,
        vector_sums[6],
        shrink_grad,
        vector_sums[7],
    )


CHUNKS = 4
LOG2E = 1.4426950408889634
MESH = pl.DeviceIdType.MESH


def remote(src, dst, send, recv, peer):
    return pltpu.make_async_remote_copy(
        src_ref=src,
        dst_ref=dst,
        send_sem=send,
        recv_sem=recv,
        device_id=peer,
        device_id_type=MESH,
    )


def greet(peers):
    barrier = pltpu.get_barrier_semaphore()
    for peer in peers:
        pl.semaphore_signal(barrier, inc=1, device_id=peer, device_id_type=MESH)
    pl.semaphore_wait(barrier, len(peers))


class Corner:
    def __init__(self):
        self.c = lax.axis_index("dp")
        self.y = lax.axis_index("y")
        self.x = lax.axis_index("x")
        self.ax = self.x + (1 - self.c) * (1 - 2 * self.x)
        self.ay = self.y + self.c * (1 - 2 * self.y)
        self.bx = self.x + self.c * (1 - 2 * self.x)
        self.by = self.y + (1 - self.c) * (1 - 2 * self.y)
        self.dx = 1 - self.x
        self.dy = 1 - self.y
        self.peer_a = {"y": self.ay, "x": self.ax}
        self.peer_b = {"y": self.by, "x": self.bx}
        self.sibling = {"dp": 1 - self.c}

    def slots(self, core):
        return [
            (core * 2 + y) * 2 + x
            for y, x in (
                (self.dy, self.dx),
                (self.by, self.bx),
                (self.ay, self.ax),
                (self.y, self.x),
            )
        ]


def gather_kernel(deep, whole, *refs):
    if deep:
        rows_ref, deep_ref, all_ref, moved_ref, local_sem, send, recv, deep_send, deep_recv = refs
    else:
        rows_ref, all_ref, local_sem, send, recv = refs
    at = Corner()
    slot_d, slot_b, slot_a, me = at.slots(at.c)
    step = rows_ref.shape[0] // CHUNKS
    peers = [at.peer_a, at.peer_b, at.sibling]
    sent, moves = [], []
    if deep:
        z = lax.axis_index("z")
        plane_at = [lax.rem(z + i, 4) for i in range(4)]
        peers += [{"z": plane_at[i]} for i in range(1, 4)]
    greet(peers)
    locals_ = [pltpu.make_async_copy(rows_ref, all_ref.at[me], local_sem.at[0])]
    if deep:
        block = deep_ref if whole else deep_ref.at[z]
        locals_.append(pltpu.make_async_copy(block, moved_ref.at[z], local_sem.at[1]))
    for one in locals_:
        one.start()

    def copy(kind, k, slot, peer):
        part = pl.ds(k * step, step)
        src = rows_ref.at[part] if kind < 3 else all_ref.at[slot, part]
        return remote(src, all_ref.at[slot, part], send.at[kind, k], recv.at[kind, k], peer)

    def arrived(kind, k, slot, peer):
        part = pl.ds(k * step, step)
        block = all_ref.at[slot, part]
        remote(block, block, send.at[kind, k], recv.at[kind, k], peer).wait_recv()

    def start(kind, k, slot, peer):
        one = copy(kind, k, slot, peer)
        one.start()
        sent.append(one)

    for i in range(1, 4) if deep else ():
        sems = deep_send.at[i - 1], deep_recv.at[i - 1]
        block = deep_ref if whole else deep_ref.at[plane_at[i]]
        one = remote(block, moved_ref.at[z], *sems, {"z": plane_at[i]})
        one.start()
        sent.append(one)
        landing = moved_ref.at[plane_at[4 - i]]
        moves.append(remote(landing, landing, *sems, {"z": plane_at[i]}))
    for k in range(CHUNKS):
        start(0, k, me, at.peer_a)
        start(1, k, me, at.peer_b)
    for k in range(CHUNKS):
        start(2, k, me, at.sibling)
    for k in range(CHUNKS):
        arrived(0, k, slot_a, at.peer_a)
        start(3, k, slot_a, at.peer_b)
        start(4, k, slot_a, at.sibling)
    for k in range(CHUNKS):
        arrived(1, k, slot_b, at.peer_b)
        start(5, k, slot_b, at.sibling)
    for k in range(CHUNKS):
        arrived(3, k, slot_d, at.peer_b)
        start(6, k, slot_d, at.sibling)
    other_d, other_b, other_a, other_me = at.slots(1 - at.c)
    for k in range(CHUNKS):
        arrived(2, k, other_me, at.sibling)
        arrived(4, k, other_b, at.sibling)
        arrived(5, k, other_a, at.sibling)
        arrived(6, k, other_d, at.sibling)
    for one in moves:
        one.wait_recv()
    for one in sent:
        one.wait_send()
    for one in locals_:
        one.wait()


def gather_tokens(identity, rows, deep=None, whole=False):
    count, width = rows.shape
    operands = [rows]
    shapes = [jax.ShapeDtypeStruct((8, count, width), rows.dtype)]
    scratch = [
        pltpu.SemaphoreType.DMA((2,)),
        pltpu.SemaphoreType.DMA((7, CHUNKS)),
        pltpu.SemaphoreType.DMA((7, CHUNKS)),
    ]
    if deep is not None:
        operands.append(deep)
        moved_shape = (4,) + deep.shape if whole else deep.shape
        shapes.append(jax.ShapeDtypeStruct(moved_shape, deep.dtype))
        scratch += [pltpu.SemaphoreType.DMA((3,)), pltpu.SemaphoreType.DMA((3,))]
    all_rows, *moved = pl.pallas_call(
        functools.partial(gather_kernel, deep is not None, whole),
        out_shape=shapes,
        in_specs=[pl.BlockSpec(memory_space=pl.ANY)] * len(operands),
        out_specs=[pl.BlockSpec(memory_space=pl.ANY)] * len(shapes),
        scratch_shapes=scratch,
        compiler_params=pltpu.CompilerParams(
            collective_id=identity, has_side_effects=True
        ),
        cost_estimate=pl.CostEstimate(
            flops=0, bytes_accessed=16 * count * width * 4, transcendentals=0
        ),
        name="gather_tokens",
    )(*operands)
    return (all_rows.reshape(8 * count, width), *moved)


def after(value, *others):
    return lax.optimization_barrier((value, *others))[0]


def scatter_kernel(turned, term, left_ref, right_ref, *refs):
    if term:
        rows_ref, grads_ref, own_ref, term_ref, *refs = refs
    else:
        own_ref, *refs = refs
    part_ref, from_core, from_b, from_a, send, recv = refs
    at = Corner()
    slot_d, slot_b, slot_a, me = at.slots(at.c)
    other_d, other_b, other_a, other_me = at.slots(1 - at.c)
    _, width = own_ref.shape
    step = width // CHUNKS
    wide = jnp.float32
    greet([at.peer_a, at.peer_b, at.sibling])
    sent = []

    def start(kind, k, src, dst, peer):
        one = remote(src, dst, send.at[kind, k], recv.at[kind, k], peer)
        one.start()
        sent.append(one)

    def arrived(kind, k, dst, peer):
        remote(dst, dst, send.at[kind, k], recv.at[kind, k], peer).wait_recv()

    def multiply_columns(slot, cols):
        right = right_ref[cols] if turned else right_ref[:, cols]
        product = lax.dot_general(
            left_ref[slot],
            right,
            (((1,), (1 if turned else 0,)), ((), ())),
            preferred_element_type=wide,
        )
        part_ref[slot, :, cols] = product.astype(part_ref.dtype)

    def multiply(slot):
        def columns(t, carry):
            multiply_columns(slot, pl.ds(pl.multiple_of(t * step, step), step))
            return carry

        lax.fori_loop(0, CHUNKS, columns, 0)

    def multiply_term(first, last):
        if not term:
            return
        lanes = min(256, rows_ref.shape[1] // 8)

        def features(t, carry):
            cols = pl.ds(pl.multiple_of(t * lanes, lanes), lanes)
            product = lax.dot_general(
                rows_ref[:, cols],
                grads_ref[...],
                (((0,), (0,)), ((), ())),
                preferred_element_type=wide,
            )
            term_ref[cols] = product.astype(term_ref.dtype)
            return carry

        count = rows_ref.shape[1] // lanes
        lax.fori_loop(count * first // 8, count * last // 8, features, 0)

    def share(q, slot, chunks):
        for k in chunks:
            part = pl.ds(k * step, step)
            start(q, k, part_ref.at[slot, :, part], from_core.at[q, :, part], at.sibling)

    def to_b(q, slot, chunks):
        for k in chunks:
            part = pl.ds(k * step, step)
            arrived(q, k, from_core.at[q, :, part], at.sibling)
            total = part_ref[slot, :, part].astype(wide) + from_core[q, :, part].astype(wide)
            from_core[q, :, part] = total.astype(from_core.dtype)
            start(4 + q, k, from_core.at[q, :, part], from_b.at[q, :, part], at.peer_b)

    everything = range(CHUNKS)
    for k in everything:
        multiply_columns(other_d, pl.ds(k * step, step))
        share(0, other_d, [k])
        multiply_columns(slot_d, pl.ds(k * step, step))
        if k:
            to_b(0, slot_d, [k - 1])
    to_b(0, slot_d, [CHUNKS - 1])
    multiply(other_a)
    share(1, other_a, everything)
    multiply(slot_b)
    to_b(1, slot_b, everything)
    multiply(other_b)
    share(2, other_b, everything)
    multiply(slot_a)
    multiply_term(0, 2)
    for k in everything:
        part = pl.ds(k * step, step)
        arrived(2, k, from_core.at[2, :, part], at.sibling)
        arrived(4, k, from_b.at[0, :, part], at.peer_b)
        total = part_ref[slot_a, :, part].astype(wide) + from_core[2, :, part].astype(wide)
        total = total + from_b[0, :, part].astype(wide)
        from_core[2, :, part] = total.astype(from_core.dtype)
        start(6, k, from_core.at[2, :, part], from_a.at[:, part], at.peer_a)
    multiply(other_me)
    share(3, other_me, everything)
    multiply(me)
    multiply_term(2, 8)
    for k in everything:
        part = pl.ds(k * step, step)
        arrived(3, k, from_core.at[3, :, part], at.sibling)
        arrived(5, k, from_b.at[1, :, part], at.peer_b)
        arrived(6, k, from_a.at[:, part], at.peer_a)
        total = part_ref[me, :, part].astype(wide) + from_core[3, :, part].astype(wide)
        total = total + from_b[1, :, part].astype(wide)
        own_ref[:, part] = total + from_a[:, part].astype(wide)
    for one in sent:
        one.wait_send()


def scatter_tokens(identity, left, right, turned=False, term=()):
    count, depth = left.shape[0] // 8, left.shape[1]
    width = right.shape[0] if turned else right.shape[1]
    half = left.dtype
    shapes = [jax.ShapeDtypeStruct((count, width), jnp.float32)]
    if term:
        shapes.append(jax.ShapeDtypeStruct((term[0].shape[1], term[1].shape[1]), half))
    vmem = pl.BlockSpec(memory_space=pltpu.VMEM)
    return pl.pallas_call(
        functools.partial(scatter_kernel, turned, bool(term)),
        out_shape=shapes,
        in_specs=[vmem] * (2 + len(term)),
        out_specs=[vmem] * len(shapes),
        scratch_shapes=[
            pltpu.VMEM((8, count, width), half),
            pltpu.VMEM((4, count, width), half),
            pltpu.VMEM((2, count, width), half),
            pltpu.VMEM((count, width), half),
            pltpu.SemaphoreType.DMA((7, CHUNKS)),
            pltpu.SemaphoreType.DMA((7, CHUNKS)),
        ],
        compiler_params=pltpu.CompilerParams(
            collective_id=identity, has_side_effects=True, vmem_limit_bytes=58 * 2**20
        ),
        cost_estimate=pl.CostEstimate(
            flops=2 * left.size * width, bytes_accessed=64 * count * width, transcendentals=0
        ),
        name="scatter_tokens",
    )(left.reshape(8, count, depth), right, *term)


def exchange_kernel(last, triple_step, *refs):
    refs = list(refs)
    take = lambda n: [refs.pop(0) for _ in range(n)]
    deep_in, turn_in, triple_in, vec_in = take(4)
    expand_in = take(1)[0] if last else None
    deep_out, turn_out, triple_out = take(3)
    if last:
        expand_out = take(1)[0]
    vec_out = take(1)[0]
    if last:
        triple_columns, expand_columns = triple_out, expand_out
        triple_out, expand_out, near, far, here = take(5)
    send, recv, local_sem = take(3)
    c, z = lax.axis_index("dp"), lax.axis_index("z")
    y, x = lax.axis_index("y"), lax.axis_index("x")
    place = y * 2 + x
    rank = c * 4 + place

    def deep(i):
        return lax.rem(z + i, 4)

    def flat(i):
        return lax.rem(place + i, 4)

    def wide(i):
        return lax.rem(rank + i, 8)

    def deep_peer(i):
        return {"z": deep(i)}

    def flat_peer(i):
        return {"y": flat(i) // 2, "x": lax.rem(flat(i), 2)}

    def wide_peer(i):
        return {
            "dp": wide(i) // 4,
            "y": lax.rem(wide(i), 4) // 2,
            "x": lax.rem(wide(i), 2),
        }

    low = lax.rem(z, 2)
    turn_from = {"z": z - low + 1 - x, "x": low}
    turn_to = {"z": z - low + x, "x": 1 - low}
    if last:
        turn_from, turn_to = turn_to, turn_from
    others = range(1, 4)
    greet([deep_peer(i) for i in others] + [wide_peer(i) for i in range(1, 8)])
    sent, waits, kept = [], [], []
    count = [0]

    def post(src, dst, peer, landing):
        k = count[0]
        count[0] += 1
        one = remote(src, dst, send.at[k], recv.at[k], peer)
        one.start()
        sent.append(one)
        return remote(landing, landing, send.at[k], recv.at[k], peer)

    def keep(src, dst):
        one = pltpu.make_async_copy(src, dst, local_sem.at[len(kept)])
        one.start()
        kept.append(one)

    def parts(src, dst, order, block):
        if last:
            return [(src.at[block], dst.at[place])]
        steps = src.shape[1] // 4 // order[0]
        step = order[0]
        return [
            (
                src.at[:, pl.ds(pl.multiple_of((i * 4 + order[1](block)) * step, step), step)],
                dst.at[place, :, pl.ds(i * step, step)],
            )
            for i in range(steps)
        ]

    def turn_columns(src, dst, order):
        for i in others:
            for n, (a, b) in enumerate(parts(src, dst, order, flat(i))):
                landing = dst.at[flat(4 - i)]
                if not last:
                    landing = landing.at[:, pl.ds(n * order[0], order[0])]
                waits.append(post(a, b, flat_peer(i), landing))

    triple_order = (triple_step, lambda p: 2 * (1 - lax.rem(p, 2)) + p // 2)
    stage, late = [], []
    turn_columns(triple_in, triple_out, triple_order)
    for i in others:
        late.append(post(deep_in.at[deep(i)], deep_out.at[z], deep_peer(i), deep_out.at[deep(4 - i)]))
    for i in range(1, 8):
        if last:
            landing = near.at[wide(8 - i)]
            stage.append(post(vec_in.at[wide(i)], near.at[rank], wide_peer(i), landing))
        else:
            landing = vec_out.at[z, wide(8 - i)]
            stage.append(post(vec_in, vec_out.at[z, rank], wide_peer(i), landing))
    late.append(post(turn_in, turn_out, turn_to, turn_out))
    if last:
        turn_columns(expand_in, expand_out, None)
        keep(expand_in.at[place], expand_out.at[place])
    keep(deep_in.at[z], deep_out.at[z])
    for a, b in parts(triple_in, triple_out, triple_order, place):
        keep(a, b)
    if last:
        own = pltpu.make_async_copy(vec_in.at[rank], near.at[rank], local_sem.at[len(kept)])
        own.start()
        for one in stage:
            one.wait_recv()
        own.wait()
        here[...] = jnp.sum(near[...], 0)
        stage = []
        for i in others:
            landing = far.at[deep(4 - i)]
            stage.append(post(here.at[deep(i)], far.at[z], deep_peer(i), landing))
        far[z] = here[z]
        for one in stage:
            one.wait_recv()
        vec_out[...] = jnp.sum(far[...], 0)
    else:
        own = pltpu.make_async_copy(vec_in, vec_out.at[z, rank], local_sem.at[len(kept)])
        own.start()
        for one in stage:
            one.wait_recv()
        own.wait()
        for i in others:
            landing = vec_out.at[deep(4 - i)]
            late.append(post(vec_out.at[z], vec_out.at[z], deep_peer(i), landing))
    for one in waits:
        one.wait_recv()
    for one in kept:
        one.wait()
    if last:
        for (steps, order), blocks, columns in zip(
            last, (triple_out, expand_out), (triple_columns, expand_columns)
        ):
            step = blocks.shape[2] // steps
            for i in range(steps):
                for p in range(4):
                    first = (i * 4 + order[p]) * step
                    columns[:, first : first + step] = blocks[p, :, i * step : (i + 1) * step]
    for one in late:
        one.wait_recv()
    for one in sent:
        one.wait_send()


def exchange(identity, deep, turned, triple, vector, step, expand=None, last=None):
    half = triple.dtype
    operands = [deep, turned, triple, vector] + ([expand] if last else [])
    shapes = [jax.ShapeDtypeStruct(a.shape, a.dtype) for a in (deep, turned)]
    hbm, vmem = pl.BlockSpec(memory_space=pl.ANY), pl.BlockSpec(memory_space=pltpu.VMEM)
    scratch = []
    if last:
        tile = vector.shape[2:]
        shapes += [jax.ShapeDtypeStruct((a.shape[1], 4 * a.shape[2]), half) for a in (triple, expand)]
        shapes.append(jax.ShapeDtypeStruct(tile, vector.dtype))
        scratch = [pltpu.VMEM(triple.shape, half), pltpu.VMEM(expand.shape, half)]
        scratch += [pltpu.VMEM(n + tile, vector.dtype) for n in ((8, 4), (4,), (4,))]
        places = [hbm, hbm, vmem, vmem, vmem]
        copies = 14 + 6
    else:
        rows, columns = triple.shape
        shapes.append(jax.ShapeDtypeStruct((4, rows, columns // 4), half))
        shapes.append(jax.ShapeDtypeStruct((4, 8) + vector.shape, vector.dtype))
        places = [hbm] * 4
        copies = 14 + 3 * (columns // 4 // step)
    moved = sum(a.size * a.dtype.itemsize for a in operands)
    return pl.pallas_call(
        functools.partial(exchange_kernel, last, step),
        out_shape=shapes,
        in_specs=[hbm] * len(operands),
        out_specs=places,
        scratch_shapes=scratch
        + [
            pltpu.SemaphoreType.DMA((copies,)),
            pltpu.SemaphoreType.DMA((copies,)),
            pltpu.SemaphoreType.DMA((8,)),
        ],
        compiler_params=pltpu.CompilerParams(
            collective_id=identity, has_side_effects=True, vmem_limit_bytes=24 * 2**20
        ),
        cost_estimate=pl.CostEstimate(flops=0, bytes_accessed=16 * moved, transcendentals=0),
        name="exchange",
    )(*operands)


def turn_kernel(step, src_ref, dst_ref, send, recv, local_sem):
    place = lax.axis_index("y") * 2 + lax.axis_index("x")
    count = dst_ref.shape[2] // step

    def peer(i):
        chip = lax.rem(place + i, 4)
        return {"y": chip // 2, "x": lax.rem(chip, 2)}

    def columns(chip, n):
        return src_ref.at[:, pl.ds(pl.multiple_of((n * 4 + chip) * step, step), step)]

    greet([peer(i) for i in range(1, 4)])
    moves, waits = [], []
    for i in range(1, 4):
        for n in range(count):
            part = pl.ds(n * step, step)
            sems = send.at[i - 1, n], recv.at[i - 1, n]
            block = columns(lax.rem(place + i, 4), n)
            one = remote(block, dst_ref.at[place, :, part], *sems, peer(i))
            one.start()
            moves.append(one)
            landing = dst_ref.at[lax.rem(place + 4 - i, 4), :, part]
            waits.append(remote(landing, landing, *sems, peer(i)))
    kept = []
    for n in range(count):
        part = pl.ds(n * step, step)
        kept.append(
            pltpu.make_async_copy(
                columns(place, n), dst_ref.at[place, :, part], local_sem.at[n]
            )
        )
        kept[-1].start()
    for one in waits:
        one.wait_recv()
    for one in moves:
        one.wait_send()
    for one in kept:
        one.wait()


def turn_columns(rows, step):
    count, columns = rows.shape
    steps = columns // 4 // step
    return pl.pallas_call(
        functools.partial(turn_kernel, step),
        out_shape=jax.ShapeDtypeStruct((4, count, columns // 4), rows.dtype),
        in_specs=[pl.BlockSpec(memory_space=pl.ANY)],
        out_specs=pl.BlockSpec(memory_space=pl.ANY),
        scratch_shapes=[
            pltpu.SemaphoreType.DMA((3, steps)),
            pltpu.SemaphoreType.DMA((3, steps)),
            pltpu.SemaphoreType.DMA((steps,)),
        ],
        compiler_params=pltpu.CompilerParams(collective_id=7, has_side_effects=True),
        cost_estimate=pl.CostEstimate(
            flops=0, bytes_accessed=16 * count * columns, transcendentals=0
        ),
        name="turn_columns",
    )(rows)


def scores_of(item_ref, first, block, slope, prefix, depth, seq_rows):
    length = item_ref.shape[0]
    head_dim = item_ref.shape[1] // 3
    own_rows = depth * seq_rows
    chips = length // own_rows

    def position(index):
        chip = index // own_rows
        rest = index % own_rows
        return ((rest // seq_rows) * chips + chip) * seq_rows + rest % seq_rows

    queries = item_ref[first : first + block, :head_dim]
    keys = item_ref[:, head_dim : 2 * head_dim]
    raw = lax.dot_general(
        keys, queries, (((1,), (1,)), ((), ())), preferred_element_type=jnp.float32
    )
    key_pos = position(lax.broadcasted_iota(jnp.int32, (length, 1), 0))
    query_pos = position(first + lax.broadcasted_iota(jnp.int32, (1, block), 1))
    bound = jnp.where(key_pos < prefix, -1, key_pos)
    distance = jnp.abs(
        query_pos.astype(jnp.float32) - key_pos.astype(jnp.float32)
    )
    scores = raw * (LOG2E / math.sqrt(head_dim)) - (slope * LOG2E) * distance
    return jnp.where(bound <= query_pos, scores, jnp.float32(-1e30))


def forward_kernel(depth, seq_rows, block, prefix_ref, slope_ref, item_ref, mixed_ref, total_ref):
    prefix = prefix_ref[pl.program_id(0)]
    slope = slope_ref[pl.program_id(1)]
    length = item_ref.shape[0]
    head_dim = item_ref.shape[1] // 3
    for first in range(0, length, block):
        scores = scores_of(item_ref, first, block, slope, prefix, depth, seq_rows)
        top = jnp.max(scores, 0, keepdims=True)
        powers = jnp.exp2(scores - top)
        total = jnp.sum(powers, 0, keepdims=True)
        probs = (powers * (1.0 / total)).astype(jnp.bfloat16)
        mixed = lax.dot_general(
            probs,
            item_ref[:, 2 * head_dim :],
            (((0,), (0,)), ((), ())),
            preferred_element_type=jnp.float32,
        )
        mixed_ref[first : first + block, :] = mixed.astype(mixed_ref.dtype)
        total_ref[0, :, first : first + block] = top + jnp.log2(total)


def attend_forward(projected, slopes, prefixes, own_heads, head_dim, depth, seq_rows):
    cores = prefixes.shape[0]
    length = projected.shape[0] // cores
    block = min(256, length)
    scores = cores * own_heads * length * length
    return pl.pallas_call(
        functools.partial(forward_kernel, depth, seq_rows, block),
        grid=(cores, own_heads),
        out_shape=[
            jax.ShapeDtypeStruct((cores * length, own_heads * head_dim), projected.dtype),
            jax.ShapeDtypeStruct((cores * own_heads, 1, length), jnp.float32),
        ],
        in_specs=[
            pl.BlockSpec(memory_space=pltpu.SMEM),
            pl.BlockSpec(memory_space=pltpu.SMEM),
            pl.BlockSpec((length, 3 * head_dim), lambda s, h: (s, h)),
        ],
        out_specs=[
            pl.BlockSpec((length, head_dim), lambda s, h: (s, h)),
            pl.BlockSpec((1, 1, length), lambda s, h: (s * own_heads + h, 0, 0)),
        ],
        compiler_params=pltpu.CompilerParams(vmem_limit_bytes=48 * 2**20),
        cost_estimate=pl.CostEstimate(
            flops=4 * scores * head_dim,
            bytes_accessed=2 * projected.size * 2,
            transcendentals=scores,
        ),
        name="attend_forward",
    )(prefixes, slopes, projected)


def backward_kernel(
    depth, seq_rows, block, prefix_ref, slope_ref, item_ref, grad_ref, total_ref, out_ref, key_sum, value_sum
):
    prefix = prefix_ref[pl.program_id(0)]
    slope = slope_ref[pl.program_id(1)]
    length = item_ref.shape[0]
    head_dim = item_ref.shape[1] // 3
    scale = 1.0 / math.sqrt(head_dim)
    half = jnp.bfloat16
    wide = jnp.float32
    for first in range(0, length, block):
        scores = scores_of(item_ref, first, block, slope, prefix, depth, seq_rows)
        probs = jnp.exp2(scores - total_ref[0, :, first : first + block])
        grad = grad_ref[first : first + block, :]
        grad_probs = lax.dot_general(
            item_ref[:, 2 * head_dim :],
            grad,
            (((1,), (1,)), ((), ())),
            preferred_element_type=wide,
        )
        inner = jnp.sum(grad_probs * probs, 0, keepdims=True)
        grad_scores = (probs * (grad_probs - inner)).astype(half)
        key_term = jnp.dot(
            grad_scores, item_ref[first : first + block, :head_dim], preferred_element_type=wide
        )
        value_term = jnp.dot(probs.astype(half), grad, preferred_element_type=wide)
        query_grad = lax.dot_general(
            grad_scores,
            item_ref[:, head_dim : 2 * head_dim],
            (((0,), (0,)), ((), ())),
            preferred_element_type=wide,
        )
        out_ref[first : first + block, :head_dim] = (query_grad * scale).astype(half)
        if first == 0:
            key_sum[...] = key_term
            value_sum[...] = value_term
        else:
            key_sum[...] += key_term
            value_sum[...] += value_term
    out_ref[:, head_dim : 2 * head_dim] = (key_sum[...] * scale).astype(half)
    out_ref[:, 2 * head_dim :] = value_sum[...].astype(half)


def attend_backward(
    projected, grad_mixed, totals, slopes, prefixes, own_heads, head_dim, depth, seq_rows
):
    cores = prefixes.shape[0]
    length = projected.shape[0] // cores
    block = min(256, length)
    scores = cores * own_heads * length * length
    return pl.pallas_call(
        functools.partial(backward_kernel, depth, seq_rows, block),
        grid=(cores, own_heads),
        out_shape=jax.ShapeDtypeStruct(projected.shape, projected.dtype),
        in_specs=[
            pl.BlockSpec(memory_space=pltpu.SMEM),
            pl.BlockSpec(memory_space=pltpu.SMEM),
            pl.BlockSpec((length, 3 * head_dim), lambda s, h: (s, h)),
            pl.BlockSpec((length, head_dim), lambda s, h: (s, h)),
            pl.BlockSpec((1, 1, length), lambda s, h: (s * own_heads + h, 0, 0)),
        ],
        out_specs=pl.BlockSpec((length, 3 * head_dim), lambda s, h: (s, h)),
        scratch_shapes=[
            pltpu.VMEM((length, head_dim), jnp.float32),
            pltpu.VMEM((length, head_dim), jnp.float32),
        ],
        compiler_params=pltpu.CompilerParams(vmem_limit_bytes=48 * 2**20),
        cost_estimate=pl.CostEstimate(
            flops=10 * scores * head_dim,
            bytes_accessed=2 * projected.size * 2,
            transcendentals=scores,
        ),
        name="attend_backward",
    )(prefixes, slopes, projected, grad_mixed, totals)


def planar(
    hidden,
    prefix_lengths,
    cotangent,
    first_gain,
    first_shift,
    triple_weight,
    pair_bias,
    dense_weight,
    dense_shift,
    second_gain,
    second_shift,
    expand_weight,
    expand_shift,
    shrink_weight,
    shrink_shift,
):
    wide = jnp.float32
    half = jnp.bfloat16
    cores = lax.axis_size("dp")
    depth = lax.axis_size("z")
    rows_y = lax.axis_size("y")
    rows_x = lax.axis_size("x")
    plane = rows_y * rows_x
    core = lax.axis_index("dp")
    at_y = lax.axis_index("y")
    at_x = lax.axis_index("x")
    place = at_y * rows_x + at_x
    seq_rows = hidden.shape[2]
    width = hidden.shape[3]
    head_dim = triple_weight.shape[3]
    heads = triple_weight.shape[1]
    own_heads = heads // plane
    own_rows = seq_rows * depth
    units = expand_weight.shape[1]
    own_units = units // plane
    row_block = expand_weight.shape[0]
    shrink_rows = shrink_weight.shape[0]

    pieces = [
        first_gain,
        first_shift,
        dense_shift,
        second_gain,
        second_shift,
        shrink_shift,
        pair_bias,
        expand_shift,
    ]
    piece_total = sum(p.shape[0] for p in pieces)
    lanes = 128
    vector_rows = -(-piece_total // (lanes * 16)) * 16
    vector_tile = jnp.pad(
        jnp.concatenate(pieces), (0, vector_rows * lanes - piece_total)
    ).reshape(vector_rows, lanes)
    inputs, dense_turned, triple_turned, packed = exchange(
        3,
        hidden[:, 0],
        dense_weight,
        triple_weight.reshape(row_block, heads * 3 * head_dim),
        vector_tile,
        3 * head_dim,
    )
    packed = (
        packed.reshape(depth, cores, plane, vector_rows * lanes)
        .transpose(1, 0, 2, 3)
        .reshape(-1, vector_rows * lanes)
    )
    vectors = []
    offset = 0
    for piece in pieces:
        vectors.append(packed[:, offset : offset + piece.shape[0]].reshape(-1).astype(wide))
        offset += piece.shape[0]
    gain_one, shift_one, dense_bias, gain_two, shift_two, shrink_bias, pair_full, unit_full = vectors
    pair_heads = pair_full.reshape(cores, own_heads, rows_x, rows_y, 2, head_dim)[
        core, :, 1 - at_x, at_y
    ]
    triple_bias = jnp.stack(
        [pair_heads[:, 0], jnp.zeros_like(pair_heads[:, 0]), pair_heads[:, 1]], 1
    ).reshape(-1)
    unit_bias = unit_full.reshape(cores, depth, plane, shrink_rows)[core, :, place].reshape(-1)

    triple_own = lax.all_gather(
        triple_turned.reshape(-1, triple_turned.shape[2]), "z", axis=0, tiled=True
    )
    inputs = inputs.reshape(own_rows, width).astype(wide)

    normed_own = layer_norm(inputs, gain_one, shift_one).astype(half)
    normed, upstream = gather_tokens(6, normed_own, cotangent[:, 0])
    upstream = upstream.reshape(own_rows, width)
    expand_turned = turn_columns(after(expand_weight, normed), shrink_rows)
    upstream_all, dense_own = gather_tokens(1, after(upstream, expand_turned), dense_turned, True)
    dense_own = dense_own.reshape(own_heads * head_dim, width)
    expand_own = lax.all_gather(
        expand_turned.reshape(-1, own_units), "z", axis=0, tiled=True
    )
    projected = (
        jnp.dot(normed, triple_own, preferred_element_type=wide) + triple_bias
    ).astype(half)

    shrink_own = lax.all_gather(after(shrink_weight, projected), "z", axis=0, tiled=True)
    head_index = core * heads + jnp.arange(own_heads) * plane + (1 - at_x) * rows_y + at_y
    slopes = jnp.power(
        jnp.float32(2.0), -8.0 * (head_index.astype(wide) + 1.0) / (heads * cores)
    )
    at_z = lax.axis_index("z")
    prefixes = lax.dynamic_index_in_dim(prefix_lengths, at_z, 0, False)
    mixed, log_totals = attend_forward(
        projected, slopes, prefixes, own_heads, head_dim, depth, seq_rows
    )
    (dense_sum,) = scatter_tokens(2, mixed, dense_own)
    middle = inputs + dense_sum + dense_bias
    normed_two_own, norm_two_pull = jax.vjp(layer_norm, middle, gain_two, shift_two)
    (normed_two,) = gather_tokens(5, normed_two_own.astype(half))
    hidden_pre = jnp.dot(normed_two, expand_own, preferred_element_type=wide) + unit_bias
    activated, gelu_pull = jax.vjp(gelu_tanh, hidden_pre)
    activated = activated.astype(half)
    shrink_term = jnp.einsum(
        "tu,td->ud", activated, upstream_all, preferred_element_type=wide
    ).astype(half)
    shrink_own = after(shrink_own, shrink_term)
    grad_act = jnp.einsum("tf,uf->tu", upstream_all, shrink_own, preferred_element_type=wide)
    grad_pre = gelu_pull(grad_act)[0].astype(half)
    shrink_grad = lax.psum_scatter(shrink_term, "z", scatter_dimension=0, tiled=True)
    feed_sum, expand_term = scatter_tokens(
        8, after(activated, shrink_term), shrink_own, term=(normed_two, grad_pre)
    )
    expand_turned = lax.psum_scatter(expand_term, "z", scatter_dimension=0, tiled=True)
    layer_output = (middle + feed_sum + shrink_bias).astype(half)

    (norm_two_sum,) = scatter_tokens(9, after(grad_pre, feed_sum), expand_own, True)
    grad_norm_two, gain_two_term, shift_two_term = norm_two_pull(norm_two_sum)
    grad_middle = upstream.astype(wide) + grad_norm_two
    branch_own = grad_middle.astype(half)
    branch, layer_output = gather_tokens(
        6, branch_own, layer_output.reshape(depth, seq_rows, width)
    )

    grad_mixed = jnp.einsum("tf,ef->te", branch, dense_own, preferred_element_type=wide).astype(
        half
    )
    dense_term = jnp.einsum("te,tf->ef", mixed, branch, preferred_element_type=wide).astype(half)
    dense_turned = lax.psum_scatter(dense_term, "z", scatter_dimension=0, tiled=True)
    grad_project = attend_backward(
        projected,
        after(grad_mixed, dense_term),
        log_totals,
        slopes,
        prefixes,
        own_heads,
        head_dim,
        depth,
        seq_rows,
    )
    triple_term = jnp.einsum(
        "td,tc->dc", normed, grad_project, preferred_element_type=wide
    ).astype(half)
    triple_turned = lax.psum_scatter(triple_term, "z", scatter_dimension=0, tiled=True)
    (norm_one_sum,) = scatter_tokens(10, after(grad_project, triple_term), triple_own, True)
    grad_norm_one, gain_one_term, shift_one_term = jax.vjp(
        layer_norm, inputs, gain_one, shift_one
    )[1](norm_one_sum)
    hidden_grad = (grad_middle + grad_norm_one).astype(half)
    head_sums = jnp.sum(grad_project, 0, dtype=wide).reshape(own_heads, 3, head_dim)
    pair_term = jnp.stack([head_sums[:, 0], head_sums[:, 2]], 1)
    pair_zero = jnp.zeros((cores, own_heads, rows_x, rows_y, 2, head_dim), wide)
    pair_wide = lax.dynamic_update_slice(
        pair_zero, pair_term[None, :, None, None], (core, 0, 1 - at_x, at_y, 0, 0)
    ).reshape(-1)
    unit_term = jnp.sum(grad_pre, 0, dtype=wide).reshape(1, depth, 1, shrink_rows)
    unit_wide = lax.dynamic_update_slice(
        jnp.zeros((cores, depth, plane, shrink_rows), wide), unit_term, (core, 0, place, 0)
    ).reshape(-1)
    terms = [
        gain_one_term,
        shift_one_term,
        jnp.sum(branch_own, 0, dtype=wide),
        gain_two_term,
        shift_two_term,
        jnp.sum(upstream, 0, dtype=wide),
        pair_wide,
        unit_wide,
    ]
    devices = cores * depth * plane
    term_rows = -(-piece_total // (lanes * 8)) * 8
    term_tiles = jnp.pad(
        jnp.concatenate([t.reshape(devices, -1) for t in terms], 1),
        ((0, 0), (0, term_rows * lanes - piece_total)),
    )
    term_tiles = (
        term_tiles.reshape(cores, depth, plane, term_rows, lanes)
        .transpose(0, 2, 1, 3, 4)
        .reshape(cores * plane, depth, term_rows, lanes)
    )
    hidden_grad, dense_grad, triple_grad, expand_grad, summed = exchange(
        4,
        hidden_grad.reshape(depth, seq_rows, width),
        dense_turned,
        triple_turned.reshape(plane, row_block, -1),
        term_tiles,
        3 * head_dim,
        expand_turned.reshape(plane, row_block, own_units),
        last=((own_heads, (2, 0, 3, 1)), (depth, (0, 1, 2, 3))),
    )
    layer_output = layer_output[:, None]
    hidden_grad = hidden_grad[:, None]
    triple_grad = triple_grad.astype(wide).reshape(row_block, heads, 3, head_dim)
    summed = summed.reshape(-1)
    vector_grads = []
    offset = 0
    for piece in pieces:
        vector_grads.append(summed[offset : offset + piece.shape[0]])
        offset += piece.shape[0]
    return (
        layer_output,
        hidden_grad,
        vector_grads[0],
        vector_grads[1],
        triple_grad,
        vector_grads[6],
        dense_grad.astype(wide),
        vector_grads[2],
        vector_grads[3],
        vector_grads[4],
        expand_grad.astype(wide),
        vector_grads[7],
        shrink_grad.astype(wide),
        vector_grads[5],
    )


def layer(*args):
    return planar(*args)


def solution(mesh):
    depth = 4
    sides = (2, 2)
    planar_plan = mesh.shape["seq"] == depth * sides[0] * sides[1]
    if planar_plan:
        grid = Mesh(
            mesh.devices.reshape(mesh.shape["dp"], depth, *sides), ("dp", "z", "y", "x")
        )
        seq = ("z", "y", "x")
    else:
        grid = mesh
        seq = ("seq",)
    tokens = P(None, "dp", seq, None)
    vector = P(("dp",) + seq)
    matrix = P(("dp",) + seq, None)
    placed = (
        tokens,
        P(),
        tokens,
        vector,
        vector,
        P(seq, "dp", None, None),
        vector,
        matrix,
        vector,
        vector,
        vector,
        P(seq, "dp"),
        vector,
        matrix,
        vector,
    )
    results = (
        tokens,
        tokens,
        vector,
        vector,
        P(seq, "dp", None, None),
        vector,
        matrix,
        vector,
        vector,
        vector,
        P(seq, "dp"),
        vector,
        matrix,
        vector,
    )
    return jax.shard_map(
        layer if planar_plan else shards,
        mesh=grid,
        in_specs=placed,
        out_specs=results,
        check_vma=False,
    )
```

```python
import functools
import math

import jax
import jax.numpy as jnp
from jax import lax
from jax.experimental import pallas as pl
from jax.experimental.pallas import tpu as pltpu
from jax.sharding import Mesh
from jax.sharding import PartitionSpec as P


EPSILON = 1e-05
GELU_SCALE = 0.7978845608028654


def layer_norm(inputs, norm_gain, norm_shift):
    centered = inputs - jnp.mean(inputs, -1, keepdims=True)
    variance = jnp.mean(centered * centered, -1, keepdims=True)
    return centered * lax.rsqrt(variance + EPSILON) * norm_gain + norm_shift


def gelu_tanh(values):
    return (
        0.5 * values * (1.0 + jnp.tanh(GELU_SCALE * (values + 0.044715 * values * values * values)))
    )


def split_norm(inputs, gain_rows, shift_rows):
    return layer_norm(inputs, gain_rows[None, :, None, :], shift_rows[None, :, None, :])


def place_half(values, half_index, group_count):
    chosen = (jnp.arange(group_count, dtype=jnp.int32) == half_index).astype(values.dtype)
    return (chosen[:, None] * values.reshape(1, -1)).reshape(-1)


def shards(
    hidden,
    prefix_lengths,
    cotangent,
    first_gain,
    first_shift,
    triple_weight,
    pair_bias,
    dense_weight,
    dense_shift,
    second_gain,
    second_shift,
    expand_weight,
    expand_shift,
    shrink_weight,
    shrink_shift,
):
    wide_type = jnp.float32
    half_type = jnp.bfloat16
    seq_count = lax.axis_size("seq")
    group_count = lax.axis_size("dp")
    dp_index = lax.axis_index("dp")
    seq_index = lax.axis_index("seq")
    micro_count = hidden.shape[0]
    seq_rows = hidden.shape[2]
    model_width = hidden.shape[3]
    seq_length = seq_rows * seq_count
    local_heads = triple_weight.shape[1]
    head_dim = triple_weight.shape[3]
    head_total = local_heads * group_count
    pair_local = micro_count * group_count * local_heads // seq_count
    unit_local = expand_weight.shape[1]
    project_width = 3 * local_heads * head_dim
    token_total = micro_count * group_count * seq_rows
    score_scale = 1.0 / math.sqrt(head_dim)
    block_rows = min(512, seq_length)
    block_count = seq_length // block_rows
    key_pos = jnp.arange(seq_length, dtype=jnp.int32)
    gathered = (
        lax.all_gather(triple_weight, "seq", axis=0, tiled=True),
        lax.all_gather(dense_weight, "seq", axis=0, tiled=True),
        lax.all_gather(expand_weight, "seq", axis=0, tiled=True),
        lax.all_gather(shrink_weight, "seq", axis=0, tiled=True),
        lax.all_gather(first_gain, "seq", axis=0, tiled=True),
        lax.all_gather(first_shift, "seq", axis=0, tiled=True),
        lax.all_gather(pair_bias, "seq", axis=0, tiled=True),
        lax.all_gather(dense_shift, "seq", axis=0, tiled=True),
        lax.all_gather(second_gain, "seq", axis=0, tiled=True),
        lax.all_gather(second_shift, "seq", axis=0, tiled=True),
        lax.all_gather(expand_shift, "seq", axis=0, tiled=True),
        lax.all_gather(shrink_shift, "seq", axis=0, tiled=True),
    )
    triple_full, dense_full, expand_full, shrink_full = (
        gathered[0],
        gathered[1],
        gathered[2],
        gathered[3],
    )
    row_sets = (
        lax.all_gather(hidden, "dp", axis=1, tiled=True),
        lax.all_gather(cotangent, "dp", axis=1, tiled=True),
        lax.all_gather(gathered[4], "dp", axis=0, tiled=True),
        lax.all_gather(gathered[5], "dp", axis=0, tiled=True),
        lax.all_gather(gathered[6], "dp", axis=0, tiled=True),
        lax.all_gather(gathered[7], "dp", axis=0, tiled=True),
        lax.all_gather(gathered[8], "dp", axis=0, tiled=True),
        lax.all_gather(gathered[9], "dp", axis=0, tiled=True),
        lax.all_gather(gathered[10], "dp", axis=0, tiled=True),
        lax.all_gather(gathered[11], "dp", axis=0, tiled=True),
    )
    hidden_both = row_sets[0]
    upstream_low = row_sets[1]
    gain_one, shift_one, pair_full, dense_bias, gain_two, shift_two, expand_bias, shrink_bias = [
        vector.astype(wide_type) for vector in row_sets[2:]
    ]
    inputs_both = hidden_both.astype(wide_type)
    normed_low = layer_norm(inputs_both, gain_one, shift_one).astype(half_type)
    pair_heads = lax.dynamic_slice_in_dim(
        pair_full.reshape(head_total, 2, head_dim), dp_index * local_heads, local_heads, 0
    )
    triple_bias = jnp.stack(
        [pair_heads[:, 0], jnp.zeros_like(pair_heads[:, 0]), pair_heads[:, 1]], 0
    )
    projected = jnp.einsum(
        "mstd,dhce->cmshte", normed_low, triple_full, preferred_element_type=wide_type
    )
    projected = projected + triple_bias[:, None, None, :, None, :]
    project_low = projected.astype(half_type).reshape(3, seq_count, pair_local, seq_rows, head_dim)
    pair_rows = lax.all_to_all(project_low, "seq", split_axis=1, concat_axis=3, tiled=True)[:, 0]
    query_all, key_all, value_all = (pair_rows[0], pair_rows[1], pair_rows[2])
    pair_index = seq_index * pair_local + jnp.arange(pair_local, dtype=jnp.int32)
    head_index = dp_index * local_heads + pair_index % local_heads
    sequence_index = pair_index // local_heads
    slopes = jnp.power(jnp.float32(2.0), -8.0 * (head_index.astype(wide_type) + 1.0) / head_total)
    prefix_flat = prefix_lengths.reshape(-1)
    prefix_slots = jnp.arange(prefix_flat.shape[0], dtype=jnp.int32)
    prefixes = jnp.sum(
        jnp.where(prefix_slots[None, :] == sequence_index[:, None], prefix_flat[None, :], 0), 1
    )

    def block_scores(pair_item, first_row):
        query_block = lax.dynamic_slice_in_dim(
            lax.dynamic_index_in_dim(query_all, pair_item, 0, False), first_row, block_rows, 0
        )
        keys_item = lax.dynamic_index_in_dim(key_all, pair_item, 0, False)
        head_slope = lax.dynamic_index_in_dim(slopes, pair_item, 0, False)
        prefix = lax.dynamic_index_in_dim(prefixes, pair_item, 0, False)
        query_pos = first_row + jnp.arange(block_rows, dtype=jnp.int32)
        raw_scores = (
            jnp.einsum("qe,ke->qk", query_block, keys_item, preferred_element_type=wide_type)
            * score_scale
        )
        distance = jnp.abs(query_pos[:, None] - key_pos[None, :]).astype(wide_type)
        raw_scores = raw_scores - head_slope * distance
        allowed = (key_pos[None, :] <= query_pos[:, None]) | (key_pos[None, :] < prefix)
        return (query_block, jnp.where(allowed, raw_scores, jnp.float32(-1e30)))

    def forward_block(flat_index):
        pair_item = flat_index // block_count
        first_row = flat_index % block_count * block_rows
        _, scores = block_scores(pair_item, first_row)
        row_max = jnp.max(scores, -1, keepdims=True)
        powers = jnp.exp(scores - row_max)
        row_total = jnp.sum(powers, -1, keepdims=True)
        probs_low = (powers / row_total).astype(half_type)
        values_item = lax.dynamic_index_in_dim(value_all, pair_item, 0, False)
        mixed = jnp.dot(probs_low, values_item, preferred_element_type=wide_type).astype(half_type)
        return (mixed, (row_max + jnp.log(row_total))[:, 0])

    mixed_blocks, log_blocks = lax.map(
        forward_block, jnp.arange(pair_local * block_count, dtype=jnp.int32)
    )
    mixed_pairs = mixed_blocks.reshape(pair_local, seq_count, seq_rows, head_dim)
    log_totals = log_blocks.reshape(pair_local, seq_length)
    mixed_home = lax.all_to_all(mixed_pairs, "seq", split_axis=1, concat_axis=0, tiled=True)
    mixed_tokens = jnp.transpose(
        mixed_home.reshape(micro_count, group_count, local_heads, seq_rows, head_dim),
        (0, 1, 3, 2, 4),
    ).reshape(micro_count, group_count, seq_rows, local_heads * head_dim)
    dense_part = jnp.einsum(
        "mstk,kf->mstf", mixed_tokens, dense_full, preferred_element_type=wide_type
    )
    attention_sum = lax.psum(dense_part.astype(jnp.bfloat16), "dp").astype(jnp.float32)
    middle = inputs_both + attention_sum + dense_bias
    gain_rows_two = jnp.broadcast_to(gain_two[None, :], (group_count, model_width))
    shift_rows_two = jnp.broadcast_to(shift_two[None, :], (group_count, model_width))
    normed_two, norm_two_pull = jax.vjp(split_norm, middle, gain_rows_two, shift_rows_two)
    normed_two_low = normed_two.astype(half_type)
    unit_bias = lax.dynamic_slice_in_dim(expand_bias, dp_index * unit_local, unit_local, 0)
    hidden_pre = (
        jnp.einsum("mstd,df->mstf", normed_two_low, expand_full, preferred_element_type=wide_type)
        + unit_bias
    )
    activated_value, gelu_pull = jax.vjp(gelu_tanh, hidden_pre)
    activated_low = activated_value.astype(half_type)
    feed_part = jnp.einsum(
        "mstf,fd->mstd", activated_low, shrink_full, preferred_element_type=wide_type
    )
    feed_sum = lax.psum_scatter(
        feed_part.astype(jnp.bfloat16), "dp", scatter_dimension=1, tiled=True
    ).astype(jnp.float32)
    middle_own = lax.dynamic_slice_in_dim(middle, dp_index, 1, 1)
    layer_output = (middle_own + feed_sum + shrink_bias).astype(half_type)
    triple_back, dense_back, expand_back, shrink_back = (
        lax.all_gather(triple_weight, "seq", axis=0, tiled=True),
        lax.all_gather(dense_weight, "seq", axis=0, tiled=True),
        lax.all_gather(expand_weight, "seq", axis=0, tiled=True),
        lax.all_gather(shrink_weight, "seq", axis=0, tiled=True),
    )
    grad_act = jnp.einsum(
        "mstd,fd->mstf", upstream_low, shrink_back, preferred_element_type=wide_type
    )
    grad_pre_low = gelu_pull(grad_act)[0].astype(half_type)
    norm_two_part = jnp.einsum(
        "mstf,df->mstd", grad_pre_low, expand_back, preferred_element_type=wide_type
    )
    grad_normed_two = lax.psum(norm_two_part.astype(jnp.bfloat16), "dp").astype(jnp.float32)
    grad_middle_norm, grad_gain_rows_two, grad_shift_rows_two = norm_two_pull(grad_normed_two)
    grad_middle = upstream_low.astype(wide_type) + grad_middle_norm
    grad_branch_low = grad_middle.astype(half_type)
    go_pairs = jnp.einsum(
        "mstf,hef->mshte",
        grad_branch_low,
        dense_back.reshape(local_heads, head_dim, model_width),
        preferred_element_type=wide_type,
    ).astype(half_type)
    go_pairs = go_pairs.reshape(seq_count, pair_local, seq_rows, head_dim)
    grad_mixed_pairs = lax.all_to_all(go_pairs, "seq", split_axis=0, concat_axis=2, tiled=True)[0]

    def backward_item(pair_item):
        keys_item = lax.dynamic_index_in_dim(key_all, pair_item, 0, False)
        values_item = lax.dynamic_index_in_dim(value_all, pair_item, 0, False)
        grad_mixed_item = lax.dynamic_index_in_dim(grad_mixed_pairs, pair_item, 0, False)
        totals_item = lax.dynamic_index_in_dim(log_totals, pair_item, 0, False)

        def backward_block(running, block_index):
            key_grad, value_grad = running
            first_row = block_index * block_rows
            query_block, scores = block_scores(pair_item, first_row)
            soft_probs = jnp.exp(
                scores - lax.dynamic_slice_in_dim(totals_item, first_row, block_rows, 0)[:, None]
            )
            grad_block = lax.dynamic_slice_in_dim(grad_mixed_item, first_row, block_rows, 0)
            grad_probs = jnp.einsum(
                "qe,ke->qk", grad_block, values_item, preferred_element_type=wide_type
            )
            row_inner = jnp.sum(grad_probs * soft_probs, -1, keepdims=True)
            grad_scores_low = (soft_probs * (grad_probs - row_inner)).astype(half_type)
            query_grad = (
                jnp.dot(grad_scores_low, keys_item, preferred_element_type=wide_type) * score_scale
            )
            key_grad = (
                key_grad
                + jnp.einsum(
                    "qk,qe->ke", grad_scores_low, query_block, preferred_element_type=wide_type
                )
                * score_scale
            )
            value_grad = value_grad + jnp.einsum(
                "qk,qe->ke",
                soft_probs.astype(half_type),
                grad_block,
                preferred_element_type=wide_type,
            )
            return ((key_grad, value_grad), query_grad)

        zero_rows = jnp.zeros((seq_length, head_dim), wide_type)
        (key_grad, value_grad), query_grads = lax.scan(
            backward_block, (zero_rows, zero_rows), jnp.arange(block_count, dtype=jnp.int32)
        )
        return jnp.stack(
            [query_grads.reshape(seq_length, head_dim), key_grad, value_grad], 0
        ).astype(half_type)

    grad_pairs = lax.map(backward_item, jnp.arange(pair_local, dtype=jnp.int32))
    grad_split = grad_pairs.reshape(pair_local, 3, seq_count, seq_rows, head_dim)
    grad_home = lax.all_to_all(grad_split, "seq", split_axis=2, concat_axis=0, tiled=True)
    grad_project_low = jnp.transpose(
        grad_home.reshape(micro_count, group_count, local_heads, 3, seq_rows, head_dim),
        (0, 1, 4, 2, 3, 5),
    ).reshape(micro_count, group_count, seq_rows, project_width)
    norm_one_part = jnp.einsum(
        "mstc,dc->mstd",
        grad_project_low,
        triple_back.reshape(model_width, project_width),
        preferred_element_type=wide_type,
    )
    grad_normed_one = lax.psum_scatter(
        norm_one_part.astype(jnp.bfloat16), "dp", scatter_dimension=1, tiled=True
    ).astype(jnp.float32)
    inputs_own = hidden.astype(wide_type)
    grad_inputs_norm, grad_gain_one, grad_shift_one = jax.vjp(
        layer_norm, inputs_own, gain_one, shift_one
    )[1](grad_normed_one)
    grad_middle_own = lax.dynamic_slice_in_dim(grad_middle, dp_index, 1, 1)
    hidden_grad = (grad_middle_own + grad_inputs_norm).astype(half_type)
    head_sums = jnp.sum(
        grad_project_low.reshape(micro_count, group_count, seq_rows, local_heads, 3, head_dim),
        (0, 1, 2),
        dtype=wide_type,
    )
    pair_grad = place_half(jnp.stack([head_sums[:, 0], head_sums[:, 2]], 1), dp_index, group_count)
    unit_grad = place_half(jnp.sum(grad_pre_low, (0, 1, 2), dtype=wide_type), dp_index, group_count)
    dense_shift_term = jnp.sum(
        lax.dynamic_slice_in_dim(grad_branch_low, dp_index, 1, 1), (0, 1, 2), dtype=wide_type
    )
    shrink_shift_term = jnp.sum(cotangent, (0, 1, 2), dtype=wide_type)
    gain_two_term = lax.dynamic_index_in_dim(grad_gain_rows_two, dp_index, 0, False)
    shift_two_term = lax.dynamic_index_in_dim(grad_shift_rows_two, dp_index, 0, False)
    vector_sums = (
        lax.psum_scatter(grad_gain_one, ("dp", "seq"), scatter_dimension=0, tiled=True),
        lax.psum_scatter(grad_shift_one, ("dp", "seq"), scatter_dimension=0, tiled=True),
        lax.psum_scatter(pair_grad, ("dp", "seq"), scatter_dimension=0, tiled=True),
        lax.psum_scatter(dense_shift_term, ("dp", "seq"), scatter_dimension=0, tiled=True),
        lax.psum_scatter(gain_two_term, ("dp", "seq"), scatter_dimension=0, tiled=True),
        lax.psum_scatter(shift_two_term, ("dp", "seq"), scatter_dimension=0, tiled=True),
        lax.psum_scatter(unit_grad, ("dp", "seq"), scatter_dimension=0, tiled=True),
        lax.psum_scatter(shrink_shift_term, ("dp", "seq"), scatter_dimension=0, tiled=True),
    )
    normed_flat = normed_low.reshape(token_total, model_width)
    project_flat = grad_project_low.reshape(token_total, project_width)
    normed_two_flat = normed_two_low.reshape(token_total, model_width)
    pre_flat = grad_pre_low.reshape(token_total, unit_local)
    column_sums = lax.psum_scatter(
        jnp.concatenate(
            [
                jnp.einsum(
                    "tr,tc->rc", normed_flat, project_flat, preferred_element_type=wide_type
                ),
                jnp.einsum(
                    "tr,tc->rc", normed_two_flat, pre_flat, preferred_element_type=wide_type
                ),
            ],
            1,
        ),
        "seq",
        scatter_dimension=0,
        tiled=True,
    )
    triple_grad = column_sums[:, :project_width].reshape(
        model_width // seq_count, local_heads, 3, head_dim
    )
    expand_grad = column_sums[:, project_width:]
    dense_rows = dense_weight.shape[0]
    shrink_rows = shrink_weight.shape[0]
    row_block = dense_rows + shrink_rows
    mixed_flat = mixed_tokens.reshape(token_total, local_heads * head_dim)
    branch_flat = grad_branch_low.reshape(token_total, model_width)
    active_flat = activated_low.reshape(token_total, unit_local)
    upstream_flat = upstream_low.reshape(token_total, model_width)
    block_number = row_block * lax.axis_size("seq") // row_block
    dense_term = jnp.einsum("tr,td->rd", mixed_flat, branch_flat, preferred_element_type=wide_type)
    shrink_term = jnp.einsum(
        "tr,td->rd", active_flat, upstream_flat, preferred_element_type=wide_type
    )
    row_sums = lax.psum_scatter(
        jnp.concatenate(
            [
                dense_term.reshape(block_number, dense_rows, model_width),
                shrink_term.reshape(block_number, shrink_rows, model_width),
            ],
            1,
        ).reshape(row_block * lax.axis_size("seq"), model_width),
        "seq",
        scatter_dimension=0,
        tiled=True,
    )
    dense_grad = row_sums[:dense_rows]
    shrink_grad = row_sums[dense_rows:]
    return (
        layer_output,
        hidden_grad,
        vector_sums[0],
        vector_sums[1],
        triple_grad,
        vector_sums[2],
        dense_grad,
        vector_sums[3],
        vector_sums[4],
        vector_sums[5],
        expand_grad,
        vector_sums[6],
        shrink_grad,
        vector_sums[7],
    )


CHUNKS = 4
LOG2E = 1.4426950408889634
MESH = pl.DeviceIdType.MESH


def remote(src, dst, send, recv, peer):
    return pltpu.make_async_remote_copy(
        src_ref=src,
        dst_ref=dst,
        send_sem=send,
        recv_sem=recv,
        device_id=peer,
        device_id_type=MESH,
    )


def greet(peers):
    barrier = pltpu.get_barrier_semaphore()
    for peer in peers:
        pl.semaphore_signal(barrier, inc=1, device_id=peer, device_id_type=MESH)
    pl.semaphore_wait(barrier, len(peers))


class Corner:
    def __init__(self):
        self.c = lax.axis_index("dp")
        self.y = lax.axis_index("y")
        self.x = lax.axis_index("x")
        self.ax = self.x + (1 - self.c) * (1 - 2 * self.x)
        self.ay = self.y + self.c * (1 - 2 * self.y)
        self.bx = self.x + self.c * (1 - 2 * self.x)
        self.by = self.y + (1 - self.c) * (1 - 2 * self.y)
        self.dx = 1 - self.x
        self.dy = 1 - self.y
        self.peer_a = {"y": self.ay, "x": self.ax}
        self.peer_b = {"y": self.by, "x": self.bx}
        self.sibling = {"dp": 1 - self.c}

    def slots(self, core):
        return [
            (core * 2 + y) * 2 + x
            for y, x in (
                (self.dy, self.dx),
                (self.by, self.bx),
                (self.ay, self.ax),
                (self.y, self.x),
            )
        ]


def gather_kernel(deep, whole, *refs):
    if deep:
        rows_ref, deep_ref, all_ref, moved_ref, local_sem, send, recv, deep_send, deep_recv = refs
    else:
        rows_ref, all_ref, local_sem, send, recv = refs
    at = Corner()
    slot_d, slot_b, slot_a, me = at.slots(at.c)
    step = rows_ref.shape[0] // CHUNKS
    peers = [at.peer_a, at.peer_b, at.sibling]
    sent, moves = [], []
    if deep:
        z = lax.axis_index("z")
        plane_at = [lax.rem(z + i, 4) for i in range(4)]
        peers += [{"z": plane_at[i]} for i in range(1, 4)]
    greet(peers)
    locals_ = [pltpu.make_async_copy(rows_ref, all_ref.at[me], local_sem.at[0])]
    if deep:
        block = deep_ref if whole else deep_ref.at[z]
        locals_.append(pltpu.make_async_copy(block, moved_ref.at[z], local_sem.at[1]))
    for one in locals_:
        one.start()

    def copy(kind, k, slot, peer):
        part = pl.ds(k * step, step)
        src = rows_ref.at[part] if kind < 3 else all_ref.at[slot, part]
        return remote(src, all_ref.at[slot, part], send.at[kind, k], recv.at[kind, k], peer)

    def arrived(kind, k, slot, peer):
        part = pl.ds(k * step, step)
        block = all_ref.at[slot, part]
        remote(block, block, send.at[kind, k], recv.at[kind, k], peer).wait_recv()

    def start(kind, k, slot, peer):
        one = copy(kind, k, slot, peer)
        one.start()
        sent.append(one)

    for i in range(1, 4) if deep else ():
        sems = deep_send.at[i - 1], deep_recv.at[i - 1]
        block = deep_ref if whole else deep_ref.at[plane_at[i]]
        one = remote(block, moved_ref.at[z], *sems, {"z": plane_at[i]})
        one.start()
        sent.append(one)
        landing = moved_ref.at[plane_at[4 - i]]
        moves.append(remote(landing, landing, *sems, {"z": plane_at[i]}))
    for k in range(CHUNKS):
        start(0, k, me, at.peer_a)
        start(1, k, me, at.peer_b)
    for k in range(CHUNKS):
        start(2, k, me, at.sibling)
    for k in range(CHUNKS):
        arrived(0, k, slot_a, at.peer_a)
        start(3, k, slot_a, at.peer_b)
        start(4, k, slot_a, at.sibling)
    for k in range(CHUNKS):
        arrived(1, k, slot_b, at.peer_b)
        start(5, k, slot_b, at.sibling)
    for k in range(CHUNKS):
        arrived(3, k, slot_d, at.peer_b)
        start(6, k, slot_d, at.sibling)
    other_d, other_b, other_a, other_me = at.slots(1 - at.c)
    for k in range(CHUNKS):
        arrived(2, k, other_me, at.sibling)
        arrived(4, k, other_b, at.sibling)
        arrived(5, k, other_a, at.sibling)
        arrived(6, k, other_d, at.sibling)
    for one in moves:
        one.wait_recv()
    for one in sent:
        one.wait_send()
    for one in locals_:
        one.wait()


def gather_tokens(identity, rows, deep=None, whole=False):
    count, width = rows.shape
    operands = [rows]
    shapes = [jax.ShapeDtypeStruct((8, count, width), rows.dtype)]
    scratch = [
        pltpu.SemaphoreType.DMA((2,)),
        pltpu.SemaphoreType.DMA((7, CHUNKS)),
        pltpu.SemaphoreType.DMA((7, CHUNKS)),
    ]
    if deep is not None:
        operands.append(deep)
        moved_shape = (4,) + deep.shape if whole else deep.shape
        shapes.append(jax.ShapeDtypeStruct(moved_shape, deep.dtype))
        scratch += [pltpu.SemaphoreType.DMA((3,)), pltpu.SemaphoreType.DMA((3,))]
    all_rows, *moved = pl.pallas_call(
        functools.partial(gather_kernel, deep is not None, whole),
        out_shape=shapes,
        in_specs=[pl.BlockSpec(memory_space=pl.ANY)] * len(operands),
        out_specs=[pl.BlockSpec(memory_space=pl.ANY)] * len(shapes),
        scratch_shapes=scratch,
        compiler_params=pltpu.CompilerParams(
            collective_id=identity, has_side_effects=True
        ),
        cost_estimate=pl.CostEstimate(
            flops=0, bytes_accessed=16 * count * width * 4, transcendentals=0
        ),
        name="gather_tokens",
    )(*operands)
    return (all_rows.reshape(8 * count, width), *moved)


def after(value, *others):
    return lax.optimization_barrier((value, *others))[0]


def scatter_kernel(turned, term, left_ref, right_ref, *refs):
    if term:
        rows_ref, grads_ref, own_ref, term_ref, *refs = refs
    else:
        own_ref, *refs = refs
    part_ref, from_core, from_b, from_a, send, recv = refs
    at = Corner()
    slot_d, slot_b, slot_a, me = at.slots(at.c)
    other_d, other_b, other_a, other_me = at.slots(1 - at.c)
    _, width = own_ref.shape
    step = width // CHUNKS
    wide = jnp.float32
    greet([at.peer_a, at.peer_b, at.sibling])
    sent = []

    def start(kind, k, src, dst, peer):
        one = remote(src, dst, send.at[kind, k], recv.at[kind, k], peer)
        one.start()
        sent.append(one)

    def arrived(kind, k, dst, peer):
        remote(dst, dst, send.at[kind, k], recv.at[kind, k], peer).wait_recv()

    def multiply_columns(slot, cols):
        right = right_ref[cols] if turned else right_ref[:, cols]
        product = lax.dot_general(
            left_ref[slot],
            right,
            (((1,), (1 if turned else 0,)), ((), ())),
            preferred_element_type=wide,
        )
        part_ref[slot, :, cols] = product.astype(part_ref.dtype)

    def multiply(slot):
        def columns(t, carry):
            multiply_columns(slot, pl.ds(pl.multiple_of(t * step, step), step))
            return carry

        lax.fori_loop(0, CHUNKS, columns, 0)

    def multiply_term(first, last):
        if not term:
            return
        lanes = min(256, rows_ref.shape[1] // 8)

        def features(t, carry):
            cols = pl.ds(pl.multiple_of(t * lanes, lanes), lanes)
            product = lax.dot_general(
                rows_ref[:, cols],
                grads_ref[...],
                (((0,), (0,)), ((), ())),
                preferred_element_type=wide,
            )
            term_ref[cols] = product.astype(term_ref.dtype)
            return carry

        count = rows_ref.shape[1] // lanes
        lax.fori_loop(count * first // 8, count * last // 8, features, 0)

    def share(q, slot, chunks):
        for k in chunks:
            part = pl.ds(k * step, step)
            start(q, k, part_ref.at[slot, :, part], from_core.at[q, :, part], at.sibling)

    def to_b(q, slot, chunks):
        for k in chunks:
            part = pl.ds(k * step, step)
            arrived(q, k, from_core.at[q, :, part], at.sibling)
            total = part_ref[slot, :, part].astype(wide) + from_core[q, :, part].astype(wide)
            from_core[q, :, part] = total.astype(from_core.dtype)
            start(4 + q, k, from_core.at[q, :, part], from_b.at[q, :, part], at.peer_b)

    everything = range(CHUNKS)
    for k in everything:
        multiply_columns(other_d, pl.ds(k * step, step))
        share(0, other_d, [k])
        multiply_columns(slot_d, pl.ds(k * step, step))
        if k:
            to_b(0, slot_d, [k - 1])
    to_b(0, slot_d, [CHUNKS - 1])
    multiply(other_a)
    share(1, other_a, everything)
    multiply(slot_b)
    to_b(1, slot_b, everything)
    multiply(other_b)
    share(2, other_b, everything)
    multiply(slot_a)
    multiply_term(0, 2)
    for k in everything:
        part = pl.ds(k * step, step)
        arrived(2, k, from_core.at[2, :, part], at.sibling)
        arrived(4, k, from_b.at[0, :, part], at.peer_b)
        total = part_ref[slot_a, :, part].astype(wide) + from_core[2, :, part].astype(wide)
        total = total + from_b[0, :, part].astype(wide)
        from_core[2, :, part] = total.astype(from_core.dtype)
        start(6, k, from_core.at[2, :, part], from_a.at[:, part], at.peer_a)
    multiply(other_me)
    share(3, other_me, everything)
    multiply(me)
    multiply_term(2, 8)
    for k in everything:
        part = pl.ds(k * step, step)
        arrived(3, k, from_core.at[3, :, part], at.sibling)
        arrived(5, k, from_b.at[1, :, part], at.peer_b)
        arrived(6, k, from_a.at[:, part], at.peer_a)
        total = part_ref[me, :, part].astype(wide) + from_core[3, :, part].astype(wide)
        total = total + from_b[1, :, part].astype(wide)
        own_ref[:, part] = total + from_a[:, part].astype(wide)
    for one in sent:
        one.wait_send()


def scatter_tokens(identity, left, right, turned=False, term=()):
    count, depth = left.shape[0] // 8, left.shape[1]
    width = right.shape[0] if turned else right.shape[1]
    half = left.dtype
    shapes = [jax.ShapeDtypeStruct((count, width), jnp.float32)]
    if term:
        shapes.append(jax.ShapeDtypeStruct((term[0].shape[1], term[1].shape[1]), half))
    vmem = pl.BlockSpec(memory_space=pltpu.VMEM)
    return pl.pallas_call(
        functools.partial(scatter_kernel, turned, bool(term)),
        out_shape=shapes,
        in_specs=[vmem] * (2 + len(term)),
        out_specs=[vmem] * len(shapes),
        scratch_shapes=[
            pltpu.VMEM((8, count, width), half),
            pltpu.VMEM((4, count, width), half),
            pltpu.VMEM((2, count, width), half),
            pltpu.VMEM((count, width), half),
            pltpu.SemaphoreType.DMA((7, CHUNKS)),
            pltpu.SemaphoreType.DMA((7, CHUNKS)),
        ],
        compiler_params=pltpu.CompilerParams(
            collective_id=identity, has_side_effects=True, vmem_limit_bytes=58 * 2**20
        ),
        cost_estimate=pl.CostEstimate(
            flops=2 * left.size * width, bytes_accessed=64 * count * width, transcendentals=0
        ),
        name="scatter_tokens",
    )(left.reshape(8, count, depth), right, *term)


def exchange_kernel(last, triple_step, *refs):
    refs = list(refs)
    take = lambda n: [refs.pop(0) for _ in range(n)]
    deep_in, turn_in, triple_in, vec_in = take(4)
    expand_in = take(1)[0] if last else None
    deep_out, turn_out, triple_out = take(3)
    if last:
        expand_out = take(1)[0]
    vec_out = take(1)[0]
    if last:
        triple_columns, expand_columns = triple_out, expand_out
        triple_out, expand_out, near, far, here = take(5)
    send, recv, local_sem = take(3)
    c, z = lax.axis_index("dp"), lax.axis_index("z")
    y, x = lax.axis_index("y"), lax.axis_index("x")
    place = y * 2 + x
    rank = c * 4 + place

    def deep(i):
        return lax.rem(z + i, 4)

    def flat(i):
        return lax.rem(place + i, 4)

    def wide(i):
        return lax.rem(rank + i, 8)

    def deep_peer(i):
        return {"z": deep(i)}

    def flat_peer(i):
        return {"y": flat(i) // 2, "x": lax.rem(flat(i), 2)}

    def wide_peer(i):
        return {
            "dp": wide(i) // 4,
            "y": lax.rem(wide(i), 4) // 2,
            "x": lax.rem(wide(i), 2),
        }

    low = lax.rem(z, 2)
    turn_from = {"z": z - low + 1 - x, "x": low}
    turn_to = {"z": z - low + x, "x": 1 - low}
    if last:
        turn_from, turn_to = turn_to, turn_from
    others = range(1, 4)
    greet([deep_peer(i) for i in others] + [wide_peer(i) for i in range(1, 8)])
    sent, waits, kept = [], [], []
    count = [0]

    def post(src, dst, peer, landing):
        k = count[0]
        count[0] += 1
        one = remote(src, dst, send.at[k], recv.at[k], peer)
        one.start()
        sent.append(one)
        return remote(landing, landing, send.at[k], recv.at[k], peer)

    def keep(src, dst):
        one = pltpu.make_async_copy(src, dst, local_sem.at[len(kept)])
        one.start()
        kept.append(one)

    def parts(src, dst, order, block):
        if last:
            return [(src.at[block], dst.at[place])]
        steps = src.shape[1] // 4 // order[0]
        step = order[0]
        return [
            (
                src.at[:, pl.ds(pl.multiple_of((i * 4 + order[1](block)) * step, step), step)],
                dst.at[place, :, pl.ds(i * step, step)],
            )
            for i in range(steps)
        ]

    def turn_columns(src, dst, order):
        for i in others:
            for n, (a, b) in enumerate(parts(src, dst, order, flat(i))):
                landing = dst.at[flat(4 - i)]
                if not last:
                    landing = landing.at[:, pl.ds(n * order[0], order[0])]
                waits.append(post(a, b, flat_peer(i), landing))

    triple_order = (triple_step, lambda p: 2 * (1 - lax.rem(p, 2)) + p // 2)
    stage, late = [], []
    for i in others:
        if last:
            landing = near.at[deep(4 - i)]
            stage.append(post(vec_in.at[:, deep(i)], near.at[z], deep_peer(i), landing))
        else:
            landing = vec_out.at[deep(4 - i), rank]
            stage.append(post(vec_in, vec_out.at[z, rank], deep_peer(i), landing))
    turn_columns(triple_in, triple_out, triple_order)
    for i in others:
        late.append(post(deep_in.at[deep(i)], deep_out.at[z], deep_peer(i), deep_out.at[deep(4 - i)]))
    late.append(post(turn_in, turn_out, turn_to, turn_out))
    if last:
        turn_columns(expand_in, expand_out, None)
        keep(expand_in.at[place], expand_out.at[place])
    keep(deep_in.at[z], deep_out.at[z])
    for a, b in parts(triple_in, triple_out, triple_order, place):
        keep(a, b)
    if last:
        own = pltpu.make_async_copy(vec_in.at[:, z], near.at[z], local_sem.at[len(kept)])
        own.start()
        for one in stage:
            one.wait_recv()
        own.wait()
        here[...] = jnp.sum(near[...], 0)
        stage = []
        for i in range(1, 8):
            landing = far.at[wide(8 - i)]
            stage.append(post(here.at[wide(i)], far.at[rank], wide_peer(i), landing))
        far[rank] = here[rank]
        for one in stage:
            one.wait_recv()
        vec_out[...] = jnp.sum(far[...], 0)
    else:
        own = pltpu.make_async_copy(vec_in, vec_out.at[z, rank], local_sem.at[len(kept)])
        own.start()
        for one in stage:
            one.wait_recv()
        own.wait()
        for i in range(1, 8):
            landing = vec_out.at[:, wide(8 - i)]
            late.append(post(vec_out.at[:, rank], vec_out.at[:, rank], wide_peer(i), landing))
    for one in waits:
        one.wait_recv()
    for one in kept:
        one.wait()
    if last:
        for (steps, order), blocks, columns in zip(
            last, (triple_out, expand_out), (triple_columns, expand_columns)
        ):
            step = blocks.shape[2] // steps
            for i in range(steps):
                for p in range(4):
                    first = (i * 4 + order[p]) * step
                    columns[:, first : first + step] = blocks[p, :, i * step : (i + 1) * step]
    for one in late:
        one.wait_recv()
    for one in sent:
        one.wait_send()


def exchange(identity, deep, turned, triple, vector, step, expand=None, last=None):
    half = triple.dtype
    operands = [deep, turned, triple, vector] + ([expand] if last else [])
    shapes = [jax.ShapeDtypeStruct(a.shape, a.dtype) for a in (deep, turned)]
    hbm, vmem = pl.BlockSpec(memory_space=pl.ANY), pl.BlockSpec(memory_space=pltpu.VMEM)
    scratch = []
    if last:
        tile = vector.shape[2:]
        shapes += [jax.ShapeDtypeStruct((a.shape[1], 4 * a.shape[2]), half) for a in (triple, expand)]
        shapes.append(jax.ShapeDtypeStruct(tile, vector.dtype))
        scratch = [pltpu.VMEM(triple.shape, half), pltpu.VMEM(expand.shape, half)]
        scratch += [pltpu.VMEM(n + tile, vector.dtype) for n in ((4, 8), (8,), (8,))]
        places = [hbm, hbm, vmem, vmem, vmem]
        copies = 14 + 6
    else:
        rows, columns = triple.shape
        shapes.append(jax.ShapeDtypeStruct((4, rows, columns // 4), half))
        shapes.append(jax.ShapeDtypeStruct((4, 8) + vector.shape, vector.dtype))
        places = [hbm] * 4
        copies = 14 + 3 * (columns // 4 // step)
    moved = sum(a.size * a.dtype.itemsize for a in operands)
    return pl.pallas_call(
        functools.partial(exchange_kernel, last, step),
        out_shape=shapes,
        in_specs=[hbm] * len(operands),
        out_specs=places,
        scratch_shapes=scratch
        + [
            pltpu.SemaphoreType.DMA((copies,)),
            pltpu.SemaphoreType.DMA((copies,)),
            pltpu.SemaphoreType.DMA((8,)),
        ],
        compiler_params=pltpu.CompilerParams(
            collective_id=identity,
            has_side_effects=True,
            vmem_limit_bytes=(60 if last else 24) * 2**20,
        ),
        cost_estimate=pl.CostEstimate(flops=0, bytes_accessed=16 * moved, transcendentals=0),
        name="exchange",
    )(*operands)


def turn_kernel(step, src_ref, dst_ref, send, recv, local_sem):
    place = lax.axis_index("y") * 2 + lax.axis_index("x")
    count = dst_ref.shape[2] // step

    def peer(i):
        chip = lax.rem(place + i, 4)
        return {"y": chip // 2, "x": lax.rem(chip, 2)}

    def columns(chip, n):
        return src_ref.at[:, pl.ds(pl.multiple_of((n * 4 + chip) * step, step), step)]

    greet([peer(i) for i in range(1, 4)])
    moves, waits = [], []
    for i in range(1, 4):
        for n in range(count):
            part = pl.ds(n * step, step)
            sems = send.at[i - 1, n], recv.at[i - 1, n]
            block = columns(lax.rem(place + i, 4), n)
            one = remote(block, dst_ref.at[place, :, part], *sems, peer(i))
            one.start()
            moves.append(one)
            landing = dst_ref.at[lax.rem(place + 4 - i, 4), :, part]
            waits.append(remote(landing, landing, *sems, peer(i)))
    kept = []
    for n in range(count):
        part = pl.ds(n * step, step)
        kept.append(
            pltpu.make_async_copy(
                columns(place, n), dst_ref.at[place, :, part], local_sem.at[n]
            )
        )
        kept[-1].start()
    for one in waits:
        one.wait_recv()
    for one in moves:
        one.wait_send()
    for one in kept:
        one.wait()


def turn_columns(rows, step):
    count, columns = rows.shape
    steps = columns // 4 // step
    return pl.pallas_call(
        functools.partial(turn_kernel, step),
        out_shape=jax.ShapeDtypeStruct((4, count, columns // 4), rows.dtype),
        in_specs=[pl.BlockSpec(memory_space=pl.ANY)],
        out_specs=pl.BlockSpec(memory_space=pl.ANY),
        scratch_shapes=[
            pltpu.SemaphoreType.DMA((3, steps)),
            pltpu.SemaphoreType.DMA((3, steps)),
            pltpu.SemaphoreType.DMA((steps,)),
        ],
        compiler_params=pltpu.CompilerParams(collective_id=7, has_side_effects=True),
        cost_estimate=pl.CostEstimate(
            flops=0, bytes_accessed=16 * count * columns, transcendentals=0
        ),
        name="turn_columns",
    )(rows)


def scores_of(item_ref, first, block, slope, prefix, depth, seq_rows):
    length = item_ref.shape[0]
    head_dim = item_ref.shape[1] // 3
    own_rows = depth * seq_rows
    chips = length // own_rows

    def position(index):
        chip = index // own_rows
        rest = index % own_rows
        return ((rest // seq_rows) * chips + chip) * seq_rows + rest % seq_rows

    queries = item_ref[first : first + block, :head_dim]
    keys = item_ref[:, head_dim : 2 * head_dim]
    raw = lax.dot_general(
        keys, queries, (((1,), (1,)), ((), ())), preferred_element_type=jnp.float32
    )
    key_pos = position(lax.broadcasted_iota(jnp.int32, (length, 1), 0))
    query_pos = position(first + lax.broadcasted_iota(jnp.int32, (1, block), 1))
    bound = jnp.where(key_pos < prefix, -1, key_pos)
    distance = jnp.abs(
        query_pos.astype(jnp.float32) - key_pos.astype(jnp.float32)
    )
    scores = raw * (LOG2E / math.sqrt(head_dim)) - (slope * LOG2E) * distance
    return jnp.where(bound <= query_pos, scores, jnp.float32(-1e30))


def forward_kernel(depth, seq_rows, block, prefix_ref, slope_ref, item_ref, mixed_ref, total_ref):
    prefix = prefix_ref[pl.program_id(0)]
    slope = slope_ref[pl.program_id(1)]
    length = item_ref.shape[0]
    head_dim = item_ref.shape[1] // 3
    for first in range(0, length, block):
        scores = scores_of(item_ref, first, block, slope, prefix, depth, seq_rows)
        top = jnp.max(scores, 0, keepdims=True)
        powers = jnp.exp2(scores - top)
        total = jnp.sum(powers, 0, keepdims=True)
        probs = (powers * (1.0 / total)).astype(jnp.bfloat16)
        mixed = lax.dot_general(
            probs,
            item_ref[:, 2 * head_dim :],
            (((0,), (0,)), ((), ())),
            preferred_element_type=jnp.float32,
        )
        mixed_ref[first : first + block, :] = mixed.astype(mixed_ref.dtype)
        total_ref[0, :, first : first + block] = top + jnp.log2(total)


def attend_forward(projected, slopes, prefixes, own_heads, head_dim, depth, seq_rows):
    cores = prefixes.shape[0]
    length = projected.shape[0] // cores
    block = min(256, length)
    scores = cores * own_heads * length * length
    return pl.pallas_call(
        functools.partial(forward_kernel, depth, seq_rows, block),
        grid=(cores, own_heads),
        out_shape=[
            jax.ShapeDtypeStruct((cores * length, own_heads * head_dim), projected.dtype),
            jax.ShapeDtypeStruct((cores * own_heads, 1, length), jnp.float32),
        ],
        in_specs=[
            pl.BlockSpec(memory_space=pltpu.SMEM),
            pl.BlockSpec(memory_space=pltpu.SMEM),
            pl.BlockSpec((length, 3 * head_dim), lambda s, h: (s, h)),
        ],
        out_specs=[
            pl.BlockSpec((length, head_dim), lambda s, h: (s, h)),
            pl.BlockSpec((1, 1, length), lambda s, h: (s * own_heads + h, 0, 0)),
        ],
        compiler_params=pltpu.CompilerParams(vmem_limit_bytes=48 * 2**20),
        cost_estimate=pl.CostEstimate(
            flops=4 * scores * head_dim,
            bytes_accessed=2 * projected.size * 2,
            transcendentals=scores,
        ),
        name="attend_forward",
    )(prefixes, slopes, projected)


def backward_kernel(
    depth, seq_rows, block, prefix_ref, slope_ref, item_ref, grad_ref, total_ref, out_ref, key_sum, value_sum
):
    prefix = prefix_ref[pl.program_id(0)]
    slope = slope_ref[pl.program_id(1)]
    length = item_ref.shape[0]
    head_dim = item_ref.shape[1] // 3
    scale = 1.0 / math.sqrt(head_dim)
    half = jnp.bfloat16
    wide = jnp.float32
    for first in range(0, length, block):
        scores = scores_of(item_ref, first, block, slope, prefix, depth, seq_rows)
        probs = jnp.exp2(scores - total_ref[0, :, first : first + block])
        grad = grad_ref[first : first + block, :]
        grad_probs = lax.dot_general(
            item_ref[:, 2 * head_dim :],
            grad,
            (((1,), (1,)), ((), ())),
            preferred_element_type=wide,
        )
        inner = jnp.sum(grad_probs * probs, 0, keepdims=True)
        grad_scores = (probs * (grad_probs - inner)).astype(half)
        key_term = jnp.dot(
            grad_scores, item_ref[first : first + block, :head_dim], preferred_element_type=wide
        )
        value_term = jnp.dot(probs.astype(half), grad, preferred_element_type=wide)
        query_grad = lax.dot_general(
            grad_scores,
            item_ref[:, head_dim : 2 * head_dim],
            (((0,), (0,)), ((), ())),
            preferred_element_type=wide,
        )
        out_ref[first : first + block, :head_dim] = (query_grad * scale).astype(half)
        if first == 0:
            key_sum[...] = key_term
            value_sum[...] = value_term
        else:
            key_sum[...] += key_term
            value_sum[...] += value_term
    out_ref[:, head_dim : 2 * head_dim] = (key_sum[...] * scale).astype(half)
    out_ref[:, 2 * head_dim :] = value_sum[...].astype(half)


def attend_backward(
    projected, grad_mixed, totals, slopes, prefixes, own_heads, head_dim, depth, seq_rows
):
    cores = prefixes.shape[0]
    length = projected.shape[0] // cores
    block = min(256, length)
    scores = cores * own_heads * length * length
    return pl.pallas_call(
        functools.partial(backward_kernel, depth, seq_rows, block),
        grid=(cores, own_heads),
        out_shape=jax.ShapeDtypeStruct(projected.shape, projected.dtype),
        in_specs=[
            pl.BlockSpec(memory_space=pltpu.SMEM),
            pl.BlockSpec(memory_space=pltpu.SMEM),
            pl.BlockSpec((length, 3 * head_dim), lambda s, h: (s, h)),
            pl.BlockSpec((length, head_dim), lambda s, h: (s, h)),
            pl.BlockSpec((1, 1, length), lambda s, h: (s * own_heads + h, 0, 0)),
        ],
        out_specs=pl.BlockSpec((length, 3 * head_dim), lambda s, h: (s, h)),
        scratch_shapes=[
            pltpu.VMEM((length, head_dim), jnp.float32),
            pltpu.VMEM((length, head_dim), jnp.float32),
        ],
        compiler_params=pltpu.CompilerParams(vmem_limit_bytes=48 * 2**20),
        cost_estimate=pl.CostEstimate(
            flops=10 * scores * head_dim,
            bytes_accessed=2 * projected.size * 2,
            transcendentals=scores,
        ),
        name="attend_backward",
    )(prefixes, slopes, projected, grad_mixed, totals)


def planar(
    hidden,
    prefix_lengths,
    cotangent,
    first_gain,
    first_shift,
    triple_weight,
    pair_bias,
    dense_weight,
    dense_shift,
    second_gain,
    second_shift,
    expand_weight,
    expand_shift,
    shrink_weight,
    shrink_shift,
):
    wide = jnp.float32
    half = jnp.bfloat16
    cores = lax.axis_size("dp")
    depth = lax.axis_size("z")
    rows_y = lax.axis_size("y")
    rows_x = lax.axis_size("x")
    plane = rows_y * rows_x
    core = lax.axis_index("dp")
    at_y = lax.axis_index("y")
    at_x = lax.axis_index("x")
    place = at_y * rows_x + at_x
    seq_rows = hidden.shape[2]
    width = hidden.shape[3]
    head_dim = triple_weight.shape[3]
    heads = triple_weight.shape[1]
    own_heads = heads // plane
    own_rows = seq_rows * depth
    units = expand_weight.shape[1]
    own_units = units // plane
    row_block = expand_weight.shape[0]
    shrink_rows = shrink_weight.shape[0]

    pieces = [
        first_gain,
        first_shift,
        dense_shift,
        second_gain,
        second_shift,
        shrink_shift,
        pair_bias,
        expand_shift,
    ]
    piece_total = sum(p.shape[0] for p in pieces)
    lanes = 128
    vector_rows = -(-piece_total // (lanes * 16)) * 16
    vector_tile = jnp.pad(
        jnp.concatenate(pieces), (0, vector_rows * lanes - piece_total)
    ).reshape(vector_rows, lanes)
    inputs, dense_turned, triple_turned, packed = exchange(
        3,
        hidden[:, 0],
        dense_weight,
        triple_weight.reshape(row_block, heads * 3 * head_dim),
        vector_tile,
        3 * head_dim,
    )
    packed = (
        packed.reshape(depth, cores, plane, vector_rows * lanes)
        .transpose(1, 0, 2, 3)
        .reshape(-1, vector_rows * lanes)
    )
    vectors = []
    offset = 0
    for piece in pieces:
        vectors.append(packed[:, offset : offset + piece.shape[0]].reshape(-1).astype(wide))
        offset += piece.shape[0]
    gain_one, shift_one, dense_bias, gain_two, shift_two, shrink_bias, pair_full, unit_full = vectors
    pair_heads = pair_full.reshape(cores, own_heads, rows_x, rows_y, 2, head_dim)[
        core, :, 1 - at_x, at_y
    ]
    triple_bias = jnp.stack(
        [pair_heads[:, 0], jnp.zeros_like(pair_heads[:, 0]), pair_heads[:, 1]], 1
    ).reshape(-1)
    unit_bias = unit_full.reshape(cores, depth, plane, shrink_rows)[core, :, place].reshape(-1)

    triple_own = lax.all_gather(
        triple_turned.reshape(-1, triple_turned.shape[2]), "z", axis=0, tiled=True
    )
    inputs = inputs.reshape(own_rows, width).astype(wide)

    normed_own = layer_norm(inputs, gain_one, shift_one).astype(half)
    normed, upstream = gather_tokens(6, normed_own, cotangent[:, 0])
    upstream = upstream.reshape(own_rows, width)
    expand_turned = turn_columns(after(expand_weight, normed), shrink_rows)
    upstream_all, dense_own = gather_tokens(1, after(upstream, expand_turned), dense_turned, True)
    dense_own = dense_own.reshape(own_heads * head_dim, width)
    expand_own = lax.all_gather(
        expand_turned.reshape(-1, own_units), "z", axis=0, tiled=True
    )
    projected = (
        jnp.dot(normed, triple_own, preferred_element_type=wide) + triple_bias
    ).astype(half)

    shrink_own = lax.all_gather(after(shrink_weight, projected), "z", axis=0, tiled=True)
    head_index = core * heads + jnp.arange(own_heads) * plane + (1 - at_x) * rows_y + at_y
    slopes = jnp.power(
        jnp.float32(2.0), -8.0 * (head_index.astype(wide) + 1.0) / (heads * cores)
    )
    at_z = lax.axis_index("z")
    prefixes = lax.dynamic_index_in_dim(prefix_lengths, at_z, 0, False)
    mixed, log_totals = attend_forward(
        projected, slopes, prefixes, own_heads, head_dim, depth, seq_rows
    )
    (dense_sum,) = scatter_tokens(2, mixed, dense_own)
    middle = inputs + dense_sum + dense_bias
    normed_two_own, norm_two_pull = jax.vjp(layer_norm, middle, gain_two, shift_two)
    (normed_two,) = gather_tokens(5, normed_two_own.astype(half))
    hidden_pre = jnp.dot(normed_two, expand_own, preferred_element_type=wide) + unit_bias
    activated, gelu_pull = jax.vjp(gelu_tanh, hidden_pre)
    activated = activated.astype(half)
    shrink_term = jnp.einsum(
        "tu,td->ud", activated, upstream_all, preferred_element_type=wide
    ).astype(half)
    shrink_own = after(shrink_own, shrink_term)
    grad_act = jnp.einsum("tf,uf->tu", upstream_all, shrink_own, preferred_element_type=wide)
    grad_pre = gelu_pull(grad_act)[0].astype(half)
    shrink_grad = lax.psum_scatter(shrink_term, "z", scatter_dimension=0, tiled=True)
    feed_sum, expand_term = scatter_tokens(
        8, after(activated, shrink_term), shrink_own, term=(normed_two, grad_pre)
    )
    expand_turned = lax.psum_scatter(expand_term, "z", scatter_dimension=0, tiled=True)
    layer_output = (middle + feed_sum + shrink_bias).astype(half)

    (norm_two_sum,) = scatter_tokens(9, after(grad_pre, feed_sum), expand_own, True)
    grad_norm_two, gain_two_term, shift_two_term = norm_two_pull(norm_two_sum)
    grad_middle = upstream.astype(wide) + grad_norm_two
    branch_own = grad_middle.astype(half)
    branch, layer_output = gather_tokens(
        6, branch_own, layer_output.reshape(depth, seq_rows, width)
    )

    grad_mixed = jnp.einsum("tf,ef->te", branch, dense_own, preferred_element_type=wide).astype(
        half
    )
    dense_term = jnp.einsum("te,tf->ef", mixed, branch, preferred_element_type=wide).astype(half)
    dense_turned = lax.psum_scatter(dense_term, "z", scatter_dimension=0, tiled=True)
    grad_project = attend_backward(
        projected,
        after(grad_mixed, dense_term),
        log_totals,
        slopes,
        prefixes,
        own_heads,
        head_dim,
        depth,
        seq_rows,
    )
    triple_term = jnp.einsum(
        "td,tc->dc", normed, grad_project, preferred_element_type=wide
    ).astype(half)
    triple_turned = lax.psum_scatter(triple_term, "z", scatter_dimension=0, tiled=True)
    (norm_one_sum,) = scatter_tokens(10, after(grad_project, triple_term), triple_own, True)
    grad_norm_one, gain_one_term, shift_one_term = jax.vjp(
        layer_norm, inputs, gain_one, shift_one
    )[1](norm_one_sum)
    hidden_grad = (grad_middle + grad_norm_one).astype(half)
    head_sums = jnp.sum(grad_project, 0, dtype=wide).reshape(own_heads, 3, head_dim)
    pair_term = jnp.stack([head_sums[:, 0], head_sums[:, 2]], 1)
    pair_zero = jnp.zeros((cores, own_heads, rows_x, rows_y, 2, head_dim), wide)
    pair_wide = lax.dynamic_update_slice(
        pair_zero, pair_term[None, :, None, None], (core, 0, 1 - at_x, at_y, 0, 0)
    ).reshape(-1)
    unit_term = jnp.sum(grad_pre, 0, dtype=wide).reshape(1, depth, 1, shrink_rows)
    unit_wide = lax.dynamic_update_slice(
        jnp.zeros((cores, depth, plane, shrink_rows), wide), unit_term, (core, 0, place, 0)
    ).reshape(-1)
    terms = [
        gain_one_term,
        shift_one_term,
        jnp.sum(branch_own, 0, dtype=wide),
        gain_two_term,
        shift_two_term,
        jnp.sum(upstream, 0, dtype=wide),
        pair_wide,
        unit_wide,
    ]
    devices = cores * depth * plane
    term_rows = -(-piece_total // (lanes * 8)) * 8
    term_tiles = jnp.pad(
        jnp.concatenate([t.reshape(devices, -1) for t in terms], 1),
        ((0, 0), (0, term_rows * lanes - piece_total)),
    )
    term_tiles = (
        term_tiles.reshape(cores, depth, plane, term_rows, lanes)
        .transpose(0, 2, 1, 3, 4)
        .reshape(cores * plane, depth, term_rows, lanes)
    )
    hidden_grad, dense_grad, triple_grad, expand_grad, summed = exchange(
        4,
        hidden_grad.reshape(depth, seq_rows, width),
        dense_turned,
        triple_turned.reshape(plane, row_block, -1),
        term_tiles,
        3 * head_dim,
        expand_turned.reshape(plane, row_block, own_units),
        last=((own_heads, (2, 0, 3, 1)), (depth, (0, 1, 2, 3))),
    )
    layer_output = layer_output[:, None]
    hidden_grad = hidden_grad[:, None]
    triple_grad = triple_grad.astype(wide).reshape(row_block, heads, 3, head_dim)
    summed = summed.reshape(-1)
    vector_grads = []
    offset = 0
    for piece in pieces:
        vector_grads.append(summed[offset : offset + piece.shape[0]])
        offset += piece.shape[0]
    return (
        layer_output,
        hidden_grad,
        vector_grads[0],
        vector_grads[1],
        triple_grad,
        vector_grads[6],
        dense_grad.astype(wide),
        vector_grads[2],
        vector_grads[3],
        vector_grads[4],
        expand_grad.astype(wide),
        vector_grads[7],
        shrink_grad.astype(wide),
        vector_grads[5],
    )


def layer(*args):
    return planar(*args)


def solution(mesh):
    depth = 4
    sides = (2, 2)
    planar_plan = mesh.shape["seq"] == depth * sides[0] * sides[1]
    if planar_plan:
        grid = Mesh(
            mesh.devices.reshape(mesh.shape["dp"], depth, *sides), ("dp", "z", "y", "x")
        )
        seq = ("z", "y", "x")
    else:
        grid = mesh
        seq = ("seq",)
    tokens = P(None, "dp", seq, None)
    vector = P(("dp",) + seq)
    matrix = P(("dp",) + seq, None)
    placed = (
        tokens,
        P(),
        tokens,
        vector,
        vector,
        P(seq, "dp", None, None),
        vector,
        matrix,
        vector,
        vector,
        vector,
        P(seq, "dp"),
        vector,
        matrix,
        vector,
    )
    results = (
        tokens,
        tokens,
        vector,
        vector,
        P(seq, "dp", None, None),
        vector,
        matrix,
        vector,
        vector,
        vector,
        P(seq, "dp"),
        vector,
        matrix,
        vector,
    )
    return jax.shard_map(
        layer if planar_plan else shards,
        mesh=grid,
        in_specs=placed,
        out_specs=results,
        check_vma=False,
    )
```
